32 devices in a mesh: expert: 8 (over z, x), weight: 4 (over y, core).
Axes of the slice: x: 2, y: 2, z: 4, core: 2. Of those that a mesh axis runs over, the one named last changes fastest.
Arguments:
- tokens: bfloat16 [5120, 2048], P(('expert', 'weight')), may hold values from -6 to 6
- cotangent: bfloat16 [5120, 2048], P(('expert', 'weight')), may hold values from -6 to 6
- segments: int32 [8, 640], P('expert'), may hold values from 0 to 2, never falling along the last dimension, each value on 1 to 512 neighbouring positions
- routes: int32 [5120, 6], P(('expert', 'weight')), may hold values from 0 to 63, all different within a row; in each aligned block of 160 rows (0 to 159, 160 to 319, ...) at most 20 rows name the same one
- first_gain: float32 [2048], replicated, may hold values from 0.1 to 1.9
- query_weight: bfloat16 [2048, 3072], P(None, 'weight'), may hold values from -0.125 to 0.125
- latent_weight: bfloat16 [2048, 576], replicated, may hold values from -0.125 to 0.125
- latent_gain: float32 [512], replicated, may hold values from 0.1 to 1.9
- expand_weight: bfloat16 [512, 4096], P(None, 'weight'), may hold values from -0.25 to 0.25
- output_weight: bfloat16 [2048, 2048], P('weight'), may hold values from -0.5 to 0.5
- second_gain: float32 [2048], replicated, may hold values from 0.1 to 1.9
- router_weight: bfloat16 [2048, 64], replicated, may hold values from -0.125 to 0.125
- shared_gate: bfloat16 [2048, 2816], P(None, 'weight'), may hold values from -0.125 to 0.125
- shared_up: bfloat16 [2048, 2816], P(None, 'weight'), may hold values from -0.125 to 0.125
- shared_down: bfloat16 [2816, 2048], P('weight'), may hold values from -0.109375 to 0.109375
- expert_gate: bfloat16 [64, 2048, 1408], P('expert', None, 'weight'), may hold values from -0.125 to 0.125
- expert_up: bfloat16 [64, 2048, 1408], P('expert', None, 'weight'), may hold values from -0.125 to 0.125
- expert_down: bfloat16 [64, 1408, 2048], P('expert', 'weight'), may hold values from -0.15625 to 0.15625
Outputs:
- layer_out: bfloat16 [5120, 2048], P(('expert', 'weight'))
- token_gradient: float32 [5120, 2048], P(('expert', 'weight'))
- first_gain_gradient: float32 [2048], replicated
- query_gradient: float32 [2048, 3072], P('expert', 'weight')
- latent_weight_gradient: float32 [2048, 576], replicated
- latent_gain_gradient: float32 [512], replicated
- expand_gradient: float32 [512, 4096], P('expert', 'weight')
- output_gradient: float32 [2048, 2048], P('weight', 'expert')
- second_gain_gradient: float32 [2048], replicated
- router_gradient: float32 [2048, 64], replicated
- shared_gate_gradient: float32 [2048, 2816], P('expert', 'weight')
- shared_up_gradient: float32 [2048, 2816], P('expert', 'weight')
- shared_down_gradient: float32 [2816, 2048], P('weight', 'expert')
- expert_gate_gradient: float32 [64, 2048, 1408], P('expert', None, 'weight')
- expert_up_gradient: float32 [64, 2048, 1408], P('expert', None, 'weight')
- expert_down_gradient: float32 [64, 1408, 2048], P('expert', 'weight')
The draws below stay inside these ranges and needn't reach their ends.
Inputs may be any that keep to these rules, and one draw needn't show every extreme that they name: `segments`: ids never fall along a row; each of the 3 sequences of an index of expert is present, and the longest has 512 tokens. `routes`: each token names 6 different experts; no expert is named by more than 20 of one device's tokens, a bound that some device's tokens reach.
All inputs are finite; a program needn't handle non-finite values.
Results may differ from the reference program's by a relative error of at most 0.02.
Values may be sent and summed in bfloat16 or wider, within the bound.
A program may use at most 512 MiB of HBM per device.

```python
import math
import jax
import jax.numpy as jnp
import numpy as np
from jax import lax

D = 2048
HEADS = 16
NOPE = 128
ROPE = 64
VDIM = 128
LATENT = 512
EXPERTS = 64
TOPK = 6
E_FF = 1408
SH_FF = 2816
TOK_DEV = 160
SEQS = 3
CAP = 20
GROUP = 640
TOKENS = 5120
LONGEST = 512
N_EXPERT = 8
N_WEIGHT = 4


def levels(key, shape, cuts, low, largest):
    def one(position, shards_of):
        heights = jax.random.uniform(jax.random.fold_in(jax.random.fold_in(key, 6), position), (shards_of,), jnp.float32, low / len(cuts), largest / len(cuts))
        return jnp.repeat(jnp.exp(heights), shape[position] // shards_of).reshape((-1,) + (1,) * (len(shape) - position - 1))

    level = one(*cuts[0])
    for cut in cuts[1:]:
        level = level * one(*cut)
    return level


def length_profile(number_of, total, bound, lean):
    loads = [(1 << 20) // math.isqrt(standing ** lean) + 1 for standing in range(2, number_of + 1)]
    spare, holding = total - bound - (number_of - 1), [1] * (number_of - 1)
    while spare > 0:
        candidates = [i for i in range(number_of - 1) if holding[i] < bound]
        whole, left = sum([loads[i] for i in candidates]), spare
        for i in candidates:
            addition = min(bound - holding[i], max(1, left * loads[i] // whole), spare)
            holding[i] = holding[i] + addition
            spare = spare - addition
    return np.array([bound] + holding)


def uneven(own_key, count, total, reach, slope):
    if count == 2:
        one = jax.random.randint(own_key, (), max(1, total - reach), min(reach, total - 1) + 1)
        return jnp.stack([one, total - one])
    sizes = jnp.asarray(length_profile(count, total, reach, slope), jnp.int32)
    couples = (count - 1) // 2
    donor, receiver = sizes[1:1 + 2 * couples:2], sizes[2:2 + 2 * couples:2]
    room = jnp.minimum(donor - 1, reach - receiver)
    shifted = jax.random.randint(jax.random.fold_in(own_key, 1), (couples,), 0, 1 << 20) % (room + 1)
    sizes = sizes.at[1:1 + 2 * couples:2].set(donor - shifted).at[2:2 + 2 * couples:2].set(receiver + shifted)
    return sizes[jax.random.permutation(jax.random.fold_in(own_key, 2), count)]


def assign_block(key, own, number, rows, amount, top, reach, skew):
    ranking = jax.random.permutation(key, amount)
    heavy_load, ordinary = load_shares(amount, rows * top, reach, skew, True), load_shares(amount, rows * top, reach, skew, False)
    places = jnp.arange(amount)

    def named(sizes, rotation):
        used = int((sizes > 0).sum())
        fixed = max(1, used // 4)
        shifted = fixed + (places - fixed + rotation * (used - fixed)) % max(1, amount - fixed)
        return jnp.zeros((amount,), jnp.int32).at[ranking[jnp.where(places < fixed, places, shifted)]].set(jnp.asarray(sizes, jnp.int32))

    sizes = jnp.where(number % 4 == 0, named(heavy_load, number // 4), named(ordinary, number - number // 4 - 1))
    mixed = jax.random.permutation(jax.random.fold_in(own, 3), amount)
    source_of, taker = mixed[0:amount // 2 * 2:2], mixed[1:amount // 2 * 2:2]
    margin = jnp.minimum(sizes[source_of] - 1, reach - sizes[taker]) // 2
    margin = jnp.where((source_of == ranking[0]) | (taker == ranking[0]) | (sizes[taker] == 0), 0, jnp.maximum(margin, 0))
    shifted = jax.random.randint(jax.random.fold_in(own, 4), (amount // 2,), 0, 1 << 20) % (margin + 1)
    sizes = sizes.at[source_of].add(-shifted).at[taker].add(shifted)
    members = jnp.searchsorted(jnp.cumsum(sizes), jnp.arange(rows * top), side="right").astype(jnp.int32)
    table = members.reshape(top, rows).T
    table = table[jax.random.permutation(jax.random.fold_in(own, 1), rows)]
    rotation = jax.random.randint(jax.random.fold_in(own, 2), (rows, 1), 0, top)
    return jnp.take_along_axis(table, (jnp.arange(top)[None, :] + rotation) % top, axis=1)


def load_shares(number_of, total, reach, slope, full):
    loads = [(1 << 20) // math.isqrt(standing ** slope) + 1 for standing in range(1, number_of + 1)]
    largest = reach if full else min(reach, max(-(-total // number_of), total * loads[0] // sum(loads)))
    least = 1 if total - largest >= number_of - 1 else 0
    counts, spare = [largest] + [least] * (number_of - 1), total - largest - least * (number_of - 1)
    while spare > 0:
        candidates = [i for i in range(1, number_of) if counts[i] < largest] or [i for i in range(1, number_of) if counts[i] < reach]
        pool, remaining = sum([loads[i] for i in candidates]), spare
        for i in candidates:
            extra = min(reach - counts[i], max(1, remaining * loads[i] // pool), spare)
            counts[i] = counts[i] + extra
            spare = spare - extra
    return np.array(counts)


def centred(stream_key, extent, deviation, reach, cuts=(), held_as=jnp.bfloat16):
    factor_of = levels(stream_key, extent, cuts, -0.22, 0.18) if cuts else 1.0
    values = jax.random.normal(stream_key, extent, jnp.float32) * deviation * factor_of
    return jnp.minimum(jnp.maximum(values, -reach), reach).astype(held_as)


def setup_inputs(seed: int = 0) -> dict:
    key_list = jax.random.split(jax.random.key(seed), 19)
    tokens = centred(key_list[0], (TOKENS, D), 1.0, 6.0, ((0, 32),))
    cotangent = centred(key_list[1], (TOKENS, D), 1.0, 6.0, ((0, 32),))
    segments = jax.vmap(lambda own: jnp.searchsorted(jnp.cumsum(uneven(own, SEQS, GROUP, LONGEST, 2)), jnp.arange(GROUP), side="right"))(jax.random.split(key_list[2], N_EXPERT)).reshape((N_EXPERT, GROUP)).astype(jnp.int32)
    routes_keys = jax.random.split(jax.random.fold_in(key_list[3], 1), TOKENS // TOK_DEV)
    routes_turns = jax.random.permutation(jax.random.fold_in(key_list[3], 3), TOKENS // TOK_DEV)
    routes = jax.vmap(lambda own, number: assign_block(jax.random.fold_in(key_list[3], 2), own, number, TOK_DEV, EXPERTS, TOPK, CAP, 1))(routes_keys, routes_turns).reshape((TOKENS, TOPK))
    first_gain = jnp.clip(1.0 + 0.18 * jax.random.normal(key_list[4], (D,), jnp.float32), 0.1, 1.9)
    query_weight = centred(key_list[5], (D, HEADS * (NOPE + ROPE)), D ** -0.5, 0.125, ((1, 4),))
    latent_weight = centred(key_list[6], (D, LATENT + ROPE), D ** -0.5, 0.125)
    latent_gain = jnp.clip(1.0 + 0.18 * jax.random.normal(key_list[7], (LATENT,), jnp.float32), 0.1, 1.9)
    expand_weight = centred(key_list[8], (LATENT, HEADS * (NOPE + VDIM)), LATENT ** -0.5, 0.25, ((1, 4),))
    output_weight = centred(key_list[9], (HEADS * VDIM, D), (HEADS * VDIM // 16) ** -0.5, 0.5, ((0, 4),))
    second_gain = jnp.clip(1.0 + 0.18 * jax.random.normal(key_list[10], (D,), jnp.float32), 0.1, 1.9)
    router_weight = centred(key_list[11], (D, EXPERTS), D ** -0.5, 0.125)
    shared_gate = centred(key_list[12], (D, SH_FF), D ** -0.5, 0.125, ((1, 4),))
    shared_up = centred(key_list[13], (D, SH_FF), D ** -0.5, 0.125, ((1, 4),))
    shared_down = centred(key_list[14], (SH_FF, D), SH_FF ** -0.5, 0.109375, ((0, 4),))
    expert_gate = centred(key_list[15], (EXPERTS, D, E_FF), D ** -0.5, 0.125, ((0, 8), (2, 4)))
    expert_up = centred(key_list[16], (EXPERTS, D, E_FF), D ** -0.5, 0.125, ((0, 8), (2, 4)))
    expert_down = centred(key_list[17], (EXPERTS, E_FF, D), E_FF ** -0.5, 0.15625, ((0, 8), (1, 4)))
    return {"tokens": tokens, "cotangent": cotangent, "segments": segments, "routes": routes, "first_gain": first_gain, "query_weight": query_weight, "latent_weight": latent_weight, "latent_gain": latent_gain, "expand_weight": expand_weight, "output_weight": output_weight, "second_gain": second_gain, "router_weight": router_weight, "shared_gate": shared_gate, "shared_up": shared_up, "shared_down": shared_down, "expert_gate": expert_gate, "expert_up": expert_up, "expert_down": expert_down}


eps = 1e-06
route_scale = 2.446
rope_base = 50000.0
highest = lax.Precision.HIGHEST

@jax.custom_vjp
def low(v):
    return lax.optimization_barrier(v.astype(jnp.bfloat16)).astype(jnp.float32)

@jax.custom_vjp
def low_back(v):
    return v

def low_keep(v):
    return (low(v), None)

def low_pass(kept, grad):
    return (grad,)

def back_keep(v):
    return (v, None)

def back_low(kept, grad):
    return (low(grad),)
low.defvjp(low_keep, low_pass)
low_back.defvjp(back_keep, back_low)

def both_ways(value):
    return low_back(low(value))

def matmul(left, right):
    return jnp.dot(left, right, precision=highest)

def inv_rms(value):
    return lax.rsqrt(lax.optimization_barrier(jnp.mean(value * value, axis=-1, keepdims=True)) + eps)

def rope_tables(seg):
    size = seg.shape[0]
    index = jnp.arange(size, dtype=jnp.int32)
    fresh = jnp.concatenate([jnp.ones((1,), dtype=bool), seg[1:] != seg[:-1]])
    first = lax.cummax(jnp.where(fresh, index, jnp.zeros_like(index)), axis=0)
    place = (index - first).astype(jnp.float32)
    half = ROPE // 2
    freqs = rope_base ** (-(jnp.arange(half, dtype=jnp.float32) * 2.0 / ROPE))
    angle = place[:, None] * freqs[None, :]
    return (jnp.cos(angle), jnp.sin(angle))

def rotate(value, cosine, sine):
    half = value.shape[-1] // 2
    first, second = (value[..., :half], value[..., half:])
    return jnp.concatenate([first * cosine - second * sine, second * cosine + first * sine], axis=-1)

def group_attention(packed):
    query, key, value, seg = packed
    size = seg.shape[0]
    index = jnp.arange(size, dtype=jnp.int32)
    allowed = (seg[:, None] == seg[None, :]) & (index[None, :] <= index[:, None])
    score_scale = (NOPE + ROPE) ** (-0.5)
    raw = low_back(jnp.einsum('ihd,jhd->hij', query, key, precision=highest) * score_scale)
    scores = jnp.where(allowed[None], raw, -1e+30)
    peak = lax.optimization_barrier(jnp.max(scores, axis=-1, keepdims=True))
    weights = jnp.exp(scores - peak)
    probs = weights / lax.optimization_barrier(jnp.sum(weights, axis=-1, keepdims=True))
    return jnp.einsum('hij,jhd->ihd', low(probs), value, precision=highest)

def expert_apply(packed):
    slot_rows, gate_matrix, up_matrix, down_matrix = packed
    gate = low_back(matmul(slot_rows, gate_matrix))
    lift = low_back(matmul(slot_rows, up_matrix))
    return both_ways(matmul(low(jax.nn.silu(gate) * lift), down_matrix))

def reference(tokens, cotangent, segments, routes, first_gain, query_weight, latent_weight, latent_gain, expand_weight, output_weight, second_gain, router_weight, shared_gate, shared_up, shared_down, expert_gate, expert_up, expert_down):
    token_count = tokens.shape[0]
    flat_ids = routes.reshape(-1)
    slots_per = N_EXPERT * N_WEIGHT * CAP
    hits = (flat_ids[:, None] == jnp.arange(EXPERTS, dtype=jnp.int32)[None, :]).astype(jnp.int32)
    blocked = hits.reshape(N_EXPERT * N_WEIGHT, TOK_DEV * TOPK, EXPERTS)
    place = (lax.optimization_barrier(jnp.sum(jnp.cumsum(blocked, axis=1) * blocked, axis=2)) - 1).reshape(-1)
    device = jnp.arange(token_count * TOPK, dtype=jnp.int32) // (TOK_DEV * TOPK)
    slot_of = (flat_ids * slots_per + device * CAP + place).astype(jnp.int32)
    slot_token = jnp.zeros((EXPERTS * slots_per,), jnp.int32).at[slot_of].set(jnp.arange(token_count * TOPK, dtype=jnp.int32) // TOPK)
    slot_used = jnp.zeros((EXPERTS * slots_per,), jnp.float32).at[slot_of].set(1.0)
    cosine, sine = jax.vmap(rope_tables)(segments)
    cosine = cosine.reshape(token_count, -1)
    sine = sine.reshape(token_count, -1)
    group = segments.shape[1]

    def split(value):
        return value.reshape((segments.shape[0], group) + value.shape[1:])

    def forward(activations, gain_one, query_matrix, latent_matrix, gain_latent, expand_matrix, output_matrix, gain_two, router_matrix, sh_gate, sh_up, sh_down, ex_gate, ex_up, ex_down):
        normed = low(activations * inv_rms(activations) * gain_one)
        query = low_back(matmul(normed, query_matrix)).reshape(token_count, HEADS, NOPE + ROPE)
        query = low(jnp.concatenate([query[..., :NOPE], rotate(query[..., NOPE:], cosine[:, None, :], sine[:, None, :])], axis=-1))
        compressed = matmul(normed, latent_matrix)
        latent = compressed[:, :LATENT]
        key_rope = low(rotate(compressed[:, LATENT:], cosine, sine))
        latent_normed = low(latent * inv_rms(latent) * gain_latent)
        expanded = both_ways(matmul(latent_normed, expand_matrix)).reshape(token_count, HEADS, NOPE + VDIM)
        key = jnp.concatenate([expanded[..., :NOPE], jnp.broadcast_to(key_rope[:, None, :], (token_count, HEADS, ROPE))], axis=-1)
        values = expanded[..., NOPE:]
        mixed = lax.map(jax.checkpoint(group_attention), (split(query), split(key), split(values), segments))
        mixed = both_ways(mixed.reshape(token_count, HEADS * VDIM))
        hidden_one = activations + low_back(matmul(mixed, output_matrix))
        normed_two = low(hidden_one * inv_rms(hidden_one) * gain_two)
        gates = jax.nn.sigmoid(matmul(normed_two, router_matrix))
        chosen = jnp.take_along_axis(gates, routes, axis=1)
        mixing = route_scale * chosen / lax.optimization_barrier(jnp.sum(chosen, axis=1, keepdims=True))
        shared_gate_value = low_back(matmul(normed_two, sh_gate))
        shared_lift = low_back(matmul(normed_two, sh_up))
        shared_out = matmul(low(jax.nn.silu(shared_gate_value) * shared_lift), sh_down)
        slot_rows = low_back(normed_two[slot_token] * slot_used[:, None]).reshape(EXPERTS, slots_per, D)
        produced = lax.map(jax.checkpoint(expert_apply), (slot_rows, ex_gate, ex_up, ex_down))
        picked = produced.reshape(EXPERTS * slots_per, D)[slot_of].reshape(token_count, TOPK, D)
        return hidden_one + shared_out + lax.optimization_barrier(jnp.sum(mixing[:, :, None] * picked, axis=1))
    layer_value, pull = jax.vjp(forward, tokens.astype(jnp.float32), first_gain.astype(jnp.float32), query_weight.astype(jnp.float32), latent_weight.astype(jnp.float32), latent_gain.astype(jnp.float32), expand_weight.astype(jnp.float32), output_weight.astype(jnp.float32), second_gain.astype(jnp.float32), router_weight.astype(jnp.float32), shared_gate.astype(jnp.float32), shared_up.astype(jnp.float32), shared_down.astype(jnp.float32), expert_gate.astype(jnp.float32), expert_up.astype(jnp.float32), expert_down.astype(jnp.float32))
    grads = pull(cotangent.astype(jnp.float32))
    return (layer_value.astype(jnp.bfloat16), grads[0], grads[1], grads[2], grads[3], grads[4], grads[5], grads[6], grads[7], grads[8], grads[9], grads[10], grads[11], grads[12], grads[13], grads[14])
```

```python
import functools

import jax
import jax.numpy as jnp
from jax import lax
from jax.experimental import pallas as pl
from jax.experimental.pallas import tpu as pltpu
from jax.sharding import PartitionSpec as P

NOPE = 128
ROPE = 64
VDIM = 128
LATENT = 512
TOPK = 6
CAP = 20


eps = 1e-06
route_scale = 2.446
rope_base = 50000.0
highest = lax.Precision.HIGHEST


def matmul(left, right):
    return jnp.dot(left, right, preferred_element_type=jnp.float32)


def trans_times(left, right):
    return lax.dot_general(
        left, right, (((0,), (0,)), ((), ())), preferred_element_type=jnp.float32
    )


def times_trans(left, right):
    return lax.dot_general(
        left, right, (((1,), (1,)), ((), ())), preferred_element_type=jnp.float32
    )


def inv_rms(value):
    return lax.rsqrt(jnp.mean(value * value, axis=-1, keepdims=True) + eps)


def norm_back(grad_out, value, scale, gain):
    scaled = grad_out * gain
    grad_in = scale * scaled - value * scale**3 * jnp.mean(scaled * value, axis=-1, keepdims=True)
    gain_grad = jnp.sum(grad_out * value * scale, axis=0)
    return (grad_in, gain_grad)


def rope_tables(seg):
    size = seg.shape[0]
    index = jnp.arange(size, dtype=jnp.int32)
    fresh = jnp.concatenate([jnp.ones((1,), dtype=bool), seg[1:] != seg[:-1]])
    first = lax.cummax(jnp.where(fresh, index, jnp.zeros_like(index)), axis=0)
    place = (index - first).astype(jnp.float32)
    half = ROPE // 2
    freqs = rope_base ** (-(jnp.arange(half, dtype=jnp.float32) * 2.0 / ROPE))
    angle = place[:, None] * freqs[None, :]
    return (jnp.cos(angle), jnp.sin(angle))


def attention_mask(seg):
    index = jnp.arange(seg.shape[0], dtype=jnp.int32)
    return (seg[:, None] == seg[None, :]) & (index[None, :] <= index[:, None])


def rotate(value, cosine, sine):
    half = value.shape[-1] // 2
    first, second = (value[..., :half], value[..., half:])
    return jnp.concatenate(
        [first * cosine - second * sine, second * cosine + first * sine], axis=-1
    )


def unrotate(value, cosine, sine):
    half = value.shape[-1] // 2
    first, second = (value[..., :half], value[..., half:])
    return jnp.concatenate(
        [first * cosine + second * sine, second * cosine - first * sine], axis=-1
    )


lanes = 128
vmem_limit = 64 * 1024 * 1024 - 131072


def token_slots(marks, here, local_experts, half):
    codes = times_trans(here, marks)
    count = codes.shape[1]
    rank = jnp.floor(codes * (1.0 / 32.0))
    place = codes - 32.0 * rank
    token = lax.broadcasted_iota(jnp.int32, codes.shape, 1)
    slot = jnp.where(codes >= 0, place + jnp.where(token >= half, float(CAP), 0.0), -1.0)
    row = lax.broadcasted_iota(jnp.int32, (2 * CAP, count), 0).astype(jnp.float32)
    picks = [jnp.where(row == slot[e : e + 1], 1.0, 0.0) for e in range(local_experts)]
    return picks, rank


def gather_rows(picks, values, out_ref):
    rows = jnp.dot(
        jnp.concatenate(picks, axis=0).astype(jnp.bfloat16),
        values,
        preferred_element_type=jnp.float32,
    )
    for e in range(len(picks)):
        out_ref[e] = rows[e * 2 * CAP : (e + 1) * 2 * CAP].astype(jnp.bfloat16)


def grads_kernel(here_ref, value_ref, down_ref, rows_ref, back_ref):
    width = rows_ref.shape[2]
    local_experts, half = rows_ref.shape[0], value_ref.shape[0] // 2
    picks, _ = token_slots(value_ref[:, width:], here_ref[...], local_experts, half)
    values = value_ref[:, :width]
    gather_rows(picks, values, rows_ref)
    back_ref[...] = times_trans(values, down_ref[...])


def rows_kernel(
    here_ref,
    twice_ref,
    marks_ref,
    value_ref,
    back_ref,
    gate_ref,
    up_ref,
    rows_ref,
    mix_ref,
    hidden_ref,
    gate_grad_ref,
    lift_grad_ref,
):
    width = rows_ref.shape[2]
    local_experts, half = rows_ref.shape[0], value_ref.shape[0] // 2
    picks, _ = token_slots(marks_ref[...], here_ref[...], local_experts, half)
    values = value_ref[:, :width]
    gather_rows(picks, values, rows_ref)
    mixing = times_trans(twice_ref[...], value_ref[:, width:])
    for e in range(local_experts):
        column = jnp.sum(picks[e] * mixing[e : e + 1], axis=1, keepdims=True)
        mix_ref[e] = jnp.broadcast_to(column, mix_ref.shape[1:])
    gate = times_trans(values, gate_ref[...])
    lift = times_trans(values, up_ref[...])
    back = back_ref[...]
    sigma = jax.nn.sigmoid(gate)
    active = gate * sigma
    hidden_ref[...] = (active * lift).astype(jnp.bfloat16)
    gate_grad_ref[...] = (back * lift * sigma * (1.0 + gate * (1.0 - sigma))).astype(jnp.bfloat16)
    lift_grad_ref[...] = (back * active).astype(jnp.bfloat16)


def experts_kernel(
    rows_ref,
    grads_ref,
    mix_ref,
    gate_ref,
    up_ref,
    down_ref,
    hidden_ref,
    gate_grad_ref,
    lift_grad_ref,
    returned_ref,
    mix_grad_ref,
):
    rows, gate_matrix, up_matrix = rows_ref[0], gate_ref[0], up_ref[0]
    gate = times_trans(rows, gate_matrix)
    lift = times_trans(rows, up_matrix)
    back = times_trans(grads_ref[0], down_ref[0])
    mix = mix_ref[0][:, :1]
    sigma = jax.nn.sigmoid(gate)
    active = gate * sigma
    hidden = active * lift
    mix_grad = jnp.sum(hidden * back, axis=1, keepdims=True)
    mix_grad_ref[0] = jnp.broadcast_to(mix_grad, mix_grad_ref.shape[1:])
    hidden_ref[0] = (mix * hidden).astype(jnp.bfloat16)
    back = back * mix
    gate_grad = (back * lift * sigma * (1.0 + gate * (1.0 - sigma))).astype(jnp.bfloat16)
    lift_grad = (back * active).astype(jnp.bfloat16)
    gate_grad_ref[0] = gate_grad
    lift_grad_ref[0] = lift_grad
    returned = matmul(gate_grad, gate_matrix) + matmul(lift_grad, up_matrix)
    returned_ref[0] = returned.astype(jnp.bfloat16)


def produce_kernel(hidden_ref, down_ref, out_ref):
    out_ref[0] = matmul(hidden_ref[0], down_ref[0]).astype(jnp.bfloat16)


def spread_rows(picks, rows_ref):
    rows = jnp.concatenate([rows_ref[e].astype(jnp.float32) for e in range(len(picks))], axis=0)
    pick = jnp.concatenate(picks, axis=0).astype(jnp.bfloat16)
    return trans_times(pick, rows.astype(jnp.bfloat16))


def back_kernel(
    here_ref,
    high_ref,
    low_ref,
    marks_ref,
    rows_ref,
    mix_grad_ref,
    gate_grad_ref,
    lift_grad_ref,
    gate_ref,
    up_ref,
    out_ref,
):
    width = rows_ref.shape[2]
    local_experts, half = rows_ref.shape[0], out_ref.shape[0] // 2
    picks, rank = token_slots(marks_ref[...], here_ref[...], local_experts, half)
    total = spread_rows(picks, rows_ref)
    total = total + matmul(gate_grad_ref[...], gate_ref[...])
    total = total + matmul(lift_grad_ref[...], up_ref[...])
    out_ref[:, :width] = total.astype(jnp.bfloat16)
    choice = lax.broadcasted_iota(jnp.int32, rank.shape, 0).astype(jnp.float32)
    mix_grad = jnp.zeros(rank.shape, jnp.float32)
    for e in range(local_experts):
        row = jnp.sum(picks[e] * mix_grad_ref[e][:, :1], axis=0, keepdims=True)
        mix_grad = mix_grad + jnp.where(choice == rank[e : e + 1], row, 0.0)
    high = mix_grad.astype(jnp.bfloat16)
    low = (mix_grad - high.astype(jnp.float32)).astype(jnp.bfloat16)
    sent = trans_times(high, high_ref[...]) + trans_times(low, low_ref[...])
    out_ref[:, width:] = sent.astype(jnp.bfloat16)


def out_kernel(here_ref, marks_ref, rows_ref, hidden_ref, down_ref, out_ref):
    local_experts, half = rows_ref.shape[0], out_ref.shape[0] // 2
    picks, _ = token_slots(marks_ref[...], here_ref[...], local_experts, half)
    total = spread_rows(picks, rows_ref)
    total = total + matmul(hidden_ref[...], down_ref[...])
    out_ref[...] = total.astype(jnp.bfloat16)


def whole_spec(array):
    zeros = (0,) * array.ndim
    return pl.BlockSpec(array.shape, lambda i: zeros)


def pair_spec(array, pairs):
    block = (array.shape[0] // pairs,) + array.shape[1:]
    zeros = (0,) * (array.ndim - 1)
    return pl.BlockSpec(block, lambda i: (i,) + zeros)


def slots_spec(array, pairs):
    block = (array.shape[0], array.shape[1] // pairs) + array.shape[2:]
    return pl.BlockSpec(block, lambda i: (0, i, 0))


def cost(flops, *arrays):
    moved = sum(a.size * a.dtype.itemsize for a in arrays)
    return pl.CostEstimate(flops=int(flops), bytes_accessed=int(moved), transcendentals=0)


def call(kernel, grid, ins, outs, flops):
    arrays = [a for a, _ in ins]
    shapes = [s for s, _ in outs]
    return pl.pallas_call(
        kernel,
        grid=(grid,),
        in_specs=[s for _, s in ins],
        out_specs=[s for _, s in outs],
        out_shape=shapes,
        cost_estimate=cost(flops, *arrays, *shapes),
        compiler_params=pltpu.CompilerParams(vmem_limit_bytes=vmem_limit),
    )(*arrays)


MESH = pl.DeviceIdType.MESH


def places():
    expert, weight = lax.axis_index("expert"), lax.axis_index("weight")
    return lax.div(expert, 2), lax.rem(expert, 2), lax.div(weight, 2), lax.rem(weight, 2)


def device(z, x, y, c):
    return (z * 2 + x, y * 2 + c)


def shard(z, x, y, c):
    return z * 8 + x * 4 + y * 2 + c


def push(source, target, send, receive, to):
    return pltpu.make_async_remote_copy(
        src_ref=source,
        dst_ref=target,
        send_sem=send,
        recv_sem=receive,
        device_id=to,
        device_id_type=MESH,
    )


class Sends:
    def __init__(self, semaphores):
        self.semaphores = semaphores
        self.started = []

    def start(self, source, target, receive, to, when=None):
        copy = push(source, target, self.semaphores.at[len(self.started)], receive, to)
        self.started.append((copy, when))
        if when is None:
            copy.start()
        else:
            pl.when(when)(copy.start)

    def finish(self):
        for copy, when in self.started:
            if when is None:
                copy.wait_send()
            else:
                pl.when(when)(copy.wait_send)


def landed(target, receive, to):
    push(target, target, receive, receive, to).wait_recv()


def greet(devices):
    barrier = pltpu.get_barrier_semaphore()
    count = 0
    for to, when in devices:
        signal = functools.partial(
            pl.semaphore_signal, barrier, inc=1, device_id=to, device_id_type=MESH
        )
        if when is None:
            signal()
            count = count + 1
        else:
            pl.when(when)(signal)
            count = count + when.astype(jnp.int32)
    pl.semaphore_wait(barrier, count)


def add_rows(target, sources, start, rows):
    step = 16

    def body(i, carry):
        part = pl.ds(pl.multiple_of(start + i * step, step), step)
        total = target[part].astype(jnp.float32)
        for source, offset in sources:
            there = pl.ds(pl.multiple_of(start - offset + i * step, step), step)
            total = total + source[there].astype(jnp.float32)
        target[part] = total.astype(target.dtype)
        return carry

    lax.fori_loop(0, rows // step, body, 0)


def ordered(z, first, second):
    upper = lax.div(z, 2)
    inner = z + upper * (3 - 2 * z)
    value = first + inner * (second - first)
    return value + upper * (3 - 2 * value)


def gather_all_kernel(x_ref, out_ref, send_sems, recv_sems, local_sem):
    z, x, y, c = places()
    half = x_ref.shape[0] // 2
    over, side, mate = device(z, 1 - x, y, c), device(z, x, 1 - y, c), device(z, x, y, 1 - c)
    up, down = device(z + 1, x, y, c), device(z - 1, x, y, c)
    greet([(over, None), (side, None), (mate, None), (up, z < 3), (down, z > 0)])
    sends = Sends(send_sems)
    own = shard(z, x, y, c)
    keep = pltpu.make_async_copy(x_ref, out_ref.at[own], local_sem)
    keep.start()

    def halves(i, h):
        return out_ref.at[i, pl.ds(h * half, half)]

    def whole(step):
        zz = ordered(z, (0, 1, 2, 3)[step], (1, 0, 2, 3)[step])
        i = shard(zz, x, y, c)
        source, receive = out_ref.at[i], recv_sems.at[i, 0]
        if step == 0:
            source = x_ref
        else:
            landed(out_ref.at[i], receive, mate)
        sends.start(source, out_ref.at[i], receive, up, (zz <= z) & (z < 3))
        sends.start(source, out_ref.at[i], receive, down, (zz >= z) & (z > 0))
        sends.start(source, out_ref.at[i], receive, over)
        sends.start(source, out_ref.at[i], receive, side)
        sends.start(source, out_ref.at[i], receive, mate)

    def relay(step):
        zz = ordered(z, (0, 1, 2, 3)[step], (1, 0, 2, 3)[step])
        i = shard(zz, 1 - x, y, c)
        landed(out_ref.at[i], recv_sems.at[i, 0], mate)
        sends.start(halves(i, 0), halves(i, 0), recv_sems.at[i, 0], side)
        sends.start(out_ref.at[i], out_ref.at[i], recv_sems.at[i, 0], mate)
        i = shard(zz, x, 1 - y, c)
        landed(out_ref.at[i], recv_sems.at[i, 0], mate)
        sends.start(halves(i, 1), halves(i, 1), recv_sems.at[i, 1], over)
        sends.start(out_ref.at[i], out_ref.at[i], recv_sems.at[i, 0], mate)

    def corner(step):
        zz = ordered(z, (0, 1, 2, 3)[step], (1, 0, 2, 3)[step])
        i = shard(zz, 1 - x, 1 - y, c)
        for h in range(2):
            landed(halves(i, h), recv_sems.at[i, h], mate)
            sends.start(halves(i, h), halves(i, h), recv_sems.at[i, h], mate)

    whole(0)
    whole(1)
    relay(0)
    whole(2)
    relay(1)
    corner(0)
    whole(3)
    relay(2)
    corner(1)
    relay(3)
    corner(2)
    corner(3)
    for step in range(4):
        zz = ordered(z, (0, 1, 2, 3)[step], (1, 0, 2, 3)[step])
        for i in (shard(zz, x, y, 1 - c), shard(zz, 1 - x, y, 1 - c), shard(zz, x, 1 - y, 1 - c)):
            landed(out_ref.at[i], recv_sems.at[i, 0], mate)
        i = shard(zz, 1 - x, 1 - y, 1 - c)
        for h in range(2):
            landed(halves(i, h), recv_sems.at[i, h], mate)
    sends.finish()
    keep.wait()


def gather_all(value, number):
    if lax.axis_size("expert") != 8 or lax.axis_size("weight") != 4:
        return lax.all_gather(value, ("expert", "weight"), axis=0)
    out = jax.ShapeDtypeStruct((32,) + value.shape, value.dtype)
    return pl.pallas_call(
        gather_all_kernel,
        out_shape=out,
        in_specs=[pl.BlockSpec(memory_space=pltpu.VMEM)],
        out_specs=pl.BlockSpec(memory_space=pl.ANY),
        scratch_shapes=[
            pltpu.SemaphoreType.DMA((44,)),
            pltpu.SemaphoreType.DMA((32, 2)),
            pltpu.SemaphoreType.DMA,
        ],
        compiler_params=pltpu.CompilerParams(collective_id=number, has_side_effects=True),
        cost_estimate=cost(0, value, out),
    )(value)


def sum_all_kernel(
    p_ref,
    out_ref,
    own,
    mates,
    over_half,
    side_half,
    over_full,
    side_full,
    below,
    above,
    send_sems,
    mate_sems,
    half_sems,
    full_sems,
    line_sems,
    local_sems,
):
    z, x, y, c = places()
    rows = out_ref.shape[0]
    half = rows // 2
    over, side, mate = device(z, 1 - x, y, c), device(z, x, 1 - y, c), device(z, x, y, 1 - c)
    up, down = device(z + 1, x, y, c), device(z - 1, x, y, c)
    greet([(over, None), (side, None), (mate, None), (up, z < 3), (down, z > 0)])
    sends = Sends(send_sems)
    targets = [ordered(z, (3, 2, 1, 0)[step], (3, 0, 2, 1)[step]) for step in range(4)]
    spots = [(1 - x, 1 - y), (1 - x, y), (x, 1 - y), (x, y)]
    loads = []
    for step in range(4):
        zz = targets[step]
        for j, (xx, yy) in enumerate(spots):
            slot = step * 4 + j
            sends.start(
                p_ref.at[shard(zz, xx, yy, 1 - c)], mates.at[slot], mate_sems.at[slot], mate
            )
            load = pltpu.make_async_copy(
                p_ref.at[shard(zz, xx, yy, c)], own.at[slot], local_sems.at[slot]
            )
            load.start()
            loads.append(load)

    def join(slot):
        loads[slot].wait()
        landed(mates.at[slot], mate_sems.at[slot], mate)

    def corner(step):
        slot = step * 4
        join(slot)
        add_rows(own.at[slot], [(mates.at[slot], 0)], 0, rows)
        sends.start(
            own.at[slot, pl.ds(half, half)], over_half.at[step], half_sems.at[step, 0], over
        )
        sends.start(own.at[slot, pl.ds(0, half)], side_half.at[step], half_sems.at[step, 1], side)

    def relay(step):
        slot = step * 4 + 1
        join(slot)
        add_rows(own.at[slot], [(mates.at[slot], 0)], half, half)
        landed(side_half.at[step], half_sems.at[step, 1], mate)
        add_rows(own.at[slot], [(mates.at[slot], 0), (side_half.at[step], 0)], 0, half)
        sends.start(own.at[slot], over_full.at[step], full_sems.at[step, 0], over)
        slot = step * 4 + 2
        join(slot)
        add_rows(own.at[slot], [(mates.at[slot], 0)], 0, half)
        landed(over_half.at[step], half_sems.at[step, 0], mate)
        add_rows(own.at[slot], [(mates.at[slot], 0), (over_half.at[step], half)], half, half)
        sends.start(own.at[slot], side_full.at[step], full_sems.at[step, 1], side)

    def whole(step):
        zz = targets[step]
        slot = step * 4 + 3
        join(slot)
        landed(over_full.at[step], full_sems.at[step, 0], mate)
        landed(side_full.at[step], full_sems.at[step, 1], mate)
        add_rows(
            own.at[slot],
            [(mates.at[slot], 0), (over_full.at[step], 0), (side_full.at[step], 0)],
            0,
            rows,
        )

        @pl.when((zz >= z) & (z > 0))
        def _():
            landed(below.at[zz], line_sems.at[zz, 0], mate)
            add_rows(own.at[slot], [(below.at[zz], 0)], 0, rows)

        @pl.when((zz <= z) & (z < 3))
        def _():
            landed(above.at[zz], line_sems.at[zz, 1], mate)
            add_rows(own.at[slot], [(above.at[zz], 0)], 0, rows)

        if step < 3:
            sends.start(own.at[slot], below.at[zz], line_sems.at[zz, 0], up, zz > z)
            sends.start(own.at[slot], above.at[zz], line_sems.at[zz, 1], down, zz < z)

    corner(0)
    corner(1)
    relay(0)
    corner(2)
    relay(1)
    whole(0)
    corner(3)
    relay(2)
    whole(1)
    relay(3)
    whole(2)
    whole(3)
    out_ref[...] = own[15].astype(out_ref.dtype)
    sends.finish()


def sum_all(value, number):
    if lax.axis_size("expert") != 8 or lax.axis_size("weight") != 4:
        summed = lax.psum_scatter(
            value.reshape(-1, value.shape[2]), ("expert", "weight"), scatter_dimension=0, tiled=True
        )
        return summed.astype(jnp.float32)
    _, rows, width = value.shape
    out = jax.ShapeDtypeStruct((rows, width), jnp.float32)
    buffer = lambda n, r: pltpu.VMEM((n, r, width), value.dtype)
    return pl.pallas_call(
        sum_all_kernel,
        out_shape=out,
        in_specs=[pl.BlockSpec(memory_space=pl.ANY)],
        out_specs=pl.BlockSpec(memory_space=pltpu.VMEM),
        scratch_shapes=[
            buffer(16, rows),
            buffer(16, rows),
            buffer(4, rows // 2),
            buffer(4, rows // 2),
            buffer(4, rows),
            buffer(4, rows),
            buffer(4, rows),
            buffer(4, rows),
            pltpu.SemaphoreType.DMA((40,)),
            pltpu.SemaphoreType.DMA((16,)),
            pltpu.SemaphoreType.DMA((4, 2)),
            pltpu.SemaphoreType.DMA((4, 2)),
            pltpu.SemaphoreType.DMA((4, 2)),
            pltpu.SemaphoreType.DMA((16,)),
        ],
        compiler_params=pltpu.CompilerParams(
            collective_id=number, has_side_effects=True, vmem_limit_bytes=vmem_limit
        ),
        cost_estimate=cost(0, value, out),
    )(value)


def gather_group_kernel(x_ref, out_ref, send_sems, recv_sems, local_sem):
    z, x, y, c = places()
    half = x_ref.shape[0] // 2
    side, mate = device(z, x, 1 - y, c), device(z, x, y, 1 - c)
    greet([(side, None), (mate, None)])
    sends = Sends(send_sems)
    own, across = y * 2 + c, (1 - y) * 2 + c
    keep = pltpu.make_async_copy(x_ref, out_ref.at[own], local_sem)
    keep.start()

    def part(i, h):
        return out_ref.at[i, pl.ds(h * half, half)]

    for h in range(2):
        piece = x_ref.at[pl.ds(h * half, half)]
        sends.start(piece, part(own, h), recv_sems.at[own, h], side)
    for h in range(2):
        piece = x_ref.at[pl.ds(h * half, half)]
        sends.start(piece, part(own, h), recv_sems.at[own, h], mate)
    for h in range(2):
        landed(part(across, h), recv_sems.at[across, h], mate)
        sends.start(part(across, h), part(across, h), recv_sems.at[across, h], mate)
    for i in (y * 2 + 1 - c, (1 - y) * 2 + 1 - c):
        for h in range(2):
            landed(part(i, h), recv_sems.at[i, h], mate)
    sends.finish()
    keep.wait()


def gather_group(value, number):
    if lax.axis_size("expert") != 8 or lax.axis_size("weight") != 4:
        return lax.all_gather(value, "weight", axis=0, tiled=True)
    out = jax.ShapeDtypeStruct((4,) + value.shape, value.dtype)
    return pl.pallas_call(
        gather_group_kernel,
        out_shape=out,
        in_specs=[pl.BlockSpec(memory_space=pltpu.VMEM)],
        out_specs=pl.BlockSpec(memory_space=pltpu.VMEM),
        scratch_shapes=[
            pltpu.SemaphoreType.DMA((6,)),
            pltpu.SemaphoreType.DMA((4, 2)),
            pltpu.SemaphoreType.DMA,
        ],
        compiler_params=pltpu.CompilerParams(collective_id=number, has_side_effects=True),
        cost_estimate=cost(0, value, out),
    )(value).reshape(-1, value.shape[1])


def sum_group_kernel(p_ref, out_ref, mates, sides, carried, send_sems, mate_sems, side_sems):
    z, x, y, c = places()
    rows = out_ref.shape[0]
    half = rows // 2
    side, mate = device(z, x, 1 - y, c), device(z, x, y, 1 - c)
    greet([(side, None), (mate, None)])
    sends = Sends(send_sems)

    for j, yy in enumerate((1 - y, y)):
        for h in range(2):
            part = pl.ds(h * half, half)
            sends.start(
                p_ref.at[yy * 2 + 1 - c, part], mates.at[j, part], mate_sems.at[j, h], mate
            )

    def add(target, sources, h):
        step = 16

        def body(i, carry):
            part = pl.ds(pl.multiple_of(h * half + i * step, step), step)
            total = sources[0][part].astype(jnp.float32)
            for source in sources[1:]:
                total = total + source[part].astype(jnp.float32)
            target[part] = total.astype(target.dtype)
            return carry

        lax.fori_loop(0, half // step, body, 0)

    for h in range(2):
        part = pl.ds(h * half, half)
        landed(mates.at[0, part], mate_sems.at[0, h], mate)
        add(carried, [p_ref.at[(1 - y) * 2 + c], mates.at[0]], h)
        sends.start(carried.at[part], sides.at[part], side_sems.at[h], side)
    for h in range(2):
        part = pl.ds(h * half, half)
        landed(mates.at[1, part], mate_sems.at[1, h], mate)
        landed(sides.at[part], side_sems.at[h], mate)
        add(out_ref, [p_ref.at[y * 2 + c], mates.at[1], sides], h)
    sends.finish()


def sum_group(value, number):
    if lax.axis_size("expert") != 8 or lax.axis_size("weight") != 4:
        summed = lax.psum_scatter(value, "weight", scatter_dimension=0, tiled=True)
        return summed.astype(jnp.float32)
    rows, width = value.shape[0] // 4, value.shape[1]
    value = value.reshape(4, rows, width)
    out = jax.ShapeDtypeStruct((rows, width), jnp.float32)
    return pl.pallas_call(
        sum_group_kernel,
        out_shape=out,
        in_specs=[pl.BlockSpec(memory_space=pltpu.VMEM)],
        out_specs=pl.BlockSpec(memory_space=pltpu.VMEM),
        scratch_shapes=[
            pltpu.VMEM((2, rows, width), value.dtype),
            pltpu.VMEM((rows, width), value.dtype),
            pltpu.VMEM((rows, width), value.dtype),
            pltpu.SemaphoreType.DMA((6,)),
            pltpu.SemaphoreType.DMA((2, 2)),
            pltpu.SemaphoreType.DMA((2,)),
        ],
        compiler_params=pltpu.CompilerParams(collective_id=number, has_side_effects=True),
        cost_estimate=cost(0, value, out),
    )(value)


def per_device(
    tokens,
    cotangent,
    segments,
    routes,
    first_gain,
    query_weight,
    latent_weight,
    latent_gain,
    expand_weight,
    output_weight,
    second_gain,
    router_weight,
    shared_gate,
    shared_up,
    shared_down,
    expert_gate,
    expert_up,
    expert_down,
):
    weight_count = lax.axis_size("weight")
    token_rows = tokens.shape[0]
    width = tokens.shape[1]
    group_rows = token_rows * weight_count
    query_width = NOPE + ROPE
    heads_here = query_weight.shape[1] // query_width
    expert_count = router_weight.shape[1]
    local_experts = expert_gate.shape[0]
    score_scale = query_width ** (-0.5)
    activations = tokens.astype(jnp.float32)
    first_scale = inv_rms(activations)
    normed = (activations * first_scale * first_gain).astype(jnp.bfloat16)
    normed_all = gather_group(normed, 0)
    both = ("expert", "weight")
    expert_index = lax.axis_index("expert")
    expert_lanes = lax.axis_size("expert")
    blocks = expert_lanes * weight_count
    pairs = blocks // 2
    pair_rows = 2 * token_rows
    all_rows = blocks * token_rows
    slot_rows = blocks * CAP
    choose = (
        routes[:, :, None] == jnp.arange(expert_count, dtype=jnp.int32)[None, None, :]
    ).astype(jnp.float32)
    hit = jnp.sum(choose, axis=1)
    order = jnp.arange(token_rows, dtype=jnp.int32)
    before = (order[None, :] < order[:, None]).astype(jnp.bfloat16)
    place = matmul(before, hit.astype(jnp.bfloat16))
    rank = jnp.sum(choose * jnp.arange(routes.shape[1], dtype=jnp.float32)[None, :, None], axis=1)
    code = jnp.where(hit > 0, 32.0 * rank + place, -1.0)
    extra = jnp.pad(code, ((0, 0), (0, lanes - expert_count)), constant_values=-1.0)
    cotangent_wide = jnp.concatenate([cotangent, extra.astype(jnp.bfloat16)], axis=1)
    column = jnp.arange(lanes, dtype=jnp.int32)[None, :]
    row = jnp.arange(8, dtype=jnp.int32)[:, None]
    first_here = expert_index * local_experts
    here = (row < local_experts) & (column == first_here + row)
    twice = here | ((row < local_experts) & (column == first_here + row + expert_count))
    here, twice = here.astype(jnp.bfloat16), twice.astype(jnp.bfloat16)
    weight_index = lax.axis_index("weight")
    high_column = 2 * (row * weight_count + weight_index)
    known = row < routes.shape[1]
    high_at = (known & (column == high_column)).astype(jnp.bfloat16)
    low_at = (known & (column == high_column + 1)).astype(jnp.bfloat16)
    shared_here = shared_gate.shape[1] // expert_lanes
    shared_wide = -(-shared_here // lanes) * lanes
    start = expert_index * shared_here

    def shared_part(matrix):
        part = lax.dynamic_slice_in_dim(matrix, start, shared_here, axis=0)
        return jnp.pad(part, ((0, shared_wide - shared_here), (0, 0)))

    gate_part = shared_part(shared_gate.T)
    up_part = shared_part(shared_up.T)
    down_part = shared_part(shared_down)
    shape = jax.ShapeDtypeStruct
    whole = lambda array: (array, whole_spec(array))
    slots = shape((local_experts, slot_rows, width), jnp.bfloat16)
    slots_one = shape((local_experts, slot_rows, lanes), jnp.float32)
    gather_flops = 2 * all_rows * width * (2 * CAP * local_experts + shared_wide)
    cotangent_all = lax.all_gather(cotangent_wide, both, axis=0, tiled=True)
    marks = (cotangent_all, pl.BlockSpec((pair_rows, lanes), lambda i: (i, width // lanes)))
    grads_slots, shared_raw = call(
        grads_kernel,
        pairs,
        [whole(here), (cotangent_all, pair_spec(cotangent_all, pairs)), whole(down_part)],
        [
            (slots, slots_spec(slots, pairs)),
            (shape((all_rows, shared_wide), jnp.float32), pl.BlockSpec((pair_rows, shared_wide), lambda i: (i, 0))),
        ],
        gather_flops,
    )
    cosine, sine = rope_tables(segments[0])
    allowed = attention_mask(segments[0])
    query_full = matmul(normed_all, query_weight).reshape(group_rows, heads_here, query_width)
    query = jnp.concatenate(
        [
            query_full[..., :NOPE],
            rotate(query_full[..., NOPE:], cosine[:, None, :], sine[:, None, :]),
        ],
        axis=-1,
    ).astype(jnp.bfloat16)
    compressed = matmul(normed_all, latent_weight)
    latent = compressed[:, :LATENT]
    latent_scale = inv_rms(latent)
    latent_normed = (latent * latent_scale * latent_gain).astype(jnp.bfloat16)
    key_rope = rotate(compressed[:, LATENT:], cosine, sine).astype(jnp.bfloat16)
    expanded = (
        matmul(latent_normed, expand_weight)
        .astype(jnp.bfloat16)
        .reshape(group_rows, heads_here, NOPE + VDIM)
    )
    key_nope = expanded[..., :NOPE]
    values = expanded[..., NOPE:]

    def score_block():
        raw = jnp.einsum(
            "ihd,jhd->hij", query[..., :NOPE], key_nope, preferred_element_type=jnp.float32
        )
        raw = raw + jnp.einsum(
            "ihd,jd->hij", query[..., NOPE:], key_rope, preferred_element_type=jnp.float32
        )
        return jnp.where(allowed[None], raw * score_scale, -1e30)

    scores = score_block()
    peak = jnp.max(scores, axis=-1, keepdims=True)
    weights = jnp.exp(scores - peak)
    total = jnp.sum(weights, axis=-1, keepdims=True)
    log_total = peak + jnp.log(total)
    mixed = jnp.einsum(
        "hij,jhd->ihd",
        (weights / total).astype(jnp.bfloat16),
        values,
        preferred_element_type=jnp.float32,
    )
    mixed = mixed.astype(jnp.bfloat16).reshape(group_rows, heads_here * VDIM)
    attended = sum_group(matmul(mixed, output_weight).astype(jnp.bfloat16), 1)
    hidden_one = activations + attended
    second_scale = inv_rms(hidden_one)
    normed_two = (hidden_one * second_scale * second_gain).astype(jnp.bfloat16)
    gates = jax.nn.sigmoid(matmul(normed_two, router_weight))
    chosen = jnp.sum(choose * gates[:, None, :], axis=-1)
    chosen_total = jnp.sum(chosen, axis=1, keepdims=True)
    mixing = route_scale * chosen / chosen_total
    upstream = cotangent.astype(jnp.float32)
    mixing_at = jnp.sum(choose * mixing[:, :, None], axis=1)
    mixing_high = mixing_at.astype(jnp.bfloat16)
    mixing_low = (mixing_at - mixing_high.astype(jnp.float32)).astype(jnp.bfloat16)
    normed_wide = jnp.concatenate([normed_two, mixing_high, mixing_low], axis=1)
    normed_tokens = gather_all(normed_wide, 2).reshape(all_rows, -1)
    token_spec = pl.BlockSpec((pair_rows, shared_wide), lambda i: (i, 0))
    token_shape = shape((all_rows, shared_wide), jnp.bfloat16)
    rows_slots, mix_slots, shared_hidden, shared_gate_grad, shared_lift_grad = call(
        rows_kernel,
        pairs,
        [
            whole(here),
            whole(twice),
            marks,
            (normed_tokens, pair_spec(normed_tokens, pairs)),
            (shared_raw, token_spec),
            whole(gate_part),
            whole(up_part),
        ],
        [
            (slots, slots_spec(slots, pairs)),
            (slots_one, slots_spec(slots_one, pairs)),
            (token_shape, token_spec),
            (token_shape, token_spec),
            (token_shape, token_spec),
        ],
        gather_flops + 2 * all_rows * width * shared_wide,
    )
    hidden_here = expert_gate.shape[2]
    gate_rows, up_rows = expert_gate.transpose(0, 2, 1), expert_up.transpose(0, 2, 1)
    tile = slot_rows // 2
    tile_spec = lambda n: pl.BlockSpec((1, tile, n), lambda i: (i // 2, i % 2, 0))
    expert_spec = lambda m: pl.BlockSpec((1,) + m.shape[1:], lambda i: (i // 2, 0, 0))
    narrow = shape((local_experts, slot_rows, hidden_here), jnp.bfloat16)
    one_matmul = 2 * local_experts * slot_rows * width * hidden_here
    routed_hidden, gate_grad, lift_grad, returned, mix_grad_slots = call(
        experts_kernel,
        2 * local_experts,
        [
            (rows_slots, tile_spec(width)),
            (grads_slots, tile_spec(width)),
            (mix_slots, tile_spec(lanes)),
            (gate_rows, expert_spec(gate_rows)),
            (up_rows, expert_spec(up_rows)),
            (expert_down, expert_spec(expert_down)),
        ],
        [
            (narrow, tile_spec(hidden_here)),
            (narrow, tile_spec(hidden_here)),
            (narrow, tile_spec(hidden_here)),
            (slots, tile_spec(width)),
            (slots_one, tile_spec(lanes)),
        ],
        5 * one_matmul,
    )
    dense = shape((all_rows, width), jnp.bfloat16)
    dense_spec = pl.BlockSpec((pair_rows, width), lambda i: (i, 0))
    dense_wide = shape((all_rows, width + lanes), jnp.bfloat16)
    (back_dense,) = call(
        back_kernel,
        pairs,
        [
            whole(here),
            whole(high_at),
            whole(low_at),
            marks,
            (returned, slots_spec(slots, pairs)),
            (mix_grad_slots, slots_spec(slots_one, pairs)),
            (shared_gate_grad, token_spec),
            (shared_lift_grad, token_spec),
            whole(gate_part),
            whole(up_part),
        ],
        [(dense_wide, pair_spec(dense_wide, pairs))],
        gather_flops + 2 * all_rows * width * shared_wide,
    )
    back_here = sum_all(back_dense.reshape(blocks, token_rows, -1), 3)
    routed_back = back_here[:, :width]
    mix_grad = back_here[:, width : width + 2 * weight_count * routes.shape[1]]
    mix_grad = jnp.sum(mix_grad.reshape(token_rows, routes.shape[1], -1), axis=2)
    (produced,) = call(
        produce_kernel,
        2 * local_experts,
        [(routed_hidden, tile_spec(hidden_here)), (expert_down, expert_spec(expert_down))],
        [(slots, tile_spec(width))],
        one_matmul,
    )
    (out_dense,) = call(
        out_kernel,
        pairs,
        [
            whole(here),
            marks,
            (produced, slots_spec(slots, pairs)),
            (shared_hidden, token_spec),
            whole(down_part),
        ],
        [(dense, dense_spec)],
        gather_flops,
    )
    routed_out = lax.psum_scatter(out_dense, both, scatter_dimension=0, tiled=True).astype(jnp.float32)
    expert_grads = (
        jnp.einsum("jsf,jsd->jfd", gate_grad, rows_slots, preferred_element_type=jnp.float32).transpose(0, 2, 1),
        jnp.einsum("jsf,jsd->jfd", lift_grad, rows_slots, preferred_element_type=jnp.float32).transpose(0, 2, 1),
        jnp.einsum("jsf,jsd->jfd", routed_hidden, grads_slots, preferred_element_type=jnp.float32),
    )
    normed_plain, cotangent_plain = normed_tokens[:, :width], cotangent_all[:, :width]
    shared_grads = jnp.concatenate(
        [
            trans_times(shared_gate_grad, normed_plain)[:shared_here],
            trans_times(shared_lift_grad, normed_plain)[:shared_here],
            trans_times(shared_hidden, cotangent_plain)[:shared_here],
        ],
        axis=0,
    ).astype(jnp.bfloat16)
    swapped = lax.all_to_all(shared_grads, "expert", split_axis=1, concat_axis=0, tiled=True)
    swapped = swapped.reshape(expert_lanes, 3, shared_here, -1).astype(jnp.float32)
    shared_gradients = [swapped[:, i].reshape(expert_lanes * shared_here, -1) for i in range(3)]
    layer_out = (hidden_one + routed_out).astype(jnp.bfloat16)
    chosen_grad = route_scale * (
        mix_grad / chosen_total
        - jnp.sum(mix_grad * chosen, axis=1, keepdims=True) / chosen_total**2
    )
    logit_grad = jnp.sum(choose * chosen_grad[:, :, None], axis=1) * gates * (1.0 - gates)
    normed_two_grad = (
        routed_back
        + jnp.dot(logit_grad, router_weight.astype(jnp.float32).T, precision=highest)
    )
    router_gradient = jnp.dot(normed_two.astype(jnp.float32).T, logit_grad, precision=highest)
    back_two, second_gain_gradient = norm_back(
        normed_two_grad, hidden_one, second_scale, second_gain
    )
    hidden_grad = upstream + back_two
    hidden_group = gather_group(hidden_grad.astype(jnp.bfloat16), 4)
    output_gradient = trans_times(mixed, hidden_group)
    mixed_grad = (
        times_trans(hidden_group, output_weight)
        .astype(jnp.bfloat16)
        .reshape(group_rows, heads_here, VDIM)
    )
    probs = jnp.exp(score_block() - log_total)
    prob_grad = jnp.einsum("ihd,jhd->hij", mixed_grad, values, preferred_element_type=jnp.float32)
    centre = jnp.sum(probs * prob_grad, axis=-1, keepdims=True)
    score_grad = (probs * (prob_grad - centre)).astype(jnp.bfloat16)
    value_grad = jnp.einsum(
        "hij,ihd->jhd", probs.astype(jnp.bfloat16), mixed_grad, preferred_element_type=jnp.float32
    )
    query_nope_grad = (
        jnp.einsum("hij,jhd->ihd", score_grad, key_nope, preferred_element_type=jnp.float32)
        * score_scale
    )
    query_rope_grad = (
        jnp.einsum("hij,jd->ihd", score_grad, key_rope, preferred_element_type=jnp.float32)
        * score_scale
    )
    key_nope_grad = (
        jnp.einsum(
            "hij,ihd->jhd", score_grad, query[..., :NOPE], preferred_element_type=jnp.float32
        )
        * score_scale
    )
    key_rope_grad = (
        jnp.einsum("hij,ihd->jd", score_grad, query[..., NOPE:], preferred_element_type=jnp.float32)
        * score_scale
    )
    query_grad = jnp.concatenate(
        [query_nope_grad, unrotate(query_rope_grad, cosine[:, None, :], sine[:, None, :])], axis=-1
    )
    query_grad = query_grad.astype(jnp.bfloat16).reshape(group_rows, heads_here * query_width)
    expand_grad = (
        jnp.concatenate([key_nope_grad, value_grad], axis=-1)
        .astype(jnp.bfloat16)
        .reshape(group_rows, heads_here * (NOPE + VDIM))
    )
    query_gradient = trans_times(normed_all, query_grad)
    expand_gradient = trans_times(latent_normed, expand_grad)
    latent_normed_grad = times_trans(expand_grad, expand_weight)
    latent_back, latent_gain_gradient = norm_back(
        latent_normed_grad, latent, latent_scale, latent_gain
    )
    compressed_grad = jnp.concatenate([latent_back, unrotate(key_rope_grad, cosine, sine)], axis=-1)
    compressed_grad = compressed_grad.astype(jnp.bfloat16)
    latent_weight_gradient = trans_times(normed_all, compressed_grad)
    normed_grad = sum_group(
        (
            times_trans(query_grad, query_weight) + times_trans(compressed_grad, latent_weight)
        ).astype(jnp.bfloat16),
        5,
    )
    back_one, first_gain_gradient = norm_back(normed_grad, activations, first_scale, first_gain)
    token_gradient = hidden_grad + back_one
    shards = (
        lax.psum_scatter(
            query_gradient.astype(jnp.bfloat16), "expert", scatter_dimension=0, tiled=True
        ).astype(jnp.float32),
        lax.psum_scatter(
            expand_gradient.astype(jnp.bfloat16), "expert", scatter_dimension=0, tiled=True
        ).astype(jnp.float32),
        lax.psum_scatter(
            output_gradient.astype(jnp.bfloat16), "expert", scatter_dimension=1, tiled=True
        ).astype(jnp.float32),
    )
    totals = lax.psum(
        (
            latent_weight_gradient,
            latent_gain_gradient,
            router_gradient,
            first_gain_gradient,
            second_gain_gradient,
        ),
        ("expert", "weight"),
    )
    return (
        layer_out,
        token_gradient,
        totals[3],
        shards[0],
        totals[0],
        totals[1],
        shards[1],
        shards[2],
        totals[4],
        totals[2],
        shared_gradients[0].T,
        shared_gradients[1].T,
        shared_gradients[2],
        expert_grads[0],
        expert_grads[1],
        expert_grads[2],
    )


def solution(mesh):
    return jax.shard_map(
        per_device,
        mesh=mesh,
        in_specs=(
            P(("expert", "weight"), None),
            P(("expert", "weight"), None),
            P("expert", None),
            P(("expert", "weight"), None),
            P(),
            P(None, "weight"),
            P(),
            P(),
            P(None, "weight"),
            P("weight", None),
            P(),
            P(),
            P(None, "weight"),
            P(None, "weight"),
            P("weight", None),
            P("expert", None, "weight"),
            P("expert", None, "weight"),
            P("expert", "weight", None),
        ),
        out_specs=(
            P(("expert", "weight"), None),
            P(("expert", "weight"), None),
            P(),
            P("expert", "weight"),
            P(),
            P(),
            P("expert", "weight"),
            P("weight", "expert"),
            P(),
            P(),
            P("expert", "weight"),
            P("expert", "weight"),
            P("weight", "expert"),
            P("expert", None, "weight"),
            P("expert", None, "weight"),
            P("expert", "weight", None),
        ),
        check_vma=False,
    )
```

```python
import functools

import jax
import jax.numpy as jnp
from jax import lax
from jax.experimental import pallas as pl
from jax.experimental.pallas import tpu as pltpu
from jax.sharding import PartitionSpec as P

NOPE = 128
ROPE = 64
VDIM = 128
LATENT = 512
TOPK = 6
CAP = 20


eps = 1e-06
route_scale = 2.446
rope_base = 50000.0
highest = lax.Precision.HIGHEST


def matmul(left, right):
    return jnp.dot(left, right, preferred_element_type=jnp.float32)


def trans_times(left, right):
    return lax.dot_general(
        left, right, (((0,), (0,)), ((), ())), preferred_element_type=jnp.float32
    )


def times_trans(left, right):
    return lax.dot_general(
        left, right, (((1,), (1,)), ((), ())), preferred_element_type=jnp.float32
    )


def inv_rms(value):
    return lax.rsqrt(jnp.mean(value * value, axis=-1, keepdims=True) + eps)


def norm_back(grad_out, value, scale, gain):
    scaled = grad_out * gain
    grad_in = scale * scaled - value * scale**3 * jnp.mean(scaled * value, axis=-1, keepdims=True)
    gain_grad = jnp.sum(grad_out * value * scale, axis=0)
    return (grad_in, gain_grad)


def rope_tables(seg):
    size = seg.shape[0]
    index = jnp.arange(size, dtype=jnp.int32)
    fresh = jnp.concatenate([jnp.ones((1,), dtype=bool), seg[1:] != seg[:-1]])
    first = lax.cummax(jnp.where(fresh, index, jnp.zeros_like(index)), axis=0)
    place = (index - first).astype(jnp.float32)
    half = ROPE // 2
    freqs = rope_base ** (-(jnp.arange(half, dtype=jnp.float32) * 2.0 / ROPE))
    angle = place[:, None] * freqs[None, :]
    return (jnp.cos(angle), jnp.sin(angle))


def attention_mask(seg):
    index = jnp.arange(seg.shape[0], dtype=jnp.int32)
    return (seg[:, None] == seg[None, :]) & (index[None, :] <= index[:, None])


def rotate(value, cosine, sine):
    half = value.shape[-1] // 2
    first, second = (value[..., :half], value[..., half:])
    return jnp.concatenate(
        [first * cosine - second * sine, second * cosine + first * sine], axis=-1
    )


def unrotate(value, cosine, sine):
    half = value.shape[-1] // 2
    first, second = (value[..., :half], value[..., half:])
    return jnp.concatenate(
        [first * cosine + second * sine, second * cosine - first * sine], axis=-1
    )


lanes = 128
vmem_limit = 64 * 1024 * 1024 - 131072


def token_slots(marks, here, local_experts, half):
    codes = times_trans(here, marks)
    count = codes.shape[1]
    rank = jnp.floor(codes * (1.0 / 32.0))
    place = codes - 32.0 * rank
    token = lax.broadcasted_iota(jnp.int32, codes.shape, 1)
    slot = jnp.where(codes >= 0, place + jnp.where(token >= half, float(CAP), 0.0), -1.0)
    row = lax.broadcasted_iota(jnp.int32, (2 * CAP, count), 0).astype(jnp.float32)
    picks = [jnp.where(row == slot[e : e + 1], 1.0, 0.0) for e in range(local_experts)]
    return picks, rank


def gather_rows(picks, values, out_ref):
    rows = jnp.dot(
        jnp.concatenate(picks, axis=0).astype(jnp.bfloat16),
        values,
        preferred_element_type=jnp.float32,
    )
    for e in range(len(picks)):
        out_ref[e] = rows[e * 2 * CAP : (e + 1) * 2 * CAP].astype(jnp.bfloat16)


def grads_kernel(here_ref, value_ref, down_ref, rows_ref, back_ref):
    width = rows_ref.shape[2]
    local_experts, half = rows_ref.shape[0], value_ref.shape[0] // 2
    picks, _ = token_slots(value_ref[:, width:], here_ref[...], local_experts, half)
    values = value_ref[:, :width]
    gather_rows(picks, values, rows_ref)
    back_ref[...] = times_trans(values, down_ref[...])


def rows_kernel(
    here_ref,
    twice_ref,
    marks_ref,
    value_ref,
    back_ref,
    gate_ref,
    up_ref,
    rows_ref,
    mix_ref,
    hidden_ref,
    gate_grad_ref,
    lift_grad_ref,
):
    width = rows_ref.shape[2]
    local_experts, half = rows_ref.shape[0], value_ref.shape[0] // 2
    picks, _ = token_slots(marks_ref[...], here_ref[...], local_experts, half)
    values = value_ref[:, :width]
    gather_rows(picks, values, rows_ref)
    mixing = times_trans(twice_ref[...], value_ref[:, width:])
    for e in range(local_experts):
        column = jnp.sum(picks[e] * mixing[e : e + 1], axis=1, keepdims=True)
        mix_ref[e] = jnp.broadcast_to(column, mix_ref.shape[1:])
    gate = times_trans(values, gate_ref[...])
    lift = times_trans(values, up_ref[...])
    back = back_ref[...]
    sigma = jax.nn.sigmoid(gate)
    active = gate * sigma
    hidden_ref[...] = (active * lift).astype(jnp.bfloat16)
    gate_grad_ref[...] = (back * lift * sigma * (1.0 + gate * (1.0 - sigma))).astype(jnp.bfloat16)
    lift_grad_ref[...] = (back * active).astype(jnp.bfloat16)


def experts_kernel(
    rows_ref,
    grads_ref,
    mix_ref,
    gate_ref,
    up_ref,
    down_ref,
    hidden_ref,
    gate_grad_ref,
    lift_grad_ref,
    returned_ref,
    mix_grad_ref,
):
    rows, gate_matrix, up_matrix = rows_ref[0], gate_ref[0], up_ref[0]
    gate = times_trans(rows, gate_matrix)
    lift = times_trans(rows, up_matrix)
    back = times_trans(grads_ref[0], down_ref[0])
    mix = mix_ref[0][:, :1]
    sigma = jax.nn.sigmoid(gate)
    active = gate * sigma
    hidden = active * lift
    mix_grad = jnp.sum(hidden * back, axis=1, keepdims=True)
    mix_grad_ref[0] = jnp.broadcast_to(mix_grad, mix_grad_ref.shape[1:])
    hidden_ref[0] = (mix * hidden).astype(jnp.bfloat16)
    back = back * mix
    gate_grad = (back * lift * sigma * (1.0 + gate * (1.0 - sigma))).astype(jnp.bfloat16)
    lift_grad = (back * active).astype(jnp.bfloat16)
    gate_grad_ref[0] = gate_grad
    lift_grad_ref[0] = lift_grad
    returned = matmul(gate_grad, gate_matrix) + matmul(lift_grad, up_matrix)
    returned_ref[0] = returned.astype(jnp.bfloat16)


def produce_kernel(hidden_ref, down_ref, out_ref):
    out_ref[0] = matmul(hidden_ref[0], down_ref[0]).astype(jnp.bfloat16)


def spread_rows(picks, rows_ref):
    rows = jnp.concatenate([rows_ref[e].astype(jnp.float32) for e in range(len(picks))], axis=0)
    pick = jnp.concatenate(picks, axis=0).astype(jnp.bfloat16)
    return trans_times(pick, rows.astype(jnp.bfloat16))


def back_kernel(
    here_ref,
    high_ref,
    low_ref,
    marks_ref,
    rows_ref,
    mix_grad_ref,
    gate_grad_ref,
    lift_grad_ref,
    gate_ref,
    up_ref,
    out_ref,
):
    width = rows_ref.shape[2]
    local_experts, half = rows_ref.shape[0], out_ref.shape[0] // 2
    picks, rank = token_slots(marks_ref[...], here_ref[...], local_experts, half)
    total = spread_rows(picks, rows_ref)
    total = total + matmul(gate_grad_ref[...], gate_ref[...])
    total = total + matmul(lift_grad_ref[...], up_ref[...])
    out_ref[:, :width] = total.astype(jnp.bfloat16)
    choice = lax.broadcasted_iota(jnp.int32, rank.shape, 0).astype(jnp.float32)
    mix_grad = jnp.zeros(rank.shape, jnp.float32)
    for e in range(local_experts):
        row = jnp.sum(picks[e] * mix_grad_ref[e][:, :1], axis=0, keepdims=True)
        mix_grad = mix_grad + jnp.where(choice == rank[e : e + 1], row, 0.0)
    high = mix_grad.astype(jnp.bfloat16)
    low = (mix_grad - high.astype(jnp.float32)).astype(jnp.bfloat16)
    sent = trans_times(high, high_ref[...]) + trans_times(low, low_ref[...])
    out_ref[:, width:] = sent.astype(jnp.bfloat16)


def out_kernel(here_ref, marks_ref, rows_ref, hidden_ref, down_ref, out_ref):
    local_experts, half = rows_ref.shape[0], out_ref.shape[0] // 2
    picks, _ = token_slots(marks_ref[...], here_ref[...], local_experts, half)
    total = spread_rows(picks, rows_ref)
    total = total + matmul(hidden_ref[...], down_ref[...])
    out_ref[...] = total.astype(jnp.bfloat16)


def whole_spec(array):
    zeros = (0,) * array.ndim
    return pl.BlockSpec(array.shape, lambda i: zeros)


def pair_spec(array, pairs):
    block = (array.shape[0] // pairs,) + array.shape[1:]
    zeros = (0,) * (array.ndim - 1)
    return pl.BlockSpec(block, lambda i: (i,) + zeros)


def slots_spec(array, pairs):
    block = (array.shape[0], array.shape[1] // pairs) + array.shape[2:]
    return pl.BlockSpec(block, lambda i: (0, i, 0))


def cost(flops, *arrays):
    moved = sum(a.size * a.dtype.itemsize for a in arrays)
    return pl.CostEstimate(flops=int(flops), bytes_accessed=int(moved), transcendentals=0)


def call(kernel, grid, ins, outs, flops):
    arrays = [a for a, _ in ins]
    shapes = [s for s, _ in outs]
    return pl.pallas_call(
        kernel,
        grid=(grid,),
        in_specs=[s for _, s in ins],
        out_specs=[s for _, s in outs],
        out_shape=shapes,
        cost_estimate=cost(flops, *arrays, *shapes),
        compiler_params=pltpu.CompilerParams(vmem_limit_bytes=vmem_limit),
    )(*arrays)


MESH = pl.DeviceIdType.MESH


def places():
    expert, weight = lax.axis_index("expert"), lax.axis_index("weight")
    return lax.div(expert, 2), lax.rem(expert, 2), lax.div(weight, 2), lax.rem(weight, 2)


def device(z, x, y, c):
    return (z * 2 + x, y * 2 + c)


def shard(z, x, y, c):
    return z * 8 + x * 4 + y * 2 + c


def push(source, target, send, receive, to):
    return pltpu.make_async_remote_copy(
        src_ref=source,
        dst_ref=target,
        send_sem=send,
        recv_sem=receive,
        device_id=to,
        device_id_type=MESH,
    )


class Sends:
    def __init__(self, semaphores):
        self.semaphores = semaphores
        self.started = []

    def plan(self, source, target, receive, to, when=None):
        copy = push(source, target, self.semaphores.at[len(self.started)], receive, to)
        self.started.append((copy, when))
        return copy

    def start(self, source, target, receive, to, when=None):
        copy = self.plan(source, target, receive, to, when)
        if when is None:
            copy.start()
        else:
            pl.when(when)(copy.start)

    def finish(self):
        for copy, when in self.started:
            if when is None:
                copy.wait_send()
            else:
                pl.when(when)(copy.wait_send)


def landed(target, receive, to):
    push(target, target, receive, receive, to).wait_recv()


def greet(devices):
    barrier = pltpu.get_barrier_semaphore()
    count = 0
    for to, when in devices:
        signal = functools.partial(
            pl.semaphore_signal, barrier, inc=1, device_id=to, device_id_type=MESH
        )
        if when is None:
            signal()
            count = count + 1
        else:
            pl.when(when)(signal)
            count = count + when.astype(jnp.int32)
    pl.semaphore_wait(barrier, count)


def add_rows(target, sources, start, rows):
    step = 16

    def body(i, carry):
        part = pl.ds(pl.multiple_of(start + i * step, step), step)
        total = target[part].astype(jnp.float32)
        for source, offset in sources:
            there = pl.ds(pl.multiple_of(start - offset + i * step, step), step)
            total = total + source[there].astype(jnp.float32)
        target[part] = total.astype(target.dtype)
        return carry

    lax.fori_loop(0, rows // step, body, 0)


def ordered(z, first, second):
    upper = lax.div(z, 2)
    inner = z + upper * (3 - 2 * z)
    value = first + inner * (second - first)
    return value + upper * (3 - 2 * value)


def gather_all_kernel(x_ref, out_ref, send_sems, recv_sems, local_sem):
    z, x, y, c = places()
    half = x_ref.shape[0] // 2
    over, side, mate = device(z, 1 - x, y, c), device(z, x, 1 - y, c), device(z, x, y, 1 - c)
    up, down = device(z + 1, x, y, c), device(z - 1, x, y, c)
    greet([(over, None), (side, None), (mate, None), (up, z < 3), (down, z > 0)])
    sends = Sends(send_sems)
    own = shard(z, x, y, c)
    keep = pltpu.make_async_copy(x_ref, out_ref.at[own], local_sem)
    keep.start()

    def halves(i, h):
        return out_ref.at[i, pl.ds(h * half, half)]

    def whole(step):
        zz = ordered(z, (0, 1, 2, 3)[step], (1, 0, 2, 3)[step])
        i = shard(zz, x, y, c)
        source, receive = out_ref.at[i], recv_sems.at[i, 0]
        if step == 0:
            source = x_ref
        else:
            landed(out_ref.at[i], receive, mate)
        sends.start(source, out_ref.at[i], receive, up, (zz <= z) & (z < 3))
        sends.start(source, out_ref.at[i], receive, down, (zz >= z) & (z > 0))
        sends.start(source, out_ref.at[i], receive, over)
        sends.start(source, out_ref.at[i], receive, side)
        sends.start(source, out_ref.at[i], receive, mate)

    def relay(step):
        zz = ordered(z, (0, 1, 2, 3)[step], (1, 0, 2, 3)[step])
        i = shard(zz, 1 - x, y, c)
        landed(out_ref.at[i], recv_sems.at[i, 0], mate)
        sends.start(halves(i, 0), halves(i, 0), recv_sems.at[i, 0], side)
        sends.start(out_ref.at[i], out_ref.at[i], recv_sems.at[i, 0], mate)
        i = shard(zz, x, 1 - y, c)
        landed(out_ref.at[i], recv_sems.at[i, 0], mate)
        sends.start(halves(i, 1), halves(i, 1), recv_sems.at[i, 1], over)
        sends.start(out_ref.at[i], out_ref.at[i], recv_sems.at[i, 0], mate)

    def corner(step):
        zz = ordered(z, (0, 1, 2, 3)[step], (1, 0, 2, 3)[step])
        i = shard(zz, 1 - x, 1 - y, c)
        for h in range(2):
            landed(halves(i, h), recv_sems.at[i, h], mate)
            sends.start(halves(i, h), halves(i, h), recv_sems.at[i, h], mate)

    whole(0)
    whole(1)
    relay(0)
    whole(2)
    relay(1)
    corner(0)
    whole(3)
    relay(2)
    corner(1)
    relay(3)
    corner(2)
    corner(3)
    for step in range(4):
        zz = ordered(z, (0, 1, 2, 3)[step], (1, 0, 2, 3)[step])
        for i in (shard(zz, x, y, 1 - c), shard(zz, 1 - x, y, 1 - c), shard(zz, x, 1 - y, 1 - c)):
            landed(out_ref.at[i], recv_sems.at[i, 0], mate)
        i = shard(zz, 1 - x, 1 - y, 1 - c)
        for h in range(2):
            landed(halves(i, h), recv_sems.at[i, h], mate)
    sends.finish()
    keep.wait()


def gather_all(value, number):
    if lax.axis_size("expert") != 8 or lax.axis_size("weight") != 4:
        return lax.all_gather(value, ("expert", "weight"), axis=0)
    out = jax.ShapeDtypeStruct((32,) + value.shape, value.dtype)
    return pl.pallas_call(
        gather_all_kernel,
        out_shape=out,
        in_specs=[pl.BlockSpec(memory_space=pltpu.VMEM)],
        out_specs=pl.BlockSpec(memory_space=pl.ANY),
        scratch_shapes=[
            pltpu.SemaphoreType.DMA((44,)),
            pltpu.SemaphoreType.DMA((32, 2)),
            pltpu.SemaphoreType.DMA,
        ],
        compiler_params=pltpu.CompilerParams(collective_id=number, has_side_effects=True),
        cost_estimate=cost(0, value, out),
    )(value)


def sum_all_kernel(inner, cover_ins, cover_outs, p_ref, *refs):
    ins, refs = refs[:cover_ins], refs[cover_ins:]
    out_ref, refs = refs[0], refs[1:]
    outs, refs = refs[:cover_outs], refs[cover_outs:]
    own, mates, over_half, side_half, over_full, side_full, below, above = refs[:8]
    send_sems, mate_sems, half_sems, full_sems, line_sems, local_sems = refs[8:]
    z, x, y, c = places()
    turn, turns = pl.program_id(0), pl.num_programs(0)
    rows = out_ref.shape[0]
    half = rows // 2
    over, side, mate = device(z, 1 - x, y, c), device(z, x, 1 - y, c), device(z, x, y, 1 - c)
    up, down = device(z + 1, x, y, c), device(z - 1, x, y, c)
    sends = Sends(send_sems)
    targets = [ordered(z, (3, 2, 1, 0)[step], (3, 0, 2, 1)[step]) for step in range(4)]
    spots = [(1 - x, 1 - y), (1 - x, y), (x, 1 - y), (x, y)]
    shards = [[shard(zz, xx, yy, 1 - c) for xx, yy in spots] for zz in targets]
    mine = [[shard(zz, xx, yy, c) for xx, yy in spots] for zz in targets]
    higher = [zz > z for zz in targets]
    lower = [zz < z for zz in targets]
    loads = [
        pltpu.make_async_copy(p_ref.at[mine[slot // 4][slot % 4]], own.at[slot], local_sems.at[slot])
        for slot in range(16)
    ]

    mate_copies = [
        sends.plan(p_ref.at[shards[slot // 4][slot % 4]], mates.at[slot], mate_sems.at[slot], mate)
        for slot in range(16)
    ]
    corner_copies, relay_copies, line_copies = [], [], []
    for step in range(4):
        corner_copies.append(
            (
                sends.plan(
                    own.at[step * 4, pl.ds(half, half)],
                    over_half.at[step],
                    half_sems.at[step, 0],
                    over,
                ),
                sends.plan(
                    own.at[step * 4, pl.ds(0, half)], side_half.at[step], half_sems.at[step, 1], side
                ),
            )
        )
        relay_copies.append(
            (
                sends.plan(
                    own.at[step * 4 + 1], over_full.at[step], full_sems.at[step, 0], over
                ),
                sends.plan(
                    own.at[step * 4 + 2], side_full.at[step], full_sems.at[step, 1], side
                ),
            )
        )
    for step in range(3):
        zz, slot = targets[step], step * 4 + 3
        line_copies.append(
            (
                sends.plan(own.at[slot], below.at[zz], line_sems.at[zz, 0], up, higher[step]),
                sends.plan(own.at[slot], above.at[zz], line_sems.at[zz, 1], down, lower[step]),
            )
        )

    def begin():
        greet([(over, None), (side, None), (mate, None), (up, z < 3), (down, z > 0)])
        for slot in range(16):
            mate_copies[slot].start()
            loads[slot].start()

    def join(slot):
        loads[slot].wait()
        landed(mates.at[slot], mate_sems.at[slot], mate)

    def corner(step):
        slot = step * 4
        join(slot)
        add_rows(own.at[slot], [(mates.at[slot], 0)], 0, rows)
        for copy in corner_copies[step]:
            copy.start()

    def relay(step):
        slot = step * 4 + 1
        join(slot)
        add_rows(own.at[slot], [(mates.at[slot], 0)], half, half)
        landed(side_half.at[step], half_sems.at[step, 1], mate)
        add_rows(own.at[slot], [(mates.at[slot], 0), (side_half.at[step], 0)], 0, half)
        relay_copies[step][0].start()
        slot = step * 4 + 2
        join(slot)
        add_rows(own.at[slot], [(mates.at[slot], 0)], 0, half)
        landed(over_half.at[step], half_sems.at[step, 0], mate)
        add_rows(own.at[slot], [(mates.at[slot], 0), (over_half.at[step], half)], half, half)
        relay_copies[step][1].start()

    def whole(step):
        zz = targets[step]
        slot = step * 4 + 3
        join(slot)
        landed(over_full.at[step], full_sems.at[step, 0], mate)
        landed(side_full.at[step], full_sems.at[step, 1], mate)
        add_rows(
            own.at[slot],
            [(mates.at[slot], 0), (over_full.at[step], 0), (side_full.at[step], 0)],
            0,
            rows,
        )

        @pl.when((zz >= z) & (z > 0))
        def _():
            landed(below.at[zz], line_sems.at[zz, 0], mate)
            add_rows(own.at[slot], [(below.at[zz], 0)], 0, rows)

        @pl.when((zz <= z) & (z < 3))
        def _():
            landed(above.at[zz], line_sems.at[zz, 1], mate)
            add_rows(own.at[slot], [(above.at[zz], 0)], 0, rows)

        if step < 3:
            pl.when(higher[step])(line_copies[step][0].start)
            pl.when(lower[step])(line_copies[step][1].start)

    def end():
        whole(3)
        out_ref[...] = own[15].astype(out_ref.dtype)
        sends.finish()

    pieces = [
        begin,
        functools.partial(corner, 0),
        functools.partial(corner, 1),
        functools.partial(relay, 0),
        functools.partial(corner, 2),
        functools.partial(relay, 1),
        functools.partial(whole, 0),
        functools.partial(corner, 3),
        functools.partial(relay, 2),
        functools.partial(whole, 1),
        functools.partial(relay, 3),
        functools.partial(whole, 2),
    ]
    for number, piece in enumerate(pieces):
        pl.when(turn == number)(piece)
    inner(turn, ins, outs)
    pl.when(turn == turns - 1)(end)


def sum_all(value, number, inner, turns, ins, outs, flops):
    if lax.axis_size("expert") != 8 or lax.axis_size("weight") != 4:
        summed = lax.psum_scatter(
            value.reshape(-1, value.shape[2]), ("expert", "weight"), scatter_dimension=0, tiled=True
        )

        def alone(*refs):
            inner(pl.program_id(0), refs[: len(ins)], refs[len(ins) :])

        return summed.astype(jnp.float32), call(alone, turns, ins, outs, flops)
    _, rows, width = value.shape
    out = jax.ShapeDtypeStruct((rows, width), jnp.float32)
    buffer = lambda n, r: pltpu.VMEM((n, r, width), value.dtype)
    arrays, shapes = [a for a, _ in ins], [o for o, _ in outs]
    results = pl.pallas_call(
        functools.partial(sum_all_kernel, inner, len(ins), len(outs)),
        grid=(turns,),
        out_shape=[out] + shapes,
        in_specs=[pl.BlockSpec(memory_space=pl.ANY)] + [spec for _, spec in ins],
        out_specs=[pl.BlockSpec((rows, width), lambda i: (0, 0))] + [spec for _, spec in outs],
        scratch_shapes=[
            buffer(16, rows),
            buffer(16, rows),
            buffer(4, rows // 2),
            buffer(4, rows // 2),
            buffer(4, rows),
            buffer(4, rows),
            buffer(4, rows),
            buffer(4, rows),
            pltpu.SemaphoreType.DMA((40,)),
            pltpu.SemaphoreType.DMA((16,)),
            pltpu.SemaphoreType.DMA((4, 2)),
            pltpu.SemaphoreType.DMA((4, 2)),
            pltpu.SemaphoreType.DMA((4, 2)),
            pltpu.SemaphoreType.DMA((16,)),
        ],
        compiler_params=pltpu.CompilerParams(
            collective_id=number, has_side_effects=True, vmem_limit_bytes=vmem_limit
        ),
        cost_estimate=cost(flops, value, out, *arrays, *shapes),
    )(value, *arrays)
    return results[0], results[1:]


def gather_group_kernel(x_ref, out_ref, send_sems, recv_sems, local_sem):
    z, x, y, c = places()
    half = x_ref.shape[0] // 2
    side, mate = device(z, x, 1 - y, c), device(z, x, y, 1 - c)
    greet([(side, None), (mate, None)])
    sends = Sends(send_sems)
    own, across = y * 2 + c, (1 - y) * 2 + c
    keep = pltpu.make_async_copy(x_ref, out_ref.at[own], local_sem)
    keep.start()

    def part(i, h):
        return out_ref.at[i, pl.ds(h * half, half)]

    for h in range(2):
        piece = x_ref.at[pl.ds(h * half, half)]
        sends.start(piece, part(own, h), recv_sems.at[own, h], side)
    for h in range(2):
        piece = x_ref.at[pl.ds(h * half, half)]
        sends.start(piece, part(own, h), recv_sems.at[own, h], mate)
    for h in range(2):
        landed(part(across, h), recv_sems.at[across, h], mate)
        sends.start(part(across, h), part(across, h), recv_sems.at[across, h], mate)
    for i in (y * 2 + 1 - c, (1 - y) * 2 + 1 - c):
        for h in range(2):
            landed(part(i, h), recv_sems.at[i, h], mate)
    sends.finish()
    keep.wait()


def gather_group(value, number):
    if lax.axis_size("expert") != 8 or lax.axis_size("weight") != 4:
        return lax.all_gather(value, "weight", axis=0, tiled=True)
    out = jax.ShapeDtypeStruct((4,) + value.shape, value.dtype)
    return pl.pallas_call(
        gather_group_kernel,
        out_shape=out,
        in_specs=[pl.BlockSpec(memory_space=pltpu.VMEM)],
        out_specs=pl.BlockSpec(memory_space=pltpu.VMEM),
        scratch_shapes=[
            pltpu.SemaphoreType.DMA((6,)),
            pltpu.SemaphoreType.DMA((4, 2)),
            pltpu.SemaphoreType.DMA,
        ],
        compiler_params=pltpu.CompilerParams(collective_id=number, has_side_effects=True),
        cost_estimate=cost(0, value, out),
    )(value).reshape(-1, value.shape[1])


def sum_group_kernel(p_ref, out_ref, mates, sides, carried, send_sems, mate_sems, side_sems):
    z, x, y, c = places()
    rows = out_ref.shape[0]
    half = rows // 2
    side, mate = device(z, x, 1 - y, c), device(z, x, y, 1 - c)
    greet([(side, None), (mate, None)])
    sends = Sends(send_sems)

    for j, yy in enumerate((1 - y, y)):
        for h in range(2):
            part = pl.ds(h * half, half)
            sends.start(
                p_ref.at[yy * 2 + 1 - c, part], mates.at[j, part], mate_sems.at[j, h], mate
            )

    def add(target, sources, h):
        step = 16

        def body(i, carry):
            part = pl.ds(pl.multiple_of(h * half + i * step, step), step)
            total = sources[0][part].astype(jnp.float32)
            for source in sources[1:]:
                total = total + source[part].astype(jnp.float32)
            target[part] = total.astype(target.dtype)
            return carry

        lax.fori_loop(0, half // step, body, 0)

    for h in range(2):
        part = pl.ds(h * half, half)
        landed(mates.at[0, part], mate_sems.at[0, h], mate)
        add(carried, [p_ref.at[(1 - y) * 2 + c], mates.at[0]], h)
        sends.start(carried.at[part], sides.at[part], side_sems.at[h], side)
    for h in range(2):
        part = pl.ds(h * half, half)
        landed(mates.at[1, part], mate_sems.at[1, h], mate)
        landed(sides.at[part], side_sems.at[h], mate)
        add(out_ref, [p_ref.at[y * 2 + c], mates.at[1], sides], h)
    sends.finish()


def sum_group(value, number):
    if lax.axis_size("expert") != 8 or lax.axis_size("weight") != 4:
        summed = lax.psum_scatter(value, "weight", scatter_dimension=0, tiled=True)
        return summed.astype(jnp.float32)
    rows, width = value.shape[0] // 4, value.shape[1]
    value = value.reshape(4, rows, width)
    out = jax.ShapeDtypeStruct((rows, width), jnp.float32)
    return pl.pallas_call(
        sum_group_kernel,
        out_shape=out,
        in_specs=[pl.BlockSpec(memory_space=pltpu.VMEM)],
        out_specs=pl.BlockSpec(memory_space=pltpu.VMEM),
        scratch_shapes=[
            pltpu.VMEM((2, rows, width), value.dtype),
            pltpu.VMEM((rows, width), value.dtype),
            pltpu.VMEM((rows, width), value.dtype),
            pltpu.SemaphoreType.DMA((6,)),
            pltpu.SemaphoreType.DMA((2, 2)),
            pltpu.SemaphoreType.DMA((2,)),
        ],
        compiler_params=pltpu.CompilerParams(collective_id=number, has_side_effects=True),
        cost_estimate=cost(0, value, out),
    )(value)


def columns(start, size):
    return pl.ds(pl.multiple_of(start, lanes), size)


def add_block(target, sources, rows, row_start=0):
    step = 16

    def body(i, carry):
        part = pl.ds(pl.multiple_of(row_start + i * step, step), step)
        total = target[part].astype(jnp.float32)
        for source in sources:
            there = pl.ds(pl.multiple_of(i * step, step), step)
            total = total + source[there].astype(jnp.float32)
        target[part] = total.astype(target.dtype)
        return carry

    lax.fori_loop(0, rows // step, body, 0)


def total_kernel(
    p_ref, out_ref, acc, mates, first_over, first_side, next_side, next_over, line, send_sems, sems
):
    z, x, y, c = places()
    rows, width = p_ref.shape
    half, quarter, eighth, sixteenth = width // 2, width // 4, width // 8, width // 16
    strip = rows // 4
    over, side, mate = device(z, 1 - x, y, c), device(z, x, 1 - y, c), device(z, x, y, 1 - c)
    others = [lax.rem(z + d, 4) for d in (1, 2, 3)]
    greet(
        [(over, None), (side, None), (mate, None)] + [(device(zz, x, y, c), None) for zz in others]
    )
    sends = Sends(send_sems)
    base = c * half
    for j in range(2):
        sends.start(
            p_ref.at[:, columns((1 - c) * half + j * quarter, quarter)],
            mates.at[:, columns(j * quarter, quarter)],
            sems.at[j],
            mate,
        )
    kept = (x * eighth + y * sixteenth, quarter + y * eighth + x * sixteenth)
    firsts, nexts = (first_over, first_side), (next_side, next_over)
    for j in range(2):
        part = columns(j * quarter, quarter)
        landed(mates.at[:, part], sems.at[j], mate)
        wide = 16

        def join(i, carry, j=j):
            some = pl.ds(pl.multiple_of(i * wide, wide), wide)
            mine = p_ref[some, columns(base + j * quarter, quarter)].astype(jnp.float32)
            total = mine + mates[some, columns(j * quarter, quarter)].astype(jnp.float32)
            acc[some, columns(j * quarter, quarter)] = total.astype(acc.dtype)
            return carry

        lax.fori_loop(0, rows // wide, join, 0)
        away = (1 - x) * eighth if j == 0 else quarter + (1 - y) * eighth
        sends.start(
            acc.at[:, columns(away, eighth)], firsts[j], sems.at[2 + j], (over, side)[j]
        )
    for j in range(2):
        landed(firsts[j], sems.at[2 + j], mate)
        near = x * eighth if j == 0 else quarter + y * eighth
        add_block(acc.at[:, columns(near, eighth)], [firsts[j]], rows)
        away = near + ((1 - y) if j == 0 else (1 - x)) * sixteenth
        sends.start(
            acc.at[:, columns(away, sixteenth)], nexts[j], sems.at[4 + j], (side, over)[j]
        )
    for j in range(2):
        landed(nexts[j], sems.at[4 + j], mate)
        add_block(acc.at[:, columns(kept[j], sixteenth)], [nexts[j]], rows)
        for d, zz in enumerate(others):
            sends.start(
                acc.at[pl.ds(pl.multiple_of(zz * strip, 16), strip), columns(kept[j], sixteenth)],
                line.at[j, d],
                sems.at[6 + j * 3 + d],
                device(zz, x, y, c),
            )
    strip_here = pl.multiple_of(z * strip, 16)
    for j in range(2):
        for d in range(3):
            landed(line.at[j, d], sems.at[6 + j * 3 + d], mate)
        block = acc.at[:, columns(kept[j], sixteenth)]
        add_block(block, [line.at[j, d] for d in range(3)], strip, strip_here)

        def place(i, carry, j=j):
            some = pl.ds(pl.multiple_of(strip_here + i * 16, 16), 16)
            out_ref[some, columns(base + kept[j], sixteenth)] = acc[
                some, columns(kept[j], sixteenth)
            ]
            return carry

        lax.fori_loop(0, strip // 16, place, 0)
        done = out_ref.at[pl.ds(strip_here, strip), columns(base + kept[j], sixteenth)]
        for d, zz in enumerate(others):
            sends.start(done, done, sems.at[12 + j * 3 + d], device(zz, x, y, c))
    for j in range(2):
        for d in range(3):
            source = pl.multiple_of(lax.rem(z + 3 - d, 4) * strip, 16)
            landed(
                out_ref.at[pl.ds(source, strip), columns(base + kept[j], sixteenth)],
                sems.at[12 + j * 3 + d],
                mate,
            )
        part = out_ref.at[:, columns(base + kept[j], sixteenth)]
        sends.start(part, part, sems.at[18 + j], (side, over)[j])
    others_kept = (
        x * eighth + (1 - y) * sixteenth,
        quarter + y * eighth + (1 - x) * sixteenth,
    )
    for j in range(2):
        landed(out_ref.at[:, columns(base + others_kept[j], sixteenth)], sems.at[18 + j], mate)
        near = x * eighth if j == 0 else quarter + y * eighth
        part = out_ref.at[:, columns(base + near, eighth)]
        sends.start(part, part, sems.at[20 + j], (over, side)[j])
    for j in range(2):
        away = (1 - x) * eighth if j == 0 else quarter + (1 - y) * eighth
        landed(out_ref.at[:, columns(base + away, eighth)], sems.at[20 + j], mate)
        part = out_ref.at[:, columns(base + j * quarter, quarter)]
        sends.start(part, part, sems.at[22 + j], mate)
    for j in range(2):
        landed(
            out_ref.at[:, columns((1 - c) * half + j * quarter, quarter)], sems.at[22 + j], mate
        )
    sends.finish()


def total_over_all(value, number):
    if lax.axis_size("expert") != 8 or lax.axis_size("weight") != 4:
        return lax.psum(value.astype(jnp.float32), ("expert", "weight"))
    rows, width = value.shape
    out = jax.ShapeDtypeStruct(value.shape, value.dtype)
    buffer = lambda n: pltpu.VMEM((rows, n), value.dtype)
    return pl.pallas_call(
        total_kernel,
        out_shape=out,
        in_specs=[pl.BlockSpec(memory_space=pltpu.VMEM)],
        out_specs=pl.BlockSpec(memory_space=pltpu.VMEM),
        scratch_shapes=[
            buffer(width // 2),
            buffer(width // 2),
            buffer(width // 8),
            buffer(width // 8),
            buffer(width // 16),
            buffer(width // 16),
            pltpu.VMEM((2, 3, rows // 4, width // 16), value.dtype),
            pltpu.SemaphoreType.DMA((24,)),
            pltpu.SemaphoreType.DMA((24,)),
        ],
        compiler_params=pltpu.CompilerParams(collective_id=number, has_side_effects=True),
        cost_estimate=cost(0, value, out),
    )(value).astype(jnp.float32)


def shared_kernel(turn, ins, outs):
    normed_ref, cotangent_ref, gate_grad_ref, lift_grad_ref, hidden_ref = ins

    @pl.when(turn == 0)
    def _():
        for out_ref in outs:
            out_ref[...] = jnp.zeros_like(out_ref)

    normed, cotangent = normed_ref[...], cotangent_ref[...]
    outs[0][...] += trans_times(gate_grad_ref[...], normed)
    outs[1][...] += trans_times(lift_grad_ref[...], normed)
    outs[2][...] += trans_times(hidden_ref[...], cotangent)


def weight_kernel(turn, ins, outs):
    rows_ref, grads_ref, gate_grad_ref, lift_grad_ref, hidden_ref = ins
    rows = rows_ref[0]
    outs[0][0] = trans_times(gate_grad_ref[0], rows)
    outs[1][0] = trans_times(lift_grad_ref[0], rows)
    outs[2][0] = trans_times(hidden_ref[0], grads_ref[0])


def per_device(
    tokens,
    cotangent,
    segments,
    routes,
    first_gain,
    query_weight,
    latent_weight,
    latent_gain,
    expand_weight,
    output_weight,
    second_gain,
    router_weight,
    shared_gate,
    shared_up,
    shared_down,
    expert_gate,
    expert_up,
    expert_down,
):
    weight_count = lax.axis_size("weight")
    token_rows = tokens.shape[0]
    width = tokens.shape[1]
    group_rows = token_rows * weight_count
    query_width = NOPE + ROPE
    heads_here = query_weight.shape[1] // query_width
    expert_count = router_weight.shape[1]
    local_experts = expert_gate.shape[0]
    score_scale = query_width ** (-0.5)
    activations = tokens.astype(jnp.float32)
    first_scale = inv_rms(activations)
    normed = (activations * first_scale * first_gain).astype(jnp.bfloat16)
    normed_all = gather_group(normed, 0)
    both = ("expert", "weight")
    expert_index = lax.axis_index("expert")
    expert_lanes = lax.axis_size("expert")
    blocks = expert_lanes * weight_count
    pairs = blocks // 2
    pair_rows = 2 * token_rows
    all_rows = blocks * token_rows
    slot_rows = blocks * CAP
    choose = (
        routes[:, :, None] == jnp.arange(expert_count, dtype=jnp.int32)[None, None, :]
    ).astype(jnp.float32)
    hit = jnp.sum(choose, axis=1)
    order = jnp.arange(token_rows, dtype=jnp.int32)
    before = (order[None, :] < order[:, None]).astype(jnp.bfloat16)
    place = matmul(before, hit.astype(jnp.bfloat16))
    rank = jnp.sum(choose * jnp.arange(routes.shape[1], dtype=jnp.float32)[None, :, None], axis=1)
    code = jnp.where(hit > 0, 32.0 * rank + place, -1.0)
    extra = jnp.pad(code, ((0, 0), (0, lanes - expert_count)), constant_values=-1.0)
    cotangent_wide = jnp.concatenate([cotangent, extra.astype(jnp.bfloat16)], axis=1)
    column = jnp.arange(lanes, dtype=jnp.int32)[None, :]
    row = jnp.arange(8, dtype=jnp.int32)[:, None]
    first_here = expert_index * local_experts
    here = (row < local_experts) & (column == first_here + row)
    twice = here | ((row < local_experts) & (column == first_here + row + expert_count))
    here, twice = here.astype(jnp.bfloat16), twice.astype(jnp.bfloat16)
    weight_index = lax.axis_index("weight")
    high_column = 2 * (row * weight_count + weight_index)
    known = row < routes.shape[1]
    high_at = (known & (column == high_column)).astype(jnp.bfloat16)
    low_at = (known & (column == high_column + 1)).astype(jnp.bfloat16)
    shared_here = shared_gate.shape[1] // expert_lanes
    shared_wide = -(-shared_here // lanes) * lanes
    start = expert_index * shared_here

    def shared_part(matrix):
        part = lax.dynamic_slice_in_dim(matrix, start, shared_here, axis=0)
        return jnp.pad(part, ((0, shared_wide - shared_here), (0, 0)))

    gate_part = shared_part(shared_gate.T)
    up_part = shared_part(shared_up.T)
    down_part = shared_part(shared_down)
    shape = jax.ShapeDtypeStruct
    whole = lambda array: (array, whole_spec(array))
    slots = shape((local_experts, slot_rows, width), jnp.bfloat16)
    slots_one = shape((local_experts, slot_rows, lanes), jnp.float32)
    gather_flops = 2 * all_rows * width * (2 * CAP * local_experts + shared_wide)
    cotangent_all = lax.all_gather(cotangent_wide, both, axis=0, tiled=True)
    marks = (cotangent_all, pl.BlockSpec((pair_rows, lanes), lambda i: (i, width // lanes)))
    grads_slots, shared_raw = call(
        grads_kernel,
        pairs,
        [whole(here), (cotangent_all, pair_spec(cotangent_all, pairs)), whole(down_part)],
        [
            (slots, slots_spec(slots, pairs)),
            (shape((all_rows, shared_wide), jnp.float32), pl.BlockSpec((pair_rows, shared_wide), lambda i: (i, 0))),
        ],
        gather_flops,
    )
    cosine, sine = rope_tables(segments[0])
    allowed = attention_mask(segments[0])
    query_full = matmul(normed_all, query_weight).reshape(group_rows, heads_here, query_width)
    query = jnp.concatenate(
        [
            query_full[..., :NOPE],
            rotate(query_full[..., NOPE:], cosine[:, None, :], sine[:, None, :]),
        ],
        axis=-1,
    ).astype(jnp.bfloat16)
    compressed = matmul(normed_all, latent_weight)
    latent = compressed[:, :LATENT]
    latent_scale = inv_rms(latent)
    latent_normed = (latent * latent_scale * latent_gain).astype(jnp.bfloat16)
    key_rope = rotate(compressed[:, LATENT:], cosine, sine).astype(jnp.bfloat16)
    expanded = (
        matmul(latent_normed, expand_weight)
        .astype(jnp.bfloat16)
        .reshape(group_rows, heads_here, NOPE + VDIM)
    )
    key_nope = expanded[..., :NOPE]
    values = expanded[..., NOPE:]

    def score_block():
        raw = jnp.einsum(
            "ihd,jhd->hij", query[..., :NOPE], key_nope, preferred_element_type=jnp.float32
        )
        raw = raw + jnp.einsum(
            "ihd,jd->hij", query[..., NOPE:], key_rope, preferred_element_type=jnp.float32
        )
        return jnp.where(allowed[None], raw * score_scale, -1e30)

    scores = score_block()
    peak = jnp.max(scores, axis=-1, keepdims=True)
    weights = jnp.exp(scores - peak)
    total = jnp.sum(weights, axis=-1, keepdims=True)
    log_total = peak + jnp.log(total)
    mixed = jnp.einsum(
        "hij,jhd->ihd",
        (weights / total).astype(jnp.bfloat16),
        values,
        preferred_element_type=jnp.float32,
    )
    mixed = mixed.astype(jnp.bfloat16).reshape(group_rows, heads_here * VDIM)
    attended = sum_group(matmul(mixed, output_weight).astype(jnp.bfloat16), 1)
    hidden_one = activations + attended
    second_scale = inv_rms(hidden_one)
    normed_two = (hidden_one * second_scale * second_gain).astype(jnp.bfloat16)
    gates = jax.nn.sigmoid(matmul(normed_two, router_weight))
    chosen = jnp.sum(choose * gates[:, None, :], axis=-1)
    chosen_total = jnp.sum(chosen, axis=1, keepdims=True)
    mixing = route_scale * chosen / chosen_total
    upstream = cotangent.astype(jnp.float32)
    mixing_at = jnp.sum(choose * mixing[:, :, None], axis=1)
    mixing_high = mixing_at.astype(jnp.bfloat16)
    mixing_low = (mixing_at - mixing_high.astype(jnp.float32)).astype(jnp.bfloat16)
    normed_wide = jnp.concatenate([normed_two, mixing_high, mixing_low], axis=1)
    normed_tokens = gather_all(normed_wide, 2).reshape(all_rows, -1)
    token_spec = pl.BlockSpec((pair_rows, shared_wide), lambda i: (i, 0))
    token_shape = shape((all_rows, shared_wide), jnp.bfloat16)
    rows_slots, mix_slots, shared_hidden, shared_gate_grad, shared_lift_grad = call(
        rows_kernel,
        pairs,
        [
            whole(here),
            whole(twice),
            marks,
            (normed_tokens, pair_spec(normed_tokens, pairs)),
            (shared_raw, token_spec),
            whole(gate_part),
            whole(up_part),
        ],
        [
            (slots, slots_spec(slots, pairs)),
            (slots_one, slots_spec(slots_one, pairs)),
            (token_shape, token_spec),
            (token_shape, token_spec),
            (token_shape, token_spec),
        ],
        gather_flops + 2 * all_rows * width * shared_wide,
    )
    hidden_here = expert_gate.shape[2]
    gate_rows, up_rows = expert_gate.transpose(0, 2, 1), expert_up.transpose(0, 2, 1)
    tile = slot_rows // 2
    tile_spec = lambda n: pl.BlockSpec((1, tile, n), lambda i: (i // 2, i % 2, 0))
    expert_spec = lambda m: pl.BlockSpec((1,) + m.shape[1:], lambda i: (i // 2, 0, 0))
    narrow = shape((local_experts, slot_rows, hidden_here), jnp.bfloat16)
    one_matmul = 2 * local_experts * slot_rows * width * hidden_here
    routed_hidden, gate_grad, lift_grad, returned, mix_grad_slots = call(
        experts_kernel,
        2 * local_experts,
        [
            (rows_slots, tile_spec(width)),
            (grads_slots, tile_spec(width)),
            (mix_slots, tile_spec(lanes)),
            (gate_rows, expert_spec(gate_rows)),
            (up_rows, expert_spec(up_rows)),
            (expert_down, expert_spec(expert_down)),
        ],
        [
            (narrow, tile_spec(hidden_here)),
            (narrow, tile_spec(hidden_here)),
            (narrow, tile_spec(hidden_here)),
            (slots, tile_spec(width)),
            (slots_one, tile_spec(lanes)),
        ],
        5 * one_matmul,
    )
    dense = shape((all_rows, width), jnp.bfloat16)
    dense_spec = pl.BlockSpec((pair_rows, width), lambda i: (i, 0))
    dense_wide = shape((all_rows, width + lanes), jnp.bfloat16)
    (back_dense,) = call(
        back_kernel,
        pairs,
        [
            whole(here),
            whole(high_at),
            whole(low_at),
            marks,
            (returned, slots_spec(slots, pairs)),
            (mix_grad_slots, slots_spec(slots_one, pairs)),
            (shared_gate_grad, token_spec),
            (shared_lift_grad, token_spec),
            whole(gate_part),
            whole(up_part),
        ],
        [(dense_wide, pair_spec(dense_wide, pairs))],
        gather_flops + 2 * all_rows * width * shared_wide,
    )
    shared_sum = shape((shared_wide, width), jnp.float32)
    shared_out = (shared_sum, whole_spec(shared_sum))
    plain_spec = pl.BlockSpec((pair_rows, width), lambda i: (i, 0))
    back_here, shared_sums = sum_all(
        back_dense.reshape(blocks, token_rows, -1),
        3,
        shared_kernel,
        pairs,
        [
            (normed_tokens, plain_spec),
            (cotangent_all, plain_spec),
            (shared_gate_grad, token_spec),
            (shared_lift_grad, token_spec),
            (shared_hidden, token_spec),
        ],
        [shared_out] * 3,
        6 * all_rows * width * shared_wide,
    )
    routed_back = back_here[:, :width]
    mix_grad = back_here[:, width : width + 2 * weight_count * routes.shape[1]]
    mix_grad = jnp.sum(mix_grad.reshape(token_rows, routes.shape[1], -1), axis=2)
    shared_grads = jnp.concatenate([total[:shared_here] for total in shared_sums], axis=0)
    shared_grads = shared_grads.astype(jnp.bfloat16)
    swapped = lax.all_to_all(shared_grads, "expert", split_axis=1, concat_axis=0, tiled=True)
    swapped = swapped.reshape(expert_lanes, 3, shared_here, -1).astype(jnp.float32)
    shared_gradients = [swapped[:, i].reshape(expert_lanes * shared_here, -1) for i in range(3)]
    chosen_grad = route_scale * (
        mix_grad / chosen_total
        - jnp.sum(mix_grad * chosen, axis=1, keepdims=True) / chosen_total**2
    )
    logit_grad = jnp.sum(choose * chosen_grad[:, :, None], axis=1) * gates * (1.0 - gates)
    normed_two_grad = (
        routed_back
        + jnp.dot(logit_grad, router_weight.astype(jnp.float32).T, precision=highest)
    )
    router_gradient = jnp.dot(normed_two.astype(jnp.float32).T, logit_grad, precision=highest)
    back_two, second_gain_gradient = norm_back(
        normed_two_grad, hidden_one, second_scale, second_gain
    )
    hidden_grad = upstream + back_two
    hidden_group = gather_group(hidden_grad.astype(jnp.bfloat16), 4)
    output_gradient = trans_times(mixed, hidden_group)
    mixed_grad = (
        times_trans(hidden_group, output_weight)
        .astype(jnp.bfloat16)
        .reshape(group_rows, heads_here, VDIM)
    )
    probs = jnp.exp(score_block() - log_total)
    prob_grad = jnp.einsum("ihd,jhd->hij", mixed_grad, values, preferred_element_type=jnp.float32)
    centre = jnp.sum(probs * prob_grad, axis=-1, keepdims=True)
    score_grad = (probs * (prob_grad - centre)).astype(jnp.bfloat16)
    value_grad = jnp.einsum(
        "hij,ihd->jhd", probs.astype(jnp.bfloat16), mixed_grad, preferred_element_type=jnp.float32
    )
    query_nope_grad = (
        jnp.einsum("hij,jhd->ihd", score_grad, key_nope, preferred_element_type=jnp.float32)
        * score_scale
    )
    query_rope_grad = (
        jnp.einsum("hij,jd->ihd", score_grad, key_rope, preferred_element_type=jnp.float32)
        * score_scale
    )
    key_nope_grad = (
        jnp.einsum(
            "hij,ihd->jhd", score_grad, query[..., :NOPE], preferred_element_type=jnp.float32
        )
        * score_scale
    )
    key_rope_grad = (
        jnp.einsum("hij,ihd->jd", score_grad, query[..., NOPE:], preferred_element_type=jnp.float32)
        * score_scale
    )
    query_grad = jnp.concatenate(
        [query_nope_grad, unrotate(query_rope_grad, cosine[:, None, :], sine[:, None, :])], axis=-1
    )
    query_grad = query_grad.astype(jnp.bfloat16).reshape(group_rows, heads_here * query_width)
    expand_grad = (
        jnp.concatenate([key_nope_grad, value_grad], axis=-1)
        .astype(jnp.bfloat16)
        .reshape(group_rows, heads_here * (NOPE + VDIM))
    )
    (produced,) = call(
        produce_kernel,
        2 * local_experts,
        [(routed_hidden, tile_spec(hidden_here)), (expert_down, expert_spec(expert_down))],
        [(slots, tile_spec(width))],
        one_matmul,
    )
    (out_dense,) = call(
        out_kernel,
        pairs,
        [
            whole(here),
            marks,
            (produced, slots_spec(slots, pairs)),
            (shared_hidden, token_spec),
            whole(down_part),
        ],
        [(dense, dense_spec)],
        gather_flops,
    )
    column_half = width // 2
    half_spec = lambda m: pl.BlockSpec((1, m, column_half), lambda i: (i // 2, 0, i % 2))
    narrow_spec = pl.BlockSpec((1, slot_rows, hidden_here), lambda i: (i // 2, 0, 0))
    weight_shape = shape((local_experts, hidden_here, width), jnp.float32)
    out_dense, query_grad = lax.optimization_barrier((out_dense, query_grad))
    routed_out, weight_grads = sum_all(
        out_dense.reshape(blocks, token_rows, width),
        6,
        weight_kernel,
        2 * local_experts,
        [
            (rows_slots, half_spec(slot_rows)),
            (grads_slots, half_spec(slot_rows)),
            (gate_grad, narrow_spec),
            (lift_grad, narrow_spec),
            (routed_hidden, narrow_spec),
        ],
        [(weight_shape, half_spec(hidden_here))] * 3,
        3 * one_matmul,
    )
    expert_grads = (weight_grads[0].transpose(0, 2, 1), weight_grads[1].transpose(0, 2, 1), weight_grads[2])
    layer_out = (hidden_one + routed_out).astype(jnp.bfloat16)
    query_gradient = trans_times(normed_all, query_grad)
    expand_gradient = trans_times(latent_normed, expand_grad)
    latent_normed_grad = times_trans(expand_grad, expand_weight)
    latent_back, latent_gain_gradient = norm_back(
        latent_normed_grad, latent, latent_scale, latent_gain
    )
    compressed_grad = jnp.concatenate([latent_back, unrotate(key_rope_grad, cosine, sine)], axis=-1)
    compressed_grad = compressed_grad.astype(jnp.bfloat16)
    latent_weight_gradient = trans_times(compressed_grad, normed_all)
    normed_grad = sum_group(
        (
            times_trans(query_grad, query_weight) + times_trans(compressed_grad, latent_weight)
        ).astype(jnp.bfloat16),
        5,
    )
    back_one, first_gain_gradient = norm_back(normed_grad, activations, first_scale, first_gain)
    token_gradient = hidden_grad + back_one
    shards = (
        lax.psum_scatter(
            query_gradient.astype(jnp.bfloat16), "expert", scatter_dimension=0, tiled=True
        ).astype(jnp.float32),
        lax.psum_scatter(
            expand_gradient.astype(jnp.bfloat16), "expert", scatter_dimension=0, tiled=True
        ).astype(jnp.float32),
        lax.psum_scatter(
            output_gradient.astype(jnp.bfloat16), "expert", scatter_dimension=1, tiled=True
        ).astype(jnp.float32),
    )
    latent_columns = latent_weight.shape[1]
    filled = jnp.concatenate(
        [
            latent_weight_gradient,
            router_gradient.T,
            first_gain_gradient[None],
            second_gain_gradient[None],
            jnp.pad(latent_gain_gradient, (0, width - LATENT))[None],
        ],
        axis=0,
    ).astype(jnp.bfloat16)
    wanted = -(-filled.shape[0] // 64) * 64
    filled = jnp.pad(filled, ((0, wanted - filled.shape[0]), (0, 0)))
    total = total_over_all(filled, 7)
    gains_at = latent_columns + expert_count
    totals = (
        total[:latent_columns].T,
        total[gains_at + 2, :LATENT],
        total[latent_columns:gains_at].T,
        total[gains_at],
        total[gains_at + 1],
    )
    return (
        layer_out,
        token_gradient,
        totals[3],
        shards[0],
        totals[0],
        totals[1],
        shards[1],
        shards[2],
        totals[4],
        totals[2],
        shared_gradients[0].T,
        shared_gradients[1].T,
        shared_gradients[2],
        expert_grads[0],
        expert_grads[1],
        expert_grads[2],
    )


def solution(mesh):
    return jax.shard_map(
        per_device,
        mesh=mesh,
        in_specs=(
            P(("expert", "weight"), None),
            P(("expert", "weight"), None),
            P("expert", None),
            P(("expert", "weight"), None),
            P(),
            P(None, "weight"),
            P(),
            P(),
            P(None, "weight"),
            P("weight", None),
            P(),
            P(),
            P(None, "weight"),
            P(None, "weight"),
            P("weight", None),
            P("expert", None, "weight"),
            P("expert", None, "weight"),
            P("expert", "weight", None),
        ),
        out_specs=(
            P(("expert", "weight"), None),
            P(("expert", "weight"), None),
            P(),
            P("expert", "weight"),
            P(),
            P(),
            P("expert", "weight"),
            P("weight", "expert"),
            P(),
            P(),
            P("expert", "weight"),
            P("expert", "weight"),
            P("weight", "expert"),
            P("expert", None, "weight"),
            P("expert", None, "weight"),
            P("expert", "weight", None),
        ),
        check_vma=False,
    )
```

```python
import functools

import jax
import jax.numpy as jnp
from jax import lax
from jax.experimental import pallas as pl
from jax.experimental.pallas import tpu as pltpu
from jax.sharding import PartitionSpec as P

NOPE = 128
ROPE = 64
VDIM = 128
LATENT = 512
TOPK = 6
CAP = 20


eps = 1e-06
route_scale = 2.446
rope_base = 50000.0
highest = lax.Precision.HIGHEST


def matmul(left, right):
    return jnp.dot(left, right, preferred_element_type=jnp.float32)


def trans_times(left, right):
    return lax.dot_general(
        left, right, (((0,), (0,)), ((), ())), preferred_element_type=jnp.float32
    )


def times_trans(left, right):
    return lax.dot_general(
        left, right, (((1,), (1,)), ((), ())), preferred_element_type=jnp.float32
    )


def inv_rms(value):
    return lax.rsqrt(jnp.mean(value * value, axis=-1, keepdims=True) + eps)


def norm_back(grad_out, value, scale, gain):
    scaled = grad_out * gain
    grad_in = scale * scaled - value * scale**3 * jnp.mean(scaled * value, axis=-1, keepdims=True)
    gain_grad = jnp.sum(grad_out * value * scale, axis=0)
    return (grad_in, gain_grad)


def rope_tables(seg):
    size = seg.shape[0]
    index = jnp.arange(size, dtype=jnp.int32)
    fresh = jnp.concatenate([jnp.ones((1,), dtype=bool), seg[1:] != seg[:-1]])
    first = lax.cummax(jnp.where(fresh, index, jnp.zeros_like(index)), axis=0)
    place = (index - first).astype(jnp.float32)
    half = ROPE // 2
    freqs = rope_base ** (-(jnp.arange(half, dtype=jnp.float32) * 2.0 / ROPE))
    angle = place[:, None] * freqs[None, :]
    return (jnp.cos(angle), jnp.sin(angle))


def attention_mask(seg):
    index = jnp.arange(seg.shape[0], dtype=jnp.int32)
    return (seg[:, None] == seg[None, :]) & (index[None, :] <= index[:, None])


def rotate(value, cosine, sine):
    half = value.shape[-1] // 2
    first, second = (value[..., :half], value[..., half:])
    return jnp.concatenate(
        [first * cosine - second * sine, second * cosine + first * sine], axis=-1
    )


def unrotate(value, cosine, sine):
    half = value.shape[-1] // 2
    first, second = (value[..., :half], value[..., half:])
    return jnp.concatenate(
        [first * cosine + second * sine, second * cosine - first * sine], axis=-1
    )


lanes = 128
vmem_limit = 64 * 1024 * 1024 - 131072


def token_slots(marks, here, local_experts, half):
    codes = times_trans(here, marks)
    count = codes.shape[1]
    rank = jnp.floor(codes * (1.0 / 32.0))
    place = codes - 32.0 * rank
    token = lax.broadcasted_iota(jnp.int32, codes.shape, 1)
    slot = jnp.where(codes >= 0, place + jnp.where(token >= half, float(CAP), 0.0), -1.0)
    row = lax.broadcasted_iota(jnp.int32, (2 * CAP, count), 0).astype(jnp.float32)
    picks = [jnp.where(row == slot[e : e + 1], 1.0, 0.0) for e in range(local_experts)]
    return picks, rank


def pair_slots(marks_ref, here_ref, local_experts, pair):
    count = marks_ref.shape[0] // pair
    return [
        token_slots(marks_ref[j * pair : (j + 1) * pair], here_ref[...], local_experts, pair // 2)
        for j in range(count)
    ]


def slot_part(value, e):
    return value[e * 2 * CAP : (e + 1) * 2 * CAP]


def gather_rows(slots, values, pair, out_ref):
    rows = [
        jnp.dot(
            jnp.concatenate(picks, axis=0).astype(jnp.bfloat16),
            values[j * pair : (j + 1) * pair],
            preferred_element_type=jnp.float32,
        )
        for j, (picks, _) in enumerate(slots)
    ]
    for e in range(out_ref.shape[0]):
        together = jnp.concatenate([slot_part(value, e) for value in rows], axis=0)
        out_ref[e] = together.astype(jnp.bfloat16)


def spread_rows(slots, rows_ref):
    local_experts = rows_ref.shape[0]
    rows = [rows_ref[e].astype(jnp.float32) for e in range(local_experts)]
    totals = []
    for j, (picks, _) in enumerate(slots):
        part = jnp.concatenate([slot_part(value, j) for value in rows], axis=0)
        pick = jnp.concatenate(picks, axis=0).astype(jnp.bfloat16)
        totals.append(trans_times(pick, part.astype(jnp.bfloat16)))
    return jnp.concatenate(totals, axis=0)


def grads_kernel(pair, here_ref, value_ref, down_ref, rows_ref, back_ref):
    width = rows_ref.shape[2]
    slots = pair_slots(value_ref.at[:, width:], here_ref, rows_ref.shape[0], pair)
    values = value_ref[:, :width]
    gather_rows(slots, values, pair, rows_ref)
    back_ref[...] = times_trans(values, down_ref[...])


def rows_kernel(
    pair,
    here_ref,
    twice_ref,
    marks_ref,
    value_ref,
    back_ref,
    gate_ref,
    up_ref,
    rows_ref,
    mix_ref,
    hidden_ref,
    gate_grad_ref,
    lift_grad_ref,
):
    width = rows_ref.shape[2]
    slots = pair_slots(marks_ref, here_ref, rows_ref.shape[0], pair)
    values = value_ref[:, :width]
    gather_rows(slots, values, pair, rows_ref)
    for j, (picks, _) in enumerate(slots):
        mixing = times_trans(twice_ref[...], value_ref[j * pair : (j + 1) * pair, width:])
        for e, pick in enumerate(picks):
            column = jnp.sum(pick * mixing[e : e + 1], axis=1, keepdims=True)
            column = jnp.broadcast_to(column, (2 * CAP, lanes))
            mix_ref[e, j * 2 * CAP : (j + 1) * 2 * CAP] = column
    gate = times_trans(values, gate_ref[...])
    lift = times_trans(values, up_ref[...])
    back = back_ref[...]
    sigma = jax.nn.sigmoid(gate)
    active = gate * sigma
    hidden_ref[...] = (active * lift).astype(jnp.bfloat16)
    gate_grad_ref[...] = (back * lift * sigma * (1.0 + gate * (1.0 - sigma))).astype(jnp.bfloat16)
    lift_grad_ref[...] = (back * active).astype(jnp.bfloat16)


def forward_kernel(
    rows_ref,
    mix_ref,
    gate_ref,
    up_ref,
    down_ref,
    hidden_ref,
    mixed_ref,
    slope_ref,
    active_ref,
    produced_ref,
):
    rows = rows_ref[0]
    gate = times_trans(rows, gate_ref[0])
    lift = times_trans(rows, up_ref[0])
    mix = mix_ref[0][:, :1]
    sigma = jax.nn.sigmoid(gate)
    active = gate * sigma
    hidden = active * lift
    mixed_hidden = (mix * hidden).astype(jnp.bfloat16)
    hidden_ref[0] = hidden.astype(jnp.bfloat16)
    mixed_ref[0] = mixed_hidden
    slope_ref[0] = (mix * lift * sigma * (1.0 + gate * (1.0 - sigma))).astype(jnp.bfloat16)
    active_ref[0] = (mix * active).astype(jnp.bfloat16)
    produced_ref[0] = matmul(mixed_hidden, down_ref[0]).astype(jnp.bfloat16)


def backward_kernel(turn, ins, outs):
    grads_ref, hidden_ref, slope_ref, active_ref, gate_ref, up_ref, down_ref = ins
    gate_grad_ref, lift_grad_ref, returned_ref, mix_grad_ref = outs
    back = times_trans(grads_ref[0], down_ref[0])
    mix_grad = jnp.sum(hidden_ref[0].astype(jnp.float32) * back, axis=1, keepdims=True)
    mix_grad_ref[0] = jnp.broadcast_to(mix_grad, mix_grad_ref.shape[1:])
    gate_grad = (back * slope_ref[0].astype(jnp.float32)).astype(jnp.bfloat16)
    lift_grad = (back * active_ref[0].astype(jnp.float32)).astype(jnp.bfloat16)
    gate_grad_ref[0] = gate_grad
    lift_grad_ref[0] = lift_grad
    returned = matmul(gate_grad, gate_ref[0]) + matmul(lift_grad, up_ref[0])
    returned_ref[0] = returned.astype(jnp.bfloat16)


def back_kernel(
    pair,
    here_ref,
    high_ref,
    low_ref,
    marks_ref,
    rows_ref,
    mix_grad_ref,
    gate_grad_ref,
    lift_grad_ref,
    gate_ref,
    up_ref,
    out_ref,
):
    width = rows_ref.shape[2]
    slots = pair_slots(marks_ref, here_ref, rows_ref.shape[0], pair)
    total = spread_rows(slots, rows_ref)
    total = total + matmul(gate_grad_ref[...], gate_ref[...])
    total = total + matmul(lift_grad_ref[...], up_ref[...])
    out_ref[:, :width] = total.astype(jnp.bfloat16)
    for j, (picks, rank) in enumerate(slots):
        choice = lax.broadcasted_iota(jnp.int32, rank.shape, 0).astype(jnp.float32)
        mix_grad = jnp.zeros(rank.shape, jnp.float32)
        for e, pick in enumerate(picks):
            column = slot_part(mix_grad_ref[e], j)[:, :1]
            row = jnp.sum(pick * column, axis=0, keepdims=True)
            mix_grad = mix_grad + jnp.where(choice == rank[e : e + 1], row, 0.0)
        high = mix_grad.astype(jnp.bfloat16)
        low = (mix_grad - high.astype(jnp.float32)).astype(jnp.bfloat16)
        sent = trans_times(high, high_ref[...]) + trans_times(low, low_ref[...])
        out_ref[j * pair : (j + 1) * pair, width:] = sent.astype(jnp.bfloat16)


def out_kernel(pair, here_ref, marks_ref, rows_ref, hidden_ref, down_ref, out_ref):
    slots = pair_slots(marks_ref, here_ref, rows_ref.shape[0], pair)
    total = spread_rows(slots, rows_ref)
    total = total + matmul(hidden_ref[...], down_ref[...])
    out_ref[...] = total.astype(jnp.bfloat16)


def whole_spec(array):
    zeros = (0,) * array.ndim
    return pl.BlockSpec(array.shape, lambda i: zeros)


def pair_spec(array, pairs):
    block = (array.shape[0] // pairs,) + array.shape[1:]
    zeros = (0,) * (array.ndim - 1)
    return pl.BlockSpec(block, lambda i: (i,) + zeros)


def slots_spec(array, pairs):
    block = (array.shape[0], array.shape[1] // pairs) + array.shape[2:]
    return pl.BlockSpec(block, lambda i: (0, i, 0))


def cost(flops, *arrays):
    moved = sum(a.size * a.dtype.itemsize for a in arrays)
    return pl.CostEstimate(flops=int(flops), bytes_accessed=int(moved), transcendentals=0)


def call(kernel, grid, ins, outs, flops):
    arrays = [a for a, _ in ins]
    shapes = [s for s, _ in outs]
    return pl.pallas_call(
        kernel,
        grid=(grid,),
        in_specs=[s for _, s in ins],
        out_specs=[s for _, s in outs],
        out_shape=shapes,
        cost_estimate=cost(flops, *arrays, *shapes),
        compiler_params=pltpu.CompilerParams(vmem_limit_bytes=vmem_limit),
    )(*arrays)


MESH = pl.DeviceIdType.MESH


def places():
    expert, weight = lax.axis_index("expert"), lax.axis_index("weight")
    return lax.div(expert, 2), lax.rem(expert, 2), lax.div(weight, 2), lax.rem(weight, 2)


def device(z, x, y, c):
    return (z * 2 + x, y * 2 + c)


def shard(z, x, y, c):
    return z * 8 + x * 4 + y * 2 + c


def push(source, target, send, receive, to):
    return pltpu.make_async_remote_copy(
        src_ref=source,
        dst_ref=target,
        send_sem=send,
        recv_sem=receive,
        device_id=to,
        device_id_type=MESH,
    )


class Sends:
    def __init__(self, semaphores):
        self.semaphores = semaphores
        self.started = []

    def plan(self, source, target, receive, to, when=None):
        copy = push(source, target, self.semaphores.at[len(self.started)], receive, to)
        self.started.append((copy, when))
        return copy

    def start(self, source, target, receive, to, when=None):
        copy = self.plan(source, target, receive, to, when)
        if when is None:
            copy.start()
        else:
            pl.when(when)(copy.start)

    def finish(self):
        for copy, when in self.started:
            if when is None:
                copy.wait_send()
            else:
                pl.when(when)(copy.wait_send)


def landed(target, receive, to):
    push(target, target, receive, receive, to).wait_recv()


def greet(devices):
    barrier = pltpu.get_barrier_semaphore()
    count = 0
    for to, when in devices:
        signal = functools.partial(
            pl.semaphore_signal, barrier, inc=1, device_id=to, device_id_type=MESH
        )
        if when is None:
            signal()
            count = count + 1
        else:
            pl.when(when)(signal)
            count = count + when.astype(jnp.int32)
    pl.semaphore_wait(barrier, count)


def add_rows(target, sources, start, rows):
    step = 16

    def body(i, carry):
        part = pl.ds(pl.multiple_of(start + i * step, step), step)
        total = target[part].astype(jnp.float32)
        for source, offset in sources:
            there = pl.ds(pl.multiple_of(start - offset + i * step, step), step)
            total = total + source[there].astype(jnp.float32)
        target[part] = total.astype(target.dtype)
        return carry

    lax.fori_loop(0, rows // step, body, 0)


def ordered(z, first, second):
    upper = lax.div(z, 2)
    inner = z + upper * (3 - 2 * z)
    value = first + inner * (second - first)
    return value + upper * (3 - 2 * value)


def gather_all_kernel(x_ref, out_ref, send_sems, recv_sems, local_sem):
    z, x, y, c = places()
    half = x_ref.shape[0] // 2
    over, side, mate = device(z, 1 - x, y, c), device(z, x, 1 - y, c), device(z, x, y, 1 - c)
    up, down = device(z + 1, x, y, c), device(z - 1, x, y, c)
    greet([(over, None), (side, None), (mate, None), (up, z < 3), (down, z > 0)])
    sends = Sends(send_sems)
    own = shard(z, x, y, c)
    keep = pltpu.make_async_copy(x_ref, out_ref.at[own], local_sem)
    keep.start()

    def halves(i, h):
        return out_ref.at[i, pl.ds(h * half, half)]

    def whole(step):
        zz = ordered(z, (0, 1, 2, 3)[step], (1, 0, 2, 3)[step])
        i = shard(zz, x, y, c)
        source, receive = out_ref.at[i], recv_sems.at[i, 0]
        if step == 0:
            source = x_ref
        else:
            landed(out_ref.at[i], receive, mate)
        sends.start(source, out_ref.at[i], receive, up, (zz <= z) & (z < 3))
        sends.start(source, out_ref.at[i], receive, down, (zz >= z) & (z > 0))
        sends.start(source, out_ref.at[i], receive, over)
        sends.start(source, out_ref.at[i], receive, side)
        sends.start(source, out_ref.at[i], receive, mate)

    def relay(step):
        zz = ordered(z, (0, 1, 2, 3)[step], (1, 0, 2, 3)[step])
        i = shard(zz, 1 - x, y, c)
        landed(out_ref.at[i], recv_sems.at[i, 0], mate)
        sends.start(halves(i, 0), halves(i, 0), recv_sems.at[i, 0], side)
        sends.start(out_ref.at[i], out_ref.at[i], recv_sems.at[i, 0], mate)
        i = shard(zz, x, 1 - y, c)
        landed(out_ref.at[i], recv_sems.at[i, 0], mate)
        sends.start(halves(i, 1), halves(i, 1), recv_sems.at[i, 1], over)
        sends.start(out_ref.at[i], out_ref.at[i], recv_sems.at[i, 0], mate)

    def corner(step):
        zz = ordered(z, (0, 1, 2, 3)[step], (1, 0, 2, 3)[step])
        i = shard(zz, 1 - x, 1 - y, c)
        for h in range(2):
            landed(halves(i, h), recv_sems.at[i, h], mate)
            sends.start(halves(i, h), halves(i, h), recv_sems.at[i, h], mate)

    whole(0)
    whole(1)
    relay(0)
    whole(2)
    relay(1)
    corner(0)
    whole(3)
    relay(2)
    corner(1)
    relay(3)
    corner(2)
    corner(3)
    for step in range(4):
        zz = ordered(z, (0, 1, 2, 3)[step], (1, 0, 2, 3)[step])
        for i in (shard(zz, x, y, 1 - c), shard(zz, 1 - x, y, 1 - c), shard(zz, x, 1 - y, 1 - c)):
            landed(out_ref.at[i], recv_sems.at[i, 0], mate)
        i = shard(zz, 1 - x, 1 - y, 1 - c)
        for h in range(2):
            landed(halves(i, h), recv_sems.at[i, h], mate)
    sends.finish()
    keep.wait()


def gather_all(value, number):
    if lax.axis_size("expert") != 8 or lax.axis_size("weight") != 4:
        return lax.all_gather(value, ("expert", "weight"), axis=0)
    out = jax.ShapeDtypeStruct((32,) + value.shape, value.dtype)
    return pl.pallas_call(
        gather_all_kernel,
        out_shape=out,
        in_specs=[pl.BlockSpec(memory_space=pltpu.VMEM)],
        out_specs=pl.BlockSpec(memory_space=pl.ANY),
        scratch_shapes=[
            pltpu.SemaphoreType.DMA((44,)),
            pltpu.SemaphoreType.DMA((32, 2)),
            pltpu.SemaphoreType.DMA,
        ],
        compiler_params=pltpu.CompilerParams(collective_id=number, has_side_effects=True),
        cost_estimate=cost(0, value, out),
    )(value)


def sum_all_kernel(inner, cover_ins, cover_outs, p_ref, *refs):
    ins, refs = refs[:cover_ins], refs[cover_ins:]
    out_ref, refs = refs[0], refs[1:]
    outs, refs = refs[:cover_outs], refs[cover_outs:]
    own, mates, over_half, side_half, over_full, side_full, below, above = refs[:8]
    send_sems, mate_sems, half_sems, full_sems, line_sems, local_sems = refs[8:]
    z, x, y, c = places()
    turn, turns = pl.program_id(0), pl.num_programs(0)
    rows = out_ref.shape[0]
    half = rows // 2
    over, side, mate = device(z, 1 - x, y, c), device(z, x, 1 - y, c), device(z, x, y, 1 - c)
    up, down = device(z + 1, x, y, c), device(z - 1, x, y, c)
    sends = Sends(send_sems)
    targets = [ordered(z, (3, 2, 1, 0)[step], (3, 0, 2, 1)[step]) for step in range(4)]
    spots = [(1 - x, 1 - y), (1 - x, y), (x, 1 - y), (x, y)]
    shards = [[shard(zz, xx, yy, 1 - c) for xx, yy in spots] for zz in targets]
    mine = [[shard(zz, xx, yy, c) for xx, yy in spots] for zz in targets]
    higher = [zz > z for zz in targets]
    lower = [zz < z for zz in targets]
    loads = [
        pltpu.make_async_copy(p_ref.at[mine[slot // 4][slot % 4]], own.at[slot], local_sems.at[slot])
        for slot in range(16)
    ]

    mate_copies = [
        sends.plan(p_ref.at[shards[slot // 4][slot % 4]], mates.at[slot], mate_sems.at[slot], mate)
        for slot in range(16)
    ]
    corner_copies, relay_copies, line_copies = [], [], []
    for step in range(4):
        corner_copies.append(
            (
                sends.plan(
                    own.at[step * 4, pl.ds(half, half)],
                    over_half.at[step],
                    half_sems.at[step, 0],
                    over,
                ),
                sends.plan(
                    own.at[step * 4, pl.ds(0, half)], side_half.at[step], half_sems.at[step, 1], side
                ),
            )
        )
        relay_copies.append(
            (
                sends.plan(
                    own.at[step * 4 + 1], over_full.at[step], full_sems.at[step, 0], over
                ),
                sends.plan(
                    own.at[step * 4 + 2], side_full.at[step], full_sems.at[step, 1], side
                ),
            )
        )
    for step in range(3):
        zz, slot = targets[step], step * 4 + 3
        line_copies.append(
            (
                sends.plan(own.at[slot], below.at[zz], line_sems.at[zz, 0], up, higher[step]),
                sends.plan(own.at[slot], above.at[zz], line_sems.at[zz, 1], down, lower[step]),
            )
        )

    def begin():
        greet([(over, None), (side, None), (mate, None), (up, z < 3), (down, z > 0)])
        for slot in range(16):
            mate_copies[slot].start()
            loads[slot].start()

    def join(slot):
        loads[slot].wait()
        landed(mates.at[slot], mate_sems.at[slot], mate)

    def corner(step):
        slot = step * 4
        join(slot)
        add_rows(own.at[slot], [(mates.at[slot], 0)], 0, rows)
        for copy in corner_copies[step]:
            copy.start()

    def relay(step):
        slot = step * 4 + 1
        join(slot)
        add_rows(own.at[slot], [(mates.at[slot], 0)], half, half)
        landed(side_half.at[step], half_sems.at[step, 1], mate)
        add_rows(own.at[slot], [(mates.at[slot], 0), (side_half.at[step], 0)], 0, half)
        relay_copies[step][0].start()
        slot = step * 4 + 2
        join(slot)
        add_rows(own.at[slot], [(mates.at[slot], 0)], 0, half)
        landed(over_half.at[step], half_sems.at[step, 0], mate)
        add_rows(own.at[slot], [(mates.at[slot], 0), (over_half.at[step], half)], half, half)
        relay_copies[step][1].start()

    def whole(step):
        zz = targets[step]
        slot = step * 4 + 3
        join(slot)
        landed(over_full.at[step], full_sems.at[step, 0], mate)
        landed(side_full.at[step], full_sems.at[step, 1], mate)
        add_rows(
            own.at[slot],
            [(mates.at[slot], 0), (over_full.at[step], 0), (side_full.at[step], 0)],
            0,
            rows,
        )

        @pl.when((zz >= z) & (z > 0))
        def _():
            landed(below.at[zz], line_sems.at[zz, 0], mate)
            add_rows(own.at[slot], [(below.at[zz], 0)], 0, rows)

        @pl.when((zz <= z) & (z < 3))
        def _():
            landed(above.at[zz], line_sems.at[zz, 1], mate)
            add_rows(own.at[slot], [(above.at[zz], 0)], 0, rows)

        if step < 3:
            pl.when(higher[step])(line_copies[step][0].start)
            pl.when(lower[step])(line_copies[step][1].start)

    def end():
        whole(3)
        out_ref[...] = own[15].astype(out_ref.dtype)
        sends.finish()

    pieces = [
        begin,
        functools.partial(corner, 0),
        functools.partial(corner, 1),
        functools.partial(relay, 0),
        functools.partial(corner, 2),
        functools.partial(relay, 1),
        functools.partial(whole, 0),
        functools.partial(corner, 3),
        functools.partial(relay, 2),
        functools.partial(whole, 1),
        functools.partial(relay, 3),
        functools.partial(whole, 2),
    ]
    for number, piece in enumerate(pieces):
        pl.when(turn == number)(piece)
    inner(turn, ins, outs)
    pl.when(turn == turns - 1)(end)


def sum_all(value, number, inner, turns, ins, outs, flops):
    if lax.axis_size("expert") != 8 or lax.axis_size("weight") != 4:
        summed = lax.psum_scatter(
            value.reshape(-1, value.shape[2]), ("expert", "weight"), scatter_dimension=0, tiled=True
        )

        def alone(*refs):
            inner(pl.program_id(0), refs[: len(ins)], refs[len(ins) :])

        return summed.astype(jnp.float32), call(alone, turns, ins, outs, flops)
    _, rows, width = value.shape
    out = jax.ShapeDtypeStruct((rows, width), jnp.float32)
    buffer = lambda n, r: pltpu.VMEM((n, r, width), value.dtype)
    arrays, shapes = [a for a, _ in ins], [o for o, _ in outs]
    results = pl.pallas_call(
        functools.partial(sum_all_kernel, inner, len(ins), len(outs)),
        grid=(turns,),
        out_shape=[out] + shapes,
        in_specs=[pl.BlockSpec(memory_space=pl.ANY)] + [spec for _, spec in ins],
        out_specs=[pl.BlockSpec((rows, width), lambda i: (0, 0))] + [spec for _, spec in outs],
        scratch_shapes=[
            buffer(16, rows),
            buffer(16, rows),
            buffer(4, rows // 2),
            buffer(4, rows // 2),
            buffer(4, rows),
            buffer(4, rows),
            buffer(4, rows),
            buffer(4, rows),
            pltpu.SemaphoreType.DMA((40,)),
            pltpu.SemaphoreType.DMA((16,)),
            pltpu.SemaphoreType.DMA((4, 2)),
            pltpu.SemaphoreType.DMA((4, 2)),
            pltpu.SemaphoreType.DMA((4, 2)),
            pltpu.SemaphoreType.DMA((16,)),
        ],
        compiler_params=pltpu.CompilerParams(
            collective_id=number, has_side_effects=True, vmem_limit_bytes=vmem_limit
        ),
        cost_estimate=cost(flops, value, out, *arrays, *shapes),
    )(value, *arrays)
    return results[0], results[1:]


def gather_group_kernel(x_ref, out_ref, send_sems, recv_sems, local_sem):
    z, x, y, c = places()
    half = x_ref.shape[0] // 2
    side, mate = device(z, x, 1 - y, c), device(z, x, y, 1 - c)
    greet([(side, None), (mate, None)])
    sends = Sends(send_sems)
    own, across = y * 2 + c, (1 - y) * 2 + c
    keep = pltpu.make_async_copy(x_ref, out_ref.at[own], local_sem)
    keep.start()

    def part(i, h):
        return out_ref.at[i, pl.ds(h * half, half)]

    for h in range(2):
        piece = x_ref.at[pl.ds(h * half, half)]
        sends.start(piece, part(own, h), recv_sems.at[own, h], side)
    for h in range(2):
        piece = x_ref.at[pl.ds(h * half, half)]
        sends.start(piece, part(own, h), recv_sems.at[own, h], mate)
    for h in range(2):
        landed(part(across, h), recv_sems.at[across, h], mate)
        sends.start(part(across, h), part(across, h), recv_sems.at[across, h], mate)
    for i in (y * 2 + 1 - c, (1 - y) * 2 + 1 - c):
        for h in range(2):
            landed(part(i, h), recv_sems.at[i, h], mate)
    sends.finish()
    keep.wait()


def gather_group(value, number):
    if lax.axis_size("expert") != 8 or lax.axis_size("weight") != 4:
        return lax.all_gather(value, "weight", axis=0, tiled=True)
    out = jax.ShapeDtypeStruct((4,) + value.shape, value.dtype)
    return pl.pallas_call(
        gather_group_kernel,
        out_shape=out,
        in_specs=[pl.BlockSpec(memory_space=pltpu.VMEM)],
        out_specs=pl.BlockSpec(memory_space=pltpu.VMEM),
        scratch_shapes=[
            pltpu.SemaphoreType.DMA((6,)),
            pltpu.SemaphoreType.DMA((4, 2)),
            pltpu.SemaphoreType.DMA,
        ],
        compiler_params=pltpu.CompilerParams(collective_id=number, has_side_effects=True),
        cost_estimate=cost(0, value, out),
    )(value).reshape(-1, value.shape[1])


def sum_group_kernel(p_ref, out_ref, mates, sides, carried, send_sems, mate_sems, side_sems):
    z, x, y, c = places()
    rows = out_ref.shape[0]
    half = rows // 2
    side, mate = device(z, x, 1 - y, c), device(z, x, y, 1 - c)
    greet([(side, None), (mate, None)])
    sends = Sends(send_sems)

    for j, yy in enumerate((1 - y, y)):
        for h in range(2):
            part = pl.ds(h * half, half)
            sends.start(
                p_ref.at[yy * 2 + 1 - c, part], mates.at[j, part], mate_sems.at[j, h], mate
            )

    def add(target, sources, h):
        step = 16

        def body(i, carry):
            part = pl.ds(pl.multiple_of(h * half + i * step, step), step)
            total = sources[0][part].astype(jnp.float32)
            for source in sources[1:]:
                total = total + source[part].astype(jnp.float32)
            target[part] = total.astype(target.dtype)
            return carry

        lax.fori_loop(0, half // step, body, 0)

    for h in range(2):
        part = pl.ds(h * half, half)
        landed(mates.at[0, part], mate_sems.at[0, h], mate)
        add(carried, [p_ref.at[(1 - y) * 2 + c], mates.at[0]], h)
        sends.start(carried.at[part], sides.at[part], side_sems.at[h], side)
    for h in range(2):
        part = pl.ds(h * half, half)
        landed(mates.at[1, part], mate_sems.at[1, h], mate)
        landed(sides.at[part], side_sems.at[h], mate)
        add(out_ref, [p_ref.at[y * 2 + c], mates.at[1], sides], h)
    sends.finish()


def sum_group(value, number):
    if lax.axis_size("expert") != 8 or lax.axis_size("weight") != 4:
        summed = lax.psum_scatter(value, "weight", scatter_dimension=0, tiled=True)
        return summed.astype(jnp.float32)
    rows, width = value.shape[0] // 4, value.shape[1]
    value = value.reshape(4, rows, width)
    out = jax.ShapeDtypeStruct((rows, width), jnp.float32)
    return pl.pallas_call(
        sum_group_kernel,
        out_shape=out,
        in_specs=[pl.BlockSpec(memory_space=pltpu.VMEM)],
        out_specs=pl.BlockSpec(memory_space=pltpu.VMEM),
        scratch_shapes=[
            pltpu.VMEM((2, rows, width), value.dtype),
            pltpu.VMEM((rows, width), value.dtype),
            pltpu.VMEM((rows, width), value.dtype),
            pltpu.SemaphoreType.DMA((6,)),
            pltpu.SemaphoreType.DMA((2, 2)),
            pltpu.SemaphoreType.DMA((2,)),
        ],
        compiler_params=pltpu.CompilerParams(collective_id=number, has_side_effects=True),
        cost_estimate=cost(0, value, out),
    )(value)


def columns(start, size):
    return pl.ds(pl.multiple_of(start, lanes), size)


def add_block(target, sources, rows, row_start=0):
    step = 16

    def body(i, carry):
        part = pl.ds(pl.multiple_of(row_start + i * step, step), step)
        total = target[part].astype(jnp.float32)
        for source in sources:
            there = pl.ds(pl.multiple_of(i * step, step), step)
            total = total + source[there].astype(jnp.float32)
        target[part] = total.astype(target.dtype)
        return carry

    lax.fori_loop(0, rows // step, body, 0)


def total_kernel(
    p_ref, out_ref, acc, mates, first_over, first_side, next_side, next_over, line, send_sems, sems
):
    z, x, y, c = places()
    rows, width = p_ref.shape
    half, quarter, eighth, sixteenth = width // 2, width // 4, width // 8, width // 16
    strip = rows // 4
    over, side, mate = device(z, 1 - x, y, c), device(z, x, 1 - y, c), device(z, x, y, 1 - c)
    others = [lax.rem(z + d, 4) for d in (1, 2, 3)]
    greet(
        [(over, None), (side, None), (mate, None)] + [(device(zz, x, y, c), None) for zz in others]
    )
    sends = Sends(send_sems)
    base = c * half
    for j in range(2):
        sends.start(
            p_ref.at[:, columns((1 - c) * half + j * quarter, quarter)],
            mates.at[:, columns(j * quarter, quarter)],
            sems.at[j],
            mate,
        )
    kept = (x * eighth + y * sixteenth, quarter + y * eighth + x * sixteenth)
    firsts, nexts = (first_over, first_side), (next_side, next_over)
    for j in range(2):
        part = columns(j * quarter, quarter)
        landed(mates.at[:, part], sems.at[j], mate)
        wide = 16

        def join(i, carry, j=j):
            some = pl.ds(pl.multiple_of(i * wide, wide), wide)
            mine = p_ref[some, columns(base + j * quarter, quarter)].astype(jnp.float32)
            total = mine + mates[some, columns(j * quarter, quarter)].astype(jnp.float32)
            acc[some, columns(j * quarter, quarter)] = total.astype(acc.dtype)
            return carry

        lax.fori_loop(0, rows // wide, join, 0)
        away = (1 - x) * eighth if j == 0 else quarter + (1 - y) * eighth
        sends.start(
            acc.at[:, columns(away, eighth)], firsts[j], sems.at[2 + j], (over, side)[j]
        )
    for j in range(2):
        landed(firsts[j], sems.at[2 + j], mate)
        near = x * eighth if j == 0 else quarter + y * eighth
        add_block(acc.at[:, columns(near, eighth)], [firsts[j]], rows)
        away = near + ((1 - y) if j == 0 else (1 - x)) * sixteenth
        sends.start(
            acc.at[:, columns(away, sixteenth)], nexts[j], sems.at[4 + j], (side, over)[j]
        )
    for j in range(2):
        landed(nexts[j], sems.at[4 + j], mate)
        add_block(acc.at[:, columns(kept[j], sixteenth)], [nexts[j]], rows)
        for d, zz in enumerate(others):
            sends.start(
                acc.at[pl.ds(pl.multiple_of(zz * strip, 16), strip), columns(kept[j], sixteenth)],
                line.at[j, d],
                sems.at[6 + j * 3 + d],
                device(zz, x, y, c),
            )
    strip_here = pl.multiple_of(z * strip, 16)
    for j in range(2):
        for d in range(3):
            landed(line.at[j, d], sems.at[6 + j * 3 + d], mate)
        block = acc.at[:, columns(kept[j], sixteenth)]
        add_block(block, [line.at[j, d] for d in range(3)], strip, strip_here)

        def place(i, carry, j=j):
            some = pl.ds(pl.multiple_of(strip_here + i * 16, 16), 16)
            out_ref[some, columns(base + kept[j], sixteenth)] = acc[
                some, columns(kept[j], sixteenth)
            ]
            return carry

        lax.fori_loop(0, strip // 16, place, 0)
        done = out_ref.at[pl.ds(strip_here, strip), columns(base + kept[j], sixteenth)]
        for d, zz in enumerate(others):
            sends.start(done, done, sems.at[12 + j * 3 + d], device(zz, x, y, c))
    for j in range(2):
        for d in range(3):
            source = pl.multiple_of(lax.rem(z + 3 - d, 4) * strip, 16)
            landed(
                out_ref.at[pl.ds(source, strip), columns(base + kept[j], sixteenth)],
                sems.at[12 + j * 3 + d],
                mate,
            )
        part = out_ref.at[:, columns(base + kept[j], sixteenth)]
        sends.start(part, part, sems.at[18 + j], (side, over)[j])
    others_kept = (
        x * eighth + (1 - y) * sixteenth,
        quarter + y * eighth + (1 - x) * sixteenth,
    )
    for j in range(2):
        landed(out_ref.at[:, columns(base + others_kept[j], sixteenth)], sems.at[18 + j], mate)
        near = x * eighth if j == 0 else quarter + y * eighth
        part = out_ref.at[:, columns(base + near, eighth)]
        sends.start(part, part, sems.at[20 + j], (over, side)[j])
    for j in range(2):
        away = (1 - x) * eighth if j == 0 else quarter + (1 - y) * eighth
        landed(out_ref.at[:, columns(base + away, eighth)], sems.at[20 + j], mate)
        part = out_ref.at[:, columns(base + j * quarter, quarter)]
        sends.start(part, part, sems.at[22 + j], mate)
    for j in range(2):
        landed(
            out_ref.at[:, columns((1 - c) * half + j * quarter, quarter)], sems.at[22 + j], mate
        )
    sends.finish()


def total_over_all(value, number):
    if lax.axis_size("expert") != 8 or lax.axis_size("weight") != 4:
        return lax.psum(value.astype(jnp.float32), ("expert", "weight"))
    rows, width = value.shape
    out = jax.ShapeDtypeStruct(value.shape, value.dtype)
    buffer = lambda n: pltpu.VMEM((rows, n), value.dtype)
    return pl.pallas_call(
        total_kernel,
        out_shape=out,
        in_specs=[pl.BlockSpec(memory_space=pltpu.VMEM)],
        out_specs=pl.BlockSpec(memory_space=pltpu.VMEM),
        scratch_shapes=[
            buffer(width // 2),
            buffer(width // 2),
            buffer(width // 8),
            buffer(width // 8),
            buffer(width // 16),
            buffer(width // 16),
            pltpu.VMEM((2, 3, rows // 4, width // 16), value.dtype),
            pltpu.SemaphoreType.DMA((24,)),
            pltpu.SemaphoreType.DMA((24,)),
        ],
        compiler_params=pltpu.CompilerParams(collective_id=number, has_side_effects=True),
        cost_estimate=cost(0, value, out),
    )(value).astype(jnp.float32)


def shared_kernel(turn, ins, outs):
    normed_ref, cotangent_ref, gate_grad_ref, lift_grad_ref, hidden_ref = ins

    @pl.when(turn == 0)
    def _():
        for out_ref in outs:
            out_ref[...] = jnp.zeros_like(out_ref)

    normed, cotangent = normed_ref[...], cotangent_ref[...]
    outs[0][...] += trans_times(gate_grad_ref[...], normed)
    outs[1][...] += trans_times(lift_grad_ref[...], normed)
    outs[2][...] += trans_times(hidden_ref[...], cotangent)


def weight_kernel(
    rows_ref, grads_ref, gate_grad_ref, lift_grad_ref, hidden_ref, gate_out, up_out, down_out
):
    rows = rows_ref[0]
    gate_out[0] = trans_times(gate_grad_ref[0], rows)
    up_out[0] = trans_times(lift_grad_ref[0], rows)
    down_out[0] = trans_times(hidden_ref[0], grads_ref[0])


def per_device(
    tokens,
    cotangent,
    segments,
    routes,
    first_gain,
    query_weight,
    latent_weight,
    latent_gain,
    expand_weight,
    output_weight,
    second_gain,
    router_weight,
    shared_gate,
    shared_up,
    shared_down,
    expert_gate,
    expert_up,
    expert_down,
):
    weight_count = lax.axis_size("weight")
    token_rows = tokens.shape[0]
    width = tokens.shape[1]
    group_rows = token_rows * weight_count
    query_width = NOPE + ROPE
    heads_here = query_weight.shape[1] // query_width
    expert_count = router_weight.shape[1]
    local_experts = expert_gate.shape[0]
    score_scale = query_width ** (-0.5)
    activations = tokens.astype(jnp.float32)
    first_scale = inv_rms(activations)
    normed = (activations * first_scale * first_gain).astype(jnp.bfloat16)
    normed_all = gather_group(normed, 0)
    both = ("expert", "weight")
    expert_index = lax.axis_index("expert")
    expert_lanes = lax.axis_size("expert")
    blocks = expert_lanes * weight_count
    pairs, quads = blocks // 2, blocks // 4
    pair_rows, quad_rows = 2 * token_rows, 4 * token_rows
    all_rows = blocks * token_rows
    slot_rows = blocks * CAP
    choose = (
        routes[:, :, None] == jnp.arange(expert_count, dtype=jnp.int32)[None, None, :]
    ).astype(jnp.float32)
    hit = jnp.sum(choose, axis=1)
    order = jnp.arange(token_rows, dtype=jnp.int32)
    before = (order[None, :] < order[:, None]).astype(jnp.bfloat16)
    place = matmul(before, hit.astype(jnp.bfloat16))
    rank = jnp.sum(choose * jnp.arange(routes.shape[1], dtype=jnp.float32)[None, :, None], axis=1)
    code = jnp.where(hit > 0, 32.0 * rank + place, -1.0)
    extra = jnp.pad(code, ((0, 0), (0, lanes - expert_count)), constant_values=-1.0)
    cotangent_wide = jnp.concatenate([cotangent, extra.astype(jnp.bfloat16)], axis=1)
    column = jnp.arange(lanes, dtype=jnp.int32)[None, :]
    row = jnp.arange(8, dtype=jnp.int32)[:, None]
    first_here = expert_index * local_experts
    here = (row < local_experts) & (column == first_here + row)
    twice = here | ((row < local_experts) & (column == first_here + row + expert_count))
    here, twice = here.astype(jnp.bfloat16), twice.astype(jnp.bfloat16)
    weight_index = lax.axis_index("weight")
    high_column = 2 * (row * weight_count + weight_index)
    known = row < routes.shape[1]
    high_at = (known & (column == high_column)).astype(jnp.bfloat16)
    low_at = (known & (column == high_column + 1)).astype(jnp.bfloat16)
    shared_here = shared_gate.shape[1] // expert_lanes
    shared_wide = -(-shared_here // lanes) * lanes
    start = expert_index * shared_here

    def shared_part(matrix):
        part = lax.dynamic_slice_in_dim(matrix, start, shared_here, axis=0)
        return jnp.pad(part, ((0, shared_wide - shared_here), (0, 0)))

    gate_part = shared_part(shared_gate.T)
    up_part = shared_part(shared_up.T)
    down_part = shared_part(shared_down)
    shape = jax.ShapeDtypeStruct
    whole = lambda array: (array, whole_spec(array))
    slots = shape((local_experts, slot_rows, width), jnp.bfloat16)
    slots_one = shape((local_experts, slot_rows, lanes), jnp.float32)
    gather_flops = 2 * all_rows * width * (2 * CAP * local_experts + shared_wide)
    cotangent_all = lax.all_gather(cotangent_wide, both, axis=0, tiled=True)
    marks = (cotangent_all, pl.BlockSpec((quad_rows, lanes), lambda i: (i, width // lanes)))
    grads_slots, shared_raw = call(
        functools.partial(grads_kernel, pair_rows),
        quads,
        [whole(here), (cotangent_all, pair_spec(cotangent_all, quads)), whole(down_part)],
        [
            (slots, slots_spec(slots, quads)),
            (shape((all_rows, shared_wide), jnp.float32), pl.BlockSpec((quad_rows, shared_wide), lambda i: (i, 0))),
        ],
        gather_flops,
    )
    cosine, sine = rope_tables(segments[0])
    allowed = attention_mask(segments[0])
    query_full = matmul(normed_all, query_weight).reshape(group_rows, heads_here, query_width)
    query = jnp.concatenate(
        [
            query_full[..., :NOPE],
            rotate(query_full[..., NOPE:], cosine[:, None, :], sine[:, None, :]),
        ],
        axis=-1,
    ).astype(jnp.bfloat16)
    compressed = matmul(normed_all, latent_weight)
    latent = compressed[:, :LATENT]
    latent_scale = inv_rms(latent)
    latent_normed = (latent * latent_scale * latent_gain).astype(jnp.bfloat16)
    key_rope = rotate(compressed[:, LATENT:], cosine, sine).astype(jnp.bfloat16)
    expanded = (
        matmul(latent_normed, expand_weight)
        .astype(jnp.bfloat16)
        .reshape(group_rows, heads_here, NOPE + VDIM)
    )
    key_nope = expanded[..., :NOPE]
    values = expanded[..., NOPE:]

    def score_block():
        raw = jnp.einsum(
            "ihd,jhd->hij", query[..., :NOPE], key_nope, preferred_element_type=jnp.float32
        )
        raw = raw + jnp.einsum(
            "ihd,jd->hij", query[..., NOPE:], key_rope, preferred_element_type=jnp.float32
        )
        return jnp.where(allowed[None], raw * score_scale, -1e30)

    scores = score_block()
    peak = jnp.max(scores, axis=-1, keepdims=True)
    weights = jnp.exp(scores - peak)
    total = jnp.sum(weights, axis=-1, keepdims=True)
    log_total = peak + jnp.log(total)
    mixed = jnp.einsum(
        "hij,jhd->ihd",
        (weights / total).astype(jnp.bfloat16),
        values,
        preferred_element_type=jnp.float32,
    )
    mixed = mixed.astype(jnp.bfloat16).reshape(group_rows, heads_here * VDIM)
    attended = sum_group(matmul(mixed, output_weight).astype(jnp.bfloat16), 1)
    hidden_one = activations + attended
    second_scale = inv_rms(hidden_one)
    normed_two = (hidden_one * second_scale * second_gain).astype(jnp.bfloat16)
    gates = jax.nn.sigmoid(matmul(normed_two, router_weight))
    chosen = jnp.sum(choose * gates[:, None, :], axis=-1)
    chosen_total = jnp.sum(chosen, axis=1, keepdims=True)
    mixing = route_scale * chosen / chosen_total
    upstream = cotangent.astype(jnp.float32)
    mixing_at = jnp.sum(choose * mixing[:, :, None], axis=1)
    mixing_high = mixing_at.astype(jnp.bfloat16)
    mixing_low = (mixing_at - mixing_high.astype(jnp.float32)).astype(jnp.bfloat16)
    normed_wide = jnp.concatenate([normed_two, mixing_high, mixing_low], axis=1)
    normed_tokens = gather_all(normed_wide, 2).reshape(all_rows, -1)
    token_spec = pl.BlockSpec((quad_rows, shared_wide), lambda i: (i, 0))
    token_shape = shape((all_rows, shared_wide), jnp.bfloat16)
    rows_slots, mix_slots, shared_hidden, shared_gate_grad, shared_lift_grad = call(
        functools.partial(rows_kernel, pair_rows),
        quads,
        [
            whole(here),
            whole(twice),
            marks,
            (normed_tokens, pair_spec(normed_tokens, quads)),
            (shared_raw, token_spec),
            whole(gate_part),
            whole(up_part),
        ],
        [
            (slots, slots_spec(slots, quads)),
            (slots_one, slots_spec(slots_one, quads)),
            (token_shape, token_spec),
            (token_shape, token_spec),
            (token_shape, token_spec),
        ],
        gather_flops + 2 * all_rows * width * shared_wide,
    )
    hidden_here = expert_gate.shape[2]
    gate_rows, up_rows = expert_gate.transpose(0, 2, 1), expert_up.transpose(0, 2, 1)

    def tile_spec(rows, n):
        per = slot_rows // rows
        return pl.BlockSpec((1, rows, n), lambda i: (i // per, i % per, 0))

    def expert_spec(rows, matrix):
        per = slot_rows // rows
        return pl.BlockSpec((1,) + matrix.shape[1:], lambda i: (i // per, 0, 0))

    large, small = 32 * CAP, 16 * CAP
    narrow = shape((local_experts, slot_rows, hidden_here), jnp.bfloat16)
    one_matmul = 2 * local_experts * slot_rows * width * hidden_here
    routed_hidden, mixed_hidden, slope, active, produced = call(
        forward_kernel,
        local_experts * (slot_rows // large),
        [
            (rows_slots, tile_spec(large, width)),
            (mix_slots, tile_spec(large, lanes)),
            (gate_rows, expert_spec(large, gate_rows)),
            (up_rows, expert_spec(large, up_rows)),
            (expert_down, expert_spec(large, expert_down)),
        ],
        [(narrow, tile_spec(large, hidden_here))] * 4 + [(slots, tile_spec(large, width))],
        3 * one_matmul,
    )
    dense = shape((all_rows, width), jnp.bfloat16)
    dense_wide = shape((all_rows, width + lanes), jnp.bfloat16)
    (out_dense,) = call(
        functools.partial(out_kernel, pair_rows),
        quads,
        [
            whole(here),
            marks,
            (produced, slots_spec(slots, quads)),
            (shared_hidden, token_spec),
            whole(down_part),
        ],
        [(dense, pair_spec(dense, quads))],
        gather_flops,
    )
    narrow_tile = tile_spec(small, hidden_here)
    routed_out, (gate_grad, lift_grad, returned, mix_grad_slots) = sum_all(
        out_dense.reshape(blocks, token_rows, width),
        6,
        backward_kernel,
        local_experts * (slot_rows // small),
        [
            (grads_slots, tile_spec(small, width)),
            (routed_hidden, narrow_tile),
            (slope, narrow_tile),
            (active, narrow_tile),
            (gate_rows, expert_spec(small, gate_rows)),
            (up_rows, expert_spec(small, up_rows)),
            (expert_down, expert_spec(small, expert_down)),
        ],
        [
            (narrow, narrow_tile),
            (narrow, narrow_tile),
            (slots, tile_spec(small, width)),
            (slots_one, tile_spec(small, lanes)),
        ],
        3 * one_matmul,
    )
    (back_dense,) = call(
        functools.partial(back_kernel, pair_rows),
        quads,
        [
            whole(here),
            whole(high_at),
            whole(low_at),
            marks,
            (returned, slots_spec(slots, quads)),
            (mix_grad_slots, slots_spec(slots_one, quads)),
            (shared_gate_grad, token_spec),
            (shared_lift_grad, token_spec),
            whole(gate_part),
            whole(up_part),
        ],
        [(dense_wide, pair_spec(dense_wide, quads))],
        gather_flops + 2 * all_rows * width * shared_wide,
    )
    shared_sum = shape((shared_wide, width), jnp.float32)
    shared_out = (shared_sum, whole_spec(shared_sum))
    plain_spec = pl.BlockSpec((pair_rows, width), lambda i: (i, 0))
    shared_spec = pl.BlockSpec((pair_rows, shared_wide), lambda i: (i, 0))
    back_here, shared_sums = sum_all(
        back_dense.reshape(blocks, token_rows, -1),
        3,
        shared_kernel,
        pairs,
        [
            (normed_tokens, plain_spec),
            (cotangent_all, plain_spec),
            (shared_gate_grad, shared_spec),
            (shared_lift_grad, shared_spec),
            (shared_hidden, shared_spec),
        ],
        [shared_out] * 3,
        6 * all_rows * width * shared_wide,
    )
    routed_back = back_here[:, :width]
    mix_grad = back_here[:, width : width + 2 * weight_count * routes.shape[1]]
    mix_grad = jnp.sum(mix_grad.reshape(token_rows, routes.shape[1], -1), axis=2)
    shared_grads = jnp.concatenate([total[:shared_here] for total in shared_sums], axis=0)
    shared_grads = shared_grads.astype(jnp.bfloat16)
    swapped = lax.all_to_all(shared_grads, "expert", split_axis=1, concat_axis=0, tiled=True)
    swapped = swapped.reshape(expert_lanes, 3, shared_here, -1).astype(jnp.float32)
    shared_gradients = [swapped[:, i].reshape(expert_lanes * shared_here, -1) for i in range(3)]
    chosen_grad = route_scale * (
        mix_grad / chosen_total
        - jnp.sum(mix_grad * chosen, axis=1, keepdims=True) / chosen_total**2
    )
    logit_grad = jnp.sum(choose * chosen_grad[:, :, None], axis=1) * gates * (1.0 - gates)
    normed_two_grad = (
        routed_back
        + jnp.dot(logit_grad, router_weight.astype(jnp.float32).T, precision=highest)
    )
    router_gradient = jnp.dot(logit_grad.T, normed_two.astype(jnp.float32), precision=highest)
    back_two, second_gain_gradient = norm_back(
        normed_two_grad, hidden_one, second_scale, second_gain
    )
    hidden_grad = upstream + back_two
    hidden_group = gather_group(hidden_grad.astype(jnp.bfloat16), 4)
    output_gradient = trans_times(mixed, hidden_group)
    mixed_grad = (
        times_trans(hidden_group, output_weight)
        .astype(jnp.bfloat16)
        .reshape(group_rows, heads_here, VDIM)
    )
    probs = jnp.exp(score_block() - log_total)
    prob_grad = jnp.einsum("ihd,jhd->hij", mixed_grad, values, preferred_element_type=jnp.float32)
    centre = jnp.sum(probs * prob_grad, axis=-1, keepdims=True)
    score_grad = (probs * (prob_grad - centre)).astype(jnp.bfloat16)
    value_grad = jnp.einsum(
        "hij,ihd->jhd", probs.astype(jnp.bfloat16), mixed_grad, preferred_element_type=jnp.float32
    )
    query_nope_grad = (
        jnp.einsum("hij,jhd->ihd", score_grad, key_nope, preferred_element_type=jnp.float32)
        * score_scale
    )
    query_rope_grad = (
        jnp.einsum("hij,jd->ihd", score_grad, key_rope, preferred_element_type=jnp.float32)
        * score_scale
    )
    key_nope_grad = (
        jnp.einsum(
            "hij,ihd->jhd", score_grad, query[..., :NOPE], preferred_element_type=jnp.float32
        )
        * score_scale
    )
    key_rope_grad = (
        jnp.einsum("hij,ihd->jd", score_grad, query[..., NOPE:], preferred_element_type=jnp.float32)
        * score_scale
    )
    query_grad = jnp.concatenate(
        [query_nope_grad, unrotate(query_rope_grad, cosine[:, None, :], sine[:, None, :])], axis=-1
    )
    query_grad = query_grad.astype(jnp.bfloat16).reshape(group_rows, heads_here * query_width)
    expand_grad = (
        jnp.concatenate([key_nope_grad, value_grad], axis=-1)
        .astype(jnp.bfloat16)
        .reshape(group_rows, heads_here * (NOPE + VDIM))
    )
    column_half = width // 2
    half_spec = lambda m: pl.BlockSpec((1, m, column_half), lambda i: (i // 2, 0, i % 2))
    narrow_spec = pl.BlockSpec((1, slot_rows, hidden_here), lambda i: (i // 2, 0, 0))
    weight_shape = shape((local_experts, hidden_here, width), jnp.float32)
    weight_grads = call(
        weight_kernel,
        2 * local_experts,
        [
            (rows_slots, half_spec(slot_rows)),
            (grads_slots, half_spec(slot_rows)),
            (gate_grad, narrow_spec),
            (lift_grad, narrow_spec),
            (mixed_hidden, narrow_spec),
        ],
        [(weight_shape, half_spec(hidden_here))] * 3,
        3 * one_matmul,
    )
    expert_grads = (weight_grads[0].transpose(0, 2, 1), weight_grads[1].transpose(0, 2, 1), weight_grads[2])
    layer_out = (hidden_one + routed_out).astype(jnp.bfloat16)
    query_gradient = trans_times(normed_all, query_grad)
    expand_gradient = trans_times(latent_normed, expand_grad)
    latent_normed_grad = times_trans(expand_grad, expand_weight)
    latent_back, latent_gain_gradient = norm_back(
        latent_normed_grad, latent, latent_scale, latent_gain
    )
    compressed_grad = jnp.concatenate([latent_back, unrotate(key_rope_grad, cosine, sine)], axis=-1)
    compressed_grad = compressed_grad.astype(jnp.bfloat16)
    latent_weight_gradient = trans_times(compressed_grad, normed_all)
    normed_grad = sum_group(
        (
            times_trans(query_grad, query_weight) + times_trans(compressed_grad, latent_weight)
        ).astype(jnp.bfloat16),
        5,
    )
    back_one, first_gain_gradient = norm_back(normed_grad, activations, first_scale, first_gain)
    token_gradient = hidden_grad + back_one
    shards = (
        lax.psum_scatter(
            query_gradient.astype(jnp.bfloat16), "expert", scatter_dimension=0, tiled=True
        ).astype(jnp.float32),
        lax.psum_scatter(
            expand_gradient.astype(jnp.bfloat16), "expert", scatter_dimension=0, tiled=True
        ).astype(jnp.float32),
        lax.psum_scatter(
            output_gradient.astype(jnp.bfloat16), "expert", scatter_dimension=1, tiled=True
        ).astype(jnp.float32),
    )
    latent_columns = latent_weight.shape[1]
    filled = jnp.concatenate(
        [
            latent_weight_gradient,
            router_gradient,
            first_gain_gradient[None],
            second_gain_gradient[None],
            jnp.pad(latent_gain_gradient, (0, width - LATENT))[None],
        ],
        axis=0,
    ).astype(jnp.bfloat16)
    wanted = -(-filled.shape[0] // 64) * 64
    filled = jnp.pad(filled, ((0, wanted - filled.shape[0]), (0, 0)))
    total = total_over_all(filled, 7)
    gains_at = latent_columns + expert_count
    totals = (
        total[:latent_columns].T,
        total[gains_at + 2, :LATENT],
        total[latent_columns:gains_at].T,
        total[gains_at],
        total[gains_at + 1],
    )
    return (
        layer_out,
        token_gradient,
        totals[3],
        shards[0],
        totals[0],
        totals[1],
        shards[1],
        shards[2],
        totals[4],
        totals[2],
        shared_gradients[0].T,
        shared_gradients[1].T,
        shared_gradients[2],
        expert_grads[0],
        expert_grads[1],
        expert_grads[2],
    )


def solution(mesh):
    return jax.shard_map(
        per_device,
        mesh=mesh,
        in_specs=(
            P(("expert", "weight"), None),
            P(("expert", "weight"), None),
            P("expert", None),
            P(("expert", "weight"), None),
            P(),
            P(None, "weight"),
            P(),
            P(),
            P(None, "weight"),
            P("weight", None),
            P(),
            P(),
            P(None, "weight"),
            P(None, "weight"),
            P("weight", None),
            P("expert", None, "weight"),
            P("expert", None, "weight"),
            P("expert", "weight", None),
        ),
        out_specs=(
            P(("expert", "weight"), None),
            P(("expert", "weight"), None),
            P(),
            P("expert", "weight"),
            P(),
            P(),
            P("expert", "weight"),
            P("weight", "expert"),
            P(),
            P(),
            P("expert", "weight"),
            P("expert", "weight"),
            P("weight", "expert"),
            P("expert", None, "weight"),
            P("expert", None, "weight"),
            P("expert", "weight", None),
        ),
        check_vma=False,
    )
```

```python
import functools

import jax
import jax.numpy as jnp
from jax import lax
from jax.experimental import pallas as pl
from jax.experimental.pallas import tpu as pltpu
from jax.sharding import PartitionSpec as P

NOPE = 128
ROPE = 64
VDIM = 128
LATENT = 512
TOPK = 6
CAP = 20


eps = 1e-06
route_scale = 2.446
rope_base = 50000.0
highest = lax.Precision.HIGHEST


def matmul(left, right):
    return jnp.dot(left, right, preferred_element_type=jnp.float32)


def trans_times(left, right):
    return lax.dot_general(
        left, right, (((0,), (0,)), ((), ())), preferred_element_type=jnp.float32
    )


def times_trans(left, right):
    return lax.dot_general(
        left, right, (((1,), (1,)), ((), ())), preferred_element_type=jnp.float32
    )


def inv_rms(value):
    return lax.rsqrt(jnp.mean(value * value, axis=-1, keepdims=True) + eps)


def norm_back(grad_out, value, scale, gain):
    scaled = grad_out * gain
    grad_in = scale * scaled - value * scale**3 * jnp.mean(scaled * value, axis=-1, keepdims=True)
    gain_grad = jnp.sum(grad_out * value * scale, axis=0)
    return (grad_in, gain_grad)


def rope_tables(seg):
    size = seg.shape[0]
    index = jnp.arange(size, dtype=jnp.int32)
    fresh = jnp.concatenate([jnp.ones((1,), dtype=bool), seg[1:] != seg[:-1]])
    first = lax.cummax(jnp.where(fresh, index, jnp.zeros_like(index)), axis=0)
    place = (index - first).astype(jnp.float32)
    half = ROPE // 2
    freqs = rope_base ** (-(jnp.arange(half, dtype=jnp.float32) * 2.0 / ROPE))
    angle = place[:, None] * freqs[None, :]
    return (jnp.cos(angle), jnp.sin(angle))


def attention_mask(seg):
    index = jnp.arange(seg.shape[0], dtype=jnp.int32)
    return (seg[:, None] == seg[None, :]) & (index[None, :] <= index[:, None])


def rotate(value, cosine, sine):
    half = value.shape[-1] // 2
    first, second = (value[..., :half], value[..., half:])
    return jnp.concatenate(
        [first * cosine - second * sine, second * cosine + first * sine], axis=-1
    )


def unrotate(value, cosine, sine):
    half = value.shape[-1] // 2
    first, second = (value[..., :half], value[..., half:])
    return jnp.concatenate(
        [first * cosine + second * sine, second * cosine - first * sine], axis=-1
    )


lanes = 128
vmem_limit = 64 * 1024 * 1024 - 131072


def token_slots(marks, here, local_experts, half):
    codes = times_trans(here, marks)
    count = codes.shape[1]
    rank = jnp.floor(codes * (1.0 / 32.0))
    place = codes - 32.0 * rank
    token = lax.broadcasted_iota(jnp.int32, codes.shape, 1)
    slot = jnp.where(codes >= 0, place + jnp.where(token >= half, float(CAP), 0.0), -1.0)
    row = lax.broadcasted_iota(jnp.int32, (2 * CAP, count), 0).astype(jnp.float32)
    picks = [jnp.where(row == slot[e : e + 1], 1.0, 0.0) for e in range(local_experts)]
    return picks, rank


def pair_slots(marks_ref, here_ref, local_experts, pair):
    count = marks_ref.shape[0] // pair
    return [
        token_slots(marks_ref[j * pair : (j + 1) * pair], here_ref[...], local_experts, pair // 2)
        for j in range(count)
    ]


def slot_part(value, e):
    return value[e * 2 * CAP : (e + 1) * 2 * CAP]


def gather_rows(slots, values, pair, out_ref):
    rows = [
        jnp.dot(
            jnp.concatenate(picks, axis=0).astype(jnp.bfloat16),
            values[j * pair : (j + 1) * pair],
            preferred_element_type=jnp.float32,
        )
        for j, (picks, _) in enumerate(slots)
    ]
    for e in range(out_ref.shape[0]):
        together = jnp.concatenate([slot_part(value, e) for value in rows], axis=0)
        out_ref[e] = together.astype(jnp.bfloat16)


def spread_rows(slots, rows_ref):
    local_experts = rows_ref.shape[0]
    rows = [rows_ref[e].astype(jnp.float32) for e in range(local_experts)]
    totals = []
    for j, (picks, _) in enumerate(slots):
        part = jnp.concatenate([slot_part(value, j) for value in rows], axis=0)
        pick = jnp.concatenate(picks, axis=0).astype(jnp.bfloat16)
        totals.append(trans_times(pick, part.astype(jnp.bfloat16)))
    return jnp.concatenate(totals, axis=0)


def grads_kernel(pair, turn, ins, outs):
    here_ref, value_ref, down_ref = ins
    rows_ref, back_ref = outs
    width = rows_ref.shape[2]
    slots = pair_slots(value_ref.at[:, width:], here_ref, rows_ref.shape[0], pair)
    values = value_ref[:, :width]
    gather_rows(slots, values, pair, rows_ref)
    back_ref[...] = times_trans(values, down_ref[...])


def rows_kernel(
    pair,
    here_ref,
    twice_ref,
    marks_ref,
    value_ref,
    back_ref,
    gate_ref,
    up_ref,
    rows_ref,
    mix_ref,
    hidden_ref,
    gate_grad_ref,
    lift_grad_ref,
):
    width = rows_ref.shape[2]
    slots = pair_slots(marks_ref, here_ref, rows_ref.shape[0], pair)
    values = value_ref[:, :width]
    gather_rows(slots, values, pair, rows_ref)
    for j, (picks, _) in enumerate(slots):
        mixing = times_trans(twice_ref[...], value_ref[j * pair : (j + 1) * pair, width:])
        for e, pick in enumerate(picks):
            column = jnp.sum(pick * mixing[e : e + 1], axis=1, keepdims=True)
            column = jnp.broadcast_to(column, (2 * CAP, lanes))
            mix_ref[e, j * 2 * CAP : (j + 1) * 2 * CAP] = column
    gate = times_trans(values, gate_ref[...])
    lift = times_trans(values, up_ref[...])
    back = back_ref[...]
    sigma = jax.nn.sigmoid(gate)
    active = gate * sigma
    hidden_ref[...] = (active * lift).astype(jnp.bfloat16)
    gate_grad_ref[...] = (back * lift * sigma * (1.0 + gate * (1.0 - sigma))).astype(jnp.bfloat16)
    lift_grad_ref[...] = (back * active).astype(jnp.bfloat16)


def forward_kernel(
    rows_ref,
    mix_ref,
    gate_ref,
    up_ref,
    down_ref,
    hidden_ref,
    mixed_ref,
    slope_ref,
    active_ref,
    produced_ref,
):
    rows = rows_ref[0]
    gate = times_trans(rows, gate_ref[0])
    lift = times_trans(rows, up_ref[0])
    mix = mix_ref[0][:, :1]
    sigma = jax.nn.sigmoid(gate)
    active = gate * sigma
    hidden = active * lift
    mixed_hidden = (mix * hidden).astype(jnp.bfloat16)
    hidden_ref[0] = hidden.astype(jnp.bfloat16)
    mixed_ref[0] = mixed_hidden
    slope_ref[0] = (mix * lift * sigma * (1.0 + gate * (1.0 - sigma))).astype(jnp.bfloat16)
    active_ref[0] = (mix * active).astype(jnp.bfloat16)
    produced_ref[0] = matmul(mixed_hidden, down_ref[0]).astype(jnp.bfloat16)


def backward_kernel(turn, ins, outs):
    grads_ref, hidden_ref, slope_ref, active_ref, gate_ref, up_ref, down_ref = ins
    gate_grad_ref, lift_grad_ref, returned_ref, mix_grad_ref = outs
    back = times_trans(grads_ref[0], down_ref[0])
    mix_grad = jnp.sum(hidden_ref[0].astype(jnp.float32) * back, axis=1, keepdims=True)
    mix_grad_ref[0] = jnp.broadcast_to(mix_grad, mix_grad_ref.shape[1:])
    gate_grad = (back * slope_ref[0].astype(jnp.float32)).astype(jnp.bfloat16)
    lift_grad = (back * active_ref[0].astype(jnp.float32)).astype(jnp.bfloat16)
    gate_grad_ref[0] = gate_grad
    lift_grad_ref[0] = lift_grad
    returned = matmul(gate_grad, gate_ref[0]) + matmul(lift_grad, up_ref[0])
    returned_ref[0] = returned.astype(jnp.bfloat16)


def back_kernel(
    pair,
    here_ref,
    high_ref,
    low_ref,
    marks_ref,
    rows_ref,
    mix_grad_ref,
    gate_grad_ref,
    lift_grad_ref,
    gate_ref,
    up_ref,
    out_ref,
):
    width = rows_ref.shape[2]
    slots = pair_slots(marks_ref, here_ref, rows_ref.shape[0], pair)
    total = spread_rows(slots, rows_ref)
    total = total + matmul(gate_grad_ref[...], gate_ref[...])
    total = total + matmul(lift_grad_ref[...], up_ref[...])
    out_ref[:, :width] = total.astype(jnp.bfloat16)
    for j, (picks, rank) in enumerate(slots):
        choice = lax.broadcasted_iota(jnp.int32, rank.shape, 0).astype(jnp.float32)
        mix_grad = jnp.zeros(rank.shape, jnp.float32)
        for e, pick in enumerate(picks):
            column = slot_part(mix_grad_ref[e], j)[:, :1]
            row = jnp.sum(pick * column, axis=0, keepdims=True)
            mix_grad = mix_grad + jnp.where(choice == rank[e : e + 1], row, 0.0)
        high = mix_grad.astype(jnp.bfloat16)
        low = (mix_grad - high.astype(jnp.float32)).astype(jnp.bfloat16)
        sent = trans_times(high, high_ref[...]) + trans_times(low, low_ref[...])
        out_ref[j * pair : (j + 1) * pair, width:] = sent.astype(jnp.bfloat16)


def out_kernel(pair, here_ref, marks_ref, rows_ref, hidden_ref, down_ref, out_ref):
    slots = pair_slots(marks_ref, here_ref, rows_ref.shape[0], pair)
    total = spread_rows(slots, rows_ref)
    total = total + matmul(hidden_ref[...], down_ref[...])
    out_ref[...] = total.astype(jnp.bfloat16)


def whole_spec(array):
    zeros = (0,) * array.ndim
    return pl.BlockSpec(array.shape, lambda i: zeros)


def pair_spec(array, pairs):
    block = (array.shape[0] // pairs,) + array.shape[1:]
    zeros = (0,) * (array.ndim - 1)
    return pl.BlockSpec(block, lambda i: (i,) + zeros)


def slots_spec(array, pairs):
    block = (array.shape[0], array.shape[1] // pairs) + array.shape[2:]
    return pl.BlockSpec(block, lambda i: (0, i, 0))


def cost(flops, *arrays):
    moved = sum(a.size * a.dtype.itemsize for a in arrays)
    return pl.CostEstimate(flops=int(flops), bytes_accessed=int(moved), transcendentals=0)


def call(kernel, grid, ins, outs, flops):
    arrays = [a for a, _ in ins]
    shapes = [s for s, _ in outs]
    return pl.pallas_call(
        kernel,
        grid=(grid,),
        in_specs=[s for _, s in ins],
        out_specs=[s for _, s in outs],
        out_shape=shapes,
        cost_estimate=cost(flops, *arrays, *shapes),
        compiler_params=pltpu.CompilerParams(vmem_limit_bytes=vmem_limit),
    )(*arrays)


MESH = pl.DeviceIdType.MESH


def places():
    expert, weight = lax.axis_index("expert"), lax.axis_index("weight")
    return lax.div(expert, 2), lax.rem(expert, 2), lax.div(weight, 2), lax.rem(weight, 2)


def device(z, x, y, c):
    return (z * 2 + x, y * 2 + c)


def shard(z, x, y, c):
    return z * 8 + x * 4 + y * 2 + c


def push(source, target, send, receive, to):
    return pltpu.make_async_remote_copy(
        src_ref=source,
        dst_ref=target,
        send_sem=send,
        recv_sem=receive,
        device_id=to,
        device_id_type=MESH,
    )


class Sends:
    def __init__(self, semaphores):
        self.semaphores = semaphores
        self.started = []

    def plan(self, source, target, receive, to, when=None):
        copy = push(source, target, self.semaphores.at[len(self.started)], receive, to)
        self.started.append((copy, when))
        return copy

    def start(self, source, target, receive, to, when=None):
        copy = self.plan(source, target, receive, to, when)
        if when is None:
            copy.start()
        else:
            pl.when(when)(copy.start)

    def finish(self):
        for copy, when in self.started:
            if when is None:
                copy.wait_send()
            else:
                pl.when(when)(copy.wait_send)


def landed(target, receive, to):
    push(target, target, receive, receive, to).wait_recv()


def greet(devices):
    barrier = pltpu.get_barrier_semaphore()
    count = 0
    for to, when in devices:
        signal = functools.partial(
            pl.semaphore_signal, barrier, inc=1, device_id=to, device_id_type=MESH
        )
        if when is None:
            signal()
            count = count + 1
        else:
            pl.when(when)(signal)
            count = count + when.astype(jnp.int32)
    pl.semaphore_wait(barrier, count)


def add_rows(target, sources, start, rows):
    step = 16

    def body(i, carry):
        part = pl.ds(pl.multiple_of(start + i * step, step), step)
        total = target[part].astype(jnp.float32)
        for source, offset in sources:
            there = pl.ds(pl.multiple_of(start - offset + i * step, step), step)
            total = total + source[there].astype(jnp.float32)
        target[part] = total.astype(target.dtype)
        return carry

    lax.fori_loop(0, rows // step, body, 0)


def ordered(z, first, second):
    upper = lax.div(z, 2)
    inner = z + upper * (3 - 2 * z)
    value = first + inner * (second - first)
    return value + upper * (3 - 2 * value)


class Gather:
    def __init__(self, x_ref, out_ref, sends, recv_sems, local_sem, place):
        z, x, y, c = place
        half = x_ref.shape[0] // 2
        over, side, mate = device(z, 1 - x, y, c), device(z, x, 1 - y, c), device(z, x, y, 1 - c)
        up, down = device(z + 1, x, y, c), device(z - 1, x, y, c)
        self.out_ref, self.recv_sems, self.mate, self.half = out_ref, recv_sems, mate, half
        planes = [ordered(z, (0, 1, 2, 3)[step], (1, 0, 2, 3)[step]) for step in range(4)]
        self.rising = [(zz <= z) & (z < 3) for zz in planes]
        self.falling = [(zz >= z) & (z > 0) for zz in planes]
        self.mine = [shard(zz, x, y, c) for zz in planes]
        self.overs = [shard(zz, 1 - x, y, c) for zz in planes]
        self.sides = [shard(zz, x, 1 - y, c) for zz in planes]
        self.corners = [shard(zz, 1 - x, 1 - y, c) for zz in planes]
        self.mates = [
            (shard(zz, x, y, 1 - c), shard(zz, 1 - x, y, 1 - c), shard(zz, x, 1 - y, 1 - c))
            for zz in planes
        ]
        self.mate_corners = [shard(zz, 1 - x, 1 - y, 1 - c) for zz in planes]
        self.keep = pltpu.make_async_copy(x_ref, out_ref.at[self.mine[0]], local_sem)
        self.whole_copies, self.relay_copies, self.corner_copies = [], [], []

        def copy(ref, receive, to, when=None, source=None):
            return sends.plan(ref if source is None else source, ref, receive, to, when)

        for step in range(4):
            i = self.mine[step]
            source = x_ref if step == 0 else None
            there, receive = out_ref.at[i], recv_sems.at[i, 0]
            self.whole_copies.append(
                [
                    (copy(there, receive, up, self.rising[step], source), self.rising[step]),
                    (copy(there, receive, down, self.falling[step], source), self.falling[step]),
                    (copy(there, receive, over, None, source), None),
                    (copy(there, receive, side, None, source), None),
                    (copy(there, receive, mate, None, source), None),
                ]
            )
            i, j = self.overs[step], self.sides[step]
            self.relay_copies.append(
                [
                    copy(self.halves(i, 0), recv_sems.at[i, 0], side),
                    copy(out_ref.at[i], recv_sems.at[i, 0], mate),
                    copy(self.halves(j, 1), recv_sems.at[j, 1], over),
                    copy(out_ref.at[j], recv_sems.at[j, 0], mate),
                ]
            )
            i = self.corners[step]
            self.corner_copies.append(
                [copy(self.halves(i, h), recv_sems.at[i, h], mate) for h in range(2)]
            )

    def halves(self, i, h):
        return self.out_ref.at[i, pl.ds(h * self.half, self.half)]

    def full_here(self, i):
        landed(self.out_ref.at[i], self.recv_sems.at[i, 0], self.mate)

    def half_here(self, i, h):
        landed(self.halves(i, h), self.recv_sems.at[i, h], self.mate)

    def whole(self, step):
        if step == 0:
            self.keep.start()
        else:
            self.full_here(self.mine[step])
        for copy, when in self.whole_copies[step]:
            if when is None:
                copy.start()
            else:
                pl.when(when)(copy.start)

    def relay(self, step):
        self.full_here(self.overs[step])
        self.relay_copies[step][0].start()
        self.relay_copies[step][1].start()
        self.full_here(self.sides[step])
        self.relay_copies[step][2].start()
        self.relay_copies[step][3].start()

    def corner(self, step):
        for h in range(2):
            self.half_here(self.corners[step], h)
            self.corner_copies[step][h].start()

    def last(self):
        for step in range(4):
            for i in self.mates[step]:
                self.full_here(i)
            for h in range(2):
                self.half_here(self.mate_corners[step], h)
        self.keep.wait()


def gather_neighbours(place):
    z, x, y, c = place
    return [
        (device(z, 1 - x, y, c), None),
        (device(z, x, 1 - y, c), None),
        (device(z, x, y, 1 - c), None),
        (device(z + 1, x, y, c), z < 3),
        (device(z - 1, x, y, c), z > 0),
    ]


def gather_all_kernel(inner, cover_ins, cover_outs, x_ref, *refs):
    ins, refs = refs[:cover_ins], refs[cover_ins:]
    out_ref, refs = refs[0], refs[1:]
    outs, refs = refs[:cover_outs], refs[cover_outs:]
    send_sems, recv_sems, local_sem = refs
    turn, turns = pl.program_id(0), pl.num_programs(0)
    place = places()
    sends = Sends(send_sems)
    gather = Gather(x_ref, out_ref, sends, recv_sems, local_sem, place)

    def begin():
        greet(gather_neighbours(place))
        gather.whole(0)

    def end():
        gather.whole(3)
        gather.relay(2)
        gather.corner(1)
        gather.relay(3)
        gather.corner(2)
        gather.corner(3)
        gather.last()
        sends.finish()

    def early():
        gather.relay(1)
        gather.corner(0)

    pieces = [
        begin,
        lambda: None,
        functools.partial(gather.whole, 1),
        functools.partial(gather.relay, 0),
        functools.partial(gather.whole, 2),
        lambda: None,
        early,
    ]
    for number, piece in enumerate(pieces):
        pl.when(turn == number)(piece)
    inner(turn, ins, outs)
    pl.when(turn == turns - 1)(end)


def gather_all(value, number, inner, turns, ins, outs, flops):
    if lax.axis_size("expert") != 8 or lax.axis_size("weight") != 4:

        def alone(*refs):
            inner(pl.program_id(0), refs[: len(ins)], refs[len(ins) :])

        gathered = lax.all_gather(value, ("expert", "weight"), axis=0)
        return gathered, call(alone, turns, ins, outs, flops)
    out = jax.ShapeDtypeStruct((32,) + value.shape, value.dtype)
    arrays, shapes = [a for a, _ in ins], [o for o, _ in outs]
    results = pl.pallas_call(
        functools.partial(gather_all_kernel, inner, len(ins), len(outs)),
        grid=(turns,),
        out_shape=[out] + shapes,
        in_specs=[whole_spec(value)] + [spec for _, spec in ins],
        out_specs=[pl.BlockSpec(memory_space=pl.ANY)] + [spec for _, spec in outs],
        scratch_shapes=[
            pltpu.SemaphoreType.DMA((44,)),
            pltpu.SemaphoreType.DMA((32, 2)),
            pltpu.SemaphoreType.DMA,
        ],
        compiler_params=pltpu.CompilerParams(
            collective_id=number, has_side_effects=True, vmem_limit_bytes=vmem_limit
        ),
        cost_estimate=cost(flops, value, out, *arrays, *shapes),
    )(value, *arrays)
    return results[0], results[1:]


def attention_kernel(
    score_scale,
    normed_ref,
    value_ref,
    cosine_ref,
    sine_ref,
    segment_row_ref,
    segment_column_ref,
    gain_ref,
    query_hbm,
    latent_hbm,
    expand_hbm,
    output_hbm,
    value_out,
    normed_out,
    query_out,
    latent_out,
    scale_out,
    latent_normed_out,
    key_rope_out,
    expanded_out,
    log_out,
    mixed_out,
    attended_out,
    query_matrix,
    latent_matrix,
    expand_matrix,
    output_matrix,
    partial,
    mates,
    sides,
    carried,
    send_sems,
    recv_sems,
    local_sems,
    group_sends,
    group_sems,
    sum_sends,
    mate_sems,
    side_sems,
):
    place = places()
    z, x, y, c = place
    side, mate = device(z, x, 1 - y, c), device(z, x, y, 1 - c)
    rows = normed_ref.shape[0]
    half = rows // 2
    heads = query_out.shape[0]
    greet(gather_neighbours(place))
    near = Sends(group_sends)
    own, across = y * 2 + c, (1 - y) * 2 + c
    keep = pltpu.make_async_copy(normed_ref, normed_out.at[own], local_sems.at[0])
    keep.start()

    def part(i, h):
        return normed_out.at[i, pl.ds(h * half, half)]

    for to in (side, mate):
        for h in range(2):
            piece = normed_ref.at[pl.ds(h * half, half)]
            near.start(piece, part(own, h), group_sems.at[own, h], to)
    sends = Sends(send_sems)
    gather = Gather(value_ref, value_out, sends, recv_sems, local_sems.at[1], place)
    gather.whole(0)
    loads = [
        pltpu.make_async_copy(source, target, local_sems.at[2 + i])
        for i, (source, target) in enumerate(
            (
                (query_hbm, query_matrix),
                (latent_hbm, latent_matrix),
                (expand_hbm, expand_matrix),
                (output_hbm, output_matrix),
            )
        )
    ]
    for load in loads:
        load.start()
    for h in range(2):
        landed(part(across, h), group_sems.at[across, h], mate)
        near.start(part(across, h), part(across, h), group_sems.at[across, h], mate)
    for i in (y * 2 + 1 - c, (1 - y) * 2 + 1 - c):
        for h in range(2):
            landed(part(i, h), group_sems.at[i, h], mate)
    keep.wait()
    normed = normed_out[...].reshape(4 * rows, normed_out.shape[2])
    cosine, sine = cosine_ref[...], sine_ref[...]
    turn_half = ROPE // 2

    def turned(first, second):
        return jnp.concatenate(
            [first * cosine - second * sine, second * cosine + first * sine], axis=1
        )

    loads[0].wait()
    full = matmul(normed, query_matrix[...])
    for h in range(heads):
        start = h * (NOPE + ROPE)
        first = full[:, start + NOPE : start + NOPE + turn_half]
        second = full[:, start + NOPE + turn_half : start + NOPE + ROPE]
        query = jnp.concatenate([full[:, start : start + NOPE], turned(first, second)], axis=1)
        query_out[h] = query.astype(jnp.bfloat16)
    gather.whole(1)
    loads[1].wait()
    compressed = times_trans(normed, latent_matrix[...])
    latent = compressed[:, :LATENT]
    scale = inv_rms(latent)
    latent_out[...] = latent
    scale_out[...] = jnp.broadcast_to(scale, scale_out.shape)
    latent_normed_out[...] = (latent * scale * gain_ref[...]).astype(jnp.bfloat16)
    first = compressed[:, LATENT : LATENT + turn_half]
    second = compressed[:, LATENT + turn_half : LATENT + ROPE]
    key_rope_out[...] = turned(first, second).astype(jnp.bfloat16)
    gather.relay(0)
    loads[2].wait()
    expanded_out[...] = matmul(latent_normed_out[...], expand_matrix[...]).astype(jnp.bfloat16)

    def head(h):
        start = h * (NOPE + VDIM)
        query = query_out[h]
        raw = times_trans(query[:, :NOPE], expanded_out[:, start : start + NOPE])
        raw = raw + times_trans(query[:, NOPE:], key_rope_out[...])
        row = lax.broadcasted_iota(jnp.int32, raw.shape, 0)
        column = lax.broadcasted_iota(jnp.int32, raw.shape, 1)
        allowed = (segment_column_ref[...] == segment_row_ref[...]) & (column <= row)
        scores = jnp.where(allowed, raw * score_scale, -1e30)
        peak = jnp.max(scores, axis=1, keepdims=True)
        weights = jnp.exp(scores - peak)
        total = jnp.sum(weights, axis=1, keepdims=True)
        log_out[h] = jnp.broadcast_to(peak + jnp.log(total), log_out.shape[1:])
        probs = (weights / total).astype(jnp.bfloat16)
        mixed = matmul(probs, expanded_out[:, start + NOPE : start + NOPE + VDIM])
        mixed_out[:, h * VDIM : (h + 1) * VDIM] = mixed.astype(jnp.bfloat16)

    middle = [
        None,
        functools.partial(gather.whole, 2),
        functools.partial(gather.relay, 1),
        functools.partial(gather.corner, 0),
    ]
    for h in range(heads):
        head(h)
        if h < 4 and middle[h] is not None:
            middle[h]()
    loads[3].wait()
    for i in range(4):
        block = matmul(mixed_out[i * rows : (i + 1) * rows], output_matrix[...])
        partial[i] = block.astype(jnp.bfloat16)
    sums = Sends(sum_sends)
    for j, yy in enumerate((1 - y, y)):
        for h in range(2):
            some = pl.ds(h * half, half)
            sums.start(
                partial.at[yy * 2 + 1 - c, some], mates.at[j, some], mate_sems.at[j, h], mate
            )
    gather.whole(3)
    for h in range(2):
        some = pl.ds(h * half, half)
        landed(mates.at[0, some], mate_sems.at[0, h], mate)
        add_into(carried, [partial.at[(1 - y) * 2 + c], mates.at[0]], h * half, half)
        sums.start(carried.at[some], sides.at[some], side_sems.at[h], side)
    gather.relay(2)
    gather.corner(1)
    gather.relay(3)
    gather.corner(2)
    for h in range(2):
        some = pl.ds(h * half, half)
        landed(mates.at[1, some], mate_sems.at[1, h], mate)
        landed(sides.at[some], side_sems.at[h], mate)
        add_into(attended_out, [partial.at[y * 2 + c], mates.at[1], sides], h * half, half)
    gather.corner(3)
    gather.last()
    near.finish()
    sends.finish()
    sums.finish()


def add_into(target, sources, start, rows):
    step = 16

    def body(i, carry):
        part = pl.ds(pl.multiple_of(start + i * step, step), step)
        total = sources[0][part].astype(jnp.float32)
        for source in sources[1:]:
            total = total + source[part].astype(jnp.float32)
        target[part] = total.astype(target.dtype)
        return carry

    lax.fori_loop(0, rows // step, body, 0)


def attention_forward(
    score_scale, normed, value, cosine, sine, segment, gain, query, latent, expand, output, number
):
    rows, width = normed.shape
    group, heads = 4 * rows, query.shape[1] // (NOPE + ROPE)
    shape, low = jax.ShapeDtypeStruct, jnp.bfloat16
    vmem, away = pl.BlockSpec(memory_space=pltpu.VMEM), pl.BlockSpec(memory_space=pl.ANY)
    segment = segment.astype(jnp.float32)
    inputs = [normed, value, cosine, sine, segment[None], segment[:, None], gain[None]]
    matrices = [query, latent.T, expand, output]
    outs = [
        shape((32,) + value.shape, low),
        shape((4, rows, width), low),
        shape((heads, group, NOPE + ROPE), low),
        shape((group, LATENT), jnp.float32),
        shape((group, lanes), jnp.float32),
        shape((group, LATENT), low),
        shape((group, ROPE), low),
        shape((group, heads * (NOPE + VDIM)), low),
        shape((heads, group, lanes), jnp.float32),
        shape((group, heads * VDIM), low),
        shape((rows, width), jnp.float32),
    ]
    flops = 2 * group * (width * (query.shape[1] + latent.shape[1]) + output.size + expand.size)
    return pl.pallas_call(
        functools.partial(attention_kernel, score_scale),
        out_shape=outs,
        in_specs=[vmem] * len(inputs) + [away] * 4,
        out_specs=[away] + [vmem] * (len(outs) - 1),
        scratch_shapes=[pltpu.VMEM(m.shape, low) for m in matrices]
        + [
            pltpu.VMEM((4, rows, width), low),
            pltpu.VMEM((2, rows, width), low),
            pltpu.VMEM((rows, width), low),
            pltpu.VMEM((rows, width), low),
            pltpu.SemaphoreType.DMA((44,)),
            pltpu.SemaphoreType.DMA((32, 2)),
            pltpu.SemaphoreType.DMA((6,)),
            pltpu.SemaphoreType.DMA((6,)),
            pltpu.SemaphoreType.DMA((4, 2)),
            pltpu.SemaphoreType.DMA((6,)),
            pltpu.SemaphoreType.DMA((2, 2)),
            pltpu.SemaphoreType.DMA((2,)),
        ],
        compiler_params=pltpu.CompilerParams(
            collective_id=number, has_side_effects=True, vmem_limit_bytes=vmem_limit
        ),
        cost_estimate=cost(flops, *inputs, *matrices, *outs),
    )(*inputs, *matrices)


def sum_all_kernel(inner, cover_ins, cover_outs, p_ref, *refs):
    ins, refs = refs[:cover_ins], refs[cover_ins:]
    out_ref, refs = refs[0], refs[1:]
    outs, refs = refs[:cover_outs], refs[cover_outs:]
    own, mates, over_half, side_half, over_full, side_full, below, above = refs[:8]
    send_sems, mate_sems, half_sems, full_sems, line_sems, local_sems = refs[8:]
    z, x, y, c = places()
    turn, turns = pl.program_id(0), pl.num_programs(0)
    rows = out_ref.shape[0]
    half = rows // 2
    over, side, mate = device(z, 1 - x, y, c), device(z, x, 1 - y, c), device(z, x, y, 1 - c)
    up, down = device(z + 1, x, y, c), device(z - 1, x, y, c)
    sends = Sends(send_sems)
    targets = [ordered(z, (3, 2, 1, 0)[step], (3, 0, 2, 1)[step]) for step in range(4)]
    spots = [(1 - x, 1 - y), (1 - x, y), (x, 1 - y), (x, y)]
    shards = [[shard(zz, xx, yy, 1 - c) for xx, yy in spots] for zz in targets]
    mine = [[shard(zz, xx, yy, c) for xx, yy in spots] for zz in targets]
    higher = [zz > z for zz in targets]
    lower = [zz < z for zz in targets]
    loads = [
        pltpu.make_async_copy(p_ref.at[mine[slot // 4][slot % 4]], own.at[slot], local_sems.at[slot])
        for slot in range(16)
    ]

    mate_copies = [
        sends.plan(p_ref.at[shards[slot // 4][slot % 4]], mates.at[slot], mate_sems.at[slot], mate)
        for slot in range(16)
    ]
    corner_copies, relay_copies, line_copies = [], [], []
    for step in range(4):
        corner_copies.append(
            (
                sends.plan(
                    own.at[step * 4, pl.ds(half, half)],
                    over_half.at[step],
                    half_sems.at[step, 0],
                    over,
                ),
                sends.plan(
                    own.at[step * 4, pl.ds(0, half)], side_half.at[step], half_sems.at[step, 1], side
                ),
            )
        )
        relay_copies.append(
            (
                sends.plan(
                    own.at[step * 4 + 1], over_full.at[step], full_sems.at[step, 0], over
                ),
                sends.plan(
                    own.at[step * 4 + 2], side_full.at[step], full_sems.at[step, 1], side
                ),
            )
        )
    for step in range(3):
        zz, slot = targets[step], step * 4 + 3
        line_copies.append(
            (
                sends.plan(own.at[slot], below.at[zz], line_sems.at[zz, 0], up, higher[step]),
                sends.plan(own.at[slot], above.at[zz], line_sems.at[zz, 1], down, lower[step]),
            )
        )

    def begin():
        greet([(over, None), (side, None), (mate, None), (up, z < 3), (down, z > 0)])
        for slot in range(16):
            mate_copies[slot].start()
            loads[slot].start()

    def join(slot):
        loads[slot].wait()
        landed(mates.at[slot], mate_sems.at[slot], mate)

    def corner(step):
        slot = step * 4
        join(slot)
        add_rows(own.at[slot], [(mates.at[slot], 0)], 0, rows)
        for copy in corner_copies[step]:
            copy.start()

    def relay(step):
        slot = step * 4 + 1
        join(slot)
        add_rows(own.at[slot], [(mates.at[slot], 0)], half, half)
        landed(side_half.at[step], half_sems.at[step, 1], mate)
        add_rows(own.at[slot], [(mates.at[slot], 0), (side_half.at[step], 0)], 0, half)
        relay_copies[step][0].start()
        slot = step * 4 + 2
        join(slot)
        add_rows(own.at[slot], [(mates.at[slot], 0)], 0, half)
        landed(over_half.at[step], half_sems.at[step, 0], mate)
        add_rows(own.at[slot], [(mates.at[slot], 0), (over_half.at[step], half)], half, half)
        relay_copies[step][1].start()

    def whole(step):
        zz = targets[step]
        slot = step * 4 + 3
        join(slot)
        landed(over_full.at[step], full_sems.at[step, 0], mate)
        landed(side_full.at[step], full_sems.at[step, 1], mate)
        add_rows(
            own.at[slot],
            [(mates.at[slot], 0), (over_full.at[step], 0), (side_full.at[step], 0)],
            0,
            rows,
        )

        @pl.when((zz >= z) & (z > 0))
        def _():
            landed(below.at[zz], line_sems.at[zz, 0], mate)
            add_rows(own.at[slot], [(below.at[zz], 0)], 0, rows)

        @pl.when((zz <= z) & (z < 3))
        def _():
            landed(above.at[zz], line_sems.at[zz, 1], mate)
            add_rows(own.at[slot], [(above.at[zz], 0)], 0, rows)

        if step < 3:
            pl.when(higher[step])(line_copies[step][0].start)
            pl.when(lower[step])(line_copies[step][1].start)

    def end():
        whole(3)
        out_ref[...] = own[15].astype(out_ref.dtype)
        sends.finish()

    pieces = [
        begin,
        functools.partial(corner, 0),
        functools.partial(corner, 1),
        functools.partial(relay, 0),
        functools.partial(corner, 2),
        functools.partial(relay, 1),
        functools.partial(whole, 0),
        functools.partial(corner, 3),
        functools.partial(relay, 2),
        functools.partial(whole, 1),
        functools.partial(relay, 3),
        functools.partial(whole, 2),
    ]
    for number, piece in enumerate(pieces):
        pl.when(turn == number)(piece)
    inner(turn, ins, outs)
    pl.when(turn == turns - 1)(end)


def sum_all(value, number, inner, turns, ins, outs, flops):
    if lax.axis_size("expert") != 8 or lax.axis_size("weight") != 4:
        summed = lax.psum_scatter(
            value.reshape(-1, value.shape[2]), ("expert", "weight"), scatter_dimension=0, tiled=True
        )

        def alone(*refs):
            inner(pl.program_id(0), refs[: len(ins)], refs[len(ins) :])

        return summed.astype(jnp.float32), call(alone, turns, ins, outs, flops)
    _, rows, width = value.shape
    out = jax.ShapeDtypeStruct((rows, width), jnp.float32)
    buffer = lambda n, r: pltpu.VMEM((n, r, width), value.dtype)
    arrays, shapes = [a for a, _ in ins], [o for o, _ in outs]
    results = pl.pallas_call(
        functools.partial(sum_all_kernel, inner, len(ins), len(outs)),
        grid=(turns,),
        out_shape=[out] + shapes,
        in_specs=[pl.BlockSpec(memory_space=pl.ANY)] + [spec for _, spec in ins],
        out_specs=[pl.BlockSpec((rows, width), lambda i: (0, 0))] + [spec for _, spec in outs],
        scratch_shapes=[
            buffer(16, rows),
            buffer(16, rows),
            buffer(4, rows // 2),
            buffer(4, rows // 2),
            buffer(4, rows),
            buffer(4, rows),
            buffer(4, rows),
            buffer(4, rows),
            pltpu.SemaphoreType.DMA((40,)),
            pltpu.SemaphoreType.DMA((16,)),
            pltpu.SemaphoreType.DMA((4, 2)),
            pltpu.SemaphoreType.DMA((4, 2)),
            pltpu.SemaphoreType.DMA((4, 2)),
            pltpu.SemaphoreType.DMA((16,)),
        ],
        compiler_params=pltpu.CompilerParams(
            collective_id=number, has_side_effects=True, vmem_limit_bytes=vmem_limit
        ),
        cost_estimate=cost(flops, value, out, *arrays, *shapes),
    )(value, *arrays)
    return results[0], results[1:]


def gather_group_kernel(x_ref, out_ref, send_sems, recv_sems, local_sem):
    z, x, y, c = places()
    half = x_ref.shape[0] // 2
    side, mate = device(z, x, 1 - y, c), device(z, x, y, 1 - c)
    greet([(side, None), (mate, None)])
    sends = Sends(send_sems)
    own, across = y * 2 + c, (1 - y) * 2 + c
    keep = pltpu.make_async_copy(x_ref, out_ref.at[own], local_sem)
    keep.start()

    def part(i, h):
        return out_ref.at[i, pl.ds(h * half, half)]

    for h in range(2):
        piece = x_ref.at[pl.ds(h * half, half)]
        sends.start(piece, part(own, h), recv_sems.at[own, h], side)
    for h in range(2):
        piece = x_ref.at[pl.ds(h * half, half)]
        sends.start(piece, part(own, h), recv_sems.at[own, h], mate)
    for h in range(2):
        landed(part(across, h), recv_sems.at[across, h], mate)
        sends.start(part(across, h), part(across, h), recv_sems.at[across, h], mate)
    for i in (y * 2 + 1 - c, (1 - y) * 2 + 1 - c):
        for h in range(2):
            landed(part(i, h), recv_sems.at[i, h], mate)
    sends.finish()
    keep.wait()


def gather_group(value, number):
    if lax.axis_size("expert") != 8 or lax.axis_size("weight") != 4:
        return lax.all_gather(value, "weight", axis=0, tiled=True)
    out = jax.ShapeDtypeStruct((4,) + value.shape, value.dtype)
    return pl.pallas_call(
        gather_group_kernel,
        out_shape=out,
        in_specs=[pl.BlockSpec(memory_space=pltpu.VMEM)],
        out_specs=pl.BlockSpec(memory_space=pltpu.VMEM),
        scratch_shapes=[
            pltpu.SemaphoreType.DMA((6,)),
            pltpu.SemaphoreType.DMA((4, 2)),
            pltpu.SemaphoreType.DMA,
        ],
        compiler_params=pltpu.CompilerParams(collective_id=number, has_side_effects=True),
        cost_estimate=cost(0, value, out),
    )(value).reshape(-1, value.shape[1])


def sum_group_kernel(p_ref, out_ref, mates, sides, carried, send_sems, mate_sems, side_sems):
    z, x, y, c = places()
    rows = out_ref.shape[0]
    half = rows // 2
    side, mate = device(z, x, 1 - y, c), device(z, x, y, 1 - c)
    greet([(side, None), (mate, None)])
    sends = Sends(send_sems)

    for j, yy in enumerate((1 - y, y)):
        for h in range(2):
            part = pl.ds(h * half, half)
            sends.start(
                p_ref.at[yy * 2 + 1 - c, part], mates.at[j, part], mate_sems.at[j, h], mate
            )

    def add(target, sources, h):
        step = 16

        def body(i, carry):
            part = pl.ds(pl.multiple_of(h * half + i * step, step), step)
            total = sources[0][part].astype(jnp.float32)
            for source in sources[1:]:
                total = total + source[part].astype(jnp.float32)
            target[part] = total.astype(target.dtype)
            return carry

        lax.fori_loop(0, half // step, body, 0)

    for h in range(2):
        part = pl.ds(h * half, half)
        landed(mates.at[0, part], mate_sems.at[0, h], mate)
        add(carried, [p_ref.at[(1 - y) * 2 + c], mates.at[0]], h)
        sends.start(carried.at[part], sides.at[part], side_sems.at[h], side)
    for h in range(2):
        part = pl.ds(h * half, half)
        landed(mates.at[1, part], mate_sems.at[1, h], mate)
        landed(sides.at[part], side_sems.at[h], mate)
        add(out_ref, [p_ref.at[y * 2 + c], mates.at[1], sides], h)
    sends.finish()


def sum_group(value, number):
    if lax.axis_size("expert") != 8 or lax.axis_size("weight") != 4:
        summed = lax.psum_scatter(value, "weight", scatter_dimension=0, tiled=True)
        return summed.astype(jnp.float32)
    rows, width = value.shape[0] // 4, value.shape[1]
    value = value.reshape(4, rows, width)
    out = jax.ShapeDtypeStruct((rows, width), jnp.float32)
    return pl.pallas_call(
        sum_group_kernel,
        out_shape=out,
        in_specs=[pl.BlockSpec(memory_space=pltpu.VMEM)],
        out_specs=pl.BlockSpec(memory_space=pltpu.VMEM),
        scratch_shapes=[
            pltpu.VMEM((2, rows, width), value.dtype),
            pltpu.VMEM((rows, width), value.dtype),
            pltpu.VMEM((rows, width), value.dtype),
            pltpu.SemaphoreType.DMA((6,)),
            pltpu.SemaphoreType.DMA((2, 2)),
            pltpu.SemaphoreType.DMA((2,)),
        ],
        compiler_params=pltpu.CompilerParams(collective_id=number, has_side_effects=True),
        cost_estimate=cost(0, value, out),
    )(value)


def columns(start, size):
    return pl.ds(pl.multiple_of(start, lanes), size)


def add_block(target, sources, rows, row_start=0):
    step = 16

    def body(i, carry):
        part = pl.ds(pl.multiple_of(row_start + i * step, step), step)
        total = target[part].astype(jnp.float32)
        for source in sources:
            there = pl.ds(pl.multiple_of(i * step, step), step)
            total = total + source[there].astype(jnp.float32)
        target[part] = total.astype(target.dtype)
        return carry

    lax.fori_loop(0, rows // step, body, 0)


def total_kernel(
    p_ref, out_ref, acc, mates, first_over, first_side, next_side, next_over, line, send_sems, sems
):
    z, x, y, c = places()
    rows, width = p_ref.shape
    half, quarter, eighth, sixteenth = width // 2, width // 4, width // 8, width // 16
    strip = rows // 4
    over, side, mate = device(z, 1 - x, y, c), device(z, x, 1 - y, c), device(z, x, y, 1 - c)
    others = [lax.rem(z + d, 4) for d in (1, 2, 3)]
    greet(
        [(over, None), (side, None), (mate, None)] + [(device(zz, x, y, c), None) for zz in others]
    )
    sends = Sends(send_sems)
    base = c * half
    for j in range(2):
        sends.start(
            p_ref.at[:, columns((1 - c) * half + j * quarter, quarter)],
            mates.at[:, columns(j * quarter, quarter)],
            sems.at[j],
            mate,
        )
    kept = (x * eighth + y * sixteenth, quarter + y * eighth + x * sixteenth)
    firsts, nexts = (first_over, first_side), (next_side, next_over)
    for j in range(2):
        part = columns(j * quarter, quarter)
        landed(mates.at[:, part], sems.at[j], mate)
        wide = 16

        def join(i, carry, j=j):
            some = pl.ds(pl.multiple_of(i * wide, wide), wide)
            mine = p_ref[some, columns(base + j * quarter, quarter)].astype(jnp.float32)
            total = mine + mates[some, columns(j * quarter, quarter)].astype(jnp.float32)
            acc[some, columns(j * quarter, quarter)] = total.astype(acc.dtype)
            return carry

        lax.fori_loop(0, rows // wide, join, 0)
        away = (1 - x) * eighth if j == 0 else quarter + (1 - y) * eighth
        sends.start(
            acc.at[:, columns(away, eighth)], firsts[j], sems.at[2 + j], (over, side)[j]
        )
    for j in range(2):
        landed(firsts[j], sems.at[2 + j], mate)
        near = x * eighth if j == 0 else quarter + y * eighth
        add_block(acc.at[:, columns(near, eighth)], [firsts[j]], rows)
        away = near + ((1 - y) if j == 0 else (1 - x)) * sixteenth
        sends.start(
            acc.at[:, columns(away, sixteenth)], nexts[j], sems.at[4 + j], (side, over)[j]
        )
    for j in range(2):
        landed(nexts[j], sems.at[4 + j], mate)
        add_block(acc.at[:, columns(kept[j], sixteenth)], [nexts[j]], rows)
        for d, zz in enumerate(others):
            sends.start(
                acc.at[pl.ds(pl.multiple_of(zz * strip, 16), strip), columns(kept[j], sixteenth)],
                line.at[j, d],
                sems.at[6 + j * 3 + d],
                device(zz, x, y, c),
            )
    strip_here = pl.multiple_of(z * strip, 16)
    for j in range(2):
        for d in range(3):
            landed(line.at[j, d], sems.at[6 + j * 3 + d], mate)
        block = acc.at[:, columns(kept[j], sixteenth)]
        add_block(block, [line.at[j, d] for d in range(3)], strip, strip_here)

        def place(i, carry, j=j):
            some = pl.ds(pl.multiple_of(strip_here + i * 16, 16), 16)
            out_ref[some, columns(base + kept[j], sixteenth)] = acc[
                some, columns(kept[j], sixteenth)
            ]
            return carry

        lax.fori_loop(0, strip // 16, place, 0)
        done = out_ref.at[pl.ds(strip_here, strip), columns(base + kept[j], sixteenth)]
        for d, zz in enumerate(others):
            sends.start(done, done, sems.at[12 + j * 3 + d], device(zz, x, y, c))
    for j in range(2):
        for d in range(3):
            source = pl.multiple_of(lax.rem(z + 3 - d, 4) * strip, 16)
            landed(
                out_ref.at[pl.ds(source, strip), columns(base + kept[j], sixteenth)],
                sems.at[12 + j * 3 + d],
                mate,
            )
        part = out_ref.at[:, columns(base + kept[j], sixteenth)]
        sends.start(part, part, sems.at[18 + j], (side, over)[j])
    others_kept = (
        x * eighth + (1 - y) * sixteenth,
        quarter + y * eighth + (1 - x) * sixteenth,
    )
    for j in range(2):
        landed(out_ref.at[:, columns(base + others_kept[j], sixteenth)], sems.at[18 + j], mate)
        near = x * eighth if j == 0 else quarter + y * eighth
        part = out_ref.at[:, columns(base + near, eighth)]
        sends.start(part, part, sems.at[20 + j], (over, side)[j])
    for j in range(2):
        away = (1 - x) * eighth if j == 0 else quarter + (1 - y) * eighth
        landed(out_ref.at[:, columns(base + away, eighth)], sems.at[20 + j], mate)
        part = out_ref.at[:, columns(base + j * quarter, quarter)]
        sends.start(part, part, sems.at[22 + j], mate)
    for j in range(2):
        landed(
            out_ref.at[:, columns((1 - c) * half + j * quarter, quarter)], sems.at[22 + j], mate
        )
    sends.finish()


def total_over_all(value, number):
    if lax.axis_size("expert") != 8 or lax.axis_size("weight") != 4:
        return lax.psum(value.astype(jnp.float32), ("expert", "weight"))
    rows, width = value.shape
    out = jax.ShapeDtypeStruct(value.shape, value.dtype)
    buffer = lambda n: pltpu.VMEM((rows, n), value.dtype)
    return pl.pallas_call(
        total_kernel,
        out_shape=out,
        in_specs=[pl.BlockSpec(memory_space=pltpu.VMEM)],
        out_specs=pl.BlockSpec(memory_space=pltpu.VMEM),
        scratch_shapes=[
            buffer(width // 2),
            buffer(width // 2),
            buffer(width // 8),
            buffer(width // 8),
            buffer(width // 16),
            buffer(width // 16),
            pltpu.VMEM((2, 3, rows // 4, width // 16), value.dtype),
            pltpu.SemaphoreType.DMA((24,)),
            pltpu.SemaphoreType.DMA((24,)),
        ],
        compiler_params=pltpu.CompilerParams(collective_id=number, has_side_effects=True),
        cost_estimate=cost(0, value, out),
    )(value).astype(jnp.float32)


def shared_kernel(turn, ins, outs):
    normed_ref, cotangent_ref, gate_grad_ref, lift_grad_ref, hidden_ref = ins

    @pl.when(turn == 0)
    def _():
        for out_ref in outs:
            out_ref[...] = jnp.zeros_like(out_ref)

    normed, cotangent = normed_ref[...], cotangent_ref[...]
    outs[0][...] += trans_times(gate_grad_ref[...], normed)
    outs[1][...] += trans_times(lift_grad_ref[...], normed)
    outs[2][...] += trans_times(hidden_ref[...], cotangent)


def weight_kernel(
    rows_ref, grads_ref, gate_grad_ref, lift_grad_ref, hidden_ref, gate_out, up_out, down_out
):
    rows = rows_ref[0]
    gate_out[0] = trans_times(gate_grad_ref[0], rows)
    up_out[0] = trans_times(lift_grad_ref[0], rows)
    down_out[0] = trans_times(hidden_ref[0], grads_ref[0])


def per_device(
    tokens,
    cotangent,
    segments,
    routes,
    first_gain,
    query_weight,
    latent_weight,
    latent_gain,
    expand_weight,
    output_weight,
    second_gain,
    router_weight,
    shared_gate,
    shared_up,
    shared_down,
    expert_gate,
    expert_up,
    expert_down,
):
    weight_count = lax.axis_size("weight")
    token_rows = tokens.shape[0]
    width = tokens.shape[1]
    group_rows = token_rows * weight_count
    query_width = NOPE + ROPE
    heads_here = query_weight.shape[1] // query_width
    expert_count = router_weight.shape[1]
    local_experts = expert_gate.shape[0]
    score_scale = query_width ** (-0.5)
    activations = tokens.astype(jnp.float32)
    first_scale = inv_rms(activations)
    normed = (activations * first_scale * first_gain).astype(jnp.bfloat16)
    both = ("expert", "weight")
    expert_index = lax.axis_index("expert")
    expert_lanes = lax.axis_size("expert")
    blocks = expert_lanes * weight_count
    pairs, quads = blocks // 2, blocks // 4
    pair_rows, quad_rows = 2 * token_rows, 4 * token_rows
    all_rows = blocks * token_rows
    slot_rows = blocks * CAP
    choose = (
        routes[:, :, None] == jnp.arange(expert_count, dtype=jnp.int32)[None, None, :]
    ).astype(jnp.float32)
    hit = jnp.sum(choose, axis=1)
    order = jnp.arange(token_rows, dtype=jnp.int32)
    before = (order[None, :] < order[:, None]).astype(jnp.bfloat16)
    place = matmul(before, hit.astype(jnp.bfloat16))
    rank = jnp.sum(choose * jnp.arange(routes.shape[1], dtype=jnp.float32)[None, :, None], axis=1)
    code = jnp.where(hit > 0, 32.0 * rank + place, -1.0)
    extra = jnp.pad(code, ((0, 0), (0, lanes - expert_count)), constant_values=-1.0)
    cotangent_wide = jnp.concatenate([cotangent, extra.astype(jnp.bfloat16)], axis=1)
    column = jnp.arange(lanes, dtype=jnp.int32)[None, :]
    row = jnp.arange(8, dtype=jnp.int32)[:, None]
    first_here = expert_index * local_experts
    here = (row < local_experts) & (column == first_here + row)
    twice = here | ((row < local_experts) & (column == first_here + row + expert_count))
    here, twice = here.astype(jnp.bfloat16), twice.astype(jnp.bfloat16)
    weight_index = lax.axis_index("weight")
    high_column = 2 * (row * weight_count + weight_index)
    known = row < routes.shape[1]
    high_at = (known & (column == high_column)).astype(jnp.bfloat16)
    low_at = (known & (column == high_column + 1)).astype(jnp.bfloat16)
    shared_here = shared_gate.shape[1] // expert_lanes
    shared_wide = -(-shared_here // lanes) * lanes
    start = expert_index * shared_here

    def shared_part(matrix):
        part = lax.dynamic_slice_in_dim(matrix, start, shared_here, axis=0)
        return jnp.pad(part, ((0, shared_wide - shared_here), (0, 0)))

    gate_part = shared_part(shared_gate.T)
    up_part = shared_part(shared_up.T)
    down_part = shared_part(shared_down)
    shape = jax.ShapeDtypeStruct
    whole = lambda array: (array, whole_spec(array))
    slots = shape((local_experts, slot_rows, width), jnp.bfloat16)
    slots_one = shape((local_experts, slot_rows, lanes), jnp.float32)
    gather_flops = 2 * all_rows * width * (2 * CAP * local_experts + shared_wide)
    cosine, sine = rope_tables(segments[0])
    allowed = attention_mask(segments[0])
    sizes = (expert_lanes, weight_count)
    if sizes == (8, 4):
        (
            cotangent_all,
            normed_all,
            query,
            latent,
            latent_scale,
            latent_normed,
            key_rope,
            expanded,
            log_total,
            mixed,
            attended,
        ) = attention_forward(
            score_scale,
            normed,
            cotangent_wide,
            cosine,
            sine,
            segments[0],
            latent_gain,
            query_weight,
            latent_weight,
            expand_weight,
            output_weight,
            0,
        )
        cotangent_all = cotangent_all.reshape(all_rows, -1)
        normed_all = normed_all.reshape(group_rows, width)
        latent_scale, log_total = latent_scale[:, :1], log_total[:, :, :1]
        query = query.transpose(1, 0, 2)
        expanded = expanded.reshape(group_rows, heads_here, NOPE + VDIM)
    else:
        cotangent_all = lax.all_gather(cotangent_wide, both, axis=0, tiled=True)
        normed_all = gather_group(normed, 0)
        query_full = matmul(normed_all, query_weight).reshape(group_rows, heads_here, query_width)
        query = jnp.concatenate(
            [
                query_full[..., :NOPE],
                rotate(query_full[..., NOPE:], cosine[:, None, :], sine[:, None, :]),
            ],
            axis=-1,
        ).astype(jnp.bfloat16)
        compressed = matmul(normed_all, latent_weight)
        latent = compressed[:, :LATENT]
        latent_scale = inv_rms(latent)
        latent_normed = (latent * latent_scale * latent_gain).astype(jnp.bfloat16)
        key_rope = rotate(compressed[:, LATENT:], cosine, sine).astype(jnp.bfloat16)
        expanded = (
            matmul(latent_normed, expand_weight)
            .astype(jnp.bfloat16)
            .reshape(group_rows, heads_here, NOPE + VDIM)
        )
    key_nope = expanded[..., :NOPE]
    values = expanded[..., NOPE:]

    def score_block():
        raw = jnp.einsum(
            "ihd,jhd->hij", query[..., :NOPE], key_nope, preferred_element_type=jnp.float32
        )
        raw = raw + jnp.einsum(
            "ihd,jd->hij", query[..., NOPE:], key_rope, preferred_element_type=jnp.float32
        )
        return jnp.where(allowed[None], raw * score_scale, -1e30)

    if sizes != (8, 4):
        scores = score_block()
        peak = jnp.max(scores, axis=-1, keepdims=True)
        weights = jnp.exp(scores - peak)
        total = jnp.sum(weights, axis=-1, keepdims=True)
        log_total = peak + jnp.log(total)
        mixed = jnp.einsum(
            "hij,jhd->ihd",
            (weights / total).astype(jnp.bfloat16),
            values,
            preferred_element_type=jnp.float32,
        )
        mixed = mixed.astype(jnp.bfloat16).reshape(group_rows, heads_here * VDIM)
        attended = sum_group(matmul(mixed, output_weight).astype(jnp.bfloat16), 1)
    hidden_one = activations + attended
    second_scale = inv_rms(hidden_one)
    normed_two = (hidden_one * second_scale * second_gain).astype(jnp.bfloat16)
    gates = jax.nn.sigmoid(matmul(normed_two, router_weight))
    chosen = jnp.sum(choose * gates[:, None, :], axis=-1)
    chosen_total = jnp.sum(chosen, axis=1, keepdims=True)
    mixing = route_scale * chosen / chosen_total
    upstream = cotangent.astype(jnp.float32)
    mixing_at = jnp.sum(choose * mixing[:, :, None], axis=1)
    mixing_high = mixing_at.astype(jnp.bfloat16)
    mixing_low = (mixing_at - mixing_high.astype(jnp.float32)).astype(jnp.bfloat16)
    normed_wide = jnp.concatenate([normed_two, mixing_high, mixing_low], axis=1)
    marks = (cotangent_all, pl.BlockSpec((quad_rows, lanes), lambda i: (i, width // lanes)))
    normed_tokens, (grads_slots, shared_raw) = gather_all(
        normed_wide,
        2,
        functools.partial(grads_kernel, pair_rows),
        quads,
        [whole(here), (cotangent_all, pair_spec(cotangent_all, quads)), whole(down_part)],
        [
            (slots, slots_spec(slots, quads)),
            (shape((all_rows, shared_wide), jnp.float32), pl.BlockSpec((quad_rows, shared_wide), lambda i: (i, 0))),
        ],
        gather_flops,
    )
    normed_tokens = normed_tokens.reshape(all_rows, -1)
    token_spec = pl.BlockSpec((quad_rows, shared_wide), lambda i: (i, 0))
    token_shape = shape((all_rows, shared_wide), jnp.bfloat16)
    rows_slots, mix_slots, shared_hidden, shared_gate_grad, shared_lift_grad = call(
        functools.partial(rows_kernel, pair_rows),
        quads,
        [
            whole(here),
            whole(twice),
            marks,
            (normed_tokens, pair_spec(normed_tokens, quads)),
            (shared_raw, token_spec),
            whole(gate_part),
            whole(up_part),
        ],
        [
            (slots, slots_spec(slots, quads)),
            (slots_one, slots_spec(slots_one, quads)),
            (token_shape, token_spec),
            (token_shape, token_spec),
            (token_shape, token_spec),
        ],
        gather_flops + 2 * all_rows * width * shared_wide,
    )
    hidden_here = expert_gate.shape[2]
    gate_rows, up_rows = expert_gate.transpose(0, 2, 1), expert_up.transpose(0, 2, 1)

    def tile_spec(rows, n):
        per = slot_rows // rows
        return pl.BlockSpec((1, rows, n), lambda i: (i // per, i % per, 0))

    def expert_spec(rows, matrix):
        per = slot_rows // rows
        return pl.BlockSpec((1,) + matrix.shape[1:], lambda i: (i // per, 0, 0))

    large, small = 32 * CAP, 16 * CAP
    narrow = shape((local_experts, slot_rows, hidden_here), jnp.bfloat16)
    one_matmul = 2 * local_experts * slot_rows * width * hidden_here
    routed_hidden, mixed_hidden, slope, active, produced = call(
        forward_kernel,
        local_experts * (slot_rows // large),
        [
            (rows_slots, tile_spec(large, width)),
            (mix_slots, tile_spec(large, lanes)),
            (gate_rows, expert_spec(large, gate_rows)),
            (up_rows, expert_spec(large, up_rows)),
            (expert_down, expert_spec(large, expert_down)),
        ],
        [(narrow, tile_spec(large, hidden_here))] * 4 + [(slots, tile_spec(large, width))],
        3 * one_matmul,
    )
    dense = shape((all_rows, width), jnp.bfloat16)
    dense_wide = shape((all_rows, width + lanes), jnp.bfloat16)
    (out_dense,) = call(
        functools.partial(out_kernel, pair_rows),
        quads,
        [
            whole(here),
            marks,
            (produced, slots_spec(slots, quads)),
            (shared_hidden, token_spec),
            whole(down_part),
        ],
        [(dense, pair_spec(dense, quads))],
        gather_flops,
    )
    narrow_tile = tile_spec(small, hidden_here)
    routed_out, (gate_grad, lift_grad, returned, mix_grad_slots) = sum_all(
        out_dense.reshape(blocks, token_rows, width),
        6,
        backward_kernel,
        local_experts * (slot_rows // small),
        [
            (grads_slots, tile_spec(small, width)),
            (routed_hidden, narrow_tile),
            (slope, narrow_tile),
            (active, narrow_tile),
            (gate_rows, expert_spec(small, gate_rows)),
            (up_rows, expert_spec(small, up_rows)),
            (expert_down, expert_spec(small, expert_down)),
        ],
        [
            (narrow, narrow_tile),
            (narrow, narrow_tile),
            (slots, tile_spec(small, width)),
            (slots_one, tile_spec(small, lanes)),
        ],
        3 * one_matmul,
    )
    (back_dense,) = call(
        functools.partial(back_kernel, pair_rows),
        quads,
        [
            whole(here),
            whole(high_at),
            whole(low_at),
            marks,
            (returned, slots_spec(slots, quads)),
            (mix_grad_slots, slots_spec(slots_one, quads)),
            (shared_gate_grad, token_spec),
            (shared_lift_grad, token_spec),
            whole(gate_part),
            whole(up_part),
        ],
        [(dense_wide, pair_spec(dense_wide, quads))],
        gather_flops + 2 * all_rows * width * shared_wide,
    )
    shared_sum = shape((shared_wide, width), jnp.float32)
    shared_out = (shared_sum, whole_spec(shared_sum))
    plain_spec = pl.BlockSpec((pair_rows, width), lambda i: (i, 0))
    shared_spec = pl.BlockSpec((pair_rows, shared_wide), lambda i: (i, 0))
    back_here, shared_sums = sum_all(
        back_dense.reshape(blocks, token_rows, -1),
        3,
        shared_kernel,
        pairs,
        [
            (normed_tokens, plain_spec),
            (cotangent_all, plain_spec),
            (shared_gate_grad, shared_spec),
            (shared_lift_grad, shared_spec),
            (shared_hidden, shared_spec),
        ],
        [shared_out] * 3,
        6 * all_rows * width * shared_wide,
    )
    routed_back = back_here[:, :width]
    mix_grad = back_here[:, width : width + 2 * weight_count * routes.shape[1]]
    mix_grad = jnp.sum(mix_grad.reshape(token_rows, routes.shape[1], -1), axis=2)
    shared_grads = jnp.concatenate([total[:shared_here] for total in shared_sums], axis=0)
    shared_grads = shared_grads.astype(jnp.bfloat16)
    swapped = lax.all_to_all(shared_grads, "expert", split_axis=1, concat_axis=0, tiled=True)
    swapped = swapped.reshape(expert_lanes, 3, shared_here, -1).astype(jnp.float32)
    shared_gradients = [swapped[:, i].reshape(expert_lanes * shared_here, -1) for i in range(3)]
    chosen_grad = route_scale * (
        mix_grad / chosen_total
        - jnp.sum(mix_grad * chosen, axis=1, keepdims=True) / chosen_total**2
    )
    logit_grad = jnp.sum(choose * chosen_grad[:, :, None], axis=1) * gates * (1.0 - gates)
    normed_two_grad = (
        routed_back
        + jnp.dot(logit_grad, router_weight.astype(jnp.float32).T, precision=highest)
    )
    router_gradient = jnp.dot(logit_grad.T, normed_two.astype(jnp.float32), precision=highest)
    back_two, second_gain_gradient = norm_back(
        normed_two_grad, hidden_one, second_scale, second_gain
    )
    hidden_grad = upstream + back_two
    hidden_group = gather_group(hidden_grad.astype(jnp.bfloat16), 4)
    output_gradient = trans_times(mixed, hidden_group).astype(jnp.bfloat16)
    hidden_group, output_gradient = lax.optimization_barrier((hidden_group, output_gradient))
    mixed_grad = (
        times_trans(hidden_group, output_weight)
        .astype(jnp.bfloat16)
        .reshape(group_rows, heads_here, VDIM)
    )
    probs = jnp.exp(score_block() - log_total)
    prob_grad = jnp.einsum("ihd,jhd->hij", mixed_grad, values, preferred_element_type=jnp.float32)
    centre = jnp.sum(probs * prob_grad, axis=-1, keepdims=True)
    score_grad = (probs * (prob_grad - centre)).astype(jnp.bfloat16)
    value_grad = jnp.einsum(
        "hij,ihd->jhd", probs.astype(jnp.bfloat16), mixed_grad, preferred_element_type=jnp.float32
    )
    query_nope_grad = (
        jnp.einsum("hij,jhd->ihd", score_grad, key_nope, preferred_element_type=jnp.float32)
        * score_scale
    )
    query_rope_grad = (
        jnp.einsum("hij,jd->ihd", score_grad, key_rope, preferred_element_type=jnp.float32)
        * score_scale
    )
    key_nope_grad = (
        jnp.einsum(
            "hij,ihd->jhd", score_grad, query[..., :NOPE], preferred_element_type=jnp.float32
        )
        * score_scale
    )
    key_rope_grad = (
        jnp.einsum("hij,ihd->jd", score_grad, query[..., NOPE:], preferred_element_type=jnp.float32)
        * score_scale
    )
    query_grad = jnp.concatenate(
        [query_nope_grad, unrotate(query_rope_grad, cosine[:, None, :], sine[:, None, :])], axis=-1
    )
    query_grad = query_grad.astype(jnp.bfloat16).reshape(group_rows, heads_here * query_width)
    expand_grad = (
        jnp.concatenate([key_nope_grad, value_grad], axis=-1)
        .astype(jnp.bfloat16)
        .reshape(group_rows, heads_here * (NOPE + VDIM))
    )
    column_half = width // 2
    half_spec = lambda m: pl.BlockSpec((1, m, column_half), lambda i: (i // 2, 0, i % 2))
    narrow_spec = pl.BlockSpec((1, slot_rows, hidden_here), lambda i: (i // 2, 0, 0))
    weight_shape = shape((local_experts, hidden_here, width), jnp.float32)
    weight_grads = call(
        weight_kernel,
        2 * local_experts,
        [
            (rows_slots, half_spec(slot_rows)),
            (grads_slots, half_spec(slot_rows)),
            (gate_grad, narrow_spec),
            (lift_grad, narrow_spec),
            (mixed_hidden, narrow_spec),
        ],
        [(weight_shape, half_spec(hidden_here))] * 3,
        3 * one_matmul,
    )
    expert_grads = (weight_grads[0].transpose(0, 2, 1), weight_grads[1].transpose(0, 2, 1), weight_grads[2])
    layer_out = (hidden_one + routed_out).astype(jnp.bfloat16)
    query_gradient = trans_times(normed_all, query_grad)
    expand_gradient = trans_times(latent_normed, expand_grad)
    latent_normed_grad = times_trans(expand_grad, expand_weight)
    latent_back, latent_gain_gradient = norm_back(
        latent_normed_grad, latent, latent_scale, latent_gain
    )
    compressed_grad = jnp.concatenate([latent_back, unrotate(key_rope_grad, cosine, sine)], axis=-1)
    compressed_grad = compressed_grad.astype(jnp.bfloat16)
    latent_weight_gradient = trans_times(compressed_grad, normed_all)
    normed_grad = sum_group(
        (
            times_trans(query_grad, query_weight) + times_trans(compressed_grad, latent_weight)
        ).astype(jnp.bfloat16),
        5,
    )
    back_one, first_gain_gradient = norm_back(normed_grad, activations, first_scale, first_gain)
    token_gradient = hidden_grad + back_one
    shards = (
        lax.psum_scatter(
            query_gradient.astype(jnp.bfloat16), "expert", scatter_dimension=0, tiled=True
        ).astype(jnp.float32),
        lax.psum_scatter(
            expand_gradient.astype(jnp.bfloat16), "expert", scatter_dimension=0, tiled=True
        ).astype(jnp.float32),
        lax.psum_scatter(
            output_gradient, "expert", scatter_dimension=1, tiled=True
        ).astype(jnp.float32),
    )
    latent_columns = latent_weight.shape[1]
    filled = jnp.concatenate(
        [
            latent_weight_gradient,
            router_gradient,
            first_gain_gradient[None],
            second_gain_gradient[None],
            jnp.pad(latent_gain_gradient, (0, width - LATENT))[None],
        ],
        axis=0,
    ).astype(jnp.bfloat16)
    wanted = -(-filled.shape[0] // 64) * 64
    filled = jnp.pad(filled, ((0, wanted - filled.shape[0]), (0, 0)))
    total = total_over_all(filled, 7)
    gains_at = latent_columns + expert_count
    totals = (
        total[:latent_columns].T,
        total[gains_at + 2, :LATENT],
        total[latent_columns:gains_at].T,
        total[gains_at],
        total[gains_at + 1],
    )
    return (
        layer_out,
        token_gradient,
        totals[3],
        shards[0],
        totals[0],
        totals[1],
        shards[1],
        shards[2],
        totals[4],
        totals[2],
        shared_gradients[0].T,
        shared_gradients[1].T,
        shared_gradients[2],
        expert_grads[0],
        expert_grads[1],
        expert_grads[2],
    )


def solution(mesh):
    return jax.shard_map(
        per_device,
        mesh=mesh,
        in_specs=(
            P(("expert", "weight"), None),
            P(("expert", "weight"), None),
            P("expert", None),
            P(("expert", "weight"), None),
            P(),
            P(None, "weight"),
            P(),
            P(),
            P(None, "weight"),
            P("weight", None),
            P(),
            P(),
            P(None, "weight"),
            P(None, "weight"),
            P("weight", None),
            P("expert", None, "weight"),
            P("expert", None, "weight"),
            P("expert", "weight", None),
        ),
        out_specs=(
            P(("expert", "weight"), None),
            P(("expert", "weight"), None),
            P(),
            P("expert", "weight"),
            P(),
            P(),
            P("expert", "weight"),
            P("weight", "expert"),
            P(),
            P(),
            P("expert", "weight"),
            P("expert", "weight"),
            P("weight", "expert"),
            P("expert", None, "weight"),
            P("expert", None, "weight"),
            P("expert", "weight", None),
        ),
        check_vma=False,
    )
```

```python
import functools

import jax
import jax.numpy as jnp
from jax import lax
from jax.experimental import pallas as pl
from jax.experimental.pallas import tpu as pltpu
from jax.sharding import PartitionSpec as P

NOPE = 128
ROPE = 64
VDIM = 128
LATENT = 512
TOPK = 6
CAP = 20


eps = 1e-06
route_scale = 2.446
rope_base = 50000.0
highest = lax.Precision.HIGHEST


def matmul(left, right):
    return jnp.dot(left, right, preferred_element_type=jnp.float32)


def trans_times(left, right):
    return lax.dot_general(
        left, right, (((0,), (0,)), ((), ())), preferred_element_type=jnp.float32
    )


def times_trans(left, right):
    return lax.dot_general(
        left, right, (((1,), (1,)), ((), ())), preferred_element_type=jnp.float32
    )


def inv_rms(value):
    return lax.rsqrt(jnp.mean(value * value, axis=-1, keepdims=True) + eps)


def norm_back(grad_out, value, scale, gain):
    scaled = grad_out * gain
    grad_in = scale * scaled - value * scale**3 * jnp.mean(scaled * value, axis=-1, keepdims=True)
    gain_grad = jnp.sum(grad_out * value * scale, axis=0)
    return (grad_in, gain_grad)


def rope_tables(seg):
    size = seg.shape[0]
    index = jnp.arange(size, dtype=jnp.int32)
    fresh = jnp.concatenate([jnp.ones((1,), dtype=bool), seg[1:] != seg[:-1]])
    first = lax.cummax(jnp.where(fresh, index, jnp.zeros_like(index)), axis=0)
    place = (index - first).astype(jnp.float32)
    half = ROPE // 2
    freqs = rope_base ** (-(jnp.arange(half, dtype=jnp.float32) * 2.0 / ROPE))
    angle = place[:, None] * freqs[None, :]
    return (jnp.cos(angle), jnp.sin(angle))


def attention_mask(seg):
    index = jnp.arange(seg.shape[0], dtype=jnp.int32)
    return (seg[:, None] == seg[None, :]) & (index[None, :] <= index[:, None])


def rotate(value, cosine, sine):
    half = value.shape[-1] // 2
    first, second = (value[..., :half], value[..., half:])
    return jnp.concatenate(
        [first * cosine - second * sine, second * cosine + first * sine], axis=-1
    )


def unrotate(value, cosine, sine):
    half = value.shape[-1] // 2
    first, second = (value[..., :half], value[..., half:])
    return jnp.concatenate(
        [first * cosine + second * sine, second * cosine - first * sine], axis=-1
    )


lanes = 128
vmem_limit = 64 * 1024 * 1024 - 131072


def token_slots(marks, here, local_experts, half):
    codes = times_trans(here, marks)
    count = codes.shape[1]
    rank = jnp.floor(codes * (1.0 / 32.0))
    place = codes - 32.0 * rank
    token = lax.broadcasted_iota(jnp.int32, codes.shape, 1)
    slot = jnp.where(codes >= 0, place + jnp.where(token >= half, float(CAP), 0.0), -1.0)
    row = lax.broadcasted_iota(jnp.int32, (2 * CAP, count), 0).astype(jnp.float32)
    picks = [jnp.where(row == slot[e : e + 1], 1.0, 0.0) for e in range(local_experts)]
    return picks, rank


def pair_slots(marks_ref, here_ref, local_experts, pair):
    count = marks_ref.shape[0] // pair
    return [
        token_slots(marks_ref[j * pair : (j + 1) * pair], here_ref[...], local_experts, pair // 2)
        for j in range(count)
    ]


def slot_part(value, e):
    return value[e * 2 * CAP : (e + 1) * 2 * CAP]


def gather_rows(slots, values, pair, out_ref):
    rows = [
        jnp.dot(
            jnp.concatenate(picks, axis=0).astype(jnp.bfloat16),
            values[j * pair : (j + 1) * pair],
            preferred_element_type=jnp.float32,
        )
        for j, (picks, _) in enumerate(slots)
    ]
    for e in range(out_ref.shape[0]):
        together = jnp.concatenate([slot_part(value, e) for value in rows], axis=0)
        out_ref[e] = together.astype(jnp.bfloat16)


def spread_rows(slots, rows_ref):
    local_experts = rows_ref.shape[0]
    rows = [rows_ref[e].astype(jnp.float32) for e in range(local_experts)]
    totals = []
    for j, (picks, _) in enumerate(slots):
        part = jnp.concatenate([slot_part(value, j) for value in rows], axis=0)
        pick = jnp.concatenate(picks, axis=0).astype(jnp.bfloat16)
        totals.append(trans_times(pick, part.astype(jnp.bfloat16)))
    return jnp.concatenate(totals, axis=0)


def grads_kernel(pair, turn, ins, outs):
    here_ref, value_ref, down_ref = ins
    rows_ref, back_ref = outs
    width = rows_ref.shape[2]
    slots = pair_slots(value_ref.at[:, width:], here_ref, rows_ref.shape[0], pair)
    values = value_ref[:, :width]
    gather_rows(slots, values, pair, rows_ref)
    back_ref[...] = times_trans(values, down_ref[...])


def rows_kernel(
    pair,
    here_ref,
    twice_ref,
    marks_ref,
    value_ref,
    back_ref,
    gate_ref,
    up_ref,
    rows_ref,
    mix_ref,
    hidden_ref,
    gate_grad_ref,
    lift_grad_ref,
):
    width = rows_ref.shape[2]
    slots = pair_slots(marks_ref, here_ref, rows_ref.shape[0], pair)
    values = value_ref[:, :width]
    gather_rows(slots, values, pair, rows_ref)
    for j, (picks, _) in enumerate(slots):
        mixing = times_trans(twice_ref[...], value_ref[j * pair : (j + 1) * pair, width:])
        for e, pick in enumerate(picks):
            column = jnp.sum(pick * mixing[e : e + 1], axis=1, keepdims=True)
            column = jnp.broadcast_to(column, (2 * CAP, lanes))
            mix_ref[e, j * 2 * CAP : (j + 1) * 2 * CAP] = column
    gate = times_trans(values, gate_ref[...])
    lift = times_trans(values, up_ref[...])
    back = back_ref[...]
    sigma = jax.nn.sigmoid(gate)
    active = gate * sigma
    hidden_ref[...] = (active * lift).astype(jnp.bfloat16)
    gate_grad_ref[...] = (back * lift * sigma * (1.0 + gate * (1.0 - sigma))).astype(jnp.bfloat16)
    lift_grad_ref[...] = (back * active).astype(jnp.bfloat16)


def forward_kernel(
    rows_ref,
    mix_ref,
    gate_ref,
    up_ref,
    down_ref,
    hidden_ref,
    mixed_ref,
    slope_ref,
    active_ref,
    produced_ref,
):
    rows = rows_ref[0]
    gate = times_trans(rows, gate_ref[0])
    lift = times_trans(rows, up_ref[0])
    mix = mix_ref[0][:, :1]
    sigma = jax.nn.sigmoid(gate)
    active = gate * sigma
    hidden = active * lift
    mixed_hidden = (mix * hidden).astype(jnp.bfloat16)
    hidden_ref[0] = hidden.astype(jnp.bfloat16)
    mixed_ref[0] = mixed_hidden
    slope_ref[0] = (mix * lift * sigma * (1.0 + gate * (1.0 - sigma))).astype(jnp.bfloat16)
    active_ref[0] = (mix * active).astype(jnp.bfloat16)
    produced_ref[0] = matmul(mixed_hidden, down_ref[0]).astype(jnp.bfloat16)


def backward_kernel(turn, ins, outs):
    grads_ref, hidden_ref, slope_ref, active_ref, gate_ref, up_ref, down_ref = ins
    gate_grad_ref, lift_grad_ref, returned_ref, mix_grad_ref = outs
    back = times_trans(grads_ref[0], down_ref[0])
    mix_grad = jnp.sum(hidden_ref[0].astype(jnp.float32) * back, axis=1, keepdims=True)
    mix_grad_ref[0] = jnp.broadcast_to(mix_grad, mix_grad_ref.shape[1:])
    gate_grad = (back * slope_ref[0].astype(jnp.float32)).astype(jnp.bfloat16)
    lift_grad = (back * active_ref[0].astype(jnp.float32)).astype(jnp.bfloat16)
    gate_grad_ref[0] = gate_grad
    lift_grad_ref[0] = lift_grad
    returned = matmul(gate_grad, gate_ref[0]) + matmul(lift_grad, up_ref[0])
    returned_ref[0] = returned.astype(jnp.bfloat16)


def back_kernel(
    pair,
    here_ref,
    high_ref,
    low_ref,
    marks_ref,
    rows_ref,
    mix_grad_ref,
    gate_grad_ref,
    lift_grad_ref,
    gate_ref,
    up_ref,
    out_ref,
):
    width = rows_ref.shape[2]
    slots = pair_slots(marks_ref, here_ref, rows_ref.shape[0], pair)
    total = spread_rows(slots, rows_ref)
    total = total + matmul(gate_grad_ref[...], gate_ref[...])
    total = total + matmul(lift_grad_ref[...], up_ref[...])
    out_ref[:, :width] = total.astype(jnp.bfloat16)
    for j, (picks, rank) in enumerate(slots):
        choice = lax.broadcasted_iota(jnp.int32, rank.shape, 0).astype(jnp.float32)
        mix_grad = jnp.zeros(rank.shape, jnp.float32)
        for e, pick in enumerate(picks):
            column = slot_part(mix_grad_ref[e], j)[:, :1]
            row = jnp.sum(pick * column, axis=0, keepdims=True)
            mix_grad = mix_grad + jnp.where(choice == rank[e : e + 1], row, 0.0)
        high = mix_grad.astype(jnp.bfloat16)
        low = (mix_grad - high.astype(jnp.float32)).astype(jnp.bfloat16)
        sent = trans_times(high, high_ref[...]) + trans_times(low, low_ref[...])
        out_ref[j * pair : (j + 1) * pair, width:] = sent.astype(jnp.bfloat16)


def out_kernel(pair, here_ref, marks_ref, rows_ref, hidden_ref, down_ref, out_ref):
    slots = pair_slots(marks_ref, here_ref, rows_ref.shape[0], pair)
    total = spread_rows(slots, rows_ref)
    total = total + matmul(hidden_ref[...], down_ref[...])
    out_ref[...] = total.astype(jnp.bfloat16)


def whole_spec(array):
    zeros = (0,) * array.ndim
    return pl.BlockSpec(array.shape, lambda i: zeros)


def pair_spec(array, pairs):
    block = (array.shape[0] // pairs,) + array.shape[1:]
    zeros = (0,) * (array.ndim - 1)
    return pl.BlockSpec(block, lambda i: (i,) + zeros)


def slots_spec(array, pairs):
    block = (array.shape[0], array.shape[1] // pairs) + array.shape[2:]
    return pl.BlockSpec(block, lambda i: (0, i, 0))


def cost(flops, *arrays):
    moved = sum(a.size * a.dtype.itemsize for a in arrays)
    return pl.CostEstimate(flops=int(flops), bytes_accessed=int(moved), transcendentals=0)


def call(kernel, grid, ins, outs, flops):
    arrays = [a for a, _ in ins]
    shapes = [s for s, _ in outs]
    return pl.pallas_call(
        kernel,
        grid=(grid,),
        in_specs=[s for _, s in ins],
        out_specs=[s for _, s in outs],
        out_shape=shapes,
        cost_estimate=cost(flops, *arrays, *shapes),
        compiler_params=pltpu.CompilerParams(vmem_limit_bytes=vmem_limit),
    )(*arrays)


MESH = pl.DeviceIdType.MESH


def places():
    expert, weight = lax.axis_index("expert"), lax.axis_index("weight")
    return lax.div(expert, 2), lax.rem(expert, 2), lax.div(weight, 2), lax.rem(weight, 2)


def device(z, x, y, c):
    return (z * 2 + x, y * 2 + c)


def shard(z, x, y, c):
    return z * 8 + x * 4 + y * 2 + c


def push(source, target, send, receive, to):
    return pltpu.make_async_remote_copy(
        src_ref=source,
        dst_ref=target,
        send_sem=send,
        recv_sem=receive,
        device_id=to,
        device_id_type=MESH,
    )


class Sends:
    def __init__(self, semaphores):
        self.semaphores = semaphores
        self.started = []

    def plan(self, source, target, receive, to, when=None):
        copy = push(source, target, self.semaphores.at[len(self.started)], receive, to)
        self.started.append((copy, when))
        return copy

    def start(self, source, target, receive, to, when=None):
        copy = self.plan(source, target, receive, to, when)
        if when is None:
            copy.start()
        else:
            pl.when(when)(copy.start)

    def finish(self):
        for copy, when in self.started:
            if when is None:
                copy.wait_send()
            else:
                pl.when(when)(copy.wait_send)


def landed(target, receive, to):
    push(target, target, receive, receive, to).wait_recv()


def greet(devices):
    barrier = pltpu.get_barrier_semaphore()
    count = 0
    for to, when in devices:
        signal = functools.partial(
            pl.semaphore_signal, barrier, inc=1, device_id=to, device_id_type=MESH
        )
        if when is None:
            signal()
            count = count + 1
        else:
            pl.when(when)(signal)
            count = count + when.astype(jnp.int32)
    pl.semaphore_wait(barrier, count)


def add_rows(target, sources, start, rows):
    step = 16

    def body(i, carry):
        part = pl.ds(pl.multiple_of(start + i * step, step), step)
        total = target[part].astype(jnp.float32)
        for source, offset in sources:
            there = pl.ds(pl.multiple_of(start - offset + i * step, step), step)
            total = total + source[there].astype(jnp.float32)
        target[part] = total.astype(target.dtype)
        return carry

    lax.fori_loop(0, rows // step, body, 0)


def ordered(z, first, second):
    upper = lax.div(z, 2)
    inner = z + upper * (3 - 2 * z)
    value = first + inner * (second - first)
    return value + upper * (3 - 2 * value)


class Gather:
    def __init__(self, x_ref, out_ref, sends, recv_sems, local_sem, place, cut=None):
        z, x, y, c = place
        rows = x_ref.shape[0]
        cut = rows // 2 if cut is None else cut
        self.parts = [pl.ds(0, cut), pl.ds(cut, rows - cut)]
        over, side, mate = device(z, 1 - x, y, c), device(z, x, 1 - y, c), device(z, x, y, 1 - c)
        up, down = device(z + 1, x, y, c), device(z - 1, x, y, c)
        self.out_ref, self.recv_sems, self.mate = out_ref, recv_sems, mate
        planes = [ordered(z, (0, 1, 2, 3)[step], (1, 0, 2, 3)[step]) for step in range(4)]
        self.rising = [(zz <= z) & (z < 3) for zz in planes]
        self.falling = [(zz >= z) & (z > 0) for zz in planes]
        self.mine = [shard(zz, x, y, c) for zz in planes]
        self.overs = [shard(zz, 1 - x, y, c) for zz in planes]
        self.sides = [shard(zz, x, 1 - y, c) for zz in planes]
        self.corners = [shard(zz, 1 - x, 1 - y, c) for zz in planes]
        self.mates = [
            (shard(zz, x, y, 1 - c), shard(zz, 1 - x, y, 1 - c), shard(zz, x, 1 - y, 1 - c))
            for zz in planes
        ]
        self.mate_corners = [shard(zz, 1 - x, 1 - y, 1 - c) for zz in planes]
        self.keep = pltpu.make_async_copy(x_ref, out_ref.at[self.mine[0]], local_sem)
        self.whole_copies, self.relay_copies, self.corner_copies = [], [], []

        def copy(ref, receive, to, when=None, source=None):
            return sends.plan(ref if source is None else source, ref, receive, to, when)

        for step in range(4):
            i = self.mine[step]
            source = x_ref if step == 0 else None
            there, receive = out_ref.at[i], recv_sems.at[i, 0]
            self.whole_copies.append(
                [
                    (copy(there, receive, up, self.rising[step], source), self.rising[step]),
                    (copy(there, receive, down, self.falling[step], source), self.falling[step]),
                    (copy(there, receive, over, None, source), None),
                    (copy(there, receive, side, None, source), None),
                    (copy(there, receive, mate, None, source), None),
                ]
            )
            i, j = self.overs[step], self.sides[step]
            self.relay_copies.append(
                [
                    copy(self.halves(i, 0), recv_sems.at[i, 0], side),
                    copy(out_ref.at[i], recv_sems.at[i, 0], mate),
                    copy(self.halves(j, 1), recv_sems.at[j, 1], over),
                    copy(out_ref.at[j], recv_sems.at[j, 0], mate),
                ]
            )
            i = self.corners[step]
            self.corner_copies.append(
                [copy(self.halves(i, h), recv_sems.at[i, h], mate) for h in range(2)]
            )

    def halves(self, i, h):
        return self.out_ref.at[i, self.parts[h]]

    def full_here(self, i):
        landed(self.out_ref.at[i], self.recv_sems.at[i, 0], self.mate)

    def half_here(self, i, h):
        landed(self.halves(i, h), self.recv_sems.at[i, h], self.mate)

    def whole(self, step):
        if step == 0:
            self.keep.start()
        else:
            self.full_here(self.mine[step])
        for copy, when in self.whole_copies[step]:
            if when is None:
                copy.start()
            else:
                pl.when(when)(copy.start)

    def relay(self, step):
        self.full_here(self.overs[step])
        self.relay_copies[step][0].start()
        self.relay_copies[step][1].start()
        self.full_here(self.sides[step])
        self.relay_copies[step][2].start()
        self.relay_copies[step][3].start()

    def corner(self, step):
        for h in range(2):
            self.half_here(self.corners[step], h)
            self.corner_copies[step][h].start()

    def last(self):
        for step in range(4):
            for i in self.mates[step]:
                self.full_here(i)
            for h in range(2):
                self.half_here(self.mate_corners[step], h)
        self.keep.wait()


def gather_neighbours(place):
    z, x, y, c = place
    return [
        (device(z, 1 - x, y, c), None),
        (device(z, x, 1 - y, c), None),
        (device(z, x, y, 1 - c), None),
        (device(z + 1, x, y, c), z < 3),
        (device(z - 1, x, y, c), z > 0),
    ]


def gather_all_kernel(inner, cover_ins, cover_outs, x_ref, *refs):
    ins, refs = refs[:cover_ins], refs[cover_ins:]
    out_ref, refs = refs[0], refs[1:]
    outs, refs = refs[:cover_outs], refs[cover_outs:]
    send_sems, recv_sems, local_sem = refs
    turn, turns = pl.program_id(0), pl.num_programs(0)
    place = places()
    sends = Sends(send_sems)
    gather = Gather(x_ref, out_ref, sends, recv_sems, local_sem, place)

    def begin():
        greet(gather_neighbours(place))
        gather.whole(0)

    def end():
        gather.whole(3)
        gather.relay(2)
        gather.corner(1)
        gather.relay(3)
        gather.corner(2)
        gather.corner(3)
        gather.last()
        sends.finish()

    def early():
        gather.relay(1)
        gather.corner(0)

    pieces = [
        begin,
        lambda: None,
        functools.partial(gather.whole, 1),
        functools.partial(gather.relay, 0),
        functools.partial(gather.whole, 2),
        lambda: None,
        early,
    ]
    for number, piece in enumerate(pieces):
        pl.when(turn == number)(piece)
    inner(turn, ins, outs)
    pl.when(turn == turns - 1)(end)


def gather_all(value, number, inner, turns, ins, outs, flops):
    if lax.axis_size("expert") != 8 or lax.axis_size("weight") != 4:

        def alone(*refs):
            inner(pl.program_id(0), refs[: len(ins)], refs[len(ins) :])

        gathered = lax.all_gather(value, ("expert", "weight"), axis=0)
        return gathered, call(alone, turns, ins, outs, flops)
    out = jax.ShapeDtypeStruct((32,) + value.shape, value.dtype)
    arrays, shapes = [a for a, _ in ins], [o for o, _ in outs]
    results = pl.pallas_call(
        functools.partial(gather_all_kernel, inner, len(ins), len(outs)),
        grid=(turns,),
        out_shape=[out] + shapes,
        in_specs=[whole_spec(value)] + [spec for _, spec in ins],
        out_specs=[pl.BlockSpec(memory_space=pl.ANY)] + [spec for _, spec in outs],
        scratch_shapes=[
            pltpu.SemaphoreType.DMA((44,)),
            pltpu.SemaphoreType.DMA((32, 2)),
            pltpu.SemaphoreType.DMA,
        ],
        compiler_params=pltpu.CompilerParams(
            collective_id=number, has_side_effects=True, vmem_limit_bytes=vmem_limit
        ),
        cost_estimate=cost(flops, value, out, *arrays, *shapes),
    )(value, *arrays)
    return results[0], results[1:]


def attention_kernel(
    score_scale,
    normed_ref,
    value_ref,
    cosine_ref,
    sine_ref,
    segment_row_ref,
    segment_column_ref,
    gain_ref,
    query_hbm,
    latent_hbm,
    expand_hbm,
    output_hbm,
    value_out,
    normed_out,
    query_out,
    latent_out,
    scale_out,
    latent_normed_out,
    key_rope_out,
    expanded_out,
    log_out,
    mixed_out,
    attended_out,
    query_matrix,
    latent_matrix,
    expand_matrix,
    output_matrix,
    partial,
    mates,
    sides,
    carried,
    send_sems,
    recv_sems,
    local_sems,
    group_sends,
    group_sems,
    sum_sends,
    mate_sems,
    side_sems,
):
    place = places()
    z, x, y, c = place
    side, mate = device(z, x, 1 - y, c), device(z, x, y, 1 - c)
    rows = normed_ref.shape[0]
    half = rows // 2
    heads = query_out.shape[0]
    greet(gather_neighbours(place))
    near = Sends(group_sends)
    own, across = y * 2 + c, (1 - y) * 2 + c
    keep = pltpu.make_async_copy(normed_ref, normed_out.at[own], local_sems.at[0])
    keep.start()

    def part(i, h):
        return normed_out.at[i, pl.ds(h * half, half)]

    for to in (side, mate):
        for h in range(2):
            piece = normed_ref.at[pl.ds(h * half, half)]
            near.start(piece, part(own, h), group_sems.at[own, h], to)
    sends = Sends(send_sems)
    gather = Gather(value_ref, value_out, sends, recv_sems, local_sems.at[1], place, 48)
    gather.whole(0)
    loads = [
        pltpu.make_async_copy(source, target, local_sems.at[2 + i])
        for i, (source, target) in enumerate(
            (
                (query_hbm, query_matrix),
                (latent_hbm, latent_matrix),
                (expand_hbm, expand_matrix),
                (output_hbm, output_matrix),
            )
        )
    ]
    for load in loads:
        load.start()
    for h in range(2):
        landed(part(across, h), group_sems.at[across, h], mate)
        near.start(part(across, h), part(across, h), group_sems.at[across, h], mate)
    for i in (y * 2 + 1 - c, (1 - y) * 2 + 1 - c):
        for h in range(2):
            landed(part(i, h), group_sems.at[i, h], mate)
    keep.wait()
    normed = normed_out[...].reshape(4 * rows, normed_out.shape[2])
    cosine, sine = cosine_ref[...], sine_ref[...]
    turn_half = ROPE // 2

    def turned(first, second):
        return jnp.concatenate(
            [first * cosine - second * sine, second * cosine + first * sine], axis=1
        )

    loads[0].wait()
    full = matmul(normed, query_matrix[...])
    for h in range(heads):
        start = h * (NOPE + ROPE)
        first = full[:, start + NOPE : start + NOPE + turn_half]
        second = full[:, start + NOPE + turn_half : start + NOPE + ROPE]
        query = jnp.concatenate([full[:, start : start + NOPE], turned(first, second)], axis=1)
        query_out[h] = query.astype(jnp.bfloat16)
    gather.whole(1)
    loads[1].wait()
    compressed = times_trans(normed, latent_matrix[...])
    latent = compressed[:, :LATENT]
    scale = inv_rms(latent)
    latent_out[...] = latent
    scale_out[...] = jnp.broadcast_to(scale, scale_out.shape)
    latent_normed_out[...] = (latent * scale * gain_ref[...]).astype(jnp.bfloat16)
    first = compressed[:, LATENT : LATENT + turn_half]
    second = compressed[:, LATENT + turn_half : LATENT + ROPE]
    key_rope_out[...] = turned(first, second).astype(jnp.bfloat16)
    gather.relay(0)
    loads[2].wait()
    expanded_out[...] = matmul(latent_normed_out[...], expand_matrix[...]).astype(jnp.bfloat16)

    def head(h):
        start = h * (NOPE + VDIM)
        query = query_out[h]
        raw = times_trans(query[:, :NOPE], expanded_out[:, start : start + NOPE])
        raw = raw + times_trans(query[:, NOPE:], key_rope_out[...])
        row = lax.broadcasted_iota(jnp.int32, raw.shape, 0)
        column = lax.broadcasted_iota(jnp.int32, raw.shape, 1)
        allowed = (segment_column_ref[...] == segment_row_ref[...]) & (column <= row)
        scores = jnp.where(allowed, raw * score_scale, -1e30)
        peak = jnp.max(scores, axis=1, keepdims=True)
        weights = jnp.exp(scores - peak)
        total = jnp.sum(weights, axis=1, keepdims=True)
        log_out[h] = jnp.broadcast_to(peak + jnp.log(total), log_out.shape[1:])
        probs = (weights / total).astype(jnp.bfloat16)
        mixed = matmul(probs, expanded_out[:, start + NOPE : start + NOPE + VDIM])
        mixed_out[:, h * VDIM : (h + 1) * VDIM] = mixed.astype(jnp.bfloat16)

    middle = [
        None,
        functools.partial(gather.whole, 2),
        functools.partial(gather.relay, 1),
        functools.partial(gather.corner, 0),
    ]
    for h in range(heads):
        head(h)
        if h < 4 and middle[h] is not None:
            middle[h]()
    loads[3].wait()
    for i in range(4):
        block = matmul(mixed_out[i * rows : (i + 1) * rows], output_matrix[...])
        partial[i] = block.astype(jnp.bfloat16)
    sums = Sends(sum_sends)
    for j, yy in enumerate((1 - y, y)):
        for h in range(2):
            some = pl.ds(h * half, half)
            sums.start(
                partial.at[yy * 2 + 1 - c, some], mates.at[j, some], mate_sems.at[j, h], mate
            )
    gather.whole(3)
    for h in range(2):
        some = pl.ds(h * half, half)
        landed(mates.at[0, some], mate_sems.at[0, h], mate)
        add_into(carried, [partial.at[(1 - y) * 2 + c], mates.at[0]], h * half, half)
        sums.start(carried.at[some], sides.at[some], side_sems.at[h], side)
    gather.relay(2)
    gather.corner(1)
    gather.relay(3)
    gather.corner(2)
    for h in range(2):
        some = pl.ds(h * half, half)
        landed(mates.at[1, some], mate_sems.at[1, h], mate)
        landed(sides.at[some], side_sems.at[h], mate)
        add_into(attended_out, [partial.at[y * 2 + c], mates.at[1], sides], h * half, half)
    gather.corner(3)
    gather.last()
    near.finish()
    sends.finish()
    sums.finish()


def add_into(target, sources, start, rows):
    step = 16

    def body(i, carry):
        part = pl.ds(pl.multiple_of(start + i * step, step), step)
        total = sources[0][part].astype(jnp.float32)
        for source in sources[1:]:
            total = total + source[part].astype(jnp.float32)
        target[part] = total.astype(target.dtype)
        return carry

    lax.fori_loop(0, rows // step, body, 0)


def attention_forward(
    score_scale, normed, value, cosine, sine, segment, gain, query, latent, expand, output, number
):
    rows, width = normed.shape
    group, heads = 4 * rows, query.shape[1] // (NOPE + ROPE)
    shape, low = jax.ShapeDtypeStruct, jnp.bfloat16
    vmem, away = pl.BlockSpec(memory_space=pltpu.VMEM), pl.BlockSpec(memory_space=pl.ANY)
    segment = segment.astype(jnp.float32)
    inputs = [normed, value, cosine, sine, segment[None], segment[:, None], gain[None]]
    matrices = [query, latent.T, expand, output]
    outs = [
        shape((32,) + value.shape, low),
        shape((4, rows, width), low),
        shape((heads, group, NOPE + ROPE), low),
        shape((group, LATENT), jnp.float32),
        shape((group, lanes), jnp.float32),
        shape((group, LATENT), low),
        shape((group, ROPE), low),
        shape((group, heads * (NOPE + VDIM)), low),
        shape((heads, group, lanes), jnp.float32),
        shape((group, heads * VDIM), low),
        shape((rows, width), jnp.float32),
    ]
    flops = 2 * group * (width * (query.shape[1] + latent.shape[1]) + output.size + expand.size)
    return pl.pallas_call(
        functools.partial(attention_kernel, score_scale),
        out_shape=outs,
        in_specs=[vmem] * len(inputs) + [away] * 4,
        out_specs=[away] + [vmem] * (len(outs) - 1),
        scratch_shapes=[pltpu.VMEM(m.shape, low) for m in matrices]
        + [
            pltpu.VMEM((4, rows, width), low),
            pltpu.VMEM((2, rows, width), low),
            pltpu.VMEM((rows, width), low),
            pltpu.VMEM((rows, width), low),
            pltpu.SemaphoreType.DMA((44,)),
            pltpu.SemaphoreType.DMA((32, 2)),
            pltpu.SemaphoreType.DMA((6,)),
            pltpu.SemaphoreType.DMA((6,)),
            pltpu.SemaphoreType.DMA((4, 2)),
            pltpu.SemaphoreType.DMA((6,)),
            pltpu.SemaphoreType.DMA((2, 2)),
            pltpu.SemaphoreType.DMA((2,)),
        ],
        compiler_params=pltpu.CompilerParams(
            collective_id=number, has_side_effects=True, vmem_limit_bytes=vmem_limit
        ),
        cost_estimate=cost(flops, *inputs, *matrices, *outs),
    )(*inputs, *matrices)


def sum_all_kernel(inner, cover_ins, cover_outs, p_ref, *refs):
    ins, refs = refs[:cover_ins], refs[cover_ins:]
    out_ref, refs = refs[0], refs[1:]
    outs, refs = refs[:cover_outs], refs[cover_outs:]
    own, mates, over_half, side_half, over_full, side_full, below, above = refs[:8]
    send_sems, mate_sems, half_sems, full_sems, line_sems, local_sems = refs[8:]
    z, x, y, c = places()
    turn, turns = pl.program_id(0), pl.num_programs(0)
    rows = out_ref.shape[0]
    half = rows // 2
    over, side, mate = device(z, 1 - x, y, c), device(z, x, 1 - y, c), device(z, x, y, 1 - c)
    up, down = device(z + 1, x, y, c), device(z - 1, x, y, c)
    sends = Sends(send_sems)
    targets = [ordered(z, (3, 2, 1, 0)[step], (3, 0, 2, 1)[step]) for step in range(4)]
    spots = [(1 - x, 1 - y), (1 - x, y), (x, 1 - y), (x, y)]
    shards = [[shard(zz, xx, yy, 1 - c) for xx, yy in spots] for zz in targets]
    mine = [[shard(zz, xx, yy, c) for xx, yy in spots] for zz in targets]
    higher = [zz > z for zz in targets]
    lower = [zz < z for zz in targets]
    loads = [
        pltpu.make_async_copy(p_ref.at[mine[slot // 4][slot % 4]], own.at[slot], local_sems.at[slot])
        for slot in range(16)
    ]

    mate_copies = [
        sends.plan(p_ref.at[shards[slot // 4][slot % 4]], mates.at[slot], mate_sems.at[slot], mate)
        for slot in range(16)
    ]
    corner_copies, relay_copies, line_copies = [], [], []
    for step in range(4):
        corner_copies.append(
            (
                sends.plan(
                    own.at[step * 4, pl.ds(half, half)],
                    over_half.at[step],
                    half_sems.at[step, 0],
                    over,
                ),
                sends.plan(
                    own.at[step * 4, pl.ds(0, half)], side_half.at[step], half_sems.at[step, 1], side
                ),
            )
        )
        relay_copies.append(
            (
                sends.plan(
                    own.at[step * 4 + 1], over_full.at[step], full_sems.at[step, 0], over
                ),
                sends.plan(
                    own.at[step * 4 + 2], side_full.at[step], full_sems.at[step, 1], side
                ),
            )
        )
    for step in range(3):
        zz, slot = targets[step], step * 4 + 3
        line_copies.append(
            (
                sends.plan(own.at[slot], below.at[zz], line_sems.at[zz, 0], up, higher[step]),
                sends.plan(own.at[slot], above.at[zz], line_sems.at[zz, 1], down, lower[step]),
            )
        )

    def begin():
        greet([(over, None), (side, None), (mate, None), (up, z < 3), (down, z > 0)])
        for slot in range(16):
            mate_copies[slot].start()
            loads[slot].start()

    def join(slot):
        loads[slot].wait()
        landed(mates.at[slot], mate_sems.at[slot], mate)

    def corner(step):
        slot = step * 4
        join(slot)
        add_rows(own.at[slot], [(mates.at[slot], 0)], 0, rows)
        for copy in corner_copies[step]:
            copy.start()

    def relay(step):
        slot = step * 4 + 1
        join(slot)
        add_rows(own.at[slot], [(mates.at[slot], 0)], half, half)
        landed(side_half.at[step], half_sems.at[step, 1], mate)
        add_rows(own.at[slot], [(mates.at[slot], 0), (side_half.at[step], 0)], 0, half)
        relay_copies[step][0].start()
        slot = step * 4 + 2
        join(slot)
        add_rows(own.at[slot], [(mates.at[slot], 0)], 0, half)
        landed(over_half.at[step], half_sems.at[step, 0], mate)
        add_rows(own.at[slot], [(mates.at[slot], 0), (over_half.at[step], half)], half, half)
        relay_copies[step][1].start()

    def whole(step):
        zz = targets[step]
        slot = step * 4 + 3
        join(slot)
        landed(over_full.at[step], full_sems.at[step, 0], mate)
        landed(side_full.at[step], full_sems.at[step, 1], mate)
        add_rows(
            own.at[slot],
            [(mates.at[slot], 0), (over_full.at[step], 0), (side_full.at[step], 0)],
            0,
            rows,
        )

        @pl.when((zz >= z) & (z > 0))
        def _():
            landed(below.at[zz], line_sems.at[zz, 0], mate)
            add_rows(own.at[slot], [(below.at[zz], 0)], 0, rows)

        @pl.when((zz <= z) & (z < 3))
        def _():
            landed(above.at[zz], line_sems.at[zz, 1], mate)
            add_rows(own.at[slot], [(above.at[zz], 0)], 0, rows)

        if step < 3:
            pl.when(higher[step])(line_copies[step][0].start)
            pl.when(lower[step])(line_copies[step][1].start)

    def end():
        whole(3)
        out_ref[...] = own[15].astype(out_ref.dtype)
        sends.finish()

    pieces = [
        begin,
        functools.partial(corner, 0),
        functools.partial(corner, 1),
        functools.partial(relay, 0),
        functools.partial(corner, 2),
        functools.partial(relay, 1),
        functools.partial(whole, 0),
        functools.partial(corner, 3),
        functools.partial(relay, 2),
        functools.partial(whole, 1),
        functools.partial(relay, 3),
        functools.partial(whole, 2),
    ]
    for number, piece in enumerate(pieces):
        pl.when(turn == number)(piece)
    inner(turn, ins, outs)
    pl.when(turn == turns - 1)(end)


def sum_all(value, number, inner, turns, ins, outs, flops):
    if lax.axis_size("expert") != 8 or lax.axis_size("weight") != 4:
        summed = lax.psum_scatter(
            value.reshape(-1, value.shape[2]), ("expert", "weight"), scatter_dimension=0, tiled=True
        )

        def alone(*refs):
            inner(pl.program_id(0), refs[: len(ins)], refs[len(ins) :])

        return summed.astype(jnp.float32), call(alone, turns, ins, outs, flops)
    _, rows, width = value.shape
    out = jax.ShapeDtypeStruct((rows, width), jnp.float32)
    buffer = lambda n, r: pltpu.VMEM((n, r, width), value.dtype)
    arrays, shapes = [a for a, _ in ins], [o for o, _ in outs]
    results = pl.pallas_call(
        functools.partial(sum_all_kernel, inner, len(ins), len(outs)),
        grid=(turns,),
        out_shape=[out] + shapes,
        in_specs=[pl.BlockSpec(memory_space=pl.ANY)] + [spec for _, spec in ins],
        out_specs=[pl.BlockSpec((rows, width), lambda i: (0, 0))] + [spec for _, spec in outs],
        scratch_shapes=[
            buffer(16, rows),
            buffer(16, rows),
            buffer(4, rows // 2),
            buffer(4, rows // 2),
            buffer(4, rows),
            buffer(4, rows),
            buffer(4, rows),
            buffer(4, rows),
            pltpu.SemaphoreType.DMA((40,)),
            pltpu.SemaphoreType.DMA((16,)),
            pltpu.SemaphoreType.DMA((4, 2)),
            pltpu.SemaphoreType.DMA((4, 2)),
            pltpu.SemaphoreType.DMA((4, 2)),
            pltpu.SemaphoreType.DMA((16,)),
        ],
        compiler_params=pltpu.CompilerParams(
            collective_id=number, has_side_effects=True, vmem_limit_bytes=vmem_limit
        ),
        cost_estimate=cost(flops, value, out, *arrays, *shapes),
    )(value, *arrays)
    return results[0], results[1:]


def gather_group_kernel(x_ref, out_ref, send_sems, recv_sems, local_sem):
    z, x, y, c = places()
    half = x_ref.shape[0] // 2
    side, mate = device(z, x, 1 - y, c), device(z, x, y, 1 - c)
    greet([(side, None), (mate, None)])
    sends = Sends(send_sems)
    own, across = y * 2 + c, (1 - y) * 2 + c
    keep = pltpu.make_async_copy(x_ref, out_ref.at[own], local_sem)
    keep.start()

    def part(i, h):
        return out_ref.at[i, pl.ds(h * half, half)]

    for h in range(2):
        piece = x_ref.at[pl.ds(h * half, half)]
        sends.start(piece, part(own, h), recv_sems.at[own, h], side)
    for h in range(2):
        piece = x_ref.at[pl.ds(h * half, half)]
        sends.start(piece, part(own, h), recv_sems.at[own, h], mate)
    for h in range(2):
        landed(part(across, h), recv_sems.at[across, h], mate)
        sends.start(part(across, h), part(across, h), recv_sems.at[across, h], mate)
    for i in (y * 2 + 1 - c, (1 - y) * 2 + 1 - c):
        for h in range(2):
            landed(part(i, h), recv_sems.at[i, h], mate)
    sends.finish()
    keep.wait()


def gather_group(value, number):
    if lax.axis_size("expert") != 8 or lax.axis_size("weight") != 4:
        return lax.all_gather(value, "weight", axis=0, tiled=True)
    out = jax.ShapeDtypeStruct((4,) + value.shape, value.dtype)
    return pl.pallas_call(
        gather_group_kernel,
        out_shape=out,
        in_specs=[pl.BlockSpec(memory_space=pltpu.VMEM)],
        out_specs=pl.BlockSpec(memory_space=pltpu.VMEM),
        scratch_shapes=[
            pltpu.SemaphoreType.DMA((6,)),
            pltpu.SemaphoreType.DMA((4, 2)),
            pltpu.SemaphoreType.DMA,
        ],
        compiler_params=pltpu.CompilerParams(collective_id=number, has_side_effects=True),
        cost_estimate=cost(0, value, out),
    )(value).reshape(-1, value.shape[1])


def sum_group_kernel(p_ref, out_ref, mates, sides, carried, send_sems, mate_sems, side_sems):
    z, x, y, c = places()
    rows = out_ref.shape[0]
    half = rows // 2
    side, mate = device(z, x, 1 - y, c), device(z, x, y, 1 - c)
    greet([(side, None), (mate, None)])
    sends = Sends(send_sems)

    for j, yy in enumerate((1 - y, y)):
        for h in range(2):
            part = pl.ds(h * half, half)
            sends.start(
                p_ref.at[yy * 2 + 1 - c, part], mates.at[j, part], mate_sems.at[j, h], mate
            )

    def add(target, sources, h):
        step = 16

        def body(i, carry):
            part = pl.ds(pl.multiple_of(h * half + i * step, step), step)
            total = sources[0][part].astype(jnp.float32)
            for source in sources[1:]:
                total = total + source[part].astype(jnp.float32)
            target[part] = total.astype(target.dtype)
            return carry

        lax.fori_loop(0, half // step, body, 0)

    for h in range(2):
        part = pl.ds(h * half, half)
        landed(mates.at[0, part], mate_sems.at[0, h], mate)
        add(carried, [p_ref.at[(1 - y) * 2 + c], mates.at[0]], h)
        sends.start(carried.at[part], sides.at[part], side_sems.at[h], side)
    for h in range(2):
        part = pl.ds(h * half, half)
        landed(mates.at[1, part], mate_sems.at[1, h], mate)
        landed(sides.at[part], side_sems.at[h], mate)
        add(out_ref, [p_ref.at[y * 2 + c], mates.at[1], sides], h)
    sends.finish()


def sum_group(value, number):
    if lax.axis_size("expert") != 8 or lax.axis_size("weight") != 4:
        summed = lax.psum_scatter(value, "weight", scatter_dimension=0, tiled=True)
        return summed.astype(jnp.float32)
    rows, width = value.shape[0] // 4, value.shape[1]
    value = value.reshape(4, rows, width)
    out = jax.ShapeDtypeStruct((rows, width), jnp.float32)
    return pl.pallas_call(
        sum_group_kernel,
        out_shape=out,
        in_specs=[pl.BlockSpec(memory_space=pltpu.VMEM)],
        out_specs=pl.BlockSpec(memory_space=pltpu.VMEM),
        scratch_shapes=[
            pltpu.VMEM((2, rows, width), value.dtype),
            pltpu.VMEM((rows, width), value.dtype),
            pltpu.VMEM((rows, width), value.dtype),
            pltpu.SemaphoreType.DMA((6,)),
            pltpu.SemaphoreType.DMA((2, 2)),
            pltpu.SemaphoreType.DMA((2,)),
        ],
        compiler_params=pltpu.CompilerParams(collective_id=number, has_side_effects=True),
        cost_estimate=cost(0, value, out),
    )(value)


def columns(start, size):
    return pl.ds(pl.multiple_of(start, lanes), size)


def add_block(target, sources, rows, row_start=0):
    step = 16

    def body(i, carry):
        part = pl.ds(pl.multiple_of(row_start + i * step, step), step)
        total = target[part].astype(jnp.float32)
        for source in sources:
            there = pl.ds(pl.multiple_of(i * step, step), step)
            total = total + source[there].astype(jnp.float32)
        target[part] = total.astype(target.dtype)
        return carry

    lax.fori_loop(0, rows // step, body, 0)


def total_kernel(
    top_ref,
    rest_ref,
    out_ref,
    acc,
    mates,
    first_over,
    first_side,
    next_side,
    next_over,
    line,
    send_sems,
    sems,
):
    z, x, y, c = places()
    rows, width = out_ref.shape
    sources = [(top_ref, 0, 0), (rest_ref, top_ref.shape[0], 24)]
    half, quarter, eighth, sixteenth = width // 2, width // 4, width // 8, width // 16
    strip = rows // 4
    over, side, mate = device(z, 1 - x, y, c), device(z, x, 1 - y, c), device(z, x, y, 1 - c)
    others = [lax.rem(z + d, 4) for d in (1, 2, 3)]
    greet(
        [(over, None), (side, None), (mate, None)] + [(device(zz, x, y, c), None) for zz in others]
    )
    sends = Sends(send_sems)
    base = c * half
    for j in range(2):
        for p_ref, top, sem in sources:
            sends.start(
                p_ref.at[:, columns((1 - c) * half + j * quarter, quarter)],
                mates.at[pl.ds(top, p_ref.shape[0]), columns(j * quarter, quarter)],
                sems.at[sem + j],
                mate,
            )
    kept = (x * eighth + y * sixteenth, quarter + y * eighth + x * sixteenth)
    firsts, nexts = (first_over, first_side), (next_side, next_over)
    for j in range(2):
        part = columns(j * quarter, quarter)
        wide = 16
        for p_ref, top, sem in sources:
            landed(mates.at[pl.ds(top, p_ref.shape[0]), part], sems.at[sem + j], mate)

            def join(i, carry, j=j, p_ref=p_ref, top=top):
                mine = pl.ds(pl.multiple_of(i * wide, wide), wide)
                some = pl.ds(pl.multiple_of(top + i * wide, wide), wide)
                total = p_ref[mine, columns(base + j * quarter, quarter)].astype(jnp.float32)
                total = total + mates[some, columns(j * quarter, quarter)].astype(jnp.float32)
                acc[some, columns(j * quarter, quarter)] = total.astype(acc.dtype)
                return carry

            lax.fori_loop(0, p_ref.shape[0] // wide, join, 0)
        away = (1 - x) * eighth if j == 0 else quarter + (1 - y) * eighth
        sends.start(
            acc.at[:, columns(away, eighth)], firsts[j], sems.at[2 + j], (over, side)[j]
        )
    for j in range(2):
        landed(firsts[j], sems.at[2 + j], mate)
        near = x * eighth if j == 0 else quarter + y * eighth
        add_block(acc.at[:, columns(near, eighth)], [firsts[j]], rows)
        away = near + ((1 - y) if j == 0 else (1 - x)) * sixteenth
        sends.start(
            acc.at[:, columns(away, sixteenth)], nexts[j], sems.at[4 + j], (side, over)[j]
        )
    for j in range(2):
        landed(nexts[j], sems.at[4 + j], mate)
        add_block(acc.at[:, columns(kept[j], sixteenth)], [nexts[j]], rows)
        for d, zz in enumerate(others):
            sends.start(
                acc.at[pl.ds(pl.multiple_of(zz * strip, 16), strip), columns(kept[j], sixteenth)],
                line.at[j, d],
                sems.at[6 + j * 3 + d],
                device(zz, x, y, c),
            )
    strip_here = pl.multiple_of(z * strip, 16)
    for j in range(2):
        for d in range(3):
            landed(line.at[j, d], sems.at[6 + j * 3 + d], mate)
        block = acc.at[:, columns(kept[j], sixteenth)]
        add_block(block, [line.at[j, d] for d in range(3)], strip, strip_here)

        def place(i, carry, j=j):
            some = pl.ds(pl.multiple_of(strip_here + i * 16, 16), 16)
            out_ref[some, columns(base + kept[j], sixteenth)] = acc[
                some, columns(kept[j], sixteenth)
            ]
            return carry

        lax.fori_loop(0, strip // 16, place, 0)
        done = out_ref.at[pl.ds(strip_here, strip), columns(base + kept[j], sixteenth)]
        for d, zz in enumerate(others):
            sends.start(done, done, sems.at[12 + j * 3 + d], device(zz, x, y, c))
    for j in range(2):
        for d in range(3):
            source = pl.multiple_of(lax.rem(z + 3 - d, 4) * strip, 16)
            landed(
                out_ref.at[pl.ds(source, strip), columns(base + kept[j], sixteenth)],
                sems.at[12 + j * 3 + d],
                mate,
            )
        part = out_ref.at[:, columns(base + kept[j], sixteenth)]
        sends.start(part, part, sems.at[18 + j], (side, over)[j])
    others_kept = (
        x * eighth + (1 - y) * sixteenth,
        quarter + y * eighth + (1 - x) * sixteenth,
    )
    for j in range(2):
        landed(out_ref.at[:, columns(base + others_kept[j], sixteenth)], sems.at[18 + j], mate)
        near = x * eighth if j == 0 else quarter + y * eighth
        part = out_ref.at[:, columns(base + near, eighth)]
        sends.start(part, part, sems.at[20 + j], (over, side)[j])
    for j in range(2):
        away = (1 - x) * eighth if j == 0 else quarter + (1 - y) * eighth
        landed(out_ref.at[:, columns(base + away, eighth)], sems.at[20 + j], mate)
        part = out_ref.at[:, columns(base + j * quarter, quarter)]
        sends.start(part, part, sems.at[22 + j], mate)
    for j in range(2):
        landed(
            out_ref.at[:, columns((1 - c) * half + j * quarter, quarter)], sems.at[22 + j], mate
        )
    sends.finish()


def total_over_all(top, rest, number):
    if lax.axis_size("expert") != 8 or lax.axis_size("weight") != 4:
        value = jnp.concatenate([top, rest], axis=0).astype(jnp.float32)
        return lax.psum(value, ("expert", "weight"))
    rows, width = top.shape[0] + rest.shape[0], top.shape[1]
    out = jax.ShapeDtypeStruct((rows, width), top.dtype)
    buffer = lambda n: pltpu.VMEM((rows, n), top.dtype)
    return pl.pallas_call(
        total_kernel,
        out_shape=out,
        in_specs=[pl.BlockSpec(memory_space=pltpu.VMEM)] * 2,
        out_specs=pl.BlockSpec(memory_space=pltpu.VMEM),
        scratch_shapes=[
            buffer(width // 2),
            buffer(width // 2),
            buffer(width // 8),
            buffer(width // 8),
            buffer(width // 16),
            buffer(width // 16),
            pltpu.VMEM((2, 3, rows // 4, width // 16), top.dtype),
            pltpu.SemaphoreType.DMA((26,)),
            pltpu.SemaphoreType.DMA((26,)),
        ],
        compiler_params=pltpu.CompilerParams(collective_id=number, has_side_effects=True),
        cost_estimate=cost(0, top, rest, out),
    )(top, rest)


def shared_kernel(turn, ins, outs):
    normed_ref, cotangent_ref, gate_grad_ref, lift_grad_ref, hidden_ref = ins

    @pl.when(turn == 0)
    def _():
        for out_ref in outs:
            out_ref[...] = jnp.zeros_like(out_ref)

    normed, cotangent = normed_ref[...], cotangent_ref[...]
    outs[0][...] += trans_times(gate_grad_ref[...], normed)
    outs[1][...] += trans_times(lift_grad_ref[...], normed)
    outs[2][...] += trans_times(hidden_ref[...], cotangent)


def weight_kernel(turn, ins, outs):
    rows_ref, grads_ref, gate_grad_ref, lift_grad_ref, hidden_ref = ins
    rows = rows_ref[0]
    for out_ref, left_ref, right in (
        (outs[0], gate_grad_ref, rows),
        (outs[1], lift_grad_ref, rows),
        (outs[2], hidden_ref, grads_ref[0]),
    ):
        out_ref[0] = trans_times(left_ref[0], right).astype(out_ref.dtype)


def weights_alone(*refs):
    weight_kernel(pl.program_id(0), refs[:5], refs[5:])


def gradients_kernel(turn, ins, outs):
    shared_kernel(turn, ins[:5], outs[:3])
    weight_kernel(turn, ins[5:], outs[3:])


def per_device(
    tokens,
    cotangent,
    segments,
    routes,
    first_gain,
    query_weight,
    latent_weight,
    latent_gain,
    expand_weight,
    output_weight,
    second_gain,
    router_weight,
    shared_gate,
    shared_up,
    shared_down,
    expert_gate,
    expert_up,
    expert_down,
):
    weight_count = lax.axis_size("weight")
    token_rows = tokens.shape[0]
    width = tokens.shape[1]
    group_rows = token_rows * weight_count
    query_width = NOPE + ROPE
    heads_here = query_weight.shape[1] // query_width
    expert_count = router_weight.shape[1]
    local_experts = expert_gate.shape[0]
    score_scale = query_width ** (-0.5)
    activations = tokens.astype(jnp.float32)
    first_scale = inv_rms(activations)
    normed = (activations * first_scale * first_gain).astype(jnp.bfloat16)
    both = ("expert", "weight")
    expert_index = lax.axis_index("expert")
    expert_lanes = lax.axis_size("expert")
    blocks = expert_lanes * weight_count
    pairs, quads = blocks // 2, blocks // 4
    pair_rows, quad_rows = 2 * token_rows, 4 * token_rows
    all_rows = blocks * token_rows
    slot_rows = blocks * CAP
    choose = (
        routes[:, :, None] == jnp.arange(expert_count, dtype=jnp.int32)[None, None, :]
    ).astype(jnp.float32)
    hit = jnp.sum(choose, axis=1)
    order = jnp.arange(token_rows, dtype=jnp.int32)
    before = (order[None, :] < order[:, None]).astype(jnp.bfloat16)
    place = matmul(before, hit.astype(jnp.bfloat16))
    rank = jnp.sum(choose * jnp.arange(routes.shape[1], dtype=jnp.float32)[None, :, None], axis=1)
    code = jnp.where(hit > 0, 32.0 * rank + place, -1.0)
    extra = jnp.pad(code, ((0, 0), (0, lanes - expert_count)), constant_values=-1.0)
    cotangent_wide = jnp.concatenate([cotangent, extra.astype(jnp.bfloat16)], axis=1)
    column = jnp.arange(lanes, dtype=jnp.int32)[None, :]
    row = jnp.arange(8, dtype=jnp.int32)[:, None]
    first_here = expert_index * local_experts
    here = (row < local_experts) & (column == first_here + row)
    twice = here | ((row < local_experts) & (column == first_here + row + expert_count))
    here, twice = here.astype(jnp.bfloat16), twice.astype(jnp.bfloat16)
    weight_index = lax.axis_index("weight")
    high_column = 2 * (row * weight_count + weight_index)
    known = row < routes.shape[1]
    high_at = (known & (column == high_column)).astype(jnp.bfloat16)
    low_at = (known & (column == high_column + 1)).astype(jnp.bfloat16)
    shared_here = shared_gate.shape[1] // expert_lanes
    shared_wide = -(-shared_here // lanes) * lanes
    start = expert_index * shared_here

    def shared_part(matrix):
        part = lax.dynamic_slice_in_dim(matrix, start, shared_here, axis=0)
        return jnp.pad(part, ((0, shared_wide - shared_here), (0, 0)))

    gate_part = shared_part(shared_gate.T)
    up_part = shared_part(shared_up.T)
    down_part = shared_part(shared_down)
    shape = jax.ShapeDtypeStruct
    whole = lambda array: (array, whole_spec(array))
    slots = shape((local_experts, slot_rows, width), jnp.bfloat16)
    slots_one = shape((local_experts, slot_rows, lanes), jnp.float32)
    gather_flops = 2 * all_rows * width * (2 * CAP * local_experts + shared_wide)
    cosine, sine = rope_tables(segments[0])
    allowed = attention_mask(segments[0])
    sizes = (expert_lanes, weight_count)
    if sizes == (8, 4):
        (
            cotangent_all,
            normed_all,
            query,
            latent,
            latent_scale,
            latent_normed,
            key_rope,
            expanded,
            log_total,
            mixed,
            attended,
        ) = attention_forward(
            score_scale,
            normed,
            cotangent_wide,
            cosine,
            sine,
            segments[0],
            latent_gain,
            query_weight,
            latent_weight,
            expand_weight,
            output_weight,
            0,
        )
        cotangent_all = cotangent_all.reshape(all_rows, -1)
        normed_all = normed_all.reshape(group_rows, width)
        latent_scale, log_total = latent_scale[:, :1], log_total[:, :, :1]
        query = query.transpose(1, 0, 2)
        expanded = expanded.reshape(group_rows, heads_here, NOPE + VDIM)
    else:
        cotangent_all = lax.all_gather(cotangent_wide, both, axis=0, tiled=True)
        normed_all = gather_group(normed, 0)
        query_full = matmul(normed_all, query_weight).reshape(group_rows, heads_here, query_width)
        query = jnp.concatenate(
            [
                query_full[..., :NOPE],
                rotate(query_full[..., NOPE:], cosine[:, None, :], sine[:, None, :]),
            ],
            axis=-1,
        ).astype(jnp.bfloat16)
        compressed = matmul(normed_all, latent_weight)
        latent = compressed[:, :LATENT]
        latent_scale = inv_rms(latent)
        latent_normed = (latent * latent_scale * latent_gain).astype(jnp.bfloat16)
        key_rope = rotate(compressed[:, LATENT:], cosine, sine).astype(jnp.bfloat16)
        expanded = (
            matmul(latent_normed, expand_weight)
            .astype(jnp.bfloat16)
            .reshape(group_rows, heads_here, NOPE + VDIM)
        )
    key_nope = expanded[..., :NOPE]
    values = expanded[..., NOPE:]

    def score_block():
        raw = jnp.einsum(
            "ihd,jhd->hij", query[..., :NOPE], key_nope, preferred_element_type=jnp.float32
        )
        raw = raw + jnp.einsum(
            "ihd,jd->hij", query[..., NOPE:], key_rope, preferred_element_type=jnp.float32
        )
        return jnp.where(allowed[None], raw * score_scale, -1e30)

    if sizes != (8, 4):
        scores = score_block()
        peak = jnp.max(scores, axis=-1, keepdims=True)
        weights = jnp.exp(scores - peak)
        total = jnp.sum(weights, axis=-1, keepdims=True)
        log_total = peak + jnp.log(total)
        mixed = jnp.einsum(
            "hij,jhd->ihd",
            (weights / total).astype(jnp.bfloat16),
            values,
            preferred_element_type=jnp.float32,
        )
        mixed = mixed.astype(jnp.bfloat16).reshape(group_rows, heads_here * VDIM)
        attended = sum_group(matmul(mixed, output_weight).astype(jnp.bfloat16), 1)
    hidden_one = activations + attended
    second_scale = inv_rms(hidden_one)
    normed_two = (hidden_one * second_scale * second_gain).astype(jnp.bfloat16)
    gates = jax.nn.sigmoid(matmul(normed_two, router_weight))
    chosen = jnp.sum(choose * gates[:, None, :], axis=-1)
    chosen_total = jnp.sum(chosen, axis=1, keepdims=True)
    mixing = route_scale * chosen / chosen_total
    upstream = cotangent.astype(jnp.float32)
    mixing_at = jnp.sum(choose * mixing[:, :, None], axis=1)
    mixing_high = mixing_at.astype(jnp.bfloat16)
    mixing_low = (mixing_at - mixing_high.astype(jnp.float32)).astype(jnp.bfloat16)
    normed_wide = jnp.concatenate([normed_two, mixing_high, mixing_low], axis=1)
    marks = (cotangent_all, pl.BlockSpec((quad_rows, lanes), lambda i: (i, width // lanes)))
    normed_tokens, (grads_slots, shared_raw) = gather_all(
        normed_wide,
        2,
        functools.partial(grads_kernel, pair_rows),
        quads,
        [whole(here), (cotangent_all, pair_spec(cotangent_all, quads)), whole(down_part)],
        [
            (slots, slots_spec(slots, quads)),
            (shape((all_rows, shared_wide), jnp.float32), pl.BlockSpec((quad_rows, shared_wide), lambda i: (i, 0))),
        ],
        gather_flops,
    )
    normed_tokens = normed_tokens.reshape(all_rows, -1)
    token_spec = pl.BlockSpec((quad_rows, shared_wide), lambda i: (i, 0))
    token_shape = shape((all_rows, shared_wide), jnp.bfloat16)
    rows_slots, mix_slots, shared_hidden, shared_gate_grad, shared_lift_grad = call(
        functools.partial(rows_kernel, pair_rows),
        quads,
        [
            whole(here),
            whole(twice),
            marks,
            (normed_tokens, pair_spec(normed_tokens, quads)),
            (shared_raw, token_spec),
            whole(gate_part),
            whole(up_part),
        ],
        [
            (slots, slots_spec(slots, quads)),
            (slots_one, slots_spec(slots_one, quads)),
            (token_shape, token_spec),
            (token_shape, token_spec),
            (token_shape, token_spec),
        ],
        gather_flops + 2 * all_rows * width * shared_wide,
    )
    hidden_here = expert_gate.shape[2]
    gate_rows, up_rows = expert_gate.transpose(0, 2, 1), expert_up.transpose(0, 2, 1)

    def tile_spec(rows, n):
        per = slot_rows // rows
        return pl.BlockSpec((1, rows, n), lambda i: (i // per, i % per, 0))

    def expert_spec(rows, matrix):
        per = slot_rows // rows
        return pl.BlockSpec((1,) + matrix.shape[1:], lambda i: (i // per, 0, 0))

    large, small = 32 * CAP, 16 * CAP
    narrow = shape((local_experts, slot_rows, hidden_here), jnp.bfloat16)
    one_matmul = 2 * local_experts * slot_rows * width * hidden_here
    routed_hidden, mixed_hidden, slope, active, produced = call(
        forward_kernel,
        local_experts * (slot_rows // large),
        [
            (rows_slots, tile_spec(large, width)),
            (mix_slots, tile_spec(large, lanes)),
            (gate_rows, expert_spec(large, gate_rows)),
            (up_rows, expert_spec(large, up_rows)),
            (expert_down, expert_spec(large, expert_down)),
        ],
        [(narrow, tile_spec(large, hidden_here))] * 4 + [(slots, tile_spec(large, width))],
        3 * one_matmul,
    )
    dense = shape((all_rows, width), jnp.bfloat16)
    dense_wide = shape((all_rows, width + lanes), jnp.bfloat16)
    (out_dense,) = call(
        functools.partial(out_kernel, pair_rows),
        quads,
        [
            whole(here),
            marks,
            (produced, slots_spec(slots, quads)),
            (shared_hidden, token_spec),
            whole(down_part),
        ],
        [(dense, pair_spec(dense, quads))],
        gather_flops,
    )
    narrow_tile = tile_spec(small, hidden_here)
    routed_out, (gate_grad, lift_grad, returned, mix_grad_slots) = sum_all(
        out_dense.reshape(blocks, token_rows, width),
        6,
        backward_kernel,
        local_experts * (slot_rows // small),
        [
            (grads_slots, tile_spec(small, width)),
            (routed_hidden, narrow_tile),
            (slope, narrow_tile),
            (active, narrow_tile),
            (gate_rows, expert_spec(small, gate_rows)),
            (up_rows, expert_spec(small, up_rows)),
            (expert_down, expert_spec(small, expert_down)),
        ],
        [
            (narrow, narrow_tile),
            (narrow, narrow_tile),
            (slots, tile_spec(small, width)),
            (slots_one, tile_spec(small, lanes)),
        ],
        3 * one_matmul,
    )
    (back_dense,) = call(
        functools.partial(back_kernel, pair_rows),
        quads,
        [
            whole(here),
            whole(high_at),
            whole(low_at),
            marks,
            (returned, slots_spec(slots, quads)),
            (mix_grad_slots, slots_spec(slots_one, quads)),
            (shared_gate_grad, token_spec),
            (shared_lift_grad, token_spec),
            whole(gate_part),
            whole(up_part),
        ],
        [(dense_wide, pair_spec(dense_wide, quads))],
        gather_flops + 2 * all_rows * width * shared_wide,
    )
    shared_sum = shape((shared_wide, width), jnp.float32)
    shared_out = (shared_sum, whole_spec(shared_sum))
    plain_spec = pl.BlockSpec((pair_rows, width), lambda i: (i, 0))
    shared_spec = pl.BlockSpec((pair_rows, shared_wide), lambda i: (i, 0))
    column_half = width // 2
    half_spec = lambda m: pl.BlockSpec((1, m, column_half), lambda i: (i // 2, 0, i % 2))
    narrow_spec = pl.BlockSpec((1, slot_rows, hidden_here), lambda i: (i // 2, 0, 0))
    shared_ins = [
        (normed_tokens, plain_spec),
        (cotangent_all, plain_spec),
        (shared_gate_grad, shared_spec),
        (shared_lift_grad, shared_spec),
        (shared_hidden, shared_spec),
    ]
    weight_ins = [
        (rows_slots, half_spec(slot_rows)),
        (grads_slots, half_spec(slot_rows)),
        (gate_grad, narrow_spec),
        (lift_grad, narrow_spec),
        (mixed_hidden, narrow_spec),
    ]
    back_blocks = back_dense.reshape(blocks, token_rows, -1)
    shared_flops = 6 * all_rows * width * shared_wide
    together = pairs == 2 * local_experts
    weight_type = jnp.bfloat16 if together else jnp.float32
    weight_shape = shape((local_experts, hidden_here, width), weight_type)
    weight_outs = [(weight_shape, half_spec(hidden_here))] * 3
    if together:
        back_here, sums = sum_all(
            back_blocks,
            3,
            gradients_kernel,
            pairs,
            shared_ins + weight_ins,
            [shared_out] * 3 + weight_outs,
            shared_flops + 3 * one_matmul,
        )
        shared_sums = sums[:3]
        weight_grads = [value.astype(jnp.float32) for value in sums[3:]]
    else:
        back_here, shared_sums = sum_all(
            back_blocks, 3, shared_kernel, pairs, shared_ins, [shared_out] * 3, shared_flops
        )
        weight_grads = call(
            weights_alone, 2 * local_experts, weight_ins, weight_outs, 3 * one_matmul
        )
    routed_back = back_here[:, :width]
    mix_grad = back_here[:, width : width + 2 * weight_count * routes.shape[1]]
    mix_grad = jnp.sum(mix_grad.reshape(token_rows, routes.shape[1], -1), axis=2)
    shared_grads = jnp.concatenate([total[:shared_here] for total in shared_sums], axis=0)
    shared_grads = shared_grads.astype(jnp.bfloat16)
    swapped = lax.all_to_all(shared_grads, "expert", split_axis=1, concat_axis=0, tiled=True)
    swapped = swapped.reshape(expert_lanes, 3, shared_here, -1).astype(jnp.float32)
    shared_gradients = [swapped[:, i].reshape(expert_lanes * shared_here, -1) for i in range(3)]
    chosen_grad = route_scale * (
        mix_grad / chosen_total
        - jnp.sum(mix_grad * chosen, axis=1, keepdims=True) / chosen_total**2
    )
    logit_grad = jnp.sum(choose * chosen_grad[:, :, None], axis=1) * gates * (1.0 - gates)
    normed_two_grad = (
        routed_back
        + jnp.dot(logit_grad, router_weight.astype(jnp.float32).T, precision=highest)
    )
    router_gradient = jnp.dot(logit_grad.T, normed_two.astype(jnp.float32), precision=highest)
    back_two, second_gain_gradient = norm_back(
        normed_two_grad, hidden_one, second_scale, second_gain
    )
    hidden_grad = upstream + back_two
    hidden_group = gather_group(hidden_grad.astype(jnp.bfloat16), 4)
    output_gradient = trans_times(mixed, hidden_group).astype(jnp.bfloat16)
    hidden_group, output_gradient = lax.optimization_barrier((hidden_group, output_gradient))
    output_shard = lax.psum_scatter(output_gradient, "expert", scatter_dimension=1, tiled=True)
    mixed_grad = (
        times_trans(hidden_group, output_weight)
        .astype(jnp.bfloat16)
        .reshape(group_rows, heads_here, VDIM)
    )
    probs = jnp.exp(score_block() - log_total)
    prob_grad = jnp.einsum("ihd,jhd->hij", mixed_grad, values, preferred_element_type=jnp.float32)
    centre = jnp.sum(probs * prob_grad, axis=-1, keepdims=True)
    score_grad = (probs * (prob_grad - centre)).astype(jnp.bfloat16)
    value_grad = jnp.einsum(
        "hij,ihd->jhd", probs.astype(jnp.bfloat16), mixed_grad, preferred_element_type=jnp.float32
    )
    query_nope_grad = (
        jnp.einsum("hij,jhd->ihd", score_grad, key_nope, preferred_element_type=jnp.float32)
        * score_scale
    )
    query_rope_grad = (
        jnp.einsum("hij,jd->ihd", score_grad, key_rope, preferred_element_type=jnp.float32)
        * score_scale
    )
    key_nope_grad = (
        jnp.einsum(
            "hij,ihd->jhd", score_grad, query[..., :NOPE], preferred_element_type=jnp.float32
        )
        * score_scale
    )
    key_rope_grad = (
        jnp.einsum("hij,ihd->jd", score_grad, query[..., NOPE:], preferred_element_type=jnp.float32)
        * score_scale
    )
    query_grad = jnp.concatenate(
        [query_nope_grad, unrotate(query_rope_grad, cosine[:, None, :], sine[:, None, :])], axis=-1
    )
    query_grad = query_grad.astype(jnp.bfloat16).reshape(group_rows, heads_here * query_width)
    expand_grad = (
        jnp.concatenate([key_nope_grad, value_grad], axis=-1)
        .astype(jnp.bfloat16)
        .reshape(group_rows, heads_here * (NOPE + VDIM))
    )
    expert_grads = (weight_grads[0].transpose(0, 2, 1), weight_grads[1].transpose(0, 2, 1), weight_grads[2])
    layer_out = (hidden_one + routed_out).astype(jnp.bfloat16)
    query_gradient = trans_times(normed_all, query_grad)
    expand_gradient = trans_times(latent_normed, expand_grad).astype(jnp.bfloat16)
    expand_gradient, output_shard = lax.optimization_barrier((expand_gradient, output_shard))
    latent_normed_grad = times_trans(expand_grad, expand_weight)
    latent_back, latent_gain_gradient = norm_back(
        latent_normed_grad, latent, latent_scale, latent_gain
    )
    compressed_grad = jnp.concatenate([latent_back, unrotate(key_rope_grad, cosine, sine)], axis=-1)
    compressed_grad = compressed_grad.astype(jnp.bfloat16)
    latent_weight_gradient = trans_times(compressed_grad, normed_all)
    normed_grad = sum_group(
        (
            times_trans(query_grad, query_weight) + times_trans(compressed_grad, latent_weight)
        ).astype(jnp.bfloat16),
        5,
    )
    back_one, first_gain_gradient = norm_back(normed_grad, activations, first_scale, first_gain)
    token_gradient = hidden_grad + back_one
    shards = (
        lax.psum_scatter(
            query_gradient.astype(jnp.bfloat16), "expert", scatter_dimension=0, tiled=True
        ).astype(jnp.float32),
        lax.psum_scatter(
            expand_gradient, "expert", scatter_dimension=0, tiled=True
        ).astype(jnp.float32),
        output_shard.astype(jnp.float32),
    )
    latent_columns = latent_weight.shape[1]
    rest = jnp.concatenate(
        [
            router_gradient,
            first_gain_gradient[None],
            second_gain_gradient[None],
            jnp.pad(latent_gain_gradient, (0, width - LATENT))[None],
        ],
        axis=0,
    ).astype(jnp.bfloat16)
    wanted = -(-(latent_columns + rest.shape[0]) // 64) * 64 - latent_columns
    rest = jnp.pad(rest, ((0, wanted - rest.shape[0]), (0, 0)))
    total = total_over_all(latent_weight_gradient.astype(jnp.bfloat16), rest, 7)
    gains_at = latent_columns + expert_count
    wide = lambda value: value.astype(jnp.float32)
    totals = (
        wide(total[:latent_columns]).T,
        wide(total[gains_at + 2, :LATENT]),
        wide(total[latent_columns:gains_at]).T,
        wide(total[gains_at]),
        wide(total[gains_at + 1]),
    )
    return (
        layer_out,
        token_gradient,
        totals[3],
        shards[0],
        totals[0],
        totals[1],
        shards[1],
        shards[2],
        totals[4],
        totals[2],
        shared_gradients[0].T,
        shared_gradients[1].T,
        shared_gradients[2],
        expert_grads[0],
        expert_grads[1],
        expert_grads[2],
    )


def solution(mesh):
    return jax.shard_map(
        per_device,
        mesh=mesh,
        in_specs=(
            P(("expert", "weight"), None),
            P(("expert", "weight"), None),
            P("expert", None),
            P(("expert", "weight"), None),
            P(),
            P(None, "weight"),
            P(),
            P(),
            P(None, "weight"),
            P("weight", None),
            P(),
            P(),
            P(None, "weight"),
            P(None, "weight"),
            P("weight", None),
            P("expert", None, "weight"),
            P("expert", None, "weight"),
            P("expert", "weight", None),
        ),
        out_specs=(
            P(("expert", "weight"), None),
            P(("expert", "weight"), None),
            P(),
            P("expert", "weight"),
            P(),
            P(),
            P("expert", "weight"),
            P("weight", "expert"),
            P(),
            P(),
            P("expert", "weight"),
            P("expert", "weight"),
            P("weight", "expert"),
            P("expert", None, "weight"),
            P("expert", None, "weight"),
            P("expert", "weight", None),
        ),
        check_vma=False,
    )
```

```python
import functools

import jax
import jax.numpy as jnp
from jax import lax
from jax.experimental import pallas as pl
from jax.experimental.pallas import tpu as pltpu
from jax.sharding import PartitionSpec as P

NOPE = 128
ROPE = 64
VDIM = 128
LATENT = 512
TOPK = 6
CAP = 20


eps = 1e-06
route_scale = 2.446
rope_base = 50000.0
highest = lax.Precision.HIGHEST


def matmul(left, right):
    return jnp.dot(left, right, preferred_element_type=jnp.float32)


def trans_times(left, right):
    return lax.dot_general(
        left, right, (((0,), (0,)), ((), ())), preferred_element_type=jnp.float32
    )


def times_trans(left, right):
    return lax.dot_general(
        left, right, (((1,), (1,)), ((), ())), preferred_element_type=jnp.float32
    )


def inv_rms(value):
    return lax.rsqrt(jnp.mean(value * value, axis=-1, keepdims=True) + eps)


def norm_back(grad_out, value, scale, gain):
    scaled = grad_out * gain
    grad_in = scale * scaled - value * scale**3 * jnp.mean(scaled * value, axis=-1, keepdims=True)
    gain_grad = jnp.sum(grad_out * value * scale, axis=0)
    return (grad_in, gain_grad)


def rope_tables(seg):
    size = seg.shape[0]
    index = jnp.arange(size, dtype=jnp.int32)
    fresh = jnp.concatenate([jnp.ones((1,), dtype=bool), seg[1:] != seg[:-1]])
    first = lax.cummax(jnp.where(fresh, index, jnp.zeros_like(index)), axis=0)
    place = (index - first).astype(jnp.float32)
    half = ROPE // 2
    freqs = rope_base ** (-(jnp.arange(half, dtype=jnp.float32) * 2.0 / ROPE))
    angle = place[:, None] * freqs[None, :]
    return (jnp.cos(angle), jnp.sin(angle))


def attention_mask(seg):
    index = jnp.arange(seg.shape[0], dtype=jnp.int32)
    return (seg[:, None] == seg[None, :]) & (index[None, :] <= index[:, None])


def rotate(value, cosine, sine):
    half = value.shape[-1] // 2
    first, second = (value[..., :half], value[..., half:])
    return jnp.concatenate(
        [first * cosine - second * sine, second * cosine + first * sine], axis=-1
    )


def unrotate(value, cosine, sine):
    half = value.shape[-1] // 2
    first, second = (value[..., :half], value[..., half:])
    return jnp.concatenate(
        [first * cosine + second * sine, second * cosine - first * sine], axis=-1
    )


lanes = 128
vmem_limit = 64 * 1024 * 1024 - 131072


def token_slots(marks, here, local_experts, half):
    codes = times_trans(here, marks)
    count = codes.shape[1]
    rank = jnp.floor(codes * (1.0 / 32.0))
    place = codes - 32.0 * rank
    token = lax.broadcasted_iota(jnp.int32, codes.shape, 1)
    slot = jnp.where(codes >= 0, place + jnp.where(token >= half, float(CAP), 0.0), -1.0)
    row = lax.broadcasted_iota(jnp.int32, (2 * CAP, count), 0).astype(jnp.float32)
    picks = [jnp.where(row == slot[e : e + 1], 1.0, 0.0) for e in range(local_experts)]
    return picks, rank


def pair_slots(marks_ref, here_ref, local_experts, pair):
    count = marks_ref.shape[0] // pair
    return [
        token_slots(marks_ref[j * pair : (j + 1) * pair], here_ref[...], local_experts, pair // 2)
        for j in range(count)
    ]


def slot_part(value, e):
    return value[e * 2 * CAP : (e + 1) * 2 * CAP]


def gather_rows(slots, values, pair, out_ref):
    rows = [
        jnp.dot(
            jnp.concatenate(picks, axis=0).astype(jnp.bfloat16),
            values[j * pair : (j + 1) * pair],
            preferred_element_type=jnp.float32,
        )
        for j, (picks, _) in enumerate(slots)
    ]
    for e in range(out_ref.shape[0]):
        together = jnp.concatenate([slot_part(value, e) for value in rows], axis=0)
        out_ref[e] = together.astype(jnp.bfloat16)


def spread_rows(slots, rows_ref):
    local_experts = rows_ref.shape[0]
    rows = [rows_ref[e].astype(jnp.float32) for e in range(local_experts)]
    totals = []
    for j, (picks, _) in enumerate(slots):
        part = jnp.concatenate([slot_part(value, j) for value in rows], axis=0)
        pick = jnp.concatenate(picks, axis=0).astype(jnp.bfloat16)
        totals.append(trans_times(pick, part.astype(jnp.bfloat16)))
    return jnp.concatenate(totals, axis=0)


def grads_kernel(pair, turn, ins, outs):
    here_ref, value_ref, down_ref = ins
    rows_ref, back_ref = outs
    width = rows_ref.shape[2]
    slots = pair_slots(value_ref.at[:, width:], here_ref, rows_ref.shape[0], pair)
    values = value_ref[:, :width]
    gather_rows(slots, values, pair, rows_ref)
    back_ref[...] = times_trans(values, down_ref[...])


def rows_kernel(
    pair,
    here_ref,
    twice_ref,
    marks_ref,
    value_ref,
    back_ref,
    gate_ref,
    up_ref,
    rows_ref,
    mix_ref,
    hidden_ref,
    gate_grad_ref,
    lift_grad_ref,
):
    width = rows_ref.shape[2]
    slots = pair_slots(marks_ref, here_ref, rows_ref.shape[0], pair)
    values = value_ref[:, :width]
    gather_rows(slots, values, pair, rows_ref)
    for j, (picks, _) in enumerate(slots):
        mixing = times_trans(twice_ref[...], value_ref[j * pair : (j + 1) * pair, width:])
        for e, pick in enumerate(picks):
            column = jnp.sum(pick * mixing[e : e + 1], axis=1, keepdims=True)
            column = jnp.broadcast_to(column, (2 * CAP, lanes))
            mix_ref[e, j * 2 * CAP : (j + 1) * 2 * CAP] = column
    gate = times_trans(values, gate_ref[...])
    lift = times_trans(values, up_ref[...])
    back = back_ref[...]
    sigma = jax.nn.sigmoid(gate)
    active = gate * sigma
    hidden_ref[...] = (active * lift).astype(jnp.bfloat16)
    gate_grad_ref[...] = (back * lift * sigma * (1.0 + gate * (1.0 - sigma))).astype(jnp.bfloat16)
    lift_grad_ref[...] = (back * active).astype(jnp.bfloat16)


def forward_kernel(
    rows_ref,
    mix_ref,
    gate_ref,
    up_ref,
    down_ref,
    hidden_ref,
    mixed_ref,
    slope_ref,
    active_ref,
    produced_ref,
):
    rows = rows_ref[0]
    gate = times_trans(rows, gate_ref[0])
    lift = times_trans(rows, up_ref[0])
    mix = mix_ref[0][:, :1]
    sigma = jax.nn.sigmoid(gate)
    active = gate * sigma
    hidden = active * lift
    mixed_hidden = (mix * hidden).astype(jnp.bfloat16)
    hidden_ref[0] = hidden.astype(jnp.bfloat16)
    mixed_ref[0] = mixed_hidden
    slope_ref[0] = (mix * lift * sigma * (1.0 + gate * (1.0 - sigma))).astype(jnp.bfloat16)
    active_ref[0] = (mix * active).astype(jnp.bfloat16)
    produced_ref[0] = matmul(mixed_hidden, down_ref[0]).astype(jnp.bfloat16)


def backward_kernel(turn, ins, outs):
    grads_ref, hidden_ref, slope_ref, active_ref, gate_ref, up_ref, down_ref = ins
    gate_grad_ref, lift_grad_ref, returned_ref, mix_grad_ref = outs
    back = times_trans(grads_ref[0], down_ref[0])
    mix_grad = jnp.sum(hidden_ref[0].astype(jnp.float32) * back, axis=1, keepdims=True)
    mix_grad_ref[0] = jnp.broadcast_to(mix_grad, mix_grad_ref.shape[1:])
    gate_grad = (back * slope_ref[0].astype(jnp.float32)).astype(jnp.bfloat16)
    lift_grad = (back * active_ref[0].astype(jnp.float32)).astype(jnp.bfloat16)
    gate_grad_ref[0] = gate_grad
    lift_grad_ref[0] = lift_grad
    returned = matmul(gate_grad, gate_ref[0]) + matmul(lift_grad, up_ref[0])
    returned_ref[0] = returned.astype(jnp.bfloat16)


def back_kernel(
    pair,
    here_ref,
    high_ref,
    low_ref,
    marks_ref,
    rows_ref,
    mix_grad_ref,
    gate_grad_ref,
    lift_grad_ref,
    gate_ref,
    up_ref,
    out_ref,
):
    width = rows_ref.shape[2]
    slots = pair_slots(marks_ref, here_ref, rows_ref.shape[0], pair)
    total = spread_rows(slots, rows_ref)
    total = total + matmul(gate_grad_ref[...], gate_ref[...])
    total = total + matmul(lift_grad_ref[...], up_ref[...])
    out_ref[:, :width] = total.astype(jnp.bfloat16)
    for j, (picks, rank) in enumerate(slots):
        choice = lax.broadcasted_iota(jnp.int32, rank.shape, 0).astype(jnp.float32)
        mix_grad = jnp.zeros(rank.shape, jnp.float32)
        for e, pick in enumerate(picks):
            column = slot_part(mix_grad_ref[e], j)[:, :1]
            row = jnp.sum(pick * column, axis=0, keepdims=True)
            mix_grad = mix_grad + jnp.where(choice == rank[e : e + 1], row, 0.0)
        high = mix_grad.astype(jnp.bfloat16)
        low = (mix_grad - high.astype(jnp.float32)).astype(jnp.bfloat16)
        sent = trans_times(high, high_ref[...]) + trans_times(low, low_ref[...])
        out_ref[j * pair : (j + 1) * pair, width:] = sent.astype(jnp.bfloat16)


def out_kernel(pair, here_ref, marks_ref, rows_ref, hidden_ref, down_ref, out_ref):
    slots = pair_slots(marks_ref, here_ref, rows_ref.shape[0], pair)
    total = spread_rows(slots, rows_ref)
    total = total + matmul(hidden_ref[...], down_ref[...])
    out_ref[...] = total.astype(jnp.bfloat16)


def whole_spec(array):
    zeros = (0,) * array.ndim
    return pl.BlockSpec(array.shape, lambda i: zeros)


def pair_spec(array, pairs):
    block = (array.shape[0] // pairs,) + array.shape[1:]
    zeros = (0,) * (array.ndim - 1)
    return pl.BlockSpec(block, lambda i: (i,) + zeros)


def slots_spec(array, pairs):
    block = (array.shape[0], array.shape[1] // pairs) + array.shape[2:]
    return pl.BlockSpec(block, lambda i: (0, i, 0))


def cost(flops, *arrays):
    moved = sum(a.size * a.dtype.itemsize for a in arrays)
    return pl.CostEstimate(flops=int(flops), bytes_accessed=int(moved), transcendentals=0)


def call(kernel, grid, ins, outs, flops):
    arrays = [a for a, _ in ins]
    shapes = [s for s, _ in outs]
    return pl.pallas_call(
        kernel,
        grid=(grid,),
        in_specs=[s for _, s in ins],
        out_specs=[s for _, s in outs],
        out_shape=shapes,
        cost_estimate=cost(flops, *arrays, *shapes),
        compiler_params=pltpu.CompilerParams(vmem_limit_bytes=vmem_limit),
    )(*arrays)


MESH = pl.DeviceIdType.MESH


def places():
    expert, weight = lax.axis_index("expert"), lax.axis_index("weight")
    return lax.div(expert, 2), lax.rem(expert, 2), lax.div(weight, 2), lax.rem(weight, 2)


def device(z, x, y, c):
    return (z * 2 + x, y * 2 + c)


def shard(z, x, y, c):
    return z * 8 + x * 4 + y * 2 + c


def push(source, target, send, receive, to):
    return pltpu.make_async_remote_copy(
        src_ref=source,
        dst_ref=target,
        send_sem=send,
        recv_sem=receive,
        device_id=to,
        device_id_type=MESH,
    )


class Sends:
    def __init__(self, semaphores):
        self.semaphores = semaphores
        self.started = []

    def plan(self, source, target, receive, to, when=None):
        copy = push(source, target, self.semaphores.at[len(self.started)], receive, to)
        self.started.append((copy, when))
        return copy

    def start(self, source, target, receive, to, when=None):
        copy = self.plan(source, target, receive, to, when)
        if when is None:
            copy.start()
        else:
            pl.when(when)(copy.start)

    def finish(self):
        for copy, when in self.started:
            if when is None:
                copy.wait_send()
            else:
                pl.when(when)(copy.wait_send)


def landed(target, receive, to):
    push(target, target, receive, receive, to).wait_recv()


def greet(devices):
    barrier = pltpu.get_barrier_semaphore()
    count = 0
    for to, when in devices:
        signal = functools.partial(
            pl.semaphore_signal, barrier, inc=1, device_id=to, device_id_type=MESH
        )
        if when is None:
            signal()
            count = count + 1
        else:
            pl.when(when)(signal)
            count = count + when.astype(jnp.int32)
    pl.semaphore_wait(barrier, count)


def add_rows(target, sources, start, rows):
    step = 16

    def body(i, carry):
        part = pl.ds(pl.multiple_of(start + i * step, step), step)
        total = target[part].astype(jnp.float32)
        for source, offset in sources:
            there = pl.ds(pl.multiple_of(start - offset + i * step, step), step)
            total = total + source[there].astype(jnp.float32)
        target[part] = total.astype(target.dtype)
        return carry

    lax.fori_loop(0, rows // step, body, 0)


def ordered(z, first, second):
    upper = lax.div(z, 2)
    inner = z + upper * (3 - 2 * z)
    value = first + inner * (second - first)
    return value + upper * (3 - 2 * value)


class Gather:
    def __init__(self, x_ref, out_ref, sends, recv_sems, local_sem, place, cut=None):
        z, x, y, c = place
        rows = x_ref.shape[0]
        cut = rows // 2 if cut is None else cut
        self.parts = [pl.ds(0, cut), pl.ds(cut, rows - cut)]
        over, side, mate = device(z, 1 - x, y, c), device(z, x, 1 - y, c), device(z, x, y, 1 - c)
        up, down = device(z + 1, x, y, c), device(z - 1, x, y, c)
        self.out_ref, self.recv_sems, self.mate = out_ref, recv_sems, mate
        planes = [ordered(z, (0, 1, 2, 3)[step], (1, 0, 2, 3)[step]) for step in range(4)]
        self.rising = [(zz <= z) & (z < 3) for zz in planes]
        self.falling = [(zz >= z) & (z > 0) for zz in planes]
        self.mine = [shard(zz, x, y, c) for zz in planes]
        self.overs = [shard(zz, 1 - x, y, c) for zz in planes]
        self.sides = [shard(zz, x, 1 - y, c) for zz in planes]
        self.corners = [shard(zz, 1 - x, 1 - y, c) for zz in planes]
        self.mates = [
            (shard(zz, x, y, 1 - c), shard(zz, 1 - x, y, 1 - c), shard(zz, x, 1 - y, 1 - c))
            for zz in planes
        ]
        self.mate_corners = [shard(zz, 1 - x, 1 - y, 1 - c) for zz in planes]
        self.keep = pltpu.make_async_copy(x_ref, out_ref.at[self.mine[0]], local_sem)
        self.whole_copies, self.relay_copies, self.corner_copies = [], [], []

        def copy(ref, receive, to, when=None, source=None):
            return sends.plan(ref if source is None else source, ref, receive, to, when)

        for step in range(4):
            i = self.mine[step]
            source = x_ref if step == 0 else None
            there, receive = out_ref.at[i], recv_sems.at[i, 0]
            self.whole_copies.append(
                [
                    (copy(there, receive, up, self.rising[step], source), self.rising[step]),
                    (copy(there, receive, down, self.falling[step], source), self.falling[step]),
                    (copy(there, receive, over, None, source), None),
                    (copy(there, receive, side, None, source), None),
                    (copy(there, receive, mate, None, source), None),
                ]
            )
            i, j = self.overs[step], self.sides[step]
            self.relay_copies.append(
                [
                    copy(self.halves(i, 0), recv_sems.at[i, 0], side),
                    copy(out_ref.at[i], recv_sems.at[i, 0], mate),
                    copy(self.halves(j, 1), recv_sems.at[j, 1], over),
                    copy(out_ref.at[j], recv_sems.at[j, 0], mate),
                ]
            )
            i = self.corners[step]
            self.corner_copies.append(
                [copy(self.halves(i, h), recv_sems.at[i, h], mate) for h in range(2)]
            )

    def halves(self, i, h):
        return self.out_ref.at[i, self.parts[h]]

    def full_here(self, i):
        landed(self.out_ref.at[i], self.recv_sems.at[i, 0], self.mate)

    def half_here(self, i, h):
        landed(self.halves(i, h), self.recv_sems.at[i, h], self.mate)

    def whole(self, step):
        if step == 0:
            self.keep.start()
        else:
            self.full_here(self.mine[step])
        for copy, when in self.whole_copies[step]:
            if when is None:
                copy.start()
            else:
                pl.when(when)(copy.start)

    def relay(self, step):
        self.full_here(self.overs[step])
        self.relay_copies[step][0].start()
        self.relay_copies[step][1].start()
        self.full_here(self.sides[step])
        self.relay_copies[step][2].start()
        self.relay_copies[step][3].start()

    def corner(self, step):
        for h in range(2):
            self.half_here(self.corners[step], h)
            self.corner_copies[step][h].start()

    def last(self):
        for step in range(4):
            for i in self.mates[step]:
                self.full_here(i)
            for h in range(2):
                self.half_here(self.mate_corners[step], h)
        self.keep.wait()


def gather_neighbours(place):
    z, x, y, c = place
    return [
        (device(z, 1 - x, y, c), None),
        (device(z, x, 1 - y, c), None),
        (device(z, x, y, 1 - c), None),
        (device(z + 1, x, y, c), z < 3),
        (device(z - 1, x, y, c), z > 0),
    ]


def gather_all_kernel(inner, cover_ins, cover_outs, x_ref, *refs):
    ins, refs = refs[:cover_ins], refs[cover_ins:]
    out_ref, refs = refs[0], refs[1:]
    outs, refs = refs[:cover_outs], refs[cover_outs:]
    send_sems, recv_sems, local_sem = refs
    turn, turns = pl.program_id(0), pl.num_programs(0)
    place = places()
    sends = Sends(send_sems)
    gather = Gather(x_ref, out_ref, sends, recv_sems, local_sem, place)

    def begin():
        greet(gather_neighbours(place))
        gather.whole(0)

    def end():
        gather.whole(3)
        gather.relay(2)
        gather.corner(1)
        gather.relay(3)
        gather.corner(2)
        gather.corner(3)
        gather.last()
        sends.finish()

    def early():
        gather.relay(1)
        gather.corner(0)

    pieces = [
        begin,
        lambda: None,
        functools.partial(gather.whole, 1),
        functools.partial(gather.relay, 0),
        functools.partial(gather.whole, 2),
        lambda: None,
        early,
    ]
    for number, piece in enumerate(pieces):
        pl.when(turn == number)(piece)
    inner(turn, ins, outs)
    pl.when(turn == turns - 1)(end)


def gather_all(value, number, inner, turns, ins, outs, flops):
    if lax.axis_size("expert") != 8 or lax.axis_size("weight") != 4:

        def alone(*refs):
            inner(pl.program_id(0), refs[: len(ins)], refs[len(ins) :])

        gathered = lax.all_gather(value, ("expert", "weight"), axis=0)
        return gathered, call(alone, turns, ins, outs, flops)
    out = jax.ShapeDtypeStruct((32,) + value.shape, value.dtype)
    arrays, shapes = [a for a, _ in ins], [o for o, _ in outs]
    results = pl.pallas_call(
        functools.partial(gather_all_kernel, inner, len(ins), len(outs)),
        grid=(turns,),
        out_shape=[out] + shapes,
        in_specs=[whole_spec(value)] + [spec for _, spec in ins],
        out_specs=[pl.BlockSpec(memory_space=pl.ANY)] + [spec for _, spec in outs],
        scratch_shapes=[
            pltpu.SemaphoreType.DMA((44,)),
            pltpu.SemaphoreType.DMA((32, 2)),
            pltpu.SemaphoreType.DMA,
        ],
        compiler_params=pltpu.CompilerParams(
            collective_id=number, has_side_effects=True, vmem_limit_bytes=vmem_limit
        ),
        cost_estimate=cost(flops, value, out, *arrays, *shapes),
    )(value, *arrays)
    return results[0], results[1:]


def attention_kernel(
    score_scale,
    normed_ref,
    value_ref,
    cosine_ref,
    sine_ref,
    segment_row_ref,
    segment_column_ref,
    gain_ref,
    query_hbm,
    latent_hbm,
    expand_hbm,
    output_hbm,
    value_out,
    normed_out,
    query_out,
    latent_out,
    scale_out,
    latent_normed_out,
    key_rope_out,
    expanded_out,
    log_out,
    mixed_out,
    attended_out,
    query_matrix,
    latent_matrix,
    expand_matrix,
    output_matrix,
    partial,
    mates,
    sides,
    carried,
    send_sems,
    recv_sems,
    local_sems,
    group_sends,
    group_sems,
    sum_sends,
    mate_sems,
    side_sems,
):
    place = places()
    z, x, y, c = place
    side, mate = device(z, x, 1 - y, c), device(z, x, y, 1 - c)
    rows = normed_ref.shape[0]
    half = rows // 2
    heads = query_out.shape[0]
    greet(gather_neighbours(place))
    near = Sends(group_sends)
    own, across = y * 2 + c, (1 - y) * 2 + c
    keep = pltpu.make_async_copy(normed_ref, normed_out.at[own], local_sems.at[0])
    keep.start()

    def part(i, h):
        return normed_out.at[i, pl.ds(h * half, half)]

    for to in (side, mate):
        for h in range(2):
            piece = normed_ref.at[pl.ds(h * half, half)]
            near.start(piece, part(own, h), group_sems.at[own, h], to)
    sends = Sends(send_sems)
    gather = Gather(value_ref, value_out, sends, recv_sems, local_sems.at[1], place, 48)
    gather.whole(0)
    loads = [
        pltpu.make_async_copy(source, target, local_sems.at[2 + i])
        for i, (source, target) in enumerate(
            (
                (query_hbm, query_matrix),
                (latent_hbm, latent_matrix),
                (expand_hbm, expand_matrix),
                (output_hbm, output_matrix),
            )
        )
    ]
    for load in loads:
        load.start()
    for h in range(2):
        landed(part(across, h), group_sems.at[across, h], mate)
        near.start(part(across, h), part(across, h), group_sems.at[across, h], mate)
    for i in (y * 2 + 1 - c, (1 - y) * 2 + 1 - c):
        for h in range(2):
            landed(part(i, h), group_sems.at[i, h], mate)
    keep.wait()
    normed = normed_out[...].reshape(4 * rows, normed_out.shape[2])
    cosine, sine = cosine_ref[...], sine_ref[...]
    turn_half = ROPE // 2

    def turned(first, second):
        return jnp.concatenate(
            [first * cosine - second * sine, second * cosine + first * sine], axis=1
        )

    loads[0].wait()
    full = matmul(normed, query_matrix[...])
    for h in range(heads):
        start = h * (NOPE + ROPE)
        first = full[:, start + NOPE : start + NOPE + turn_half]
        second = full[:, start + NOPE + turn_half : start + NOPE + ROPE]
        query = jnp.concatenate([full[:, start : start + NOPE], turned(first, second)], axis=1)
        query_out[h] = query.astype(jnp.bfloat16)
    gather.whole(1)
    loads[1].wait()
    compressed = times_trans(normed, latent_matrix[...])
    latent = compressed[:, :LATENT]
    scale = inv_rms(latent)
    latent_out[...] = latent
    scale_out[...] = jnp.broadcast_to(scale, scale_out.shape)
    latent_normed_out[...] = (latent * scale * gain_ref[...]).astype(jnp.bfloat16)
    first = compressed[:, LATENT : LATENT + turn_half]
    second = compressed[:, LATENT + turn_half : LATENT + ROPE]
    key_rope_out[...] = turned(first, second).astype(jnp.bfloat16)
    gather.relay(0)
    loads[2].wait()
    expanded_out[...] = matmul(latent_normed_out[...], expand_matrix[...]).astype(jnp.bfloat16)

    def head(h):
        start = h * (NOPE + VDIM)
        query = query_out[h]
        raw = times_trans(query[:, :NOPE], expanded_out[:, start : start + NOPE])
        raw = raw + times_trans(query[:, NOPE:], key_rope_out[...])
        row = lax.broadcasted_iota(jnp.int32, raw.shape, 0)
        column = lax.broadcasted_iota(jnp.int32, raw.shape, 1)
        allowed = (segment_column_ref[...] == segment_row_ref[...]) & (column <= row)
        scores = jnp.where(allowed, raw * score_scale, -1e30)
        peak = jnp.max(scores, axis=1, keepdims=True)
        weights = jnp.exp(scores - peak)
        total = jnp.sum(weights, axis=1, keepdims=True)
        log_out[h] = jnp.broadcast_to(peak + jnp.log(total), log_out.shape[1:])
        probs = (weights / total).astype(jnp.bfloat16)
        mixed = matmul(probs, expanded_out[:, start + NOPE : start + NOPE + VDIM])
        mixed_out[:, h * VDIM : (h + 1) * VDIM] = mixed.astype(jnp.bfloat16)

    middle = [
        None,
        functools.partial(gather.whole, 2),
        functools.partial(gather.relay, 1),
        functools.partial(gather.corner, 0),
    ]
    for h in range(heads):
        head(h)
        if h < 4 and middle[h] is not None:
            middle[h]()
    loads[3].wait()
    for i in range(4):
        block = matmul(mixed_out[i * rows : (i + 1) * rows], output_matrix[...])
        partial[i] = block.astype(jnp.bfloat16)
    sums = Sends(sum_sends)
    for j, yy in enumerate((1 - y, y)):
        for h in range(2):
            some = pl.ds(h * half, half)
            sums.start(
                partial.at[yy * 2 + 1 - c, some], mates.at[j, some], mate_sems.at[j, h], mate
            )
    gather.whole(3)
    for h in range(2):
        some = pl.ds(h * half, half)
        landed(mates.at[0, some], mate_sems.at[0, h], mate)
        add_into(carried, [partial.at[(1 - y) * 2 + c], mates.at[0]], h * half, half)
        sums.start(carried.at[some], sides.at[some], side_sems.at[h], side)
    gather.relay(2)
    gather.corner(1)
    gather.relay(3)
    gather.corner(2)
    for h in range(2):
        some = pl.ds(h * half, half)
        landed(mates.at[1, some], mate_sems.at[1, h], mate)
        landed(sides.at[some], side_sems.at[h], mate)
        add_into(attended_out, [partial.at[y * 2 + c], mates.at[1], sides], h * half, half)
    gather.corner(3)
    gather.last()
    near.finish()
    sends.finish()
    sums.finish()


def add_into(target, sources, start, rows):
    step = 16

    def body(i, carry):
        part = pl.ds(pl.multiple_of(start + i * step, step), step)
        total = sources[0][part].astype(jnp.float32)
        for source in sources[1:]:
            total = total + source[part].astype(jnp.float32)
        target[part] = total.astype(target.dtype)
        return carry

    lax.fori_loop(0, rows // step, body, 0)


def attention_forward(
    score_scale, normed, value, cosine, sine, segment, gain, query, latent, expand, output, number
):
    rows, width = normed.shape
    group, heads = 4 * rows, query.shape[1] // (NOPE + ROPE)
    shape, low = jax.ShapeDtypeStruct, jnp.bfloat16
    vmem, away = pl.BlockSpec(memory_space=pltpu.VMEM), pl.BlockSpec(memory_space=pl.ANY)
    segment = segment.astype(jnp.float32)
    inputs = [normed, value, cosine, sine, segment[None], segment[:, None], gain[None]]
    matrices = [query, latent.T, expand, output]
    outs = [
        shape((32,) + value.shape, low),
        shape((4, rows, width), low),
        shape((heads, group, NOPE + ROPE), low),
        shape((group, LATENT), jnp.float32),
        shape((group, lanes), jnp.float32),
        shape((group, LATENT), low),
        shape((group, ROPE), low),
        shape((group, heads * (NOPE + VDIM)), low),
        shape((heads, group, lanes), jnp.float32),
        shape((group, heads * VDIM), low),
        shape((rows, width), jnp.float32),
    ]
    flops = 2 * group * (width * (query.shape[1] + latent.shape[1]) + output.size + expand.size)
    return pl.pallas_call(
        functools.partial(attention_kernel, score_scale),
        out_shape=outs,
        in_specs=[vmem] * len(inputs) + [away] * 4,
        out_specs=[away] + [vmem] * (len(outs) - 1),
        scratch_shapes=[pltpu.VMEM(m.shape, low) for m in matrices]
        + [
            pltpu.VMEM((4, rows, width), low),
            pltpu.VMEM((2, rows, width), low),
            pltpu.VMEM((rows, width), low),
            pltpu.VMEM((rows, width), low),
            pltpu.SemaphoreType.DMA((44,)),
            pltpu.SemaphoreType.DMA((32, 2)),
            pltpu.SemaphoreType.DMA((6,)),
            pltpu.SemaphoreType.DMA((6,)),
            pltpu.SemaphoreType.DMA((4, 2)),
            pltpu.SemaphoreType.DMA((6,)),
            pltpu.SemaphoreType.DMA((2, 2)),
            pltpu.SemaphoreType.DMA((2,)),
        ],
        compiler_params=pltpu.CompilerParams(
            collective_id=number, has_side_effects=True, vmem_limit_bytes=vmem_limit
        ),
        cost_estimate=cost(flops, *inputs, *matrices, *outs),
    )(*inputs, *matrices)


def sum_all_kernel(inner, cover_ins, cover_outs, p_ref, *refs):
    ins, refs = refs[:cover_ins], refs[cover_ins:]
    out_ref, refs = refs[0], refs[1:]
    outs, refs = refs[:cover_outs], refs[cover_outs:]
    own, mates, over_half, side_half, over_full, side_full, below, above = refs[:8]
    send_sems, mate_sems, half_sems, full_sems, line_sems, local_sems = refs[8:]
    z, x, y, c = places()
    turn, turns = pl.program_id(0), pl.num_programs(0)
    rows = out_ref.shape[0]
    half = rows // 2
    over, side, mate = device(z, 1 - x, y, c), device(z, x, 1 - y, c), device(z, x, y, 1 - c)
    up, down = device(z + 1, x, y, c), device(z - 1, x, y, c)
    sends = Sends(send_sems)
    targets = [ordered(z, (3, 2, 1, 0)[step], (3, 0, 2, 1)[step]) for step in range(4)]
    spots = [(1 - x, 1 - y), (1 - x, y), (x, 1 - y), (x, y)]
    shards = [[shard(zz, xx, yy, 1 - c) for xx, yy in spots] for zz in targets]
    mine = [[shard(zz, xx, yy, c) for xx, yy in spots] for zz in targets]
    higher = [zz > z for zz in targets]
    lower = [zz < z for zz in targets]
    loads = [
        pltpu.make_async_copy(p_ref.at[mine[slot // 4][slot % 4]], own.at[slot], local_sems.at[slot])
        for slot in range(16)
    ]

    mate_copies = [
        sends.plan(p_ref.at[shards[slot // 4][slot % 4]], mates.at[slot], mate_sems.at[slot], mate)
        for slot in range(16)
    ]
    corner_copies, relay_copies, line_copies = [], [], []
    for step in range(4):
        corner_copies.append(
            (
                sends.plan(
                    own.at[step * 4, pl.ds(half, half)],
                    over_half.at[step],
                    half_sems.at[step, 0],
                    over,
                ),
                sends.plan(
                    own.at[step * 4, pl.ds(0, half)], side_half.at[step], half_sems.at[step, 1], side
                ),
            )
        )
        relay_copies.append(
            (
                sends.plan(
                    own.at[step * 4 + 1], over_full.at[step], full_sems.at[step, 0], over
                ),
                sends.plan(
                    own.at[step * 4 + 2], side_full.at[step], full_sems.at[step, 1], side
                ),
            )
        )
    for step in range(3):
        zz, slot = targets[step], step * 4 + 3
        line_copies.append(
            (
                sends.plan(own.at[slot], below.at[zz], line_sems.at[zz, 0], up, higher[step]),
                sends.plan(own.at[slot], above.at[zz], line_sems.at[zz, 1], down, lower[step]),
            )
        )

    def begin():
        greet([(over, None), (side, None), (mate, None), (up, z < 3), (down, z > 0)])
        for slot in range(16):
            mate_copies[slot].start()
            loads[slot].start()

    def join(slot):
        loads[slot].wait()
        landed(mates.at[slot], mate_sems.at[slot], mate)

    def corner(step):
        slot = step * 4
        join(slot)
        add_rows(own.at[slot], [(mates.at[slot], 0)], 0, rows)
        for copy in corner_copies[step]:
            copy.start()

    def relay(step):
        slot = step * 4 + 1
        join(slot)
        add_rows(own.at[slot], [(mates.at[slot], 0)], half, half)
        landed(side_half.at[step], half_sems.at[step, 1], mate)
        add_rows(own.at[slot], [(mates.at[slot], 0), (side_half.at[step], 0)], 0, half)
        relay_copies[step][0].start()
        slot = step * 4 + 2
        join(slot)
        add_rows(own.at[slot], [(mates.at[slot], 0)], 0, half)
        landed(over_half.at[step], half_sems.at[step, 0], mate)
        add_rows(own.at[slot], [(mates.at[slot], 0), (over_half.at[step], half)], half, half)
        relay_copies[step][1].start()

    def whole(step):
        zz = targets[step]
        slot = step * 4 + 3
        join(slot)
        landed(over_full.at[step], full_sems.at[step, 0], mate)
        landed(side_full.at[step], full_sems.at[step, 1], mate)
        add_rows(
            own.at[slot],
            [(mates.at[slot], 0), (over_full.at[step], 0), (side_full.at[step], 0)],
            0,
            rows,
        )

        @pl.when((zz >= z) & (z > 0))
        def _():
            landed(below.at[zz], line_sems.at[zz, 0], mate)
            add_rows(own.at[slot], [(below.at[zz], 0)], 0, rows)

        @pl.when((zz <= z) & (z < 3))
        def _():
            landed(above.at[zz], line_sems.at[zz, 1], mate)
            add_rows(own.at[slot], [(above.at[zz], 0)], 0, rows)

        if step < 3:
            pl.when(higher[step])(line_copies[step][0].start)
            pl.when(lower[step])(line_copies[step][1].start)

    def end():
        whole(3)
        out_ref[...] = own[15].astype(out_ref.dtype)
        sends.finish()

    pieces = [
        begin,
        functools.partial(corner, 0),
        functools.partial(corner, 1),
        functools.partial(relay, 0),
        functools.partial(corner, 2),
        functools.partial(relay, 1),
        functools.partial(whole, 0),
        functools.partial(corner, 3),
        functools.partial(relay, 2),
        functools.partial(whole, 1),
        functools.partial(relay, 3),
        functools.partial(whole, 2),
    ]
    for number, piece in enumerate(pieces):
        pl.when(turn == number)(piece)
    inner(turn, ins, outs)
    pl.when(turn == turns - 1)(end)


def sum_all(value, number, inner, turns, ins, outs, flops):
    if lax.axis_size("expert") != 8 or lax.axis_size("weight") != 4:
        summed = lax.psum_scatter(
            value.reshape(-1, value.shape[2]), ("expert", "weight"), scatter_dimension=0, tiled=True
        )

        def alone(*refs):
            inner(pl.program_id(0), refs[: len(ins)], refs[len(ins) :])

        return summed.astype(jnp.float32), call(alone, turns, ins, outs, flops)
    _, rows, width = value.shape
    out = jax.ShapeDtypeStruct((rows, width), jnp.float32)
    buffer = lambda n, r: pltpu.VMEM((n, r, width), value.dtype)
    arrays, shapes = [a for a, _ in ins], [o for o, _ in outs]
    results = pl.pallas_call(
        functools.partial(sum_all_kernel, inner, len(ins), len(outs)),
        grid=(turns,),
        out_shape=[out] + shapes,
        in_specs=[pl.BlockSpec(memory_space=pl.ANY)] + [spec for _, spec in ins],
        out_specs=[pl.BlockSpec((rows, width), lambda i: (0, 0))] + [spec for _, spec in outs],
        scratch_shapes=[
            buffer(16, rows),
            buffer(16, rows),
            buffer(4, rows // 2),
            buffer(4, rows // 2),
            buffer(4, rows),
            buffer(4, rows),
            buffer(4, rows),
            buffer(4, rows),
            pltpu.SemaphoreType.DMA((40,)),
            pltpu.SemaphoreType.DMA((16,)),
            pltpu.SemaphoreType.DMA((4, 2)),
            pltpu.SemaphoreType.DMA((4, 2)),
            pltpu.SemaphoreType.DMA((4, 2)),
            pltpu.SemaphoreType.DMA((16,)),
        ],
        compiler_params=pltpu.CompilerParams(
            collective_id=number, has_side_effects=True, vmem_limit_bytes=vmem_limit
        ),
        cost_estimate=cost(flops, value, out, *arrays, *shapes),
    )(value, *arrays)
    return results[0], results[1:]


def gather_group_kernel(x_ref, out_ref, send_sems, recv_sems, local_sem):
    z, x, y, c = places()
    half = x_ref.shape[0] // 2
    side, mate = device(z, x, 1 - y, c), device(z, x, y, 1 - c)
    greet([(side, None), (mate, None)])
    sends = Sends(send_sems)
    own, across = y * 2 + c, (1 - y) * 2 + c
    keep = pltpu.make_async_copy(x_ref, out_ref.at[own], local_sem)
    keep.start()

    def part(i, h):
        return out_ref.at[i, pl.ds(h * half, half)]

    for h in range(2):
        piece = x_ref.at[pl.ds(h * half, half)]
        sends.start(piece, part(own, h), recv_sems.at[own, h], side)
    for h in range(2):
        piece = x_ref.at[pl.ds(h * half, half)]
        sends.start(piece, part(own, h), recv_sems.at[own, h], mate)
    for h in range(2):
        landed(part(across, h), recv_sems.at[across, h], mate)
        sends.start(part(across, h), part(across, h), recv_sems.at[across, h], mate)
    for i in (y * 2 + 1 - c, (1 - y) * 2 + 1 - c):
        for h in range(2):
            landed(part(i, h), recv_sems.at[i, h], mate)
    sends.finish()
    keep.wait()


def gather_group(value, number):
    if lax.axis_size("expert") != 8 or lax.axis_size("weight") != 4:
        return lax.all_gather(value, "weight", axis=0, tiled=True)
    out = jax.ShapeDtypeStruct((4,) + value.shape, value.dtype)
    return pl.pallas_call(
        gather_group_kernel,
        out_shape=out,
        in_specs=[pl.BlockSpec(memory_space=pltpu.VMEM)],
        out_specs=pl.BlockSpec(memory_space=pltpu.VMEM),
        scratch_shapes=[
            pltpu.SemaphoreType.DMA((6,)),
            pltpu.SemaphoreType.DMA((4, 2)),
            pltpu.SemaphoreType.DMA,
        ],
        compiler_params=pltpu.CompilerParams(collective_id=number, has_side_effects=True),
        cost_estimate=cost(0, value, out),
    )(value).reshape(-1, value.shape[1])


def sum_group_kernel(p_ref, out_ref, mates, sides, carried, send_sems, mate_sems, side_sems):
    z, x, y, c = places()
    rows = out_ref.shape[0]
    half = rows // 2
    side, mate = device(z, x, 1 - y, c), device(z, x, y, 1 - c)
    greet([(side, None), (mate, None)])
    sends = Sends(send_sems)

    for j, yy in enumerate((1 - y, y)):
        for h in range(2):
            part = pl.ds(h * half, half)
            sends.start(
                p_ref.at[yy * 2 + 1 - c, part], mates.at[j, part], mate_sems.at[j, h], mate
            )

    def add(target, sources, h):
        step = 16

        def body(i, carry):
            part = pl.ds(pl.multiple_of(h * half + i * step, step), step)
            total = sources[0][part].astype(jnp.float32)
            for source in sources[1:]:
                total = total + source[part].astype(jnp.float32)
            target[part] = total.astype(target.dtype)
            return carry

        lax.fori_loop(0, half // step, body, 0)

    for h in range(2):
        part = pl.ds(h * half, half)
        landed(mates.at[0, part], mate_sems.at[0, h], mate)
        add(carried, [p_ref.at[(1 - y) * 2 + c], mates.at[0]], h)
        sends.start(carried.at[part], sides.at[part], side_sems.at[h], side)
    for h in range(2):
        part = pl.ds(h * half, half)
        landed(mates.at[1, part], mate_sems.at[1, h], mate)
        landed(sides.at[part], side_sems.at[h], mate)
        add(out_ref, [p_ref.at[y * 2 + c], mates.at[1], sides], h)
    sends.finish()


def sum_group(value, number):
    if lax.axis_size("expert") != 8 or lax.axis_size("weight") != 4:
        summed = lax.psum_scatter(value, "weight", scatter_dimension=0, tiled=True)
        return summed.astype(jnp.float32)
    rows, width = value.shape[0] // 4, value.shape[1]
    value = value.reshape(4, rows, width)
    out = jax.ShapeDtypeStruct((rows, width), jnp.float32)
    return pl.pallas_call(
        sum_group_kernel,
        out_shape=out,
        in_specs=[pl.BlockSpec(memory_space=pltpu.VMEM)],
        out_specs=pl.BlockSpec(memory_space=pltpu.VMEM),
        scratch_shapes=[
            pltpu.VMEM((2, rows, width), value.dtype),
            pltpu.VMEM((rows, width), value.dtype),
            pltpu.VMEM((rows, width), value.dtype),
            pltpu.SemaphoreType.DMA((6,)),
            pltpu.SemaphoreType.DMA((2, 2)),
            pltpu.SemaphoreType.DMA((2,)),
        ],
        compiler_params=pltpu.CompilerParams(collective_id=number, has_side_effects=True),
        cost_estimate=cost(0, value, out),
    )(value)


def columns(start, size):
    return pl.ds(pl.multiple_of(start, lanes), size)


def add_block(target, sources, rows, row_start=0):
    step = 16

    def body(i, carry):
        part = pl.ds(pl.multiple_of(row_start + i * step, step), step)
        total = target[part].astype(jnp.float32)
        for source in sources:
            there = pl.ds(pl.multiple_of(i * step, step), step)
            total = total + source[there].astype(jnp.float32)
        target[part] = total.astype(target.dtype)
        return carry

    lax.fori_loop(0, rows // step, body, 0)


def total_kernel(
    top_ref,
    rest_ref,
    group_ref,
    out_ref,
    group_out,
    acc,
    mates,
    first_over,
    first_side,
    next_side,
    next_over,
    line,
    group_mates,
    group_sides,
    carried,
    send_sems,
    sems,
    mate_sems,
    side_sems,
):
    z, x, y, c = places()
    rows, width = out_ref.shape
    group_half = group_out.shape[0] // 2
    group_parts = [pl.ds(h * group_half, group_half) for h in range(2)]
    sources = [(top_ref, 0, 0), (rest_ref, top_ref.shape[0], 24)]
    half, quarter, eighth, sixteenth = width // 2, width // 4, width // 8, width // 16
    strip = rows // 4
    over, side, mate = device(z, 1 - x, y, c), device(z, x, 1 - y, c), device(z, x, y, 1 - c)
    others = [lax.rem(z + d, 4) for d in (1, 2, 3)]
    greet(
        [(over, None), (side, None), (mate, None)] + [(device(zz, x, y, c), None) for zz in others]
    )
    sends = Sends(send_sems)
    base = c * half
    for j in range(2):
        for p_ref, top, sem in sources:
            sends.start(
                p_ref.at[:, columns((1 - c) * half + j * quarter, quarter)],
                mates.at[pl.ds(top, p_ref.shape[0]), columns(j * quarter, quarter)],
                sems.at[sem + j],
                mate,
            )
    for i, yy in enumerate((1 - y, y)):
        for h, some in enumerate(group_parts):
            sends.start(
                group_ref.at[yy * 2 + 1 - c, some],
                group_mates.at[i, some],
                mate_sems.at[i, h],
                mate,
            )
    kept = (x * eighth + y * sixteenth, quarter + y * eighth + x * sixteenth)
    firsts, nexts = (first_over, first_side), (next_side, next_over)
    for j in range(2):
        part = columns(j * quarter, quarter)
        wide = 16
        for p_ref, top, sem in sources:
            landed(mates.at[pl.ds(top, p_ref.shape[0]), part], sems.at[sem + j], mate)

            def join(i, carry, j=j, p_ref=p_ref, top=top):
                mine = pl.ds(pl.multiple_of(i * wide, wide), wide)
                some = pl.ds(pl.multiple_of(top + i * wide, wide), wide)
                total = p_ref[mine, columns(base + j * quarter, quarter)].astype(jnp.float32)
                total = total + mates[some, columns(j * quarter, quarter)].astype(jnp.float32)
                acc[some, columns(j * quarter, quarter)] = total.astype(acc.dtype)
                return carry

            lax.fori_loop(0, p_ref.shape[0] // wide, join, 0)
        away = (1 - x) * eighth if j == 0 else quarter + (1 - y) * eighth
        sends.start(
            acc.at[:, columns(away, eighth)], firsts[j], sems.at[2 + j], (over, side)[j]
        )
    for h, some in enumerate(group_parts):
        landed(group_mates.at[0, some], mate_sems.at[0, h], mate)
        add_into(
            carried,
            [group_ref.at[(1 - y) * 2 + c], group_mates.at[0]],
            h * group_half,
            group_half,
        )
        sends.start(carried.at[some], group_sides.at[some], side_sems.at[h], side)
    for j in range(2):
        landed(firsts[j], sems.at[2 + j], mate)
        near = x * eighth if j == 0 else quarter + y * eighth
        add_block(acc.at[:, columns(near, eighth)], [firsts[j]], rows)
        away = near + ((1 - y) if j == 0 else (1 - x)) * sixteenth
        sends.start(
            acc.at[:, columns(away, sixteenth)], nexts[j], sems.at[4 + j], (side, over)[j]
        )
    for j in range(2):
        landed(nexts[j], sems.at[4 + j], mate)
        add_block(acc.at[:, columns(kept[j], sixteenth)], [nexts[j]], rows)
        for d, zz in enumerate(others):
            sends.start(
                acc.at[pl.ds(pl.multiple_of(zz * strip, 16), strip), columns(kept[j], sixteenth)],
                line.at[j, d],
                sems.at[6 + j * 3 + d],
                device(zz, x, y, c),
            )
    strip_here = pl.multiple_of(z * strip, 16)
    for j in range(2):
        for d in range(3):
            landed(line.at[j, d], sems.at[6 + j * 3 + d], mate)
        block = acc.at[:, columns(kept[j], sixteenth)]
        add_block(block, [line.at[j, d] for d in range(3)], strip, strip_here)

        def place(i, carry, j=j):
            some = pl.ds(pl.multiple_of(strip_here + i * 16, 16), 16)
            out_ref[some, columns(base + kept[j], sixteenth)] = acc[
                some, columns(kept[j], sixteenth)
            ]
            return carry

        lax.fori_loop(0, strip // 16, place, 0)
        done = out_ref.at[pl.ds(strip_here, strip), columns(base + kept[j], sixteenth)]
        for d, zz in enumerate(others):
            sends.start(done, done, sems.at[12 + j * 3 + d], device(zz, x, y, c))
    for j in range(2):
        for d in range(3):
            source = pl.multiple_of(lax.rem(z + 3 - d, 4) * strip, 16)
            landed(
                out_ref.at[pl.ds(source, strip), columns(base + kept[j], sixteenth)],
                sems.at[12 + j * 3 + d],
                mate,
            )
        part = out_ref.at[:, columns(base + kept[j], sixteenth)]
        sends.start(part, part, sems.at[18 + j], (side, over)[j])
    others_kept = (
        x * eighth + (1 - y) * sixteenth,
        quarter + y * eighth + (1 - x) * sixteenth,
    )
    for j in range(2):
        landed(out_ref.at[:, columns(base + others_kept[j], sixteenth)], sems.at[18 + j], mate)
        near = x * eighth if j == 0 else quarter + y * eighth
        part = out_ref.at[:, columns(base + near, eighth)]
        sends.start(part, part, sems.at[20 + j], (over, side)[j])
    for j in range(2):
        away = (1 - x) * eighth if j == 0 else quarter + (1 - y) * eighth
        landed(out_ref.at[:, columns(base + away, eighth)], sems.at[20 + j], mate)
        part = out_ref.at[:, columns(base + j * quarter, quarter)]
        sends.start(part, part, sems.at[22 + j], mate)
    for h, some in enumerate(group_parts):
        landed(group_mates.at[1, some], mate_sems.at[1, h], mate)
        landed(group_sides.at[some], side_sems.at[h], mate)
        add_into(
            group_out,
            [group_ref.at[y * 2 + c], group_mates.at[1], group_sides],
            h * group_half,
            group_half,
        )
    for j in range(2):
        landed(
            out_ref.at[:, columns((1 - c) * half + j * quarter, quarter)], sems.at[22 + j], mate
        )
    sends.finish()


def total_over_all(top, rest, group, number):
    if lax.axis_size("expert") != 8 or lax.axis_size("weight") != 4:
        value = jnp.concatenate([top, rest], axis=0).astype(jnp.float32)
        return lax.psum(value, ("expert", "weight")), sum_group(group, number)
    rows, width = top.shape[0] + rest.shape[0], top.shape[1]
    group = group.reshape(4, -1, width)
    group_rows = group.shape[1]
    out = jax.ShapeDtypeStruct((rows, width), top.dtype)
    group_out = jax.ShapeDtypeStruct((group_rows, width), jnp.float32)
    buffer = lambda n: pltpu.VMEM((rows, n), top.dtype)
    return pl.pallas_call(
        total_kernel,
        out_shape=[out, group_out],
        in_specs=[pl.BlockSpec(memory_space=pltpu.VMEM)] * 3,
        out_specs=[pl.BlockSpec(memory_space=pltpu.VMEM)] * 2,
        scratch_shapes=[
            buffer(width // 2),
            buffer(width // 2),
            buffer(width // 8),
            buffer(width // 8),
            buffer(width // 16),
            buffer(width // 16),
            pltpu.VMEM((2, 3, rows // 4, width // 16), top.dtype),
            pltpu.VMEM((2, group_rows, width), group.dtype),
            pltpu.VMEM((group_rows, width), group.dtype),
            pltpu.VMEM((group_rows, width), group.dtype),
            pltpu.SemaphoreType.DMA((32,)),
            pltpu.SemaphoreType.DMA((26,)),
            pltpu.SemaphoreType.DMA((2, 2)),
            pltpu.SemaphoreType.DMA((2,)),
        ],
        compiler_params=pltpu.CompilerParams(
            collective_id=number, has_side_effects=True, vmem_limit_bytes=vmem_limit
        ),
        cost_estimate=cost(0, top, rest, group, out, group_out),
    )(top, rest, group)


def shared_kernel(turn, ins, outs):
    normed_ref, cotangent_ref, gate_grad_ref, lift_grad_ref, hidden_ref = ins

    @pl.when(turn == 0)
    def _():
        for out_ref in outs:
            out_ref[...] = jnp.zeros_like(out_ref)

    normed, cotangent = normed_ref[...], cotangent_ref[...]
    outs[0][...] += trans_times(gate_grad_ref[...], normed)
    outs[1][...] += trans_times(lift_grad_ref[...], normed)
    outs[2][...] += trans_times(hidden_ref[...], cotangent)


def weight_kernel(turn, ins, outs):
    rows_ref, grads_ref, gate_grad_ref, lift_grad_ref, hidden_ref = ins
    rows = rows_ref[0]
    for out_ref, left_ref, right in (
        (outs[0], gate_grad_ref, rows),
        (outs[1], lift_grad_ref, rows),
        (outs[2], hidden_ref, grads_ref[0]),
    ):
        out_ref[0] = trans_times(left_ref[0], right).astype(out_ref.dtype)


def weights_alone(*refs):
    weight_kernel(pl.program_id(0), refs[:5], refs[5:])


def gradients_kernel(turn, ins, outs):
    shared_kernel(turn, ins[:5], outs[:3])
    weight_kernel(turn, ins[5:], outs[3:])


def per_device(
    tokens,
    cotangent,
    segments,
    routes,
    first_gain,
    query_weight,
    latent_weight,
    latent_gain,
    expand_weight,
    output_weight,
    second_gain,
    router_weight,
    shared_gate,
    shared_up,
    shared_down,
    expert_gate,
    expert_up,
    expert_down,
):
    weight_count = lax.axis_size("weight")
    token_rows = tokens.shape[0]
    width = tokens.shape[1]
    group_rows = token_rows * weight_count
    query_width = NOPE + ROPE
    heads_here = query_weight.shape[1] // query_width
    expert_count = router_weight.shape[1]
    local_experts = expert_gate.shape[0]
    score_scale = query_width ** (-0.5)
    activations = tokens.astype(jnp.float32)
    first_scale = inv_rms(activations)
    normed = (activations * first_scale * first_gain).astype(jnp.bfloat16)
    both = ("expert", "weight")
    expert_index = lax.axis_index("expert")
    expert_lanes = lax.axis_size("expert")
    blocks = expert_lanes * weight_count
    pairs, quads = blocks // 2, blocks // 4
    pair_rows, quad_rows = 2 * token_rows, 4 * token_rows
    all_rows = blocks * token_rows
    slot_rows = blocks * CAP
    choose = (
        routes[:, :, None] == jnp.arange(expert_count, dtype=jnp.int32)[None, None, :]
    ).astype(jnp.float32)
    hit = jnp.sum(choose, axis=1)
    order = jnp.arange(token_rows, dtype=jnp.int32)
    before = (order[None, :] < order[:, None]).astype(jnp.bfloat16)
    place = matmul(before, hit.astype(jnp.bfloat16))
    rank = jnp.sum(choose * jnp.arange(routes.shape[1], dtype=jnp.float32)[None, :, None], axis=1)
    code = jnp.where(hit > 0, 32.0 * rank + place, -1.0)
    extra = jnp.pad(code, ((0, 0), (0, lanes - expert_count)), constant_values=-1.0)
    cotangent_wide = jnp.concatenate([cotangent, extra.astype(jnp.bfloat16)], axis=1)
    column = jnp.arange(lanes, dtype=jnp.int32)[None, :]
    row = jnp.arange(8, dtype=jnp.int32)[:, None]
    first_here = expert_index * local_experts
    here = (row < local_experts) & (column == first_here + row)
    twice = here | ((row < local_experts) & (column == first_here + row + expert_count))
    here, twice = here.astype(jnp.bfloat16), twice.astype(jnp.bfloat16)
    weight_index = lax.axis_index("weight")
    high_column = 2 * (row * weight_count + weight_index)
    known = row < routes.shape[1]
    high_at = (known & (column == high_column)).astype(jnp.bfloat16)
    low_at = (known & (column == high_column + 1)).astype(jnp.bfloat16)
    shared_here = shared_gate.shape[1] // expert_lanes
    shared_wide = -(-shared_here // lanes) * lanes
    start = expert_index * shared_here

    def shared_part(matrix):
        part = lax.dynamic_slice_in_dim(matrix, start, shared_here, axis=0)
        return jnp.pad(part, ((0, shared_wide - shared_here), (0, 0)))

    gate_part = shared_part(shared_gate.T)
    up_part = shared_part(shared_up.T)
    down_part = shared_part(shared_down)
    shape = jax.ShapeDtypeStruct
    whole = lambda array: (array, whole_spec(array))
    slots = shape((local_experts, slot_rows, width), jnp.bfloat16)
    slots_one = shape((local_experts, slot_rows, lanes), jnp.float32)
    gather_flops = 2 * all_rows * width * (2 * CAP * local_experts + shared_wide)
    cosine, sine = rope_tables(segments[0])
    allowed = attention_mask(segments[0])
    sizes = (expert_lanes, weight_count)
    if sizes == (8, 4):
        (
            cotangent_all,
            normed_all,
            query,
            latent,
            latent_scale,
            latent_normed,
            key_rope,
            expanded,
            log_total,
            mixed,
            attended,
        ) = attention_forward(
            score_scale,
            normed,
            cotangent_wide,
            cosine,
            sine,
            segments[0],
            latent_gain,
            query_weight,
            latent_weight,
            expand_weight,
            output_weight,
            0,
        )
        cotangent_all = cotangent_all.reshape(all_rows, -1)
        normed_all = normed_all.reshape(group_rows, width)
        latent_scale, log_total = latent_scale[:, :1], log_total[:, :, :1]
        query = query.transpose(1, 0, 2)
        expanded = expanded.reshape(group_rows, heads_here, NOPE + VDIM)
    else:
        cotangent_all = lax.all_gather(cotangent_wide, both, axis=0, tiled=True)
        normed_all = gather_group(normed, 0)
        query_full = matmul(normed_all, query_weight).reshape(group_rows, heads_here, query_width)
        query = jnp.concatenate(
            [
                query_full[..., :NOPE],
                rotate(query_full[..., NOPE:], cosine[:, None, :], sine[:, None, :]),
            ],
            axis=-1,
        ).astype(jnp.bfloat16)
        compressed = matmul(normed_all, latent_weight)
        latent = compressed[:, :LATENT]
        latent_scale = inv_rms(latent)
        latent_normed = (latent * latent_scale * latent_gain).astype(jnp.bfloat16)
        key_rope = rotate(compressed[:, LATENT:], cosine, sine).astype(jnp.bfloat16)
        expanded = (
            matmul(latent_normed, expand_weight)
            .astype(jnp.bfloat16)
            .reshape(group_rows, heads_here, NOPE + VDIM)
        )
    key_nope = expanded[..., :NOPE]
    values = expanded[..., NOPE:]

    def score_block():
        raw = jnp.einsum(
            "ihd,jhd->hij", query[..., :NOPE], key_nope, preferred_element_type=jnp.float32
        )
        raw = raw + jnp.einsum(
            "ihd,jd->hij", query[..., NOPE:], key_rope, preferred_element_type=jnp.float32
        )
        return jnp.where(allowed[None], raw * score_scale, -1e30)

    if sizes != (8, 4):
        scores = score_block()
        peak = jnp.max(scores, axis=-1, keepdims=True)
        weights = jnp.exp(scores - peak)
        total = jnp.sum(weights, axis=-1, keepdims=True)
        log_total = peak + jnp.log(total)
        mixed = jnp.einsum(
            "hij,jhd->ihd",
            (weights / total).astype(jnp.bfloat16),
            values,
            preferred_element_type=jnp.float32,
        )
        mixed = mixed.astype(jnp.bfloat16).reshape(group_rows, heads_here * VDIM)
        attended = sum_group(matmul(mixed, output_weight).astype(jnp.bfloat16), 1)
    hidden_one = activations + attended
    second_scale = inv_rms(hidden_one)
    normed_two = (hidden_one * second_scale * second_gain).astype(jnp.bfloat16)
    gates = jax.nn.sigmoid(matmul(normed_two, router_weight))
    chosen = jnp.sum(choose * gates[:, None, :], axis=-1)
    chosen_total = jnp.sum(chosen, axis=1, keepdims=True)
    mixing = route_scale * chosen / chosen_total
    upstream = cotangent.astype(jnp.float32)
    mixing_at = jnp.sum(choose * mixing[:, :, None], axis=1)
    mixing_high = mixing_at.astype(jnp.bfloat16)
    mixing_low = (mixing_at - mixing_high.astype(jnp.float32)).astype(jnp.bfloat16)
    normed_wide = jnp.concatenate([normed_two, mixing_high, mixing_low], axis=1)
    marks = (cotangent_all, pl.BlockSpec((quad_rows, lanes), lambda i: (i, width // lanes)))
    normed_tokens, (grads_slots, shared_raw) = gather_all(
        normed_wide,
        2,
        functools.partial(grads_kernel, pair_rows),
        quads,
        [whole(here), (cotangent_all, pair_spec(cotangent_all, quads)), whole(down_part)],
        [
            (slots, slots_spec(slots, quads)),
            (shape((all_rows, shared_wide), jnp.float32), pl.BlockSpec((quad_rows, shared_wide), lambda i: (i, 0))),
        ],
        gather_flops,
    )
    normed_tokens = normed_tokens.reshape(all_rows, -1)
    token_spec = pl.BlockSpec((quad_rows, shared_wide), lambda i: (i, 0))
    token_shape = shape((all_rows, shared_wide), jnp.bfloat16)
    rows_slots, mix_slots, shared_hidden, shared_gate_grad, shared_lift_grad = call(
        functools.partial(rows_kernel, pair_rows),
        quads,
        [
            whole(here),
            whole(twice),
            marks,
            (normed_tokens, pair_spec(normed_tokens, quads)),
            (shared_raw, token_spec),
            whole(gate_part),
            whole(up_part),
        ],
        [
            (slots, slots_spec(slots, quads)),
            (slots_one, slots_spec(slots_one, quads)),
            (token_shape, token_spec),
            (token_shape, token_spec),
            (token_shape, token_spec),
        ],
        gather_flops + 2 * all_rows * width * shared_wide,
    )
    hidden_here = expert_gate.shape[2]
    gate_rows, up_rows = expert_gate.transpose(0, 2, 1), expert_up.transpose(0, 2, 1)

    def tile_spec(rows, n):
        per = slot_rows // rows
        return pl.BlockSpec((1, rows, n), lambda i: (i // per, i % per, 0))

    def expert_spec(rows, matrix):
        per = slot_rows // rows
        return pl.BlockSpec((1,) + matrix.shape[1:], lambda i: (i // per, 0, 0))

    large, small = 32 * CAP, 16 * CAP
    narrow = shape((local_experts, slot_rows, hidden_here), jnp.bfloat16)
    one_matmul = 2 * local_experts * slot_rows * width * hidden_here
    routed_hidden, mixed_hidden, slope, active, produced = call(
        forward_kernel,
        local_experts * (slot_rows // large),
        [
            (rows_slots, tile_spec(large, width)),
            (mix_slots, tile_spec(large, lanes)),
            (gate_rows, expert_spec(large, gate_rows)),
            (up_rows, expert_spec(large, up_rows)),
            (expert_down, expert_spec(large, expert_down)),
        ],
        [(narrow, tile_spec(large, hidden_here))] * 4 + [(slots, tile_spec(large, width))],
        3 * one_matmul,
    )
    dense = shape((all_rows, width), jnp.bfloat16)
    dense_wide = shape((all_rows, width + lanes), jnp.bfloat16)
    (out_dense,) = call(
        functools.partial(out_kernel, pair_rows),
        quads,
        [
            whole(here),
            marks,
            (produced, slots_spec(slots, quads)),
            (shared_hidden, token_spec),
            whole(down_part),
        ],
        [(dense, pair_spec(dense, quads))],
        gather_flops,
    )
    narrow_tile = tile_spec(small, hidden_here)
    routed_out, (gate_grad, lift_grad, returned, mix_grad_slots) = sum_all(
        out_dense.reshape(blocks, token_rows, width),
        6,
        backward_kernel,
        local_experts * (slot_rows // small),
        [
            (grads_slots, tile_spec(small, width)),
            (routed_hidden, narrow_tile),
            (slope, narrow_tile),
            (active, narrow_tile),
            (gate_rows, expert_spec(small, gate_rows)),
            (up_rows, expert_spec(small, up_rows)),
            (expert_down, expert_spec(small, expert_down)),
        ],
        [
            (narrow, narrow_tile),
            (narrow, narrow_tile),
            (slots, tile_spec(small, width)),
            (slots_one, tile_spec(small, lanes)),
        ],
        3 * one_matmul,
    )
    (back_dense,) = call(
        functools.partial(back_kernel, pair_rows),
        quads,
        [
            whole(here),
            whole(high_at),
            whole(low_at),
            marks,
            (returned, slots_spec(slots, quads)),
            (mix_grad_slots, slots_spec(slots_one, quads)),
            (shared_gate_grad, token_spec),
            (shared_lift_grad, token_spec),
            whole(gate_part),
            whole(up_part),
        ],
        [(dense_wide, pair_spec(dense_wide, quads))],
        gather_flops + 2 * all_rows * width * shared_wide,
    )
    shared_sum = shape((shared_wide, width), jnp.float32)
    shared_out = (shared_sum, whole_spec(shared_sum))
    plain_spec = pl.BlockSpec((pair_rows, width), lambda i: (i, 0))
    shared_spec = pl.BlockSpec((pair_rows, shared_wide), lambda i: (i, 0))
    column_half = width // 2
    half_spec = lambda m: pl.BlockSpec((1, m, column_half), lambda i: (i // 2, 0, i % 2))
    narrow_spec = pl.BlockSpec((1, slot_rows, hidden_here), lambda i: (i // 2, 0, 0))
    shared_ins = [
        (normed_tokens, plain_spec),
        (cotangent_all, plain_spec),
        (shared_gate_grad, shared_spec),
        (shared_lift_grad, shared_spec),
        (shared_hidden, shared_spec),
    ]
    weight_ins = [
        (rows_slots, half_spec(slot_rows)),
        (grads_slots, half_spec(slot_rows)),
        (gate_grad, narrow_spec),
        (lift_grad, narrow_spec),
        (mixed_hidden, narrow_spec),
    ]
    back_blocks = back_dense.reshape(blocks, token_rows, -1)
    shared_flops = 6 * all_rows * width * shared_wide
    together = pairs == 2 * local_experts
    weight_type = jnp.bfloat16 if together else jnp.float32
    weight_shape = shape((local_experts, hidden_here, width), weight_type)
    weight_outs = [(weight_shape, half_spec(hidden_here))] * 3
    if together:
        back_here, sums = sum_all(
            back_blocks,
            3,
            gradients_kernel,
            pairs,
            shared_ins + weight_ins,
            [shared_out] * 3 + weight_outs,
            shared_flops + 3 * one_matmul,
        )
        shared_sums = sums[:3]
        weight_grads = [value.astype(jnp.float32) for value in sums[3:]]
    else:
        back_here, shared_sums = sum_all(
            back_blocks, 3, shared_kernel, pairs, shared_ins, [shared_out] * 3, shared_flops
        )
        weight_grads = call(
            weights_alone, 2 * local_experts, weight_ins, weight_outs, 3 * one_matmul
        )
    routed_back = back_here[:, :width]
    mix_grad = back_here[:, width : width + 2 * weight_count * routes.shape[1]]
    mix_grad = jnp.sum(mix_grad.reshape(token_rows, routes.shape[1], -1), axis=2)
    shared_grads = jnp.concatenate([total[:shared_here] for total in shared_sums], axis=0)
    shared_grads = shared_grads.astype(jnp.bfloat16)
    swapped = lax.all_to_all(shared_grads, "expert", split_axis=1, concat_axis=0, tiled=True)
    swapped = swapped.reshape(expert_lanes, 3, shared_here, -1).astype(jnp.float32)
    shared_gradients = [swapped[:, i].reshape(expert_lanes * shared_here, -1) for i in range(3)]
    chosen_grad = route_scale * (
        mix_grad / chosen_total
        - jnp.sum(mix_grad * chosen, axis=1, keepdims=True) / chosen_total**2
    )
    logit_grad = jnp.sum(choose * chosen_grad[:, :, None], axis=1) * gates * (1.0 - gates)
    normed_two_grad = (
        routed_back
        + jnp.dot(logit_grad, router_weight.astype(jnp.float32).T, precision=highest)
    )
    router_gradient = jnp.dot(logit_grad.T, normed_two.astype(jnp.float32), precision=highest)
    back_two, second_gain_gradient = norm_back(
        normed_two_grad, hidden_one, second_scale, second_gain
    )
    hidden_grad = upstream + back_two
    hidden_group = gather_group(hidden_grad.astype(jnp.bfloat16), 4)
    output_gradient = trans_times(hidden_group, mixed).astype(jnp.bfloat16)
    hidden_group, output_gradient = lax.optimization_barrier((hidden_group, output_gradient))
    output_shard = lax.psum_scatter(output_gradient, "expert", scatter_dimension=0, tiled=True)
    mixed_grad = (
        times_trans(hidden_group, output_weight)
        .astype(jnp.bfloat16)
        .reshape(group_rows, heads_here, VDIM)
    )
    probs = jnp.exp(score_block() - log_total)
    prob_grad = jnp.einsum("ihd,jhd->hij", mixed_grad, values, preferred_element_type=jnp.float32)
    centre = jnp.sum(probs * prob_grad, axis=-1, keepdims=True)
    score_grad = (probs * (prob_grad - centre)).astype(jnp.bfloat16)
    value_grad = jnp.einsum(
        "hij,ihd->jhd", probs.astype(jnp.bfloat16), mixed_grad, preferred_element_type=jnp.float32
    )
    query_nope_grad = (
        jnp.einsum("hij,jhd->ihd", score_grad, key_nope, preferred_element_type=jnp.float32)
        * score_scale
    )
    query_rope_grad = (
        jnp.einsum("hij,jd->ihd", score_grad, key_rope, preferred_element_type=jnp.float32)
        * score_scale
    )
    key_nope_grad = (
        jnp.einsum(
            "hij,ihd->jhd", score_grad, query[..., :NOPE], preferred_element_type=jnp.float32
        )
        * score_scale
    )
    key_rope_grad = (
        jnp.einsum("hij,ihd->jd", score_grad, query[..., NOPE:], preferred_element_type=jnp.float32)
        * score_scale
    )
    query_grad = jnp.concatenate(
        [query_nope_grad, unrotate(query_rope_grad, cosine[:, None, :], sine[:, None, :])], axis=-1
    )
    query_grad = query_grad.astype(jnp.bfloat16).reshape(group_rows, heads_here * query_width)
    expand_grad = (
        jnp.concatenate([key_nope_grad, value_grad], axis=-1)
        .astype(jnp.bfloat16)
        .reshape(group_rows, heads_here * (NOPE + VDIM))
    )
    expert_grads = (weight_grads[0].transpose(0, 2, 1), weight_grads[1].transpose(0, 2, 1), weight_grads[2])
    layer_out = (hidden_one + routed_out).astype(jnp.bfloat16)
    query_gradient = trans_times(normed_all, query_grad)
    expand_gradient = trans_times(latent_normed, expand_grad).astype(jnp.bfloat16)
    latent_normed_grad = times_trans(expand_grad, expand_weight)
    latent_back, latent_gain_gradient = norm_back(
        latent_normed_grad, latent, latent_scale, latent_gain
    )
    compressed_grad = jnp.concatenate([latent_back, unrotate(key_rope_grad, cosine, sine)], axis=-1)
    compressed_grad = compressed_grad.astype(jnp.bfloat16)
    latent_weight_gradient = trans_times(compressed_grad, normed_all)
    normed_part = times_trans(query_grad, query_weight) + times_trans(compressed_grad, latent_weight)
    first_gain_gradient = jnp.sum(normed_part * normed_all.astype(jnp.float32), axis=0) / first_gain
    shards = (
        lax.psum_scatter(
            query_gradient.astype(jnp.bfloat16), "expert", scatter_dimension=0, tiled=True
        ).astype(jnp.float32),
        lax.psum_scatter(
            expand_gradient, "expert", scatter_dimension=0, tiled=True
        ).astype(jnp.float32),
        output_shard.T.astype(jnp.float32),
    )
    latent_columns = latent_weight.shape[1]
    rest = jnp.concatenate(
        [
            router_gradient,
            first_gain_gradient[None],
            second_gain_gradient[None],
            jnp.pad(latent_gain_gradient, (0, width - LATENT))[None],
        ],
        axis=0,
    ).astype(jnp.bfloat16)
    wanted = -(-(latent_columns + rest.shape[0]) // 64) * 64 - latent_columns
    rest = jnp.pad(rest, ((0, wanted - rest.shape[0]), (0, 0)))
    total, normed_grad = total_over_all(
        latent_weight_gradient.astype(jnp.bfloat16), rest, normed_part.astype(jnp.bfloat16), 7
    )
    back_one, _ = norm_back(normed_grad, activations, first_scale, first_gain)
    token_gradient = hidden_grad + back_one
    gains_at = latent_columns + expert_count
    wide = lambda value: value.astype(jnp.float32)
    totals = (
        wide(total[:latent_columns]).T,
        wide(total[gains_at + 2, :LATENT]),
        wide(total[latent_columns:gains_at]).T,
        wide(total[gains_at]),
        wide(total[gains_at + 1]),
    )
    return (
        layer_out,
        token_gradient,
        totals[3],
        shards[0],
        totals[0],
        totals[1],
        shards[1],
        shards[2],
        totals[4],
        totals[2],
        shared_gradients[0].T,
        shared_gradients[1].T,
        shared_gradients[2],
        expert_grads[0],
        expert_grads[1],
        expert_grads[2],
    )


def solution(mesh):
    return jax.shard_map(
        per_device,
        mesh=mesh,
        in_specs=(
            P(("expert", "weight"), None),
            P(("expert", "weight"), None),
            P("expert", None),
            P(("expert", "weight"), None),
            P(),
            P(None, "weight"),
            P(),
            P(),
            P(None, "weight"),
            P("weight", None),
            P(),
            P(),
            P(None, "weight"),
            P(None, "weight"),
            P("weight", None),
            P("expert", None, "weight"),
            P("expert", None, "weight"),
            P("expert", "weight", None),
        ),
        out_specs=(
            P(("expert", "weight"), None),
            P(("expert", "weight"), None),
            P(),
            P("expert", "weight"),
            P(),
            P(),
            P("expert", "weight"),
            P("weight", "expert"),
            P(),
            P(),
            P("expert", "weight"),
            P("expert", "weight"),
            P("weight", "expert"),
            P("expert", None, "weight"),
            P("expert", None, "weight"),
            P("expert", "weight", None),
        ),
        check_vma=False,
    )
```

```python
import functools

import jax
import jax.numpy as jnp
from jax import lax
from jax.experimental import pallas as pl
from jax.experimental.pallas import tpu as pltpu
from jax.sharding import PartitionSpec as P

NOPE = 128
ROPE = 64
VDIM = 128
LATENT = 512
CAP = 20


eps = 1e-06
route_scale = 2.446
rope_base = 50000.0
highest = lax.Precision.HIGHEST


def matmul(left, right):
    return jnp.dot(left, right, preferred_element_type=jnp.float32)


def trans_times(left, right):
    return lax.dot_general(
        left, right, (((0,), (0,)), ((), ())), preferred_element_type=jnp.float32
    )


def times_trans(left, right):
    return lax.dot_general(
        left, right, (((1,), (1,)), ((), ())), preferred_element_type=jnp.float32
    )


def inv_rms(value):
    return lax.rsqrt(jnp.mean(value * value, axis=-1, keepdims=True) + eps)


def norm_back(grad_out, value, scale, gain):
    scaled = grad_out * gain
    grad_in = scale * scaled - value * scale**3 * jnp.mean(scaled * value, axis=-1, keepdims=True)
    gain_grad = jnp.sum(grad_out * value * scale, axis=0)
    return (grad_in, gain_grad)


def rope_tables(seg):
    size = seg.shape[0]
    index = jnp.arange(size, dtype=jnp.int32)
    earlier = jnp.sum((seg[None, :] < seg[:, None]).astype(jnp.int32), axis=1)
    place = (index - earlier).astype(jnp.float32)
    half = ROPE // 2
    freqs = rope_base ** (-(jnp.arange(half, dtype=jnp.float32) * 2.0 / ROPE))
    angle = place[:, None] * freqs[None, :]
    return (jnp.cos(angle), jnp.sin(angle))


def attention_mask(seg):
    index = jnp.arange(seg.shape[0], dtype=jnp.int32)
    return (seg[:, None] == seg[None, :]) & (index[None, :] <= index[:, None])


def rotate(value, cosine, sine):
    half = value.shape[-1] // 2
    first, second = (value[..., :half], value[..., half:])
    return jnp.concatenate(
        [first * cosine - second * sine, second * cosine + first * sine], axis=-1
    )


def unrotate(value, cosine, sine):
    half = value.shape[-1] // 2
    first, second = (value[..., :half], value[..., half:])
    return jnp.concatenate(
        [first * cosine + second * sine, second * cosine - first * sine], axis=-1
    )


lanes = 128
vmem_limit = 64 * 1024 * 1024 - 131072


def token_slots(marks, here, local_experts, half):
    codes = times_trans(here, marks)
    count = codes.shape[1]
    rank = jnp.floor(codes * (1.0 / 32.0))
    place = codes - 32.0 * rank
    token = lax.broadcasted_iota(jnp.int32, codes.shape, 1)
    slot = jnp.where(codes >= 0, place + jnp.where(token >= half, float(CAP), 0.0), -1.0)
    row = lax.broadcasted_iota(jnp.int32, (2 * CAP, count), 0).astype(jnp.float32)
    picks = [jnp.where(row == slot[e : e + 1], 1.0, 0.0) for e in range(local_experts)]
    return picks, rank


def pair_slots(marks_ref, here_ref, local_experts, pair):
    count = marks_ref.shape[0] // pair
    return [
        token_slots(marks_ref[j * pair : (j + 1) * pair], here_ref[...], local_experts, pair // 2)
        for j in range(count)
    ]


def slot_part(value, e):
    return value[e * 2 * CAP : (e + 1) * 2 * CAP]


def gather_rows(slots, values, pair, out_ref):
    rows = [
        jnp.dot(
            jnp.concatenate(picks, axis=0).astype(jnp.bfloat16),
            values[j * pair : (j + 1) * pair],
            preferred_element_type=jnp.float32,
        )
        for j, (picks, _) in enumerate(slots)
    ]
    for e in range(out_ref.shape[0]):
        together = jnp.concatenate([slot_part(value, e) for value in rows], axis=0)
        out_ref[e] = together.astype(jnp.bfloat16)


def spread_rows(slots, rows_ref):
    local_experts = rows_ref.shape[0]
    rows = [rows_ref[e].astype(jnp.float32) for e in range(local_experts)]
    totals = []
    for j, (picks, _) in enumerate(slots):
        part = jnp.concatenate([slot_part(value, j) for value in rows], axis=0)
        pick = jnp.concatenate(picks, axis=0).astype(jnp.bfloat16)
        totals.append(trans_times(pick, part.astype(jnp.bfloat16)))
    return jnp.concatenate(totals, axis=0)


def grads_kernel(pair, turn, ins, outs):
    here_ref, value_ref, down_ref = ins
    rows_ref, back_ref = outs
    width = rows_ref.shape[2]
    slots = pair_slots(value_ref.at[:, width:], here_ref, rows_ref.shape[0], pair)
    values = value_ref[:, :width]
    gather_rows(slots, values, pair, rows_ref)
    back_ref[...] = times_trans(values, down_ref[...])


def rows_kernel(
    pair,
    here_ref,
    twice_ref,
    marks_ref,
    value_ref,
    back_ref,
    gate_ref,
    up_ref,
    rows_ref,
    mix_ref,
    hidden_ref,
    gate_grad_ref,
    lift_grad_ref,
):
    width = rows_ref.shape[2]
    slots = pair_slots(marks_ref, here_ref, rows_ref.shape[0], pair)
    values = value_ref[:, :width]
    gather_rows(slots, values, pair, rows_ref)
    for j, (picks, _) in enumerate(slots):
        mixing = times_trans(twice_ref[...], value_ref[j * pair : (j + 1) * pair, width:])
        for e, pick in enumerate(picks):
            column = jnp.sum(pick * mixing[e : e + 1], axis=1, keepdims=True)
            column = jnp.broadcast_to(column, (2 * CAP, lanes))
            mix_ref[e, j * 2 * CAP : (j + 1) * 2 * CAP] = column
    gate = times_trans(values, gate_ref[...])
    lift = times_trans(values, up_ref[...])
    back = back_ref[...]
    sigma = jax.nn.sigmoid(gate)
    active = gate * sigma
    hidden_ref[...] = (active * lift).astype(jnp.bfloat16)
    gate_grad_ref[...] = (back * lift * sigma * (1.0 + gate * (1.0 - sigma))).astype(jnp.bfloat16)
    lift_grad_ref[...] = (back * active).astype(jnp.bfloat16)


def forward_kernel(
    rows_ref,
    mix_ref,
    gate_ref,
    up_ref,
    down_ref,
    hidden_ref,
    mixed_ref,
    slope_ref,
    active_ref,
    produced_ref,
):
    rows = rows_ref[0]
    gate = times_trans(rows, gate_ref[0])
    lift = times_trans(rows, up_ref[0])
    mix = mix_ref[0][:, :1]
    sigma = jax.nn.sigmoid(gate)
    active = gate * sigma
    hidden = active * lift
    mixed_hidden = (mix * hidden).astype(jnp.bfloat16)
    hidden_ref[0] = hidden.astype(jnp.bfloat16)
    mixed_ref[0] = mixed_hidden
    slope_ref[0] = (mix * lift * sigma * (1.0 + gate * (1.0 - sigma))).astype(jnp.bfloat16)
    active_ref[0] = (mix * active).astype(jnp.bfloat16)
    produced_ref[0] = matmul(mixed_hidden, down_ref[0]).astype(jnp.bfloat16)


def backward_kernel(turn, ins, outs):
    grads_ref, hidden_ref, slope_ref, active_ref, gate_ref, up_ref, down_ref = ins
    gate_grad_ref, lift_grad_ref, returned_ref, mix_grad_ref = outs
    back = times_trans(grads_ref[0], down_ref[0])
    mix_grad = jnp.sum(hidden_ref[0].astype(jnp.float32) * back, axis=1, keepdims=True)
    mix_grad_ref[0] = jnp.broadcast_to(mix_grad, mix_grad_ref.shape[1:])
    gate_grad = (back * slope_ref[0].astype(jnp.float32)).astype(jnp.bfloat16)
    lift_grad = (back * active_ref[0].astype(jnp.float32)).astype(jnp.bfloat16)
    gate_grad_ref[0] = gate_grad
    lift_grad_ref[0] = lift_grad
    returned = matmul(gate_grad, gate_ref[0]) + matmul(lift_grad, up_ref[0])
    returned_ref[0] = returned.astype(jnp.bfloat16)


def back_kernel(
    pair,
    here_ref,
    high_ref,
    low_ref,
    marks_ref,
    rows_ref,
    mix_grad_ref,
    gate_grad_ref,
    lift_grad_ref,
    gate_ref,
    up_ref,
    out_ref,
):
    width = rows_ref.shape[2]
    slots = pair_slots(marks_ref, here_ref, rows_ref.shape[0], pair)
    total = spread_rows(slots, rows_ref)
    total = total + matmul(gate_grad_ref[...], gate_ref[...])
    total = total + matmul(lift_grad_ref[...], up_ref[...])
    out_ref[:, :width] = total.astype(jnp.bfloat16)
    for j, (picks, rank) in enumerate(slots):
        choice = lax.broadcasted_iota(jnp.int32, rank.shape, 0).astype(jnp.float32)
        mix_grad = jnp.zeros(rank.shape, jnp.float32)
        for e, pick in enumerate(picks):
            column = slot_part(mix_grad_ref[e], j)[:, :1]
            row = jnp.sum(pick * column, axis=0, keepdims=True)
            mix_grad = mix_grad + jnp.where(choice == rank[e : e + 1], row, 0.0)
        high = mix_grad.astype(jnp.bfloat16)
        low = (mix_grad - high.astype(jnp.float32)).astype(jnp.bfloat16)
        sent = trans_times(high, high_ref[...]) + trans_times(low, low_ref[...])
        out_ref[j * pair : (j + 1) * pair, width:] = sent.astype(jnp.bfloat16)


def out_kernel(pair, here_ref, marks_ref, rows_ref, hidden_ref, down_ref, out_ref):
    slots = pair_slots(marks_ref, here_ref, rows_ref.shape[0], pair)
    total = spread_rows(slots, rows_ref)
    total = total + matmul(hidden_ref[...], down_ref[...])
    out_ref[...] = total.astype(jnp.bfloat16)


def whole_spec(array):
    zeros = (0,) * array.ndim
    return pl.BlockSpec(array.shape, lambda i: zeros)


def pair_spec(array, pairs):
    block = (array.shape[0] // pairs,) + array.shape[1:]
    zeros = (0,) * (array.ndim - 1)
    return pl.BlockSpec(block, lambda i: (i,) + zeros)


def slots_spec(array, pairs):
    block = (array.shape[0], array.shape[1] // pairs) + array.shape[2:]
    return pl.BlockSpec(block, lambda i: (0, i, 0))


def cost(flops, *arrays):
    moved = sum(a.size * a.dtype.itemsize for a in arrays)
    return pl.CostEstimate(flops=int(flops), bytes_accessed=int(moved), transcendentals=0)


def call(kernel, grid, ins, outs, flops):
    arrays = [a for a, _ in ins]
    shapes = [s for s, _ in outs]
    return pl.pallas_call(
        kernel,
        grid=(grid,),
        in_specs=[s for _, s in ins],
        out_specs=[s for _, s in outs],
        out_shape=shapes,
        cost_estimate=cost(flops, *arrays, *shapes),
        compiler_params=pltpu.CompilerParams(vmem_limit_bytes=vmem_limit),
    )(*arrays)


MESH = pl.DeviceIdType.MESH


def places():
    expert, weight = lax.axis_index("expert"), lax.axis_index("weight")
    return lax.div(expert, 2), lax.rem(expert, 2), lax.div(weight, 2), lax.rem(weight, 2)


def device(z, x, y, c):
    return (z * 2 + x, y * 2 + c)


def shard(z, x, y, c):
    return z * 8 + x * 4 + y * 2 + c


def push(source, target, send, receive, to):
    return pltpu.make_async_remote_copy(
        src_ref=source,
        dst_ref=target,
        send_sem=send,
        recv_sem=receive,
        device_id=to,
        device_id_type=MESH,
    )


class Sends:
    def __init__(self, semaphores):
        self.semaphores = semaphores
        self.started = []

    def plan(self, source, target, receive, to, when=None):
        copy = push(source, target, self.semaphores.at[len(self.started)], receive, to)
        self.started.append((copy, when))
        return copy

    def start(self, source, target, receive, to, when=None):
        copy = self.plan(source, target, receive, to, when)
        if when is None:
            copy.start()
        else:
            pl.when(when)(copy.start)

    def finish(self):
        for copy, when in self.started:
            if when is None:
                copy.wait_send()
            else:
                pl.when(when)(copy.wait_send)


def landed(target, receive, to):
    push(target, target, receive, receive, to).wait_recv()


def greet(devices):
    barrier = pltpu.get_barrier_semaphore()
    count = 0
    for to, when in devices:
        signal = functools.partial(
            pl.semaphore_signal, barrier, inc=1, device_id=to, device_id_type=MESH
        )
        if when is None:
            signal()
            count = count + 1
        else:
            pl.when(when)(signal)
            count = count + when.astype(jnp.int32)
    pl.semaphore_wait(barrier, count)


def add_rows(target, sources, start, rows):
    step = 16

    def body(i, carry):
        part = pl.ds(pl.multiple_of(start + i * step, step), step)
        total = target[part].astype(jnp.float32)
        for source, offset in sources:
            there = pl.ds(pl.multiple_of(start - offset + i * step, step), step)
            total = total + source[there].astype(jnp.float32)
        target[part] = total.astype(target.dtype)
        return carry

    lax.fori_loop(0, rows // step, body, 0)


def ordered(z, first, second):
    upper = lax.div(z, 2)
    inner = z + upper * (3 - 2 * z)
    value = first + inner * (second - first)
    return value + upper * (3 - 2 * value)


class Gather:
    def __init__(self, x_ref, out_ref, sends, recv_sems, local_sem, place, cut=None):
        z, x, y, c = place
        rows = x_ref.shape[0]
        cut = rows // 2 if cut is None else cut
        self.parts = [pl.ds(0, cut), pl.ds(cut, rows - cut)]
        over, side, mate = device(z, 1 - x, y, c), device(z, x, 1 - y, c), device(z, x, y, 1 - c)
        up, down = device(z + 1, x, y, c), device(z - 1, x, y, c)
        self.out_ref, self.recv_sems, self.mate = out_ref, recv_sems, mate
        planes = [ordered(z, (0, 1, 2, 3)[step], (1, 0, 2, 3)[step]) for step in range(4)]
        self.rising = [(zz <= z) & (z < 3) for zz in planes]
        self.falling = [(zz >= z) & (z > 0) for zz in planes]
        self.mine = [shard(zz, x, y, c) for zz in planes]
        self.overs = [shard(zz, 1 - x, y, c) for zz in planes]
        self.sides = [shard(zz, x, 1 - y, c) for zz in planes]
        self.corners = [shard(zz, 1 - x, 1 - y, c) for zz in planes]
        self.mates = [
            (shard(zz, x, y, 1 - c), shard(zz, 1 - x, y, 1 - c), shard(zz, x, 1 - y, 1 - c))
            for zz in planes
        ]
        self.mate_corners = [shard(zz, 1 - x, 1 - y, 1 - c) for zz in planes]
        self.keep = pltpu.make_async_copy(x_ref, out_ref.at[self.mine[0]], local_sem)
        self.whole_copies, self.relay_copies, self.corner_copies = [], [], []

        def copy(ref, receive, to, when=None, source=None):
            return sends.plan(ref if source is None else source, ref, receive, to, when)

        for step in range(4):
            i = self.mine[step]
            source = x_ref if step == 0 else None
            there, receive = out_ref.at[i], recv_sems.at[i, 0]
            self.whole_copies.append(
                [
                    (copy(there, receive, up, self.rising[step], source), self.rising[step]),
                    (copy(there, receive, down, self.falling[step], source), self.falling[step]),
                    (copy(there, receive, over, None, source), None),
                    (copy(there, receive, side, None, source), None),
                    (copy(there, receive, mate, None, source), None),
                ]
            )
            i, j = self.overs[step], self.sides[step]
            self.relay_copies.append(
                [
                    copy(self.halves(i, 0), recv_sems.at[i, 0], side),
                    copy(out_ref.at[i], recv_sems.at[i, 0], mate),
                    copy(self.halves(j, 1), recv_sems.at[j, 1], over),
                    copy(out_ref.at[j], recv_sems.at[j, 0], mate),
                ]
            )
            i = self.corners[step]
            self.corner_copies.append(
                [copy(self.halves(i, h), recv_sems.at[i, h], mate) for h in range(2)]
            )

    def halves(self, i, h):
        return self.out_ref.at[i, self.parts[h]]

    def full_here(self, i):
        landed(self.out_ref.at[i], self.recv_sems.at[i, 0], self.mate)

    def half_here(self, i, h):
        landed(self.halves(i, h), self.recv_sems.at[i, h], self.mate)

    def whole(self, step):
        if step == 0:
            self.keep.start()
        else:
            self.full_here(self.mine[step])
        for copy, when in self.whole_copies[step]:
            if when is None:
                copy.start()
            else:
                pl.when(when)(copy.start)

    def relay(self, step):
        self.full_here(self.overs[step])
        self.relay_copies[step][0].start()
        self.relay_copies[step][1].start()
        self.full_here(self.sides[step])
        self.relay_copies[step][2].start()
        self.relay_copies[step][3].start()

    def corner(self, step):
        for h in range(2):
            self.half_here(self.corners[step], h)
            self.corner_copies[step][h].start()

    def last(self):
        for step in range(4):
            for i in self.mates[step]:
                self.full_here(i)
            for h in range(2):
                self.half_here(self.mate_corners[step], h)
        self.keep.wait()


def gather_neighbours(place):
    z, x, y, c = place
    return [
        (device(z, 1 - x, y, c), None),
        (device(z, x, 1 - y, c), None),
        (device(z, x, y, 1 - c), None),
        (device(z + 1, x, y, c), z < 3),
        (device(z - 1, x, y, c), z > 0),
    ]


def gather_all_kernel(inner, cover_ins, cover_outs, x_ref, *refs):
    ins, refs = refs[:cover_ins], refs[cover_ins:]
    out_ref, refs = refs[0], refs[1:]
    outs, refs = refs[:cover_outs], refs[cover_outs:]
    send_sems, recv_sems, local_sem = refs
    turn, turns = pl.program_id(0), pl.num_programs(0)
    place = places()
    sends = Sends(send_sems)
    gather = Gather(x_ref, out_ref, sends, recv_sems, local_sem, place)

    def begin():
        greet(gather_neighbours(place))
        gather.whole(0)

    def end():
        gather.whole(3)
        gather.relay(2)
        gather.corner(1)
        gather.relay(3)
        gather.corner(2)
        gather.corner(3)
        gather.last()
        sends.finish()

    def early():
        gather.relay(1)
        gather.corner(0)

    pieces = [
        begin,
        lambda: None,
        functools.partial(gather.whole, 1),
        functools.partial(gather.relay, 0),
        functools.partial(gather.whole, 2),
        lambda: None,
        early,
    ]
    for number, piece in enumerate(pieces):
        pl.when(turn == number)(piece)
    inner(turn, ins, outs)
    pl.when(turn == turns - 1)(end)


def gather_all(value, number, inner, turns, ins, outs, flops):
    if lax.axis_size("expert") != 8 or lax.axis_size("weight") != 4:

        def alone(*refs):
            inner(pl.program_id(0), refs[: len(ins)], refs[len(ins) :])

        gathered = lax.all_gather(value, ("expert", "weight"), axis=0)
        return gathered, call(alone, turns, ins, outs, flops)
    out = jax.ShapeDtypeStruct((32,) + value.shape, value.dtype)
    arrays, shapes = [a for a, _ in ins], [o for o, _ in outs]
    results = pl.pallas_call(
        functools.partial(gather_all_kernel, inner, len(ins), len(outs)),
        grid=(turns,),
        out_shape=[out] + shapes,
        in_specs=[whole_spec(value)] + [spec for _, spec in ins],
        out_specs=[pl.BlockSpec(memory_space=pl.ANY)] + [spec for _, spec in outs],
        scratch_shapes=[
            pltpu.SemaphoreType.DMA((44,)),
            pltpu.SemaphoreType.DMA((32, 2)),
            pltpu.SemaphoreType.DMA,
        ],
        compiler_params=pltpu.CompilerParams(
            collective_id=number, has_side_effects=True, vmem_limit_bytes=vmem_limit
        ),
        cost_estimate=cost(flops, value, out, *arrays, *shapes),
    )(value, *arrays)
    return results[0], results[1:]


def attention_kernel(
    score_scale,
    normed_ref,
    value_ref,
    cosine_ref,
    sine_ref,
    segment_row_ref,
    segment_column_ref,
    gain_ref,
    tokens_ref,
    second_gain_ref,
    router_ref,
    query_hbm,
    latent_hbm,
    expand_hbm,
    output_hbm,
    value_out,
    normed_out,
    query_out,
    latent_out,
    scale_out,
    latent_normed_out,
    key_rope_out,
    expanded_out,
    log_out,
    mixed_out,
    hidden_out,
    second_scale_out,
    gates_out,
    wide_out,
    query_matrix,
    latent_matrix,
    expand_matrix,
    output_matrix,
    partial,
    mates,
    sides,
    carried,
    send_sems,
    recv_sems,
    local_sems,
    group_sends,
    group_sems,
    sum_sends,
    mate_sems,
    side_sems,
):
    place = places()
    z, x, y, c = place
    side, mate = device(z, x, 1 - y, c), device(z, x, y, 1 - c)
    rows = normed_ref.shape[0]
    half = rows // 2
    heads = query_out.shape[0]
    greet(gather_neighbours(place))
    near = Sends(group_sends)
    own, across = y * 2 + c, (1 - y) * 2 + c
    keep = pltpu.make_async_copy(normed_ref, normed_out.at[own], local_sems.at[0])
    keep.start()

    def part(i, h):
        return normed_out.at[i, pl.ds(h * half, half)]

    for to in (side, mate):
        for h in range(2):
            piece = normed_ref.at[pl.ds(h * half, half)]
            near.start(piece, part(own, h), group_sems.at[own, h], to)
    sends = Sends(send_sems)
    gather = Gather(value_ref, value_out, sends, recv_sems, local_sems.at[1], place, 48)
    gather.whole(0)
    loads = [
        pltpu.make_async_copy(source, target, local_sems.at[2 + i])
        for i, (source, target) in enumerate(
            (
                (query_hbm, query_matrix),
                (latent_hbm, latent_matrix),
                (expand_hbm, expand_matrix),
                (output_hbm, output_matrix),
            )
        )
    ]
    for load in loads:
        load.start()
    for h in range(2):
        landed(part(across, h), group_sems.at[across, h], mate)
        near.start(part(across, h), part(across, h), group_sems.at[across, h], mate)
    for i in (y * 2 + 1 - c, (1 - y) * 2 + 1 - c):
        for h in range(2):
            landed(part(i, h), group_sems.at[i, h], mate)
    keep.wait()
    normed = normed_out[...].reshape(4 * rows, normed_out.shape[2])
    cosine, sine = cosine_ref[...], sine_ref[...]
    turn_half = ROPE // 2

    def turned(first, second):
        return jnp.concatenate(
            [first * cosine - second * sine, second * cosine + first * sine], axis=1
        )

    loads[0].wait()
    full = matmul(normed, query_matrix[...])
    for h in range(heads):
        start = h * (NOPE + ROPE)
        first = full[:, start + NOPE : start + NOPE + turn_half]
        second = full[:, start + NOPE + turn_half : start + NOPE + ROPE]
        query = jnp.concatenate([full[:, start : start + NOPE], turned(first, second)], axis=1)
        query_out[h] = query.astype(jnp.bfloat16)
    gather.whole(1)
    loads[1].wait()
    compressed = times_trans(normed, latent_matrix[...])
    latent = compressed[:, :LATENT]
    scale = inv_rms(latent)
    latent_out[...] = latent
    scale_out[...] = jnp.broadcast_to(scale, scale_out.shape)
    latent_normed_out[...] = (latent * scale * gain_ref[...]).astype(jnp.bfloat16)
    first = compressed[:, LATENT : LATENT + turn_half]
    second = compressed[:, LATENT + turn_half : LATENT + ROPE]
    key_rope_out[...] = turned(first, second).astype(jnp.bfloat16)
    gather.relay(0)
    loads[2].wait()
    expanded_out[...] = matmul(latent_normed_out[...], expand_matrix[...]).astype(jnp.bfloat16)

    def head(h):
        start = h * (NOPE + VDIM)
        query = query_out[h]
        raw = times_trans(query[:, :NOPE], expanded_out[:, start : start + NOPE])
        raw = raw + times_trans(query[:, NOPE:], key_rope_out[...])
        row = lax.broadcasted_iota(jnp.int32, raw.shape, 0)
        column = lax.broadcasted_iota(jnp.int32, raw.shape, 1)
        allowed = (segment_column_ref[...] == segment_row_ref[...]) & (column <= row)
        scores = jnp.where(allowed, raw * score_scale, -1e30)
        peak = jnp.max(scores, axis=1, keepdims=True)
        weights = jnp.exp(scores - peak)
        total = jnp.sum(weights, axis=1, keepdims=True)
        log_out[h] = jnp.broadcast_to(peak + jnp.log(total), log_out.shape[1:])
        probs = (weights / total).astype(jnp.bfloat16)
        mixed = matmul(probs, expanded_out[:, start + NOPE : start + NOPE + VDIM])
        mixed_out[:, h * VDIM : (h + 1) * VDIM] = mixed.astype(jnp.bfloat16)

    middle = [
        None,
        functools.partial(gather.whole, 2),
        functools.partial(gather.relay, 1),
        functools.partial(gather.corner, 0),
    ]
    for h in range(heads):
        head(h)
        if h < 4 and middle[h] is not None:
            middle[h]()
    loads[3].wait()
    for i in range(4):
        block = matmul(mixed_out[i * rows : (i + 1) * rows], output_matrix[...])
        partial[i] = block.astype(jnp.bfloat16)
    sums = Sends(sum_sends)
    for j, yy in enumerate((1 - y, y)):
        for h in range(2):
            some = pl.ds(h * half, half)
            sums.start(
                partial.at[yy * 2 + 1 - c, some], mates.at[j, some], mate_sems.at[j, h], mate
            )
    gather.whole(3)
    for h in range(2):
        some = pl.ds(h * half, half)
        landed(mates.at[0, some], mate_sems.at[0, h], mate)
        add_into(carried, [partial.at[(1 - y) * 2 + c], mates.at[0]], h * half, half)
        sums.start(carried.at[some], sides.at[some], side_sems.at[h], side)
    gather.relay(2)
    gather.corner(1)
    for h in range(2):
        some = pl.ds(h * half, half)
        landed(mates.at[1, some], mate_sems.at[1, h], mate)
        landed(sides.at[some], side_sems.at[h], mate)
        add_into(hidden_out, [partial.at[y * 2 + c], mates.at[1], sides], h * half, half)
    hidden = tokens_ref[...].astype(jnp.float32) + hidden_out[...]
    hidden_out[...] = hidden
    second_scale = inv_rms(hidden)
    second_scale_out[...] = jnp.broadcast_to(second_scale, second_scale_out.shape)
    normed_two = (hidden * second_scale * second_gain_ref[...]).astype(jnp.bfloat16)
    width = hidden.shape[1]
    wide_out[:, :width] = normed_two
    gates = jax.nn.sigmoid(times_trans(normed_two, router_ref[...]))
    gates_out[...] = gates
    codes = value_ref[:, width:].astype(jnp.float32)[:, : gates.shape[1]]
    weighted = jnp.where(codes >= 0, gates, 0.0)
    mixing = route_scale * weighted / jnp.sum(weighted, axis=1, keepdims=True)
    high = mixing.astype(jnp.bfloat16).astype(jnp.float32)
    wide_out[:, width:] = jnp.concatenate([high, mixing - high], axis=1).astype(jnp.bfloat16)
    gather.relay(3)
    gather.corner(2)
    gather.corner(3)
    gather.last()
    near.finish()
    sends.finish()
    sums.finish()


def add_into(target, sources, start, rows):
    step = 16

    def body(i, carry):
        part = pl.ds(pl.multiple_of(start + i * step, step), step)
        total = sources[0][part].astype(jnp.float32)
        for source in sources[1:]:
            total = total + source[part].astype(jnp.float32)
        target[part] = total.astype(target.dtype)
        return carry

    lax.fori_loop(0, rows // step, body, 0)


def attention_forward(
    score_scale,
    normed,
    value,
    cosine,
    sine,
    segment,
    gain,
    tokens,
    second_gain,
    router,
    query,
    latent,
    expand,
    output,
    number,
):
    rows, width = normed.shape
    group, heads = 4 * rows, query.shape[1] // (NOPE + ROPE)
    shape, low = jax.ShapeDtypeStruct, jnp.bfloat16
    vmem, away = pl.BlockSpec(memory_space=pltpu.VMEM), pl.BlockSpec(memory_space=pl.ANY)
    segment = segment.astype(jnp.float32)
    inputs = [normed, value, cosine, sine, segment[None], segment[:, None], gain[None]]
    inputs += [tokens, second_gain[None], router.T]
    matrices = [query, latent.T, expand, output]
    outs = [
        shape((32,) + value.shape, low),
        shape((4, rows, width), low),
        shape((heads, group, NOPE + ROPE), low),
        shape((group, LATENT), jnp.float32),
        shape((group, lanes), jnp.float32),
        shape((group, LATENT), low),
        shape((group, ROPE), low),
        shape((group, heads * (NOPE + VDIM)), low),
        shape((heads, group, lanes), jnp.float32),
        shape((group, heads * VDIM), low),
        shape((rows, width), jnp.float32),
        shape((rows, lanes), jnp.float32),
        shape((rows, router.shape[1]), jnp.float32),
        shape(value.shape, low),
    ]
    flops = 2 * group * (width * (query.shape[1] + latent.shape[1]) + output.size + expand.size)
    return pl.pallas_call(
        functools.partial(attention_kernel, score_scale),
        out_shape=outs,
        in_specs=[vmem] * len(inputs) + [away] * 4,
        out_specs=[away] + [vmem] * (len(outs) - 1),
        scratch_shapes=[pltpu.VMEM(m.shape, low) for m in matrices]
        + [
            pltpu.VMEM((4, rows, width), low),
            pltpu.VMEM((2, rows, width), low),
            pltpu.VMEM((rows, width), low),
            pltpu.VMEM((rows, width), low),
            pltpu.SemaphoreType.DMA((44,)),
            pltpu.SemaphoreType.DMA((32, 2)),
            pltpu.SemaphoreType.DMA((6,)),
            pltpu.SemaphoreType.DMA((6,)),
            pltpu.SemaphoreType.DMA((4, 2)),
            pltpu.SemaphoreType.DMA((6,)),
            pltpu.SemaphoreType.DMA((2, 2)),
            pltpu.SemaphoreType.DMA((2,)),
        ],
        compiler_params=pltpu.CompilerParams(
            collective_id=number, has_side_effects=True, vmem_limit_bytes=vmem_limit
        ),
        cost_estimate=cost(flops, *inputs, *matrices, *outs),
    )(*inputs, *matrices)


def sum_all_kernel(inner, cover_ins, cover_outs, p_ref, *refs):
    ins, refs = refs[:cover_ins], refs[cover_ins:]
    out_ref, refs = refs[0], refs[1:]
    outs, refs = refs[:cover_outs], refs[cover_outs:]
    own, mates, over_half, side_half, over_full, side_full, below, above = refs[:8]
    send_sems, mate_sems, half_sems, full_sems, line_sems, local_sems = refs[8:]
    z, x, y, c = places()
    turn, turns = pl.program_id(0), pl.num_programs(0)
    rows = out_ref.shape[0]
    half = rows // 2
    over, side, mate = device(z, 1 - x, y, c), device(z, x, 1 - y, c), device(z, x, y, 1 - c)
    up, down = device(z + 1, x, y, c), device(z - 1, x, y, c)
    sends = Sends(send_sems)
    targets = [ordered(z, (3, 2, 1, 0)[step], (3, 0, 2, 1)[step]) for step in range(4)]
    spots = [(1 - x, 1 - y), (1 - x, y), (x, 1 - y), (x, y)]
    shards = [[shard(zz, xx, yy, 1 - c) for xx, yy in spots] for zz in targets]
    mine = [[shard(zz, xx, yy, c) for xx, yy in spots] for zz in targets]
    higher = [zz > z for zz in targets]
    lower = [zz < z for zz in targets]
    loads = [
        pltpu.make_async_copy(p_ref.at[mine[slot // 4][slot % 4]], own.at[slot], local_sems.at[slot])
        for slot in range(16)
    ]

    mate_copies = [
        sends.plan(p_ref.at[shards[slot // 4][slot % 4]], mates.at[slot], mate_sems.at[slot], mate)
        for slot in range(16)
    ]
    corner_copies, relay_copies, line_copies = [], [], []
    for step in range(4):
        corner_copies.append(
            (
                sends.plan(
                    own.at[step * 4, pl.ds(half, half)],
                    over_half.at[step],
                    half_sems.at[step, 0],
                    over,
                ),
                sends.plan(
                    own.at[step * 4, pl.ds(0, half)], side_half.at[step], half_sems.at[step, 1], side
                ),
            )
        )
        relay_copies.append(
            (
                sends.plan(
                    own.at[step * 4 + 1], over_full.at[step], full_sems.at[step, 0], over
                ),
                sends.plan(
                    own.at[step * 4 + 2], side_full.at[step], full_sems.at[step, 1], side
                ),
            )
        )
    for step in range(3):
        zz, slot = targets[step], step * 4 + 3
        line_copies.append(
            (
                sends.plan(own.at[slot], below.at[zz], line_sems.at[zz, 0], up, higher[step]),
                sends.plan(own.at[slot], above.at[zz], line_sems.at[zz, 1], down, lower[step]),
            )
        )

    def begin():
        greet([(over, None), (side, None), (mate, None), (up, z < 3), (down, z > 0)])
        for slot in range(16):
            mate_copies[slot].start()
            loads[slot].start()

    def join(slot):
        loads[slot].wait()
        landed(mates.at[slot], mate_sems.at[slot], mate)

    def corner(step):
        slot = step * 4
        join(slot)
        add_rows(own.at[slot], [(mates.at[slot], 0)], 0, rows)
        for copy in corner_copies[step]:
            copy.start()

    def relay(step):
        slot = step * 4 + 1
        join(slot)
        add_rows(own.at[slot], [(mates.at[slot], 0)], half, half)
        landed(side_half.at[step], half_sems.at[step, 1], mate)
        add_rows(own.at[slot], [(mates.at[slot], 0), (side_half.at[step], 0)], 0, half)
        relay_copies[step][0].start()
        slot = step * 4 + 2
        join(slot)
        add_rows(own.at[slot], [(mates.at[slot], 0)], 0, half)
        landed(over_half.at[step], half_sems.at[step, 0], mate)
        add_rows(own.at[slot], [(mates.at[slot], 0), (over_half.at[step], half)], half, half)
        relay_copies[step][1].start()

    def whole(step):
        zz = targets[step]
        slot = step * 4 + 3
        join(slot)
        landed(over_full.at[step], full_sems.at[step, 0], mate)
        landed(side_full.at[step], full_sems.at[step, 1], mate)
        add_rows(
            own.at[slot],
            [(mates.at[slot], 0), (over_full.at[step], 0), (side_full.at[step], 0)],
            0,
            rows,
        )

        @pl.when((zz >= z) & (z > 0))
        def _():
            landed(below.at[zz], line_sems.at[zz, 0], mate)
            add_rows(own.at[slot], [(below.at[zz], 0)], 0, rows)

        @pl.when((zz <= z) & (z < 3))
        def _():
            landed(above.at[zz], line_sems.at[zz, 1], mate)
            add_rows(own.at[slot], [(above.at[zz], 0)], 0, rows)

        if step < 3:
            pl.when(higher[step])(line_copies[step][0].start)
            pl.when(lower[step])(line_copies[step][1].start)

    def end():
        whole(3)
        out_ref[...] = own[15].astype(out_ref.dtype)
        sends.finish()

    pieces = [
        begin,
        functools.partial(corner, 0),
        functools.partial(corner, 1),
        functools.partial(relay, 0),
        functools.partial(corner, 2),
        functools.partial(relay, 1),
        functools.partial(whole, 0),
        functools.partial(corner, 3),
        functools.partial(relay, 2),
        functools.partial(whole, 1),
        functools.partial(relay, 3),
        functools.partial(whole, 2),
    ]
    for number, piece in enumerate(pieces):
        pl.when(turn == number)(piece)
    inner(turn, ins, outs)
    pl.when(turn == turns - 1)(end)


def sum_all(value, number, inner, turns, ins, outs, flops):
    if lax.axis_size("expert") != 8 or lax.axis_size("weight") != 4:
        summed = lax.psum_scatter(
            value.reshape(-1, value.shape[2]), ("expert", "weight"), scatter_dimension=0, tiled=True
        )

        def alone(*refs):
            inner(pl.program_id(0), refs[: len(ins)], refs[len(ins) :])

        return summed.astype(jnp.float32), call(alone, turns, ins, outs, flops)
    _, rows, width = value.shape
    out = jax.ShapeDtypeStruct((rows, width), jnp.float32)
    buffer = lambda n, r: pltpu.VMEM((n, r, width), value.dtype)
    arrays, shapes = [a for a, _ in ins], [o for o, _ in outs]
    results = pl.pallas_call(
        functools.partial(sum_all_kernel, inner, len(ins), len(outs)),
        grid=(turns,),
        out_shape=[out] + shapes,
        in_specs=[pl.BlockSpec(memory_space=pl.ANY)] + [spec for _, spec in ins],
        out_specs=[pl.BlockSpec((rows, width), lambda i: (0, 0))] + [spec for _, spec in outs],
        scratch_shapes=[
            buffer(16, rows),
            buffer(16, rows),
            buffer(4, rows // 2),
            buffer(4, rows // 2),
            buffer(4, rows),
            buffer(4, rows),
            buffer(4, rows),
            buffer(4, rows),
            pltpu.SemaphoreType.DMA((40,)),
            pltpu.SemaphoreType.DMA((16,)),
            pltpu.SemaphoreType.DMA((4, 2)),
            pltpu.SemaphoreType.DMA((4, 2)),
            pltpu.SemaphoreType.DMA((4, 2)),
            pltpu.SemaphoreType.DMA((16,)),
        ],
        compiler_params=pltpu.CompilerParams(
            collective_id=number, has_side_effects=True, vmem_limit_bytes=vmem_limit
        ),
        cost_estimate=cost(flops, value, out, *arrays, *shapes),
    )(value, *arrays)
    return results[0], results[1:]


def gather_group_kernel(x_ref, out_ref, send_sems, recv_sems, local_sem):
    z, x, y, c = places()
    half = x_ref.shape[0] // 2
    side, mate = device(z, x, 1 - y, c), device(z, x, y, 1 - c)
    greet([(side, None), (mate, None)])
    sends = Sends(send_sems)
    own, across = y * 2 + c, (1 - y) * 2 + c
    keep = pltpu.make_async_copy(x_ref, out_ref.at[own], local_sem)
    keep.start()

    def part(i, h):
        return out_ref.at[i, pl.ds(h * half, half)]

    for h in range(2):
        piece = x_ref.at[pl.ds(h * half, half)]
        sends.start(piece, part(own, h), recv_sems.at[own, h], side)
    for h in range(2):
        piece = x_ref.at[pl.ds(h * half, half)]
        sends.start(piece, part(own, h), recv_sems.at[own, h], mate)
    for h in range(2):
        landed(part(across, h), recv_sems.at[across, h], mate)
        sends.start(part(across, h), part(across, h), recv_sems.at[across, h], mate)
    for i in (y * 2 + 1 - c, (1 - y) * 2 + 1 - c):
        for h in range(2):
            landed(part(i, h), recv_sems.at[i, h], mate)
    sends.finish()
    keep.wait()


def gather_group(value, number):
    if lax.axis_size("expert") != 8 or lax.axis_size("weight") != 4:
        return lax.all_gather(value, "weight", axis=0, tiled=True)
    out = jax.ShapeDtypeStruct((4,) + value.shape, value.dtype)
    return pl.pallas_call(
        gather_group_kernel,
        out_shape=out,
        in_specs=[pl.BlockSpec(memory_space=pltpu.VMEM)],
        out_specs=pl.BlockSpec(memory_space=pltpu.VMEM),
        scratch_shapes=[
            pltpu.SemaphoreType.DMA((6,)),
            pltpu.SemaphoreType.DMA((4, 2)),
            pltpu.SemaphoreType.DMA,
        ],
        compiler_params=pltpu.CompilerParams(collective_id=number, has_side_effects=True),
        cost_estimate=cost(0, value, out),
    )(value).reshape(-1, value.shape[1])


def sum_group_kernel(p_ref, out_ref, mates, sides, carried, send_sems, mate_sems, side_sems):
    z, x, y, c = places()
    rows = out_ref.shape[0]
    half = rows // 2
    side, mate = device(z, x, 1 - y, c), device(z, x, y, 1 - c)
    greet([(side, None), (mate, None)])
    sends = Sends(send_sems)

    for j, yy in enumerate((1 - y, y)):
        for h in range(2):
            part = pl.ds(h * half, half)
            sends.start(
                p_ref.at[yy * 2 + 1 - c, part], mates.at[j, part], mate_sems.at[j, h], mate
            )

    def add(target, sources, h):
        step = 16

        def body(i, carry):
            part = pl.ds(pl.multiple_of(h * half + i * step, step), step)
            total = sources[0][part].astype(jnp.float32)
            for source in sources[1:]:
                total = total + source[part].astype(jnp.float32)
            target[part] = total.astype(target.dtype)
            return carry

        lax.fori_loop(0, half // step, body, 0)

    for h in range(2):
        part = pl.ds(h * half, half)
        landed(mates.at[0, part], mate_sems.at[0, h], mate)
        add(carried, [p_ref.at[(1 - y) * 2 + c], mates.at[0]], h)
        sends.start(carried.at[part], sides.at[part], side_sems.at[h], side)
    for h in range(2):
        part = pl.ds(h * half, half)
        landed(mates.at[1, part], mate_sems.at[1, h], mate)
        landed(sides.at[part], side_sems.at[h], mate)
        add(out_ref, [p_ref.at[y * 2 + c], mates.at[1], sides], h)
    sends.finish()


def sum_group(value, number):
    if lax.axis_size("expert") != 8 or lax.axis_size("weight") != 4:
        summed = lax.psum_scatter(value, "weight", scatter_dimension=0, tiled=True)
        return summed.astype(jnp.float32)
    rows, width = value.shape[0] // 4, value.shape[1]
    value = value.reshape(4, rows, width)
    out = jax.ShapeDtypeStruct((rows, width), jnp.float32)
    return pl.pallas_call(
        sum_group_kernel,
        out_shape=out,
        in_specs=[pl.BlockSpec(memory_space=pltpu.VMEM)],
        out_specs=pl.BlockSpec(memory_space=pltpu.VMEM),
        scratch_shapes=[
            pltpu.VMEM((2, rows, width), value.dtype),
            pltpu.VMEM((rows, width), value.dtype),
            pltpu.VMEM((rows, width), value.dtype),
            pltpu.SemaphoreType.DMA((6,)),
            pltpu.SemaphoreType.DMA((2, 2)),
            pltpu.SemaphoreType.DMA((2,)),
        ],
        compiler_params=pltpu.CompilerParams(collective_id=number, has_side_effects=True),
        cost_estimate=cost(0, value, out),
    )(value)


def columns(start, size):
    return pl.ds(pl.multiple_of(start, lanes), size)


def add_block(target, sources, rows, row_start=0):
    step = 16

    def body(i, carry):
        part = pl.ds(pl.multiple_of(row_start + i * step, step), step)
        total = target[part].astype(jnp.float32)
        for source in sources:
            there = pl.ds(pl.multiple_of(i * step, step), step)
            total = total + source[there].astype(jnp.float32)
        target[part] = total.astype(target.dtype)
        return carry

    lax.fori_loop(0, rows // step, body, 0)


def total_kernel(
    top_ref,
    rest_ref,
    group_ref,
    out_ref,
    group_out,
    acc,
    mates,
    first_over,
    first_side,
    next_side,
    next_over,
    line,
    group_mates,
    group_sides,
    carried,
    send_sems,
    sems,
    mate_sems,
    side_sems,
):
    z, x, y, c = places()
    rows, width = out_ref.shape
    group_half = group_out.shape[0] // 2
    group_parts = [pl.ds(h * group_half, group_half) for h in range(2)]
    sources = [(top_ref, 0, 0), (rest_ref, top_ref.shape[0], 24)]
    half, quarter, eighth, sixteenth = width // 2, width // 4, width // 8, width // 16
    strip = rows // 4
    over, side, mate = device(z, 1 - x, y, c), device(z, x, 1 - y, c), device(z, x, y, 1 - c)
    others = [lax.rem(z + d, 4) for d in (1, 2, 3)]
    greet(
        [(over, None), (side, None), (mate, None)] + [(device(zz, x, y, c), None) for zz in others]
    )
    sends = Sends(send_sems)
    base = c * half
    for j in range(2):
        for p_ref, top, sem in sources:
            sends.start(
                p_ref.at[:, columns((1 - c) * half + j * quarter, quarter)],
                mates.at[pl.ds(top, p_ref.shape[0]), columns(j * quarter, quarter)],
                sems.at[sem + j],
                mate,
            )
    for i, yy in enumerate((1 - y, y)):
        for h, some in enumerate(group_parts):
            sends.start(
                group_ref.at[yy * 2 + 1 - c, some],
                group_mates.at[i, some],
                mate_sems.at[i, h],
                mate,
            )
    kept = (x * eighth + y * sixteenth, quarter + y * eighth + x * sixteenth)
    firsts, nexts = (first_over, first_side), (next_side, next_over)
    for j in range(2):
        part = columns(j * quarter, quarter)
        wide = 16
        for p_ref, top, sem in sources:
            landed(mates.at[pl.ds(top, p_ref.shape[0]), part], sems.at[sem + j], mate)

            def join(i, carry, j=j, p_ref=p_ref, top=top):
                mine = pl.ds(pl.multiple_of(i * wide, wide), wide)
                some = pl.ds(pl.multiple_of(top + i * wide, wide), wide)
                total = p_ref[mine, columns(base + j * quarter, quarter)].astype(jnp.float32)
                total = total + mates[some, columns(j * quarter, quarter)].astype(jnp.float32)
                acc[some, columns(j * quarter, quarter)] = total.astype(acc.dtype)
                return carry

            lax.fori_loop(0, p_ref.shape[0] // wide, join, 0)
        away = (1 - x) * eighth if j == 0 else quarter + (1 - y) * eighth
        sends.start(
            acc.at[:, columns(away, eighth)], firsts[j], sems.at[2 + j], (over, side)[j]
        )
    for h, some in enumerate(group_parts):
        landed(group_mates.at[0, some], mate_sems.at[0, h], mate)
        add_into(
            carried,
            [group_ref.at[(1 - y) * 2 + c], group_mates.at[0]],
            h * group_half,
            group_half,
        )
        sends.start(carried.at[some], group_sides.at[some], side_sems.at[h], side)
    for j in range(2):
        landed(firsts[j], sems.at[2 + j], mate)
        near = x * eighth if j == 0 else quarter + y * eighth
        add_block(acc.at[:, columns(near, eighth)], [firsts[j]], rows)
        away = near + ((1 - y) if j == 0 else (1 - x)) * sixteenth
        sends.start(
            acc.at[:, columns(away, sixteenth)], nexts[j], sems.at[4 + j], (side, over)[j]
        )
    for j in range(2):
        landed(nexts[j], sems.at[4 + j], mate)
        add_block(acc.at[:, columns(kept[j], sixteenth)], [nexts[j]], rows)
        for d, zz in enumerate(others):
            sends.start(
                acc.at[pl.ds(pl.multiple_of(zz * strip, 16), strip), columns(kept[j], sixteenth)],
                line.at[j, d],
                sems.at[6 + j * 3 + d],
                device(zz, x, y, c),
            )
    strip_here = pl.multiple_of(z * strip, 16)
    for j in range(2):
        for d in range(3):
            landed(line.at[j, d], sems.at[6 + j * 3 + d], mate)
        block = acc.at[:, columns(kept[j], sixteenth)]
        add_block(block, [line.at[j, d] for d in range(3)], strip, strip_here)

        def place(i, carry, j=j):
            some = pl.ds(pl.multiple_of(strip_here + i * 16, 16), 16)
            out_ref[some, columns(base + kept[j], sixteenth)] = acc[
                some, columns(kept[j], sixteenth)
            ]
            return carry

        lax.fori_loop(0, strip // 16, place, 0)
        done = out_ref.at[pl.ds(strip_here, strip), columns(base + kept[j], sixteenth)]
        for d, zz in enumerate(others):
            sends.start(done, done, sems.at[12 + j * 3 + d], device(zz, x, y, c))
    for j in range(2):
        for d in range(3):
            source = pl.multiple_of(lax.rem(z + 3 - d, 4) * strip, 16)
            landed(
                out_ref.at[pl.ds(source, strip), columns(base + kept[j], sixteenth)],
                sems.at[12 + j * 3 + d],
                mate,
            )
        part = out_ref.at[:, columns(base + kept[j], sixteenth)]
        sends.start(part, part, sems.at[18 + j], (side, over)[j])
    others_kept = (
        x * eighth + (1 - y) * sixteenth,
        quarter + y * eighth + (1 - x) * sixteenth,
    )
    for j in range(2):
        landed(out_ref.at[:, columns(base + others_kept[j], sixteenth)], sems.at[18 + j], mate)
        near = x * eighth if j == 0 else quarter + y * eighth
        part = out_ref.at[:, columns(base + near, eighth)]
        sends.start(part, part, sems.at[20 + j], (over, side)[j])
    for j in range(2):
        away = (1 - x) * eighth if j == 0 else quarter + (1 - y) * eighth
        landed(out_ref.at[:, columns(base + away, eighth)], sems.at[20 + j], mate)
        part = out_ref.at[:, columns(base + j * quarter, quarter)]
        sends.start(part, part, sems.at[22 + j], mate)
    for h, some in enumerate(group_parts):
        landed(group_mates.at[1, some], mate_sems.at[1, h], mate)
        landed(group_sides.at[some], side_sems.at[h], mate)
        add_into(
            group_out,
            [group_ref.at[y * 2 + c], group_mates.at[1], group_sides],
            h * group_half,
            group_half,
        )
    for j in range(2):
        landed(
            out_ref.at[:, columns((1 - c) * half + j * quarter, quarter)], sems.at[22 + j], mate
        )
    sends.finish()


def total_over_all(top, rest, group, number):
    if lax.axis_size("expert") != 8 or lax.axis_size("weight") != 4:
        value = jnp.concatenate([top, rest], axis=0).astype(jnp.float32)
        return lax.psum(value, ("expert", "weight")), sum_group(group, number)
    rows, width = top.shape[0] + rest.shape[0], top.shape[1]
    group = group.reshape(4, -1, width)
    group_rows = group.shape[1]
    out = jax.ShapeDtypeStruct((rows, width), top.dtype)
    group_out = jax.ShapeDtypeStruct((group_rows, width), jnp.float32)
    buffer = lambda n: pltpu.VMEM((rows, n), top.dtype)
    return pl.pallas_call(
        total_kernel,
        out_shape=[out, group_out],
        in_specs=[pl.BlockSpec(memory_space=pltpu.VMEM)] * 3,
        out_specs=[pl.BlockSpec(memory_space=pltpu.VMEM)] * 2,
        scratch_shapes=[
            buffer(width // 2),
            buffer(width // 2),
            buffer(width // 8),
            buffer(width // 8),
            buffer(width // 16),
            buffer(width // 16),
            pltpu.VMEM((2, 3, rows // 4, width // 16), top.dtype),
            pltpu.VMEM((2, group_rows, width), group.dtype),
            pltpu.VMEM((group_rows, width), group.dtype),
            pltpu.VMEM((group_rows, width), group.dtype),
            pltpu.SemaphoreType.DMA((32,)),
            pltpu.SemaphoreType.DMA((26,)),
            pltpu.SemaphoreType.DMA((2, 2)),
            pltpu.SemaphoreType.DMA((2,)),
        ],
        compiler_params=pltpu.CompilerParams(
            collective_id=number, has_side_effects=True, vmem_limit_bytes=vmem_limit
        ),
        cost_estimate=cost(0, top, rest, group, out, group_out),
    )(top, rest, group)


def shared_kernel(turn, ins, outs):
    normed_ref, cotangent_ref, gate_grad_ref, lift_grad_ref, hidden_ref = ins

    @pl.when(turn == 0)
    def _():
        for out_ref in outs:
            out_ref[...] = jnp.zeros_like(out_ref)

    normed, cotangent = normed_ref[...], cotangent_ref[...]
    outs[0][...] += trans_times(gate_grad_ref[...], normed)
    outs[1][...] += trans_times(lift_grad_ref[...], normed)
    outs[2][...] += trans_times(hidden_ref[...], cotangent)


def weight_kernel(ins, outs):
    rows_ref, grads_ref, gate_grad_ref, lift_grad_ref, hidden_ref = ins
    rows = rows_ref[0]
    for out_ref, left_ref, right in (
        (outs[0], gate_grad_ref, rows),
        (outs[1], lift_grad_ref, rows),
        (outs[2], hidden_ref, grads_ref[0]),
    ):
        out_ref[0] = trans_times(left_ref[0], right).astype(out_ref.dtype)


def weights_alone(*refs):
    weight_kernel(refs[:5], refs[5:])


def gradients_kernel(turn, ins, outs):
    shared_kernel(turn, ins[:5], outs[:3])
    weight_kernel(ins[5:], outs[3:])


def sum_shards(value):
    return lax.psum_scatter(value, "expert", scatter_dimension=0, tiled=True)


def per_device(
    tokens,
    cotangent,
    segments,
    routes,
    first_gain,
    query_weight,
    latent_weight,
    latent_gain,
    expand_weight,
    output_weight,
    second_gain,
    router_weight,
    shared_gate,
    shared_up,
    shared_down,
    expert_gate,
    expert_up,
    expert_down,
):
    weight_count = lax.axis_size("weight")
    token_rows = tokens.shape[0]
    width = tokens.shape[1]
    group_rows = token_rows * weight_count
    query_width = NOPE + ROPE
    heads_here = query_weight.shape[1] // query_width
    expert_count = router_weight.shape[1]
    local_experts = expert_gate.shape[0]
    score_scale = query_width ** (-0.5)
    activations = tokens.astype(jnp.float32)
    first_scale = inv_rms(activations)
    normed = (activations * first_scale * first_gain).astype(jnp.bfloat16)
    both = ("expert", "weight")
    expert_index = lax.axis_index("expert")
    expert_lanes = lax.axis_size("expert")
    blocks = expert_lanes * weight_count
    pairs, quads = blocks // 2, blocks // 4
    pair_rows, quad_rows = 2 * token_rows, 4 * token_rows
    all_rows = blocks * token_rows
    slot_rows = blocks * CAP
    choose = (
        routes[:, :, None] == jnp.arange(expert_count, dtype=jnp.int32)[None, None, :]
    ).astype(jnp.float32)
    hit = jnp.sum(choose, axis=1)
    order = jnp.arange(token_rows, dtype=jnp.int32)
    before = (order[None, :] < order[:, None]).astype(jnp.bfloat16)
    place = matmul(before, hit.astype(jnp.bfloat16))
    rank = jnp.sum(choose * jnp.arange(routes.shape[1], dtype=jnp.float32)[None, :, None], axis=1)
    code = jnp.where(hit > 0, 32.0 * rank + place, -1.0)
    extra = jnp.pad(code, ((0, 0), (0, lanes - expert_count)), constant_values=-1.0)
    cotangent_wide = jnp.concatenate([cotangent, extra.astype(jnp.bfloat16)], axis=1)
    column = jnp.arange(lanes, dtype=jnp.int32)[None, :]
    row = jnp.arange(8, dtype=jnp.int32)[:, None]
    first_here = expert_index * local_experts
    here = (row < local_experts) & (column == first_here + row)
    twice = here | ((row < local_experts) & (column == first_here + row + expert_count))
    here, twice = here.astype(jnp.bfloat16), twice.astype(jnp.bfloat16)
    weight_index = lax.axis_index("weight")
    high_column = 2 * (row * weight_count + weight_index)
    known = row < routes.shape[1]
    high_at = (known & (column == high_column)).astype(jnp.bfloat16)
    low_at = (known & (column == high_column + 1)).astype(jnp.bfloat16)
    shared_here = shared_gate.shape[1] // expert_lanes
    shared_wide = -(-shared_here // lanes) * lanes
    start = expert_index * shared_here

    def shared_part(matrix):
        part = lax.dynamic_slice_in_dim(matrix, start, shared_here, axis=0)
        return jnp.pad(part, ((0, shared_wide - shared_here), (0, 0)))

    gate_part = shared_part(shared_gate.T)
    up_part = shared_part(shared_up.T)
    down_part = shared_part(shared_down)
    shape = jax.ShapeDtypeStruct
    whole = lambda array: (array, whole_spec(array))
    slots = shape((local_experts, slot_rows, width), jnp.bfloat16)
    slots_one = shape((local_experts, slot_rows, lanes), jnp.float32)
    gather_flops = 2 * all_rows * width * (2 * CAP * local_experts + shared_wide)
    cosine, sine = rope_tables(segments[0])
    allowed = attention_mask(segments[0])
    sizes = (expert_lanes, weight_count)
    if sizes == (8, 4):
        (
            cotangent_all,
            normed_all,
            query,
            latent,
            latent_scale,
            latent_normed,
            key_rope,
            expanded,
            log_total,
            mixed,
            hidden_one,
            second_scale,
            gates,
            normed_wide,
        ) = attention_forward(
            score_scale,
            normed,
            cotangent_wide,
            cosine,
            sine,
            segments[0],
            latent_gain,
            tokens,
            second_gain,
            router_weight,
            query_weight,
            latent_weight,
            expand_weight,
            output_weight,
            0,
        )
        second_scale, normed_two = second_scale[:, :1], normed_wide[:, :width]
        cotangent_all = cotangent_all.reshape(all_rows, -1)
        normed_all = normed_all.reshape(group_rows, width)
        latent_scale, log_total = latent_scale[:, :1], log_total[:, :, :1]
        query = query.transpose(1, 0, 2)
        expanded = expanded.reshape(group_rows, heads_here, NOPE + VDIM)
    else:
        cotangent_all = lax.all_gather(cotangent_wide, both, axis=0, tiled=True)
        normed_all = gather_group(normed, 0)
        query_full = matmul(normed_all, query_weight).reshape(group_rows, heads_here, query_width)
        query = jnp.concatenate(
            [
                query_full[..., :NOPE],
                rotate(query_full[..., NOPE:], cosine[:, None, :], sine[:, None, :]),
            ],
            axis=-1,
        ).astype(jnp.bfloat16)
        compressed = matmul(normed_all, latent_weight)
        latent = compressed[:, :LATENT]
        latent_scale = inv_rms(latent)
        latent_normed = (latent * latent_scale * latent_gain).astype(jnp.bfloat16)
        key_rope = rotate(compressed[:, LATENT:], cosine, sine).astype(jnp.bfloat16)
        expanded = (
            matmul(latent_normed, expand_weight)
            .astype(jnp.bfloat16)
            .reshape(group_rows, heads_here, NOPE + VDIM)
        )
    key_nope = expanded[..., :NOPE]
    values = expanded[..., NOPE:]

    def score_block():
        raw = jnp.einsum(
            "ihd,jhd->hij", query[..., :NOPE], key_nope, preferred_element_type=jnp.float32
        )
        raw = raw + jnp.einsum(
            "ihd,jd->hij", query[..., NOPE:], key_rope, preferred_element_type=jnp.float32
        )
        return jnp.where(allowed[None], raw * score_scale, -1e30)

    if sizes != (8, 4):
        scores = score_block()
        peak = jnp.max(scores, axis=-1, keepdims=True)
        weights = jnp.exp(scores - peak)
        total = jnp.sum(weights, axis=-1, keepdims=True)
        log_total = peak + jnp.log(total)
        mixed = jnp.einsum(
            "hij,jhd->ihd",
            (weights / total).astype(jnp.bfloat16),
            values,
            preferred_element_type=jnp.float32,
        )
        mixed = mixed.astype(jnp.bfloat16).reshape(group_rows, heads_here * VDIM)
        attended = sum_group(matmul(mixed, output_weight).astype(jnp.bfloat16), 1)
        hidden_one = activations + attended
        second_scale = inv_rms(hidden_one)
        normed_two = (hidden_one * second_scale * second_gain).astype(jnp.bfloat16)
        gates = jax.nn.sigmoid(matmul(normed_two, router_weight))
        weighted = hit * gates
        mixing_at = route_scale * weighted / jnp.sum(weighted, axis=1, keepdims=True)
        mixing_high = mixing_at.astype(jnp.bfloat16)
        mixing_low = (mixing_at - mixing_high.astype(jnp.float32)).astype(jnp.bfloat16)
        normed_wide = jnp.concatenate([normed_two, mixing_high, mixing_low], axis=1)
    chosen = jnp.sum(choose * gates[:, None, :], axis=-1)
    chosen_total = jnp.sum(chosen, axis=1, keepdims=True)
    upstream = cotangent.astype(jnp.float32)
    marks = (cotangent_all, pl.BlockSpec((quad_rows, lanes), lambda i: (i, width // lanes)))
    normed_tokens, (grads_slots, shared_raw) = gather_all(
        normed_wide,
        2,
        functools.partial(grads_kernel, pair_rows),
        quads,
        [whole(here), (cotangent_all, pair_spec(cotangent_all, quads)), whole(down_part)],
        [
            (slots, slots_spec(slots, quads)),
            (shape((all_rows, shared_wide), jnp.float32), pl.BlockSpec((quad_rows, shared_wide), lambda i: (i, 0))),
        ],
        gather_flops,
    )
    normed_tokens = normed_tokens.reshape(all_rows, -1)
    token_spec = pl.BlockSpec((quad_rows, shared_wide), lambda i: (i, 0))
    token_shape = shape((all_rows, shared_wide), jnp.bfloat16)
    rows_slots, mix_slots, shared_hidden, shared_gate_grad, shared_lift_grad = call(
        functools.partial(rows_kernel, pair_rows),
        quads,
        [
            whole(here),
            whole(twice),
            marks,
            (normed_tokens, pair_spec(normed_tokens, quads)),
            (shared_raw, token_spec),
            whole(gate_part),
            whole(up_part),
        ],
        [
            (slots, slots_spec(slots, quads)),
            (slots_one, slots_spec(slots_one, quads)),
            (token_shape, token_spec),
            (token_shape, token_spec),
            (token_shape, token_spec),
        ],
        gather_flops + 2 * all_rows * width * shared_wide,
    )
    hidden_here = expert_gate.shape[2]
    gate_rows, up_rows = expert_gate.transpose(0, 2, 1), expert_up.transpose(0, 2, 1)

    def tile_spec(rows, n):
        per = slot_rows // rows
        return pl.BlockSpec((1, rows, n), lambda i: (i // per, i % per, 0))

    def expert_spec(rows, matrix):
        per = slot_rows // rows
        return pl.BlockSpec((1,) + matrix.shape[1:], lambda i: (i // per, 0, 0))

    large, small = 32 * CAP, 16 * CAP
    narrow = shape((local_experts, slot_rows, hidden_here), jnp.bfloat16)
    one_matmul = 2 * local_experts * slot_rows * width * hidden_here
    routed_hidden, mixed_hidden, slope, active, produced = call(
        forward_kernel,
        local_experts * (slot_rows // large),
        [
            (rows_slots, tile_spec(large, width)),
            (mix_slots, tile_spec(large, lanes)),
            (gate_rows, expert_spec(large, gate_rows)),
            (up_rows, expert_spec(large, up_rows)),
            (expert_down, expert_spec(large, expert_down)),
        ],
        [(narrow, tile_spec(large, hidden_here))] * 4 + [(slots, tile_spec(large, width))],
        3 * one_matmul,
    )
    dense = shape((all_rows, width), jnp.bfloat16)
    dense_wide = shape((all_rows, width + lanes), jnp.bfloat16)
    (out_dense,) = call(
        functools.partial(out_kernel, pair_rows),
        quads,
        [
            whole(here),
            marks,
            (produced, slots_spec(slots, quads)),
            (shared_hidden, token_spec),
            whole(down_part),
        ],
        [(dense, pair_spec(dense, quads))],
        gather_flops,
    )
    narrow_tile = tile_spec(small, hidden_here)
    routed_out, (gate_grad, lift_grad, returned, mix_grad_slots) = sum_all(
        out_dense.reshape(blocks, token_rows, width),
        6,
        backward_kernel,
        local_experts * (slot_rows // small),
        [
            (grads_slots, tile_spec(small, width)),
            (routed_hidden, narrow_tile),
            (slope, narrow_tile),
            (active, narrow_tile),
            (gate_rows, expert_spec(small, gate_rows)),
            (up_rows, expert_spec(small, up_rows)),
            (expert_down, expert_spec(small, expert_down)),
        ],
        [
            (narrow, narrow_tile),
            (narrow, narrow_tile),
            (slots, tile_spec(small, width)),
            (slots_one, tile_spec(small, lanes)),
        ],
        3 * one_matmul,
    )
    (back_dense,) = call(
        functools.partial(back_kernel, pair_rows),
        quads,
        [
            whole(here),
            whole(high_at),
            whole(low_at),
            marks,
            (returned, slots_spec(slots, quads)),
            (mix_grad_slots, slots_spec(slots_one, quads)),
            (shared_gate_grad, token_spec),
            (shared_lift_grad, token_spec),
            whole(gate_part),
            whole(up_part),
        ],
        [(dense_wide, pair_spec(dense_wide, quads))],
        gather_flops + 2 * all_rows * width * shared_wide,
    )
    shared_sum = shape((shared_wide, width), jnp.float32)
    shared_out = (shared_sum, whole_spec(shared_sum))
    plain_spec = pl.BlockSpec((pair_rows, width), lambda i: (i, 0))
    shared_spec = pl.BlockSpec((pair_rows, shared_wide), lambda i: (i, 0))
    column_half = width // 2
    half_spec = lambda m: pl.BlockSpec((1, m, column_half), lambda i: (i // 2, 0, i % 2))
    narrow_spec = pl.BlockSpec((1, slot_rows, hidden_here), lambda i: (i // 2, 0, 0))
    shared_ins = [
        (normed_tokens, plain_spec),
        (cotangent_all, plain_spec),
        (shared_gate_grad, shared_spec),
        (shared_lift_grad, shared_spec),
        (shared_hidden, shared_spec),
    ]
    weight_ins = [
        (rows_slots, half_spec(slot_rows)),
        (grads_slots, half_spec(slot_rows)),
        (gate_grad, narrow_spec),
        (lift_grad, narrow_spec),
        (mixed_hidden, narrow_spec),
    ]
    back_blocks = back_dense.reshape(blocks, token_rows, -1)
    shared_flops = 6 * all_rows * width * shared_wide
    together = pairs == 2 * local_experts
    weight_type = jnp.bfloat16 if together else jnp.float32
    weight_shape = shape((local_experts, hidden_here, width), weight_type)
    weight_outs = [(weight_shape, half_spec(hidden_here))] * 3
    if together:
        back_here, sums = sum_all(
            back_blocks,
            3,
            gradients_kernel,
            pairs,
            shared_ins + weight_ins,
            [shared_out] * 3 + weight_outs,
            shared_flops + 3 * one_matmul,
        )
        shared_sums = sums[:3]
        weight_grads = [value.astype(jnp.float32) for value in sums[3:]]
    else:
        back_here, shared_sums = sum_all(
            back_blocks, 3, shared_kernel, pairs, shared_ins, [shared_out] * 3, shared_flops
        )
        weight_grads = call(
            weights_alone, 2 * local_experts, weight_ins, weight_outs, 3 * one_matmul
        )
    routed_back = back_here[:, :width]
    mix_grad = back_here[:, width : width + 2 * weight_count * routes.shape[1]]
    mix_grad = jnp.sum(mix_grad.reshape(token_rows, routes.shape[1], -1), axis=2)
    shared_grads = jnp.concatenate([total[:shared_here] for total in shared_sums], axis=0)
    shared_grads = shared_grads.astype(jnp.bfloat16)
    swapped = lax.all_to_all(shared_grads, "expert", split_axis=1, concat_axis=0, tiled=True)
    swapped = swapped.reshape(expert_lanes, 3, shared_here, -1).astype(jnp.float32)
    shared_gradients = [swapped[:, i].reshape(expert_lanes * shared_here, -1) for i in range(3)]
    chosen_grad = route_scale * (
        mix_grad / chosen_total
        - jnp.sum(mix_grad * chosen, axis=1, keepdims=True) / chosen_total**2
    )
    logit_grad = jnp.sum(choose * chosen_grad[:, :, None], axis=1) * gates * (1.0 - gates)
    normed_two_grad = (
        routed_back
        + jnp.dot(logit_grad, router_weight.astype(jnp.float32).T, precision=highest)
    )
    router_gradient = jnp.dot(logit_grad.T, normed_two.astype(jnp.float32), precision=highest)
    back_two, second_gain_gradient = norm_back(
        normed_two_grad, hidden_one, second_scale, second_gain
    )
    hidden_grad = upstream + back_two
    hidden_group = gather_group(hidden_grad.astype(jnp.bfloat16), 4)
    output_gradient = trans_times(hidden_group, mixed).astype(jnp.bfloat16)
    hidden_group, output_gradient = lax.optimization_barrier((hidden_group, output_gradient))
    output_shard = sum_shards(output_gradient)
    mixed_grad = (
        times_trans(hidden_group, output_weight)
        .astype(jnp.bfloat16)
        .reshape(group_rows, heads_here, VDIM)
    )
    probs = jnp.exp(score_block() - log_total)
    prob_grad = jnp.einsum("ihd,jhd->hij", mixed_grad, values, preferred_element_type=jnp.float32)
    centre = jnp.sum(probs * prob_grad, axis=-1, keepdims=True)
    score_grad = (probs * (prob_grad - centre)).astype(jnp.bfloat16)
    value_grad = jnp.einsum(
        "hij,ihd->jhd", probs.astype(jnp.bfloat16), mixed_grad, preferred_element_type=jnp.float32
    )
    query_nope_grad = (
        jnp.einsum("hij,jhd->ihd", score_grad, key_nope, preferred_element_type=jnp.float32)
        * score_scale
    )
    query_rope_grad = (
        jnp.einsum("hij,jd->ihd", score_grad, key_rope, preferred_element_type=jnp.float32)
        * score_scale
    )
    key_nope_grad = (
        jnp.einsum(
            "hij,ihd->jhd", score_grad, query[..., :NOPE], preferred_element_type=jnp.float32
        )
        * score_scale
    )
    key_rope_grad = (
        jnp.einsum("hij,ihd->jd", score_grad, query[..., NOPE:], preferred_element_type=jnp.float32)
        * score_scale
    )
    query_grad = jnp.concatenate(
        [query_nope_grad, unrotate(query_rope_grad, cosine[:, None, :], sine[:, None, :])], axis=-1
    )
    query_grad = query_grad.astype(jnp.bfloat16).reshape(group_rows, heads_here * query_width)
    expand_grad = (
        jnp.concatenate([key_nope_grad, value_grad], axis=-1)
        .astype(jnp.bfloat16)
        .reshape(group_rows, heads_here * (NOPE + VDIM))
    )
    expert_grads = (weight_grads[0].transpose(0, 2, 1), weight_grads[1].transpose(0, 2, 1), weight_grads[2])
    layer_out = (hidden_one + routed_out).astype(jnp.bfloat16)
    query_gradient = trans_times(normed_all, query_grad)
    expand_gradient = trans_times(latent_normed, expand_grad).astype(jnp.bfloat16)
    latent_normed_grad = times_trans(expand_grad, expand_weight)
    latent_back, latent_gain_gradient = norm_back(
        latent_normed_grad, latent, latent_scale, latent_gain
    )
    compressed_grad = jnp.concatenate([latent_back, unrotate(key_rope_grad, cosine, sine)], axis=-1)
    compressed_grad = compressed_grad.astype(jnp.bfloat16)
    latent_weight_gradient = trans_times(compressed_grad, normed_all)
    normed_part = times_trans(query_grad, query_weight) + times_trans(compressed_grad, latent_weight)
    first_gain_gradient = jnp.sum(normed_part * normed_all.astype(jnp.float32), axis=0) / first_gain
    shards = (
        sum_shards(query_gradient.astype(jnp.bfloat16)).astype(jnp.float32),
        sum_shards(expand_gradient).astype(jnp.float32),
        output_shard.T.astype(jnp.float32),
    )
    latent_columns = latent_weight.shape[1]
    rest = jnp.concatenate(
        [
            router_gradient,
            first_gain_gradient[None],
            second_gain_gradient[None],
            jnp.pad(latent_gain_gradient, (0, width - LATENT))[None],
        ],
        axis=0,
    ).astype(jnp.bfloat16)
    wanted = -(-(latent_columns + rest.shape[0]) // 64) * 64 - latent_columns
    rest = jnp.pad(rest, ((0, wanted - rest.shape[0]), (0, 0)))
    total, normed_grad = total_over_all(
        latent_weight_gradient.astype(jnp.bfloat16), rest, normed_part.astype(jnp.bfloat16), 7
    )
    back_one, _ = norm_back(normed_grad, activations, first_scale, first_gain)
    token_gradient = hidden_grad + back_one
    gains_at = latent_columns + expert_count
    wide = lambda value: value.astype(jnp.float32)
    totals = (
        wide(total[:latent_columns]).T,
        wide(total[gains_at + 2, :LATENT]),
        wide(total[latent_columns:gains_at]).T,
        wide(total[gains_at]),
        wide(total[gains_at + 1]),
    )
    return (
        layer_out,
        token_gradient,
        totals[3],
        shards[0],
        totals[0],
        totals[1],
        shards[1],
        shards[2],
        totals[4],
        totals[2],
        shared_gradients[0].T,
        shared_gradients[1].T,
        shared_gradients[2],
        expert_grads[0],
        expert_grads[1],
        expert_grads[2],
    )


def solution(mesh):
    return jax.shard_map(
        per_device,
        mesh=mesh,
        in_specs=(
            P(("expert", "weight"), None),
            P(("expert", "weight"), None),
            P("expert", None),
            P(("expert", "weight"), None),
            P(),
            P(None, "weight"),
            P(),
            P(),
            P(None, "weight"),
            P("weight", None),
            P(),
            P(),
            P(None, "weight"),
            P(None, "weight"),
            P("weight", None),
            P("expert", None, "weight"),
            P("expert", None, "weight"),
            P("expert", "weight", None),
        ),
        out_specs=(
            P(("expert", "weight"), None),
            P(("expert", "weight"), None),
            P(),
            P("expert", "weight"),
            P(),
            P(),
            P("expert", "weight"),
            P("weight", "expert"),
            P(),
            P(),
            P("expert", "weight"),
            P("expert", "weight"),
            P("weight", "expert"),
            P("expert", None, "weight"),
            P("expert", None, "weight"),
            P("expert", "weight", None),
        ),
        check_vma=False,
    )
```

```python
import functools

import jax
import jax.numpy as jnp
from jax import lax
from jax.experimental import pallas as pl
from jax.experimental.pallas import tpu as pltpu
from jax.sharding import PartitionSpec as P

NOPE = 128
ROPE = 64
VDIM = 128
LATENT = 512
CAP = 20


eps = 1e-06
route_scale = 2.446
rope_base = 50000.0
highest = lax.Precision.HIGHEST


def matmul(left, right):
    return jnp.dot(left, right, preferred_element_type=jnp.float32)


def trans_times(left, right):
    return lax.dot_general(
        left, right, (((0,), (0,)), ((), ())), preferred_element_type=jnp.float32
    )


def times_trans(left, right):
    return lax.dot_general(
        left, right, (((1,), (1,)), ((), ())), preferred_element_type=jnp.float32
    )


def inv_rms(value):
    return lax.rsqrt(jnp.mean(value * value, axis=-1, keepdims=True) + eps)


def norm_back(grad_out, value, scale, gain):
    scaled = grad_out * gain
    grad_in = scale * scaled - value * scale**3 * jnp.mean(scaled * value, axis=-1, keepdims=True)
    gain_grad = jnp.sum(grad_out * value * scale, axis=0)
    return (grad_in, gain_grad)


def rope_tables(seg):
    size = seg.shape[0]
    index = jnp.arange(size, dtype=jnp.int32)
    earlier = jnp.sum((seg[None, :] < seg[:, None]).astype(jnp.int32), axis=1)
    place = (index - earlier).astype(jnp.float32)
    half = ROPE // 2
    freqs = rope_base ** (-(jnp.arange(half, dtype=jnp.float32) * 2.0 / ROPE))
    angle = place[:, None] * freqs[None, :]
    return (jnp.cos(angle), jnp.sin(angle))


def attention_mask(seg):
    index = jnp.arange(seg.shape[0], dtype=jnp.int32)
    return (seg[:, None] == seg[None, :]) & (index[None, :] <= index[:, None])


def rotate(value, cosine, sine):
    half = value.shape[-1] // 2
    first, second = (value[..., :half], value[..., half:])
    return jnp.concatenate(
        [first * cosine - second * sine, second * cosine + first * sine], axis=-1
    )


def unrotate(value, cosine, sine):
    half = value.shape[-1] // 2
    first, second = (value[..., :half], value[..., half:])
    return jnp.concatenate(
        [first * cosine + second * sine, second * cosine - first * sine], axis=-1
    )


lanes = 128
vmem_limit = 64 * 1024 * 1024 - 131072


def token_slots(marks, here, local_experts, half):
    codes = times_trans(here, marks)
    count = codes.shape[1]
    rank = jnp.floor(codes * (1.0 / 32.0))
    place = codes - 32.0 * rank
    token = lax.broadcasted_iota(jnp.int32, codes.shape, 1)
    slot = jnp.where(codes >= 0, place + jnp.where(token >= half, float(CAP), 0.0), -1.0)
    row = lax.broadcasted_iota(jnp.int32, (2 * CAP, count), 0).astype(jnp.float32)
    picks = [jnp.where(row == slot[e : e + 1], 1.0, 0.0) for e in range(local_experts)]
    return picks, rank


def pair_slots(marks_ref, here_ref, local_experts, pair):
    count = marks_ref.shape[0] // pair
    return [
        token_slots(marks_ref[j * pair : (j + 1) * pair], here_ref[...], local_experts, pair // 2)
        for j in range(count)
    ]


def slot_part(value, e):
    return value[e * 2 * CAP : (e + 1) * 2 * CAP]


def gather_rows(slots, values, pair, out_ref):
    rows = [
        jnp.dot(
            jnp.concatenate(picks, axis=0).astype(jnp.bfloat16),
            values[j * pair : (j + 1) * pair],
            preferred_element_type=jnp.float32,
        )
        for j, (picks, _) in enumerate(slots)
    ]
    for e in range(out_ref.shape[0]):
        together = jnp.concatenate([slot_part(value, e) for value in rows], axis=0)
        out_ref[e] = together.astype(jnp.bfloat16)


def spread_rows(slots, rows_ref):
    local_experts = rows_ref.shape[0]
    rows = [rows_ref[e].astype(jnp.float32) for e in range(local_experts)]
    totals = []
    for j, (picks, _) in enumerate(slots):
        part = jnp.concatenate([slot_part(value, j) for value in rows], axis=0)
        pick = jnp.concatenate(picks, axis=0).astype(jnp.bfloat16)
        totals.append(trans_times(pick, part.astype(jnp.bfloat16)))
    return jnp.concatenate(totals, axis=0)


def grads_kernel(pair, ins, outs):
    here_ref, value_ref, down_ref = ins
    rows_ref, back_ref = outs
    width = rows_ref.shape[2]
    slots = pair_slots(value_ref.at[:, width:], here_ref, rows_ref.shape[0], pair)
    values = value_ref[:, :width]
    gather_rows(slots, values, pair, rows_ref)
    back_ref[...] = times_trans(values, down_ref[...])


def rows_kernel(
    pair,
    here_ref,
    twice_ref,
    marks_ref,
    value_ref,
    back_ref,
    gate_ref,
    up_ref,
    rows_ref,
    mix_ref,
    hidden_ref,
    gate_grad_ref,
    lift_grad_ref,
):
    width = rows_ref.shape[2]
    slots = pair_slots(marks_ref, here_ref, rows_ref.shape[0], pair)
    values = value_ref[:, :width]
    gather_rows(slots, values, pair, rows_ref)
    for j, (picks, _) in enumerate(slots):
        mixing = times_trans(twice_ref[...], value_ref[j * pair : (j + 1) * pair, width:])
        for e, pick in enumerate(picks):
            column = jnp.sum(pick * mixing[e : e + 1], axis=1, keepdims=True)
            column = jnp.broadcast_to(column, (2 * CAP, lanes))
            mix_ref[e, j * 2 * CAP : (j + 1) * 2 * CAP] = column
    gate = times_trans(values, gate_ref[...])
    lift = times_trans(values, up_ref[...])
    back = back_ref[...]
    sigma = jax.nn.sigmoid(gate)
    active = gate * sigma
    hidden_ref[...] = (active * lift).astype(jnp.bfloat16)
    gate_grad_ref[...] = (back * lift * sigma * (1.0 + gate * (1.0 - sigma))).astype(jnp.bfloat16)
    lift_grad_ref[...] = (back * active).astype(jnp.bfloat16)


def forward_kernel(
    rows_ref,
    mix_ref,
    gate_ref,
    up_ref,
    down_ref,
    hidden_ref,
    mixed_ref,
    slope_ref,
    active_ref,
    produced_ref,
):
    rows = rows_ref[0]
    gate = times_trans(rows, gate_ref[0])
    lift = times_trans(rows, up_ref[0])
    mix = mix_ref[0][:, :1]
    sigma = jax.nn.sigmoid(gate)
    active = gate * sigma
    hidden = active * lift
    mixed_hidden = (mix * hidden).astype(jnp.bfloat16)
    hidden_ref[0] = hidden.astype(jnp.bfloat16)
    mixed_ref[0] = mixed_hidden
    slope_ref[0] = (mix * lift * sigma * (1.0 + gate * (1.0 - sigma))).astype(jnp.bfloat16)
    active_ref[0] = (mix * active).astype(jnp.bfloat16)
    produced_ref[0] = matmul(mixed_hidden, down_ref[0]).astype(jnp.bfloat16)


def backward_kernel(turn, ins, outs):
    grads_ref, hidden_ref, slope_ref, active_ref, gate_ref, up_ref, down_ref = ins
    gate_grad_ref, lift_grad_ref, returned_ref, mix_grad_ref = outs
    back = times_trans(grads_ref[0], down_ref[0])
    mix_grad = jnp.sum(hidden_ref[0].astype(jnp.float32) * back, axis=1, keepdims=True)
    mix_grad_ref[0] = jnp.broadcast_to(mix_grad, mix_grad_ref.shape[1:])
    gate_grad = (back * slope_ref[0].astype(jnp.float32)).astype(jnp.bfloat16)
    lift_grad = (back * active_ref[0].astype(jnp.float32)).astype(jnp.bfloat16)
    gate_grad_ref[0] = gate_grad
    lift_grad_ref[0] = lift_grad
    returned = matmul(gate_grad, gate_ref[0]) + matmul(lift_grad, up_ref[0])
    returned_ref[0] = returned.astype(jnp.bfloat16)


def back_kernel(
    pair,
    here_ref,
    high_ref,
    low_ref,
    marks_ref,
    rows_ref,
    mix_grad_ref,
    gate_grad_ref,
    lift_grad_ref,
    gate_ref,
    up_ref,
    out_ref,
):
    width = rows_ref.shape[2]
    slots = pair_slots(marks_ref, here_ref, rows_ref.shape[0], pair)
    total = spread_rows(slots, rows_ref)
    total = total + matmul(gate_grad_ref[...], gate_ref[...])
    total = total + matmul(lift_grad_ref[...], up_ref[...])
    out_ref[:, :width] = total.astype(jnp.bfloat16)
    for j, (picks, rank) in enumerate(slots):
        choice = lax.broadcasted_iota(jnp.int32, rank.shape, 0).astype(jnp.float32)
        mix_grad = jnp.zeros(rank.shape, jnp.float32)
        for e, pick in enumerate(picks):
            column = slot_part(mix_grad_ref[e], j)[:, :1]
            row = jnp.sum(pick * column, axis=0, keepdims=True)
            mix_grad = mix_grad + jnp.where(choice == rank[e : e + 1], row, 0.0)
        high = mix_grad.astype(jnp.bfloat16)
        low = (mix_grad - high.astype(jnp.float32)).astype(jnp.bfloat16)
        sent = trans_times(high, high_ref[...]) + trans_times(low, low_ref[...])
        out_ref[j * pair : (j + 1) * pair, width:] = sent.astype(jnp.bfloat16)


def out_kernel(pair, here_ref, marks_ref, rows_ref, hidden_ref, down_ref, out_ref):
    slots = pair_slots(marks_ref, here_ref, rows_ref.shape[0], pair)
    total = spread_rows(slots, rows_ref)
    total = total + matmul(hidden_ref[...], down_ref[...])
    out_ref[...] = total.astype(jnp.bfloat16)


def whole_spec(array):
    zeros = (0,) * array.ndim
    return pl.BlockSpec(array.shape, lambda i: zeros)


def pair_spec(array, pairs):
    block = (array.shape[0] // pairs,) + array.shape[1:]
    zeros = (0,) * (array.ndim - 1)
    return pl.BlockSpec(block, lambda i: (i,) + zeros)


def slots_spec(array, pairs):
    block = (array.shape[0], array.shape[1] // pairs) + array.shape[2:]
    return pl.BlockSpec(block, lambda i: (0, i, 0))


def cost(flops, *arrays):
    moved = sum(a.size * a.dtype.itemsize for a in arrays)
    return pl.CostEstimate(flops=int(flops), bytes_accessed=int(moved), transcendentals=0)


def call(kernel, grid, ins, outs, flops):
    arrays = [a for a, _ in ins]
    shapes = [s for s, _ in outs]
    return pl.pallas_call(
        kernel,
        grid=(grid,),
        in_specs=[s for _, s in ins],
        out_specs=[s for _, s in outs],
        out_shape=shapes,
        cost_estimate=cost(flops, *arrays, *shapes),
        compiler_params=pltpu.CompilerParams(vmem_limit_bytes=vmem_limit),
    )(*arrays)


MESH = pl.DeviceIdType.MESH


def places():
    expert, weight = lax.axis_index("expert"), lax.axis_index("weight")
    return lax.div(expert, 2), lax.rem(expert, 2), lax.div(weight, 2), lax.rem(weight, 2)


def device(z, x, y, c):
    return (z * 2 + x, y * 2 + c)


def shard(z, x, y, c):
    return z * 8 + x * 4 + y * 2 + c


def push(source, target, send, receive, to):
    return pltpu.make_async_remote_copy(
        src_ref=source,
        dst_ref=target,
        send_sem=send,
        recv_sem=receive,
        device_id=to,
        device_id_type=MESH,
    )


class Sends:
    def __init__(self, semaphores):
        self.semaphores = semaphores
        self.started = []

    def plan(self, source, target, receive, to, when=None):
        copy = push(source, target, self.semaphores.at[len(self.started)], receive, to)
        self.started.append((copy, when))
        return copy

    def start(self, source, target, receive, to, when=None):
        copy = self.plan(source, target, receive, to, when)
        if when is None:
            copy.start()
        else:
            pl.when(when)(copy.start)

    def finish(self):
        for copy, when in self.started:
            if when is None:
                copy.wait_send()
            else:
                pl.when(when)(copy.wait_send)


def landed(target, receive, to):
    push(target, target, receive, receive, to).wait_recv()


def greet(devices):
    barrier = pltpu.get_barrier_semaphore()
    count = 0
    for to, when in devices:
        signal = functools.partial(
            pl.semaphore_signal, barrier, inc=1, device_id=to, device_id_type=MESH
        )
        if when is None:
            signal()
            count = count + 1
        else:
            pl.when(when)(signal)
            count = count + when.astype(jnp.int32)
    pl.semaphore_wait(barrier, count)


def add_rows(target, sources, start, rows):
    step = 16

    def body(i, carry):
        part = pl.ds(pl.multiple_of(start + i * step, step), step)
        total = target[part].astype(jnp.float32)
        for source, offset in sources:
            there = pl.ds(pl.multiple_of(start - offset + i * step, step), step)
            total = total + source[there].astype(jnp.float32)
        target[part] = total.astype(target.dtype)
        return carry

    lax.fori_loop(0, rows // step, body, 0)


def ordered(z, first, second):
    upper = lax.div(z, 2)
    inner = z + upper * (3 - 2 * z)
    value = first + inner * (second - first)
    return value + upper * (3 - 2 * value)


class Gather:
    def __init__(self, x_ref, out_ref, sends, recv_sems, local_sem, place, cut=None):
        z, x, y, c = place
        rows = x_ref.shape[0]
        cut = rows // 2 if cut is None else cut
        self.parts = [pl.ds(0, cut), pl.ds(cut, rows - cut)]
        over, side, mate = device(z, 1 - x, y, c), device(z, x, 1 - y, c), device(z, x, y, 1 - c)
        up, down = device(z + 1, x, y, c), device(z - 1, x, y, c)
        self.out_ref, self.recv_sems, self.mate = out_ref, recv_sems, mate
        planes = [ordered(z, (0, 1, 2, 3)[step], (1, 0, 2, 3)[step]) for step in range(4)]
        self.planes = planes
        self.rising = [(zz <= z) & (z < 3) for zz in planes]
        self.falling = [(zz >= z) & (z > 0) for zz in planes]
        self.mine = [shard(zz, x, y, c) for zz in planes]
        self.overs = [shard(zz, 1 - x, y, c) for zz in planes]
        self.sides = [shard(zz, x, 1 - y, c) for zz in planes]
        self.corners = [shard(zz, 1 - x, 1 - y, c) for zz in planes]
        self.mates = [
            (shard(zz, x, y, 1 - c), shard(zz, 1 - x, y, 1 - c), shard(zz, x, 1 - y, 1 - c))
            for zz in planes
        ]
        self.mate_corners = [shard(zz, 1 - x, 1 - y, 1 - c) for zz in planes]
        self.keep = pltpu.make_async_copy(x_ref, out_ref.at[self.mine[0]], local_sem)
        self.whole_copies, self.relay_copies, self.corner_copies = [], [], []

        def copy(ref, receive, to, when=None, source=None):
            return sends.plan(ref if source is None else source, ref, receive, to, when)

        for step in range(4):
            i = self.mine[step]
            source = x_ref if step == 0 else None
            there, receive = out_ref.at[i], recv_sems.at[i, 0]
            self.whole_copies.append(
                [
                    (copy(there, receive, up, self.rising[step], source), self.rising[step]),
                    (copy(there, receive, down, self.falling[step], source), self.falling[step]),
                    (copy(there, receive, over, None, source), None),
                    (copy(there, receive, side, None, source), None),
                    (copy(there, receive, mate, None, source), None),
                ]
            )
            i, j = self.overs[step], self.sides[step]
            self.relay_copies.append(
                [
                    copy(self.halves(i, 0), recv_sems.at[i, 0], side),
                    copy(out_ref.at[i], recv_sems.at[i, 0], mate),
                    copy(self.halves(j, 1), recv_sems.at[j, 1], over),
                    copy(out_ref.at[j], recv_sems.at[j, 0], mate),
                ]
            )
            i = self.corners[step]
            self.corner_copies.append(
                [copy(self.halves(i, h), recv_sems.at[i, h], mate) for h in range(2)]
            )

    def halves(self, i, h):
        return self.out_ref.at[i, self.parts[h]]

    def full_here(self, i):
        landed(self.out_ref.at[i], self.recv_sems.at[i, 0], self.mate)

    def half_here(self, i, h):
        landed(self.halves(i, h), self.recv_sems.at[i, h], self.mate)

    def whole(self, step):
        if step == 0:
            self.keep.start()
        else:
            self.full_here(self.mine[step])
        for copy, when in self.whole_copies[step]:
            if when is None:
                copy.start()
            else:
                pl.when(when)(copy.start)

    def relay(self, step):
        self.full_here(self.overs[step])
        self.relay_copies[step][0].start()
        self.relay_copies[step][1].start()
        self.full_here(self.sides[step])
        self.relay_copies[step][2].start()
        self.relay_copies[step][3].start()

    def corner(self, step):
        for h in range(2):
            self.half_here(self.corners[step], h)
            self.corner_copies[step][h].start()

    def rest(self, step):
        for i in self.mates[step]:
            self.full_here(i)
        for h in range(2):
            self.half_here(self.mate_corners[step], h)
        if step == 0:
            self.keep.wait()

    def last(self):
        for step in range(4):
            self.rest(step)


def gather_neighbours(place):
    z, x, y, c = place
    return [
        (device(z, 1 - x, y, c), None),
        (device(z, x, 1 - y, c), None),
        (device(z, x, y, 1 - c), None),
        (device(z + 1, x, y, c), z < 3),
        (device(z - 1, x, y, c), z > 0),
    ]


def token_kernel(
    pair,
    x_ref,
    here_ref,
    value_ref,
    down_ref,
    twice_ref,
    gate_ref,
    up_ref,
    cotangent_hbm,
    out_ref,
    grads_ref,
    rows_hbm,
    mix_ref,
    hidden_ref,
    gate_grad_ref,
    lift_grad_ref,
    raw,
    arrived,
    marks,
    stage,
    send_sems,
    recv_sems,
    local_sem,
    load_sems,
    store_sems,
):
    turn, turns = pl.program_id(0), pl.num_programs(0)
    place = places()
    sends = Sends(send_sems)
    gather = Gather(x_ref, out_ref, sends, recv_sems, local_sem, place)
    quad, rows = value_ref.shape[0], x_ref.shape[0]
    count = quad // rows
    width = grads_ref.shape[2]
    slot_rows = grads_ref.shape[1]

    def begin():
        greet(gather_neighbours(place))
        gather.whole(0)

    def early():
        gather.relay(1)
        gather.corner(0)

    def part(index, size):
        return pl.ds(pl.multiple_of(index * size, 16), size)

    stores = {}

    def plane(step):
        gather.rest(step)
        loads = []
        for k in range(2):
            group = gather.planes[step] * 2 + k
            copies = [
                pltpu.make_async_copy(
                    out_ref.at[group * count + i],
                    arrived.at[k, pl.ds(i * rows, rows)],
                    load_sems.at[k, i],
                )
                for i in range(count)
            ]
            copies.append(
                pltpu.make_async_copy(
                    cotangent_hbm.at[part(group, quad), pl.ds(width, lanes)],
                    marks.at[k],
                    load_sems.at[k, count],
                )
            )
            for copy in copies:
                copy.start()
            loads.append(copies)
        for k in range(2):
            group = gather.planes[step] * 2 + k
            for copy in loads[k]:
                copy.wait()
            if k in stores:
                stores[k].wait()
            tokens = part(group, quad)
            rows_kernel(
                pair,
                here_ref,
                twice_ref,
                marks.at[k],
                arrived.at[k],
                raw.at[tokens],
                gate_ref,
                up_ref,
                stage.at[k],
                mix_ref.at[:, part(group, slot_rows)],
                hidden_ref.at[tokens],
                gate_grad_ref.at[tokens],
                lift_grad_ref.at[tokens],
            )
            stores[k] = pltpu.make_async_copy(
                stage.at[k], rows_hbm.at[:, part(group, slot_rows)], store_sems.at[k]
            )
            stores[k].start()

    def end():
        gather.whole(3)
        gather.relay(2)
        plane(0)
        gather.corner(1)
        gather.relay(3)
        plane(1)
        gather.corner(2)
        plane(2)
        gather.corner(3)
        plane(3)
        for k in range(2):
            stores[k].wait()
        sends.finish()

    pieces = [
        begin,
        lambda: None,
        functools.partial(gather.whole, 1),
        functools.partial(gather.relay, 0),
        functools.partial(gather.whole, 2),
        lambda: None,
        early,
    ]
    for number, piece in enumerate(pieces):
        pl.when(turn == number)(piece)
    grads_kernel(pair, (here_ref, value_ref, down_ref), (grads_ref, raw.at[part(turn, quad)]))
    pl.when(turn == turns - 1)(end)


def gather_tokens(
    value, cotangent, here, twice, down, gate, up, local_experts, slot_rows, pair, number
):
    rows, wide = value.shape
    width = down.shape[1]
    quad, all_rows, turns = 4 * rows, 32 * rows, 8
    shared_wide = down.shape[0]
    shape, low = jax.ShapeDtypeStruct, jnp.bfloat16
    slots = shape((local_experts, slot_rows, width), low)
    token_part = shape((all_rows, shared_wide), low)
    mix = shape((local_experts, slot_rows, lanes), jnp.float32)
    away = pl.BlockSpec(memory_space=pl.ANY)
    ins = [
        (value, whole_spec(value)),
        (here, whole_spec(here)),
        (cotangent, pair_spec(cotangent, turns)),
        (down, whole_spec(down)),
        (twice, whole_spec(twice)),
        (gate, whole_spec(gate)),
        (up, whole_spec(up)),
        (cotangent, away),
    ]
    outs = [
        (shape((32,) + value.shape, low), away),
        (slots, slots_spec(slots, turns)),
        (slots, away),
        (mix, whole_spec(mix)),
        (token_part, whole_spec(token_part)),
        (token_part, whole_spec(token_part)),
        (token_part, whole_spec(token_part)),
    ]
    part = slot_rows // turns
    flops = 4 * all_rows * width * (2 * CAP * local_experts + 2 * shared_wide)
    return pl.pallas_call(
        functools.partial(token_kernel, pair),
        grid=(turns,),
        out_shape=[o for o, _ in outs],
        in_specs=[spec for _, spec in ins],
        out_specs=[spec for _, spec in outs],
        scratch_shapes=[
            pltpu.VMEM((all_rows, shared_wide), jnp.float32),
            pltpu.VMEM((2, quad, wide), low),
            pltpu.VMEM((2, quad, lanes), low),
            pltpu.VMEM((2, local_experts, part, width), low),
            pltpu.SemaphoreType.DMA((44,)),
            pltpu.SemaphoreType.DMA((32, 2)),
            pltpu.SemaphoreType.DMA,
            pltpu.SemaphoreType.DMA((2, 5)),
            pltpu.SemaphoreType.DMA((2,)),
        ],
        compiler_params=pltpu.CompilerParams(
            collective_id=number, has_side_effects=True, vmem_limit_bytes=vmem_limit
        ),
        cost_estimate=cost(flops, *[a for a, _ in ins], *[o for o, _ in outs]),
    )(*[a for a, _ in ins])


def attention_kernel(
    score_scale,
    normed_ref,
    value_ref,
    cosine_ref,
    sine_ref,
    segment_row_ref,
    segment_column_ref,
    gain_ref,
    tokens_ref,
    second_gain_ref,
    router_ref,
    query_hbm,
    latent_hbm,
    expand_hbm,
    output_hbm,
    value_out,
    normed_out,
    query_out,
    latent_out,
    scale_out,
    latent_normed_out,
    key_rope_out,
    expanded_out,
    log_out,
    mixed_out,
    hidden_out,
    second_scale_out,
    gates_out,
    wide_out,
    query_matrix,
    latent_matrix,
    expand_matrix,
    output_matrix,
    partial,
    mates,
    sides,
    carried,
    send_sems,
    recv_sems,
    local_sems,
    group_sends,
    group_sems,
    sum_sends,
    mate_sems,
    side_sems,
):
    place = places()
    z, x, y, c = place
    side, mate = device(z, x, 1 - y, c), device(z, x, y, 1 - c)
    rows = normed_ref.shape[0]
    half = rows // 2
    heads = query_out.shape[0]
    greet(gather_neighbours(place))
    near = Sends(group_sends)
    own, across = y * 2 + c, (1 - y) * 2 + c
    keep = pltpu.make_async_copy(normed_ref, normed_out.at[own], local_sems.at[0])
    keep.start()

    def part(i, h):
        return normed_out.at[i, pl.ds(h * half, half)]

    for to in (side, mate):
        for h in range(2):
            piece = normed_ref.at[pl.ds(h * half, half)]
            near.start(piece, part(own, h), group_sems.at[own, h], to)
    sends = Sends(send_sems)
    gather = Gather(value_ref, value_out, sends, recv_sems, local_sems.at[1], place, 48)
    gather.whole(0)
    loads = [
        pltpu.make_async_copy(source, target, local_sems.at[2 + i])
        for i, (source, target) in enumerate(
            (
                (query_hbm, query_matrix),
                (latent_hbm, latent_matrix),
                (expand_hbm, expand_matrix),
                (output_hbm, output_matrix),
            )
        )
    ]
    for load in loads:
        load.start()
    for h in range(2):
        landed(part(across, h), group_sems.at[across, h], mate)
        near.start(part(across, h), part(across, h), group_sems.at[across, h], mate)
    for i in (y * 2 + 1 - c, (1 - y) * 2 + 1 - c):
        for h in range(2):
            landed(part(i, h), group_sems.at[i, h], mate)
    keep.wait()
    normed = normed_out[...].reshape(4 * rows, normed_out.shape[2])
    cosine, sine = cosine_ref[...], sine_ref[...]
    turn_half = ROPE // 2

    def turned(first, second):
        return jnp.concatenate(
            [first * cosine - second * sine, second * cosine + first * sine], axis=1
        )

    loads[0].wait()
    full = matmul(normed, query_matrix[...])
    for h in range(heads):
        start = h * (NOPE + ROPE)
        first = full[:, start + NOPE : start + NOPE + turn_half]
        second = full[:, start + NOPE + turn_half : start + NOPE + ROPE]
        query = jnp.concatenate([full[:, start : start + NOPE], turned(first, second)], axis=1)
        query_out[h] = query.astype(jnp.bfloat16)
    gather.whole(1)
    loads[1].wait()
    compressed = times_trans(normed, latent_matrix[...])
    latent = compressed[:, :LATENT]
    scale = inv_rms(latent)
    latent_out[...] = latent
    scale_out[...] = jnp.broadcast_to(scale, scale_out.shape)
    latent_normed_out[...] = (latent * scale * gain_ref[...]).astype(jnp.bfloat16)
    first = compressed[:, LATENT : LATENT + turn_half]
    second = compressed[:, LATENT + turn_half : LATENT + ROPE]
    key_rope_out[...] = turned(first, second).astype(jnp.bfloat16)
    gather.relay(0)
    loads[2].wait()
    expanded_out[...] = matmul(latent_normed_out[...], expand_matrix[...]).astype(jnp.bfloat16)

    def head(h):
        start = h * (NOPE + VDIM)
        query = query_out[h]
        raw = times_trans(query[:, :NOPE], expanded_out[:, start : start + NOPE])
        raw = raw + times_trans(query[:, NOPE:], key_rope_out[...])
        row = lax.broadcasted_iota(jnp.int32, raw.shape, 0)
        column = lax.broadcasted_iota(jnp.int32, raw.shape, 1)
        allowed = (segment_column_ref[...] == segment_row_ref[...]) & (column <= row)
        scores = jnp.where(allowed, raw * score_scale, -1e30)
        peak = jnp.max(scores, axis=1, keepdims=True)
        weights = jnp.exp(scores - peak)
        total = jnp.sum(weights, axis=1, keepdims=True)
        log_out[h] = jnp.broadcast_to(peak + jnp.log(total), log_out.shape[1:])
        probs = (weights / total).astype(jnp.bfloat16)
        mixed = matmul(probs, expanded_out[:, start + NOPE : start + NOPE + VDIM])
        mixed_out[:, h * VDIM : (h + 1) * VDIM] = mixed.astype(jnp.bfloat16)

    middle = [
        None,
        functools.partial(gather.whole, 2),
        functools.partial(gather.relay, 1),
        functools.partial(gather.corner, 0),
    ]
    for h in range(heads):
        head(h)
        if h < 4 and middle[h] is not None:
            middle[h]()
    loads[3].wait()
    for i in range(4):
        block = matmul(mixed_out[i * rows : (i + 1) * rows], output_matrix[...])
        partial[i] = block.astype(jnp.bfloat16)
    sums = Sends(sum_sends)
    for j, yy in enumerate((1 - y, y)):
        for h in range(2):
            some = pl.ds(h * half, half)
            sums.start(
                partial.at[yy * 2 + 1 - c, some], mates.at[j, some], mate_sems.at[j, h], mate
            )
    gather.whole(3)
    for h in range(2):
        some = pl.ds(h * half, half)
        landed(mates.at[0, some], mate_sems.at[0, h], mate)
        add_into(carried, [partial.at[(1 - y) * 2 + c], mates.at[0]], h * half, half)
        sums.start(carried.at[some], sides.at[some], side_sems.at[h], side)
    gather.relay(2)
    gather.corner(1)
    for h in range(2):
        some = pl.ds(h * half, half)
        landed(mates.at[1, some], mate_sems.at[1, h], mate)
        landed(sides.at[some], side_sems.at[h], mate)
        add_into(hidden_out, [partial.at[y * 2 + c], mates.at[1], sides], h * half, half)
    hidden = tokens_ref[...].astype(jnp.float32) + hidden_out[...]
    hidden_out[...] = hidden
    second_scale = inv_rms(hidden)
    second_scale_out[...] = jnp.broadcast_to(second_scale, second_scale_out.shape)
    normed_two = (hidden * second_scale * second_gain_ref[...]).astype(jnp.bfloat16)
    width = hidden.shape[1]
    wide_out[:, :width] = normed_two
    gates = jax.nn.sigmoid(times_trans(normed_two, router_ref[...]))
    gates_out[...] = gates
    codes = value_ref[:, width:].astype(jnp.float32)[:, : gates.shape[1]]
    weighted = jnp.where(codes >= 0, gates, 0.0)
    mixing = route_scale * weighted / jnp.sum(weighted, axis=1, keepdims=True)
    high = mixing.astype(jnp.bfloat16).astype(jnp.float32)
    wide_out[:, width:] = jnp.concatenate([high, mixing - high], axis=1).astype(jnp.bfloat16)
    gather.relay(3)
    gather.corner(2)
    gather.corner(3)
    gather.last()
    near.finish()
    sends.finish()
    sums.finish()


def add_into(target, sources, start, rows):
    step = 16

    def body(i, carry):
        part = pl.ds(pl.multiple_of(start + i * step, step), step)
        total = sources[0][part].astype(jnp.float32)
        for source in sources[1:]:
            total = total + source[part].astype(jnp.float32)
        target[part] = total.astype(target.dtype)
        return carry

    lax.fori_loop(0, rows // step, body, 0)


def attention_forward(
    score_scale,
    normed,
    value,
    cosine,
    sine,
    segment,
    gain,
    tokens,
    second_gain,
    router,
    query,
    latent,
    expand,
    output,
    number,
):
    rows, width = normed.shape
    group, heads = 4 * rows, query.shape[1] // (NOPE + ROPE)
    shape, low = jax.ShapeDtypeStruct, jnp.bfloat16
    vmem, away = pl.BlockSpec(memory_space=pltpu.VMEM), pl.BlockSpec(memory_space=pl.ANY)
    segment = segment.astype(jnp.float32)
    inputs = [normed, value, cosine, sine, segment[None], segment[:, None], gain[None]]
    inputs += [tokens, second_gain[None], router.T]
    matrices = [query, latent.T, expand, output]
    outs = [
        shape((32,) + value.shape, low),
        shape((4, rows, width), low),
        shape((heads, group, NOPE + ROPE), low),
        shape((group, LATENT), jnp.float32),
        shape((group, lanes), jnp.float32),
        shape((group, LATENT), low),
        shape((group, ROPE), low),
        shape((group, heads * (NOPE + VDIM)), low),
        shape((heads, group, lanes), jnp.float32),
        shape((group, heads * VDIM), low),
        shape((rows, width), jnp.float32),
        shape((rows, lanes), jnp.float32),
        shape((rows, router.shape[1]), jnp.float32),
        shape(value.shape, low),
    ]
    flops = 2 * group * (width * (query.shape[1] + latent.shape[1]) + output.size + expand.size)
    return pl.pallas_call(
        functools.partial(attention_kernel, score_scale),
        out_shape=outs,
        in_specs=[vmem] * len(inputs) + [away] * 4,
        out_specs=[away] + [vmem] * (len(outs) - 1),
        scratch_shapes=[pltpu.VMEM(m.shape, low) for m in matrices]
        + [
            pltpu.VMEM((4, rows, width), low),
            pltpu.VMEM((2, rows, width), low),
            pltpu.VMEM((rows, width), low),
            pltpu.VMEM((rows, width), low),
            pltpu.SemaphoreType.DMA((44,)),
            pltpu.SemaphoreType.DMA((32, 2)),
            pltpu.SemaphoreType.DMA((6,)),
            pltpu.SemaphoreType.DMA((6,)),
            pltpu.SemaphoreType.DMA((4, 2)),
            pltpu.SemaphoreType.DMA((6,)),
            pltpu.SemaphoreType.DMA((2, 2)),
            pltpu.SemaphoreType.DMA((2,)),
        ],
        compiler_params=pltpu.CompilerParams(
            collective_id=number, has_side_effects=True, vmem_limit_bytes=vmem_limit
        ),
        cost_estimate=cost(flops, *inputs, *matrices, *outs),
    )(*inputs, *matrices)


def sum_all_kernel(inner, cover_ins, cover_outs, p_ref, *refs):
    ins, refs = refs[:cover_ins], refs[cover_ins:]
    out_ref, refs = refs[0], refs[1:]
    outs, refs = refs[:cover_outs], refs[cover_outs:]
    own, mates, over_half, side_half, over_full, side_full, below, above = refs[:8]
    send_sems, mate_sems, half_sems, full_sems, line_sems, local_sems = refs[8:]
    z, x, y, c = places()
    turn, turns = pl.program_id(0), pl.num_programs(0)
    rows = out_ref.shape[0]
    half = rows // 2
    over, side, mate = device(z, 1 - x, y, c), device(z, x, 1 - y, c), device(z, x, y, 1 - c)
    up, down = device(z + 1, x, y, c), device(z - 1, x, y, c)
    sends = Sends(send_sems)
    targets = [ordered(z, (3, 2, 1, 0)[step], (3, 0, 2, 1)[step]) for step in range(4)]
    spots = [(1 - x, 1 - y), (1 - x, y), (x, 1 - y), (x, y)]
    shards = [[shard(zz, xx, yy, 1 - c) for xx, yy in spots] for zz in targets]
    mine = [[shard(zz, xx, yy, c) for xx, yy in spots] for zz in targets]
    higher = [zz > z for zz in targets]
    lower = [zz < z for zz in targets]
    loads = [
        pltpu.make_async_copy(p_ref.at[mine[slot // 4][slot % 4]], own.at[slot], local_sems.at[slot])
        for slot in range(16)
    ]

    mate_copies = [
        sends.plan(p_ref.at[shards[slot // 4][slot % 4]], mates.at[slot], mate_sems.at[slot], mate)
        for slot in range(16)
    ]
    corner_copies, relay_copies, line_copies = [], [], []
    for step in range(4):
        corner_copies.append(
            (
                sends.plan(
                    own.at[step * 4, pl.ds(half, half)],
                    over_half.at[step],
                    half_sems.at[step, 0],
                    over,
                ),
                sends.plan(
                    own.at[step * 4, pl.ds(0, half)], side_half.at[step], half_sems.at[step, 1], side
                ),
            )
        )
        relay_copies.append(
            (
                sends.plan(
                    own.at[step * 4 + 1], over_full.at[step], full_sems.at[step, 0], over
                ),
                sends.plan(
                    own.at[step * 4 + 2], side_full.at[step], full_sems.at[step, 1], side
                ),
            )
        )
    for step in range(3):
        zz, slot = targets[step], step * 4 + 3
        line_copies.append(
            (
                sends.plan(own.at[slot], below.at[zz], line_sems.at[zz, 0], up, higher[step]),
                sends.plan(own.at[slot], above.at[zz], line_sems.at[zz, 1], down, lower[step]),
            )
        )

    def begin():
        greet([(over, None), (side, None), (mate, None), (up, z < 3), (down, z > 0)])
        for slot in range(16):
            mate_copies[slot].start()
            loads[slot].start()

    def join(slot):
        loads[slot].wait()
        landed(mates.at[slot], mate_sems.at[slot], mate)

    def corner(step):
        slot = step * 4
        join(slot)
        add_rows(own.at[slot], [(mates.at[slot], 0)], 0, rows)
        for copy in corner_copies[step]:
            copy.start()

    def relay(step):
        slot = step * 4 + 1
        join(slot)
        add_rows(own.at[slot], [(mates.at[slot], 0)], half, half)
        landed(side_half.at[step], half_sems.at[step, 1], mate)
        add_rows(own.at[slot], [(mates.at[slot], 0), (side_half.at[step], 0)], 0, half)
        relay_copies[step][0].start()
        slot = step * 4 + 2
        join(slot)
        add_rows(own.at[slot], [(mates.at[slot], 0)], 0, half)
        landed(over_half.at[step], half_sems.at[step, 0], mate)
        add_rows(own.at[slot], [(mates.at[slot], 0), (over_half.at[step], half)], half, half)
        relay_copies[step][1].start()

    def whole(step):
        zz = targets[step]
        slot = step * 4 + 3
        join(slot)
        landed(over_full.at[step], full_sems.at[step, 0], mate)
        landed(side_full.at[step], full_sems.at[step, 1], mate)
        add_rows(
            own.at[slot],
            [(mates.at[slot], 0), (over_full.at[step], 0), (side_full.at[step], 0)],
            0,
            rows,
        )

        @pl.when((zz >= z) & (z > 0))
        def _():
            landed(below.at[zz], line_sems.at[zz, 0], mate)
            add_rows(own.at[slot], [(below.at[zz], 0)], 0, rows)

        @pl.when((zz <= z) & (z < 3))
        def _():
            landed(above.at[zz], line_sems.at[zz, 1], mate)
            add_rows(own.at[slot], [(above.at[zz], 0)], 0, rows)

        if step < 3:
            pl.when(higher[step])(line_copies[step][0].start)
            pl.when(lower[step])(line_copies[step][1].start)

    def end():
        whole(3)
        out_ref[...] = own[15].astype(out_ref.dtype)
        sends.finish()

    pieces = [
        begin,
        functools.partial(corner, 0),
        functools.partial(corner, 1),
        functools.partial(relay, 0),
        functools.partial(corner, 2),
        functools.partial(relay, 1),
        functools.partial(whole, 0),
        functools.partial(corner, 3),
        functools.partial(relay, 2),
        functools.partial(whole, 1),
        functools.partial(relay, 3),
        functools.partial(whole, 2),
    ]
    for number, piece in enumerate(pieces):
        pl.when(turn == number)(piece)
    inner(turn, ins, outs)
    pl.when(turn == turns - 1)(end)


def sum_all(value, number, inner, turns, ins, outs, flops):
    if lax.axis_size("expert") != 8 or lax.axis_size("weight") != 4:
        summed = lax.psum_scatter(
            value.reshape(-1, value.shape[2]), ("expert", "weight"), scatter_dimension=0, tiled=True
        )

        def alone(*refs):
            inner(pl.program_id(0), refs[: len(ins)], refs[len(ins) :])

        return summed.astype(jnp.float32), call(alone, turns, ins, outs, flops)
    _, rows, width = value.shape
    out = jax.ShapeDtypeStruct((rows, width), jnp.float32)
    buffer = lambda n, r: pltpu.VMEM((n, r, width), value.dtype)
    arrays, shapes = [a for a, _ in ins], [o for o, _ in outs]
    results = pl.pallas_call(
        functools.partial(sum_all_kernel, inner, len(ins), len(outs)),
        grid=(turns,),
        out_shape=[out] + shapes,
        in_specs=[pl.BlockSpec(memory_space=pl.ANY)] + [spec for _, spec in ins],
        out_specs=[pl.BlockSpec((rows, width), lambda i: (0, 0))] + [spec for _, spec in outs],
        scratch_shapes=[
            buffer(16, rows),
            buffer(16, rows),
            buffer(4, rows // 2),
            buffer(4, rows // 2),
            buffer(4, rows),
            buffer(4, rows),
            buffer(4, rows),
            buffer(4, rows),
            pltpu.SemaphoreType.DMA((40,)),
            pltpu.SemaphoreType.DMA((16,)),
            pltpu.SemaphoreType.DMA((4, 2)),
            pltpu.SemaphoreType.DMA((4, 2)),
            pltpu.SemaphoreType.DMA((4, 2)),
            pltpu.SemaphoreType.DMA((16,)),
        ],
        compiler_params=pltpu.CompilerParams(
            collective_id=number, has_side_effects=True, vmem_limit_bytes=vmem_limit
        ),
        cost_estimate=cost(flops, value, out, *arrays, *shapes),
    )(value, *arrays)
    return results[0], results[1:]


def gather_group_kernel(x_ref, out_ref, send_sems, recv_sems, local_sem):
    z, x, y, c = places()
    half = x_ref.shape[0] // 2
    side, mate = device(z, x, 1 - y, c), device(z, x, y, 1 - c)
    greet([(side, None), (mate, None)])
    sends = Sends(send_sems)
    own, across = y * 2 + c, (1 - y) * 2 + c
    keep = pltpu.make_async_copy(x_ref, out_ref.at[own], local_sem)
    keep.start()

    def part(i, h):
        return out_ref.at[i, pl.ds(h * half, half)]

    for h in range(2):
        piece = x_ref.at[pl.ds(h * half, half)]
        sends.start(piece, part(own, h), recv_sems.at[own, h], side)
    for h in range(2):
        piece = x_ref.at[pl.ds(h * half, half)]
        sends.start(piece, part(own, h), recv_sems.at[own, h], mate)
    for h in range(2):
        landed(part(across, h), recv_sems.at[across, h], mate)
        sends.start(part(across, h), part(across, h), recv_sems.at[across, h], mate)
    for i in (y * 2 + 1 - c, (1 - y) * 2 + 1 - c):
        for h in range(2):
            landed(part(i, h), recv_sems.at[i, h], mate)
    sends.finish()
    keep.wait()


def gather_group(value, number):
    if lax.axis_size("expert") != 8 or lax.axis_size("weight") != 4:
        return lax.all_gather(value, "weight", axis=0, tiled=True)
    out = jax.ShapeDtypeStruct((4,) + value.shape, value.dtype)
    return pl.pallas_call(
        gather_group_kernel,
        out_shape=out,
        in_specs=[pl.BlockSpec(memory_space=pltpu.VMEM)],
        out_specs=pl.BlockSpec(memory_space=pltpu.VMEM),
        scratch_shapes=[
            pltpu.SemaphoreType.DMA((6,)),
            pltpu.SemaphoreType.DMA((4, 2)),
            pltpu.SemaphoreType.DMA,
        ],
        compiler_params=pltpu.CompilerParams(collective_id=number, has_side_effects=True),
        cost_estimate=cost(0, value, out),
    )(value).reshape(-1, value.shape[1])


def sum_group_kernel(p_ref, out_ref, mates, sides, carried, send_sems, mate_sems, side_sems):
    z, x, y, c = places()
    rows = out_ref.shape[0]
    half = rows // 2
    side, mate = device(z, x, 1 - y, c), device(z, x, y, 1 - c)
    greet([(side, None), (mate, None)])
    sends = Sends(send_sems)

    for j, yy in enumerate((1 - y, y)):
        for h in range(2):
            part = pl.ds(h * half, half)
            sends.start(
                p_ref.at[yy * 2 + 1 - c, part], mates.at[j, part], mate_sems.at[j, h], mate
            )

    def add(target, sources, h):
        step = 16

        def body(i, carry):
            part = pl.ds(pl.multiple_of(h * half + i * step, step), step)
            total = sources[0][part].astype(jnp.float32)
            for source in sources[1:]:
                total = total + source[part].astype(jnp.float32)
            target[part] = total.astype(target.dtype)
            return carry

        lax.fori_loop(0, half // step, body, 0)

    for h in range(2):
        part = pl.ds(h * half, half)
        landed(mates.at[0, part], mate_sems.at[0, h], mate)
        add(carried, [p_ref.at[(1 - y) * 2 + c], mates.at[0]], h)
        sends.start(carried.at[part], sides.at[part], side_sems.at[h], side)
    for h in range(2):
        part = pl.ds(h * half, half)
        landed(mates.at[1, part], mate_sems.at[1, h], mate)
        landed(sides.at[part], side_sems.at[h], mate)
        add(out_ref, [p_ref.at[y * 2 + c], mates.at[1], sides], h)
    sends.finish()


def sum_group(value, number):
    if lax.axis_size("expert") != 8 or lax.axis_size("weight") != 4:
        summed = lax.psum_scatter(value, "weight", scatter_dimension=0, tiled=True)
        return summed.astype(jnp.float32)
    rows, width = value.shape[0] // 4, value.shape[1]
    value = value.reshape(4, rows, width)
    out = jax.ShapeDtypeStruct((rows, width), jnp.float32)
    return pl.pallas_call(
        sum_group_kernel,
        out_shape=out,
        in_specs=[pl.BlockSpec(memory_space=pltpu.VMEM)],
        out_specs=pl.BlockSpec(memory_space=pltpu.VMEM),
        scratch_shapes=[
            pltpu.VMEM((2, rows, width), value.dtype),
            pltpu.VMEM((rows, width), value.dtype),
            pltpu.VMEM((rows, width), value.dtype),
            pltpu.SemaphoreType.DMA((6,)),
            pltpu.SemaphoreType.DMA((2, 2)),
            pltpu.SemaphoreType.DMA((2,)),
        ],
        compiler_params=pltpu.CompilerParams(collective_id=number, has_side_effects=True),
        cost_estimate=cost(0, value, out),
    )(value)


def columns(start, size):
    return pl.ds(pl.multiple_of(start, lanes), size)


def add_block(target, sources, rows, row_start=0):
    step = 16

    def body(i, carry):
        part = pl.ds(pl.multiple_of(row_start + i * step, step), step)
        total = target[part].astype(jnp.float32)
        for source in sources:
            there = pl.ds(pl.multiple_of(i * step, step), step)
            total = total + source[there].astype(jnp.float32)
        target[part] = total.astype(target.dtype)
        return carry

    lax.fori_loop(0, rows // step, body, 0)


def total_kernel(
    top_ref,
    rest_ref,
    group_ref,
    out_ref,
    group_out,
    acc,
    mates,
    first_over,
    first_side,
    next_side,
    next_over,
    line,
    group_mates,
    group_sides,
    carried,
    send_sems,
    sems,
    mate_sems,
    side_sems,
):
    z, x, y, c = places()
    rows, width = out_ref.shape
    group_half = group_out.shape[0] // 2
    group_parts = [pl.ds(h * group_half, group_half) for h in range(2)]
    sources = [(top_ref, 0, 0), (rest_ref, top_ref.shape[0], 24)]
    half, quarter, eighth, sixteenth = width // 2, width // 4, width // 8, width // 16
    strip = rows // 4
    over, side, mate = device(z, 1 - x, y, c), device(z, x, 1 - y, c), device(z, x, y, 1 - c)
    others = [lax.rem(z + d, 4) for d in (1, 2, 3)]
    greet(
        [(over, None), (side, None), (mate, None)] + [(device(zz, x, y, c), None) for zz in others]
    )
    sends = Sends(send_sems)
    base = c * half
    for j in range(2):
        for p_ref, top, sem in sources:
            sends.start(
                p_ref.at[:, columns((1 - c) * half + j * quarter, quarter)],
                mates.at[pl.ds(top, p_ref.shape[0]), columns(j * quarter, quarter)],
                sems.at[sem + j],
                mate,
            )
    for i, yy in enumerate((1 - y, y)):
        for h, some in enumerate(group_parts):
            sends.start(
                group_ref.at[yy * 2 + 1 - c, some],
                group_mates.at[i, some],
                mate_sems.at[i, h],
                mate,
            )
    kept = (x * eighth + y * sixteenth, quarter + y * eighth + x * sixteenth)
    firsts, nexts = (first_over, first_side), (next_side, next_over)
    for j in range(2):
        part = columns(j * quarter, quarter)
        wide = 16
        for p_ref, top, sem in sources:
            landed(mates.at[pl.ds(top, p_ref.shape[0]), part], sems.at[sem + j], mate)

            def join(i, carry, j=j, p_ref=p_ref, top=top):
                mine = pl.ds(pl.multiple_of(i * wide, wide), wide)
                some = pl.ds(pl.multiple_of(top + i * wide, wide), wide)
                total = p_ref[mine, columns(base + j * quarter, quarter)].astype(jnp.float32)
                total = total + mates[some, columns(j * quarter, quarter)].astype(jnp.float32)
                acc[some, columns(j * quarter, quarter)] = total.astype(acc.dtype)
                return carry

            lax.fori_loop(0, p_ref.shape[0] // wide, join, 0)
        away = (1 - x) * eighth if j == 0 else quarter + (1 - y) * eighth
        sends.start(
            acc.at[:, columns(away, eighth)], firsts[j], sems.at[2 + j], (over, side)[j]
        )
    for h, some in enumerate(group_parts):
        landed(group_mates.at[0, some], mate_sems.at[0, h], mate)
        add_into(
            carried,
            [group_ref.at[(1 - y) * 2 + c], group_mates.at[0]],
            h * group_half,
            group_half,
        )
        sends.start(carried.at[some], group_sides.at[some], side_sems.at[h], side)
    for j in range(2):
        landed(firsts[j], sems.at[2 + j], mate)
        near = x * eighth if j == 0 else quarter + y * eighth
        add_block(acc.at[:, columns(near, eighth)], [firsts[j]], rows)
        away = near + ((1 - y) if j == 0 else (1 - x)) * sixteenth
        sends.start(
            acc.at[:, columns(away, sixteenth)], nexts[j], sems.at[4 + j], (side, over)[j]
        )
    for j in range(2):
        landed(nexts[j], sems.at[4 + j], mate)
        add_block(acc.at[:, columns(kept[j], sixteenth)], [nexts[j]], rows)
        for d, zz in enumerate(others):
            sends.start(
                acc.at[pl.ds(pl.multiple_of(zz * strip, 16), strip), columns(kept[j], sixteenth)],
                line.at[j, d],
                sems.at[6 + j * 3 + d],
                device(zz, x, y, c),
            )
    strip_here = pl.multiple_of(z * strip, 16)
    for j in range(2):
        for d in range(3):
            landed(line.at[j, d], sems.at[6 + j * 3 + d], mate)
        block = acc.at[:, columns(kept[j], sixteenth)]
        add_block(block, [line.at[j, d] for d in range(3)], strip, strip_here)

        def place(i, carry, j=j):
            some = pl.ds(pl.multiple_of(strip_here + i * 16, 16), 16)
            out_ref[some, columns(base + kept[j], sixteenth)] = acc[
                some, columns(kept[j], sixteenth)
            ]
            return carry

        lax.fori_loop(0, strip // 16, place, 0)
        done = out_ref.at[pl.ds(strip_here, strip), columns(base + kept[j], sixteenth)]
        for d, zz in enumerate(others):
            sends.start(done, done, sems.at[12 + j * 3 + d], device(zz, x, y, c))
    for j in range(2):
        for d in range(3):
            source = pl.multiple_of(lax.rem(z + 3 - d, 4) * strip, 16)
            landed(
                out_ref.at[pl.ds(source, strip), columns(base + kept[j], sixteenth)],
                sems.at[12 + j * 3 + d],
                mate,
            )
        part = out_ref.at[:, columns(base + kept[j], sixteenth)]
        sends.start(part, part, sems.at[18 + j], (side, over)[j])
    others_kept = (
        x * eighth + (1 - y) * sixteenth,
        quarter + y * eighth + (1 - x) * sixteenth,
    )
    for j in range(2):
        landed(out_ref.at[:, columns(base + others_kept[j], sixteenth)], sems.at[18 + j], mate)
        near = x * eighth if j == 0 else quarter + y * eighth
        part = out_ref.at[:, columns(base + near, eighth)]
        sends.start(part, part, sems.at[20 + j], (over, side)[j])
    for j in range(2):
        away = (1 - x) * eighth if j == 0 else quarter + (1 - y) * eighth
        landed(out_ref.at[:, columns(base + away, eighth)], sems.at[20 + j], mate)
        part = out_ref.at[:, columns(base + j * quarter, quarter)]
        sends.start(part, part, sems.at[22 + j], mate)
    for h, some in enumerate(group_parts):
        landed(group_mates.at[1, some], mate_sems.at[1, h], mate)
        landed(group_sides.at[some], side_sems.at[h], mate)
        add_into(
            group_out,
            [group_ref.at[y * 2 + c], group_mates.at[1], group_sides],
            h * group_half,
            group_half,
        )
    for j in range(2):
        landed(
            out_ref.at[:, columns((1 - c) * half + j * quarter, quarter)], sems.at[22 + j], mate
        )
    sends.finish()


def total_over_all(top, rest, group, number):
    if lax.axis_size("expert") != 8 or lax.axis_size("weight") != 4:
        value = jnp.concatenate([top, rest], axis=0).astype(jnp.float32)
        return lax.psum(value, ("expert", "weight")), sum_group(group, number)
    rows, width = top.shape[0] + rest.shape[0], top.shape[1]
    group = group.reshape(4, -1, width)
    group_rows = group.shape[1]
    out = jax.ShapeDtypeStruct((rows, width), top.dtype)
    group_out = jax.ShapeDtypeStruct((group_rows, width), jnp.float32)
    buffer = lambda n: pltpu.VMEM((rows, n), top.dtype)
    return pl.pallas_call(
        total_kernel,
        out_shape=[out, group_out],
        in_specs=[pl.BlockSpec(memory_space=pltpu.VMEM)] * 3,
        out_specs=[pl.BlockSpec(memory_space=pltpu.VMEM)] * 2,
        scratch_shapes=[
            buffer(width // 2),
            buffer(width // 2),
            buffer(width // 8),
            buffer(width // 8),
            buffer(width // 16),
            buffer(width // 16),
            pltpu.VMEM((2, 3, rows // 4, width // 16), top.dtype),
            pltpu.VMEM((2, group_rows, width), group.dtype),
            pltpu.VMEM((group_rows, width), group.dtype),
            pltpu.VMEM((group_rows, width), group.dtype),
            pltpu.SemaphoreType.DMA((32,)),
            pltpu.SemaphoreType.DMA((26,)),
            pltpu.SemaphoreType.DMA((2, 2)),
            pltpu.SemaphoreType.DMA((2,)),
        ],
        compiler_params=pltpu.CompilerParams(
            collective_id=number, has_side_effects=True, vmem_limit_bytes=vmem_limit
        ),
        cost_estimate=cost(0, top, rest, group, out, group_out),
    )(top, rest, group)


def shared_kernel(turn, ins, outs):
    normed_ref, cotangent_ref, gate_grad_ref, lift_grad_ref, hidden_ref = ins

    @pl.when(turn == 0)
    def _():
        for out_ref in outs:
            out_ref[...] = jnp.zeros_like(out_ref)

    normed, cotangent = normed_ref[...], cotangent_ref[...]
    outs[0][...] += trans_times(gate_grad_ref[...], normed)
    outs[1][...] += trans_times(lift_grad_ref[...], normed)
    outs[2][...] += trans_times(hidden_ref[...], cotangent)


def weight_kernel(ins, outs):
    rows_ref, grads_ref, gate_grad_ref, lift_grad_ref, hidden_ref = ins
    rows = rows_ref[0]
    for out_ref, left_ref, right in (
        (outs[0], gate_grad_ref, rows),
        (outs[1], lift_grad_ref, rows),
        (outs[2], hidden_ref, grads_ref[0]),
    ):
        out_ref[0] = trans_times(left_ref[0], right).astype(out_ref.dtype)


def weights_alone(*refs):
    weight_kernel(refs[:5], refs[5:])


def gradients_kernel(turn, ins, outs):
    shared_kernel(turn, ins[:5], outs[:3])
    weight_kernel(ins[5:], outs[3:])


def sum_shards(value):
    return lax.psum_scatter(value, "expert", scatter_dimension=0, tiled=True)


def per_device(
    tokens,
    cotangent,
    segments,
    routes,
    first_gain,
    query_weight,
    latent_weight,
    latent_gain,
    expand_weight,
    output_weight,
    second_gain,
    router_weight,
    shared_gate,
    shared_up,
    shared_down,
    expert_gate,
    expert_up,
    expert_down,
):
    weight_count = lax.axis_size("weight")
    token_rows = tokens.shape[0]
    width = tokens.shape[1]
    group_rows = token_rows * weight_count
    query_width = NOPE + ROPE
    heads_here = query_weight.shape[1] // query_width
    expert_count = router_weight.shape[1]
    local_experts = expert_gate.shape[0]
    score_scale = query_width ** (-0.5)
    activations = tokens.astype(jnp.float32)
    first_scale = inv_rms(activations)
    normed = (activations * first_scale * first_gain).astype(jnp.bfloat16)
    both = ("expert", "weight")
    expert_index = lax.axis_index("expert")
    expert_lanes = lax.axis_size("expert")
    blocks = expert_lanes * weight_count
    pairs, quads = blocks // 2, blocks // 4
    pair_rows, quad_rows = 2 * token_rows, 4 * token_rows
    all_rows = blocks * token_rows
    slot_rows = blocks * CAP
    choose = (
        routes[:, :, None] == jnp.arange(expert_count, dtype=jnp.int32)[None, None, :]
    ).astype(jnp.float32)
    hit = jnp.sum(choose, axis=1)
    order = jnp.arange(token_rows, dtype=jnp.int32)
    before = (order[None, :] < order[:, None]).astype(jnp.bfloat16)
    place = matmul(before, hit.astype(jnp.bfloat16))
    rank = jnp.sum(choose * jnp.arange(routes.shape[1], dtype=jnp.float32)[None, :, None], axis=1)
    code = jnp.where(hit > 0, 32.0 * rank + place, -1.0)
    extra = jnp.pad(code, ((0, 0), (0, lanes - expert_count)), constant_values=-1.0)
    cotangent_wide = jnp.concatenate([cotangent, extra.astype(jnp.bfloat16)], axis=1)
    column = jnp.arange(lanes, dtype=jnp.int32)[None, :]
    row = jnp.arange(8, dtype=jnp.int32)[:, None]
    first_here = expert_index * local_experts
    here = (row < local_experts) & (column == first_here + row)
    twice = here | ((row < local_experts) & (column == first_here + row + expert_count))
    here, twice = here.astype(jnp.bfloat16), twice.astype(jnp.bfloat16)
    weight_index = lax.axis_index("weight")
    high_column = 2 * (row * weight_count + weight_index)
    known = row < routes.shape[1]
    high_at = (known & (column == high_column)).astype(jnp.bfloat16)
    low_at = (known & (column == high_column + 1)).astype(jnp.bfloat16)
    shared_here = shared_gate.shape[1] // expert_lanes
    shared_wide = -(-shared_here // lanes) * lanes
    start = expert_index * shared_here

    def shared_part(matrix):
        part = lax.dynamic_slice_in_dim(matrix, start, shared_here, axis=0)
        return jnp.pad(part, ((0, shared_wide - shared_here), (0, 0)))

    gate_part = shared_part(shared_gate.T)
    up_part = shared_part(shared_up.T)
    down_part = shared_part(shared_down)
    shape = jax.ShapeDtypeStruct
    whole = lambda array: (array, whole_spec(array))
    slots = shape((local_experts, slot_rows, width), jnp.bfloat16)
    slots_one = shape((local_experts, slot_rows, lanes), jnp.float32)
    gather_flops = 2 * all_rows * width * (2 * CAP * local_experts + shared_wide)
    cosine, sine = rope_tables(segments[0])
    allowed = attention_mask(segments[0])
    sizes = (expert_lanes, weight_count)
    if sizes == (8, 4):
        (
            cotangent_all,
            normed_all,
            query,
            latent,
            latent_scale,
            latent_normed,
            key_rope,
            expanded,
            log_total,
            mixed,
            hidden_one,
            second_scale,
            gates,
            normed_wide,
        ) = attention_forward(
            score_scale,
            normed,
            cotangent_wide,
            cosine,
            sine,
            segments[0],
            latent_gain,
            tokens,
            second_gain,
            router_weight,
            query_weight,
            latent_weight,
            expand_weight,
            output_weight,
            0,
        )
        second_scale, normed_two = second_scale[:, :1], normed_wide[:, :width]
        cotangent_all = cotangent_all.reshape(all_rows, -1)
        normed_all = normed_all.reshape(group_rows, width)
        latent_scale, log_total = latent_scale[:, :1], log_total[:, :, :1]
        query = query.transpose(1, 0, 2)
        expanded = expanded.reshape(group_rows, heads_here, NOPE + VDIM)
    else:
        cotangent_all = lax.all_gather(cotangent_wide, both, axis=0, tiled=True)
        normed_all = gather_group(normed, 0)
        query_full = matmul(normed_all, query_weight).reshape(group_rows, heads_here, query_width)
        query = jnp.concatenate(
            [
                query_full[..., :NOPE],
                rotate(query_full[..., NOPE:], cosine[:, None, :], sine[:, None, :]),
            ],
            axis=-1,
        ).astype(jnp.bfloat16)
        compressed = matmul(normed_all, latent_weight)
        latent = compressed[:, :LATENT]
        latent_scale = inv_rms(latent)
        latent_normed = (latent * latent_scale * latent_gain).astype(jnp.bfloat16)
        key_rope = rotate(compressed[:, LATENT:], cosine, sine).astype(jnp.bfloat16)
        expanded = (
            matmul(latent_normed, expand_weight)
            .astype(jnp.bfloat16)
            .reshape(group_rows, heads_here, NOPE + VDIM)
        )
    key_nope = expanded[..., :NOPE]
    values = expanded[..., NOPE:]

    def score_block():
        raw = jnp.einsum(
            "ihd,jhd->hij", query[..., :NOPE], key_nope, preferred_element_type=jnp.float32
        )
        raw = raw + jnp.einsum(
            "ihd,jd->hij", query[..., NOPE:], key_rope, preferred_element_type=jnp.float32
        )
        return jnp.where(allowed[None], raw * score_scale, -1e30)

    if sizes != (8, 4):
        scores = score_block()
        peak = jnp.max(scores, axis=-1, keepdims=True)
        weights = jnp.exp(scores - peak)
        total = jnp.sum(weights, axis=-1, keepdims=True)
        log_total = peak + jnp.log(total)
        mixed = jnp.einsum(
            "hij,jhd->ihd",
            (weights / total).astype(jnp.bfloat16),
            values,
            preferred_element_type=jnp.float32,
        )
        mixed = mixed.astype(jnp.bfloat16).reshape(group_rows, heads_here * VDIM)
        attended = sum_group(matmul(mixed, output_weight).astype(jnp.bfloat16), 1)
        hidden_one = activations + attended
        second_scale = inv_rms(hidden_one)
        normed_two = (hidden_one * second_scale * second_gain).astype(jnp.bfloat16)
        gates = jax.nn.sigmoid(matmul(normed_two, router_weight))
        weighted = hit * gates
        mixing_at = route_scale * weighted / jnp.sum(weighted, axis=1, keepdims=True)
        mixing_high = mixing_at.astype(jnp.bfloat16)
        mixing_low = (mixing_at - mixing_high.astype(jnp.float32)).astype(jnp.bfloat16)
        normed_wide = jnp.concatenate([normed_two, mixing_high, mixing_low], axis=1)
    chosen = jnp.sum(choose * gates[:, None, :], axis=-1)
    chosen_total = jnp.sum(chosen, axis=1, keepdims=True)
    upstream = cotangent.astype(jnp.float32)
    marks = (cotangent_all, pl.BlockSpec((quad_rows, lanes), lambda i: (i, width // lanes)))
    token_spec = pl.BlockSpec((quad_rows, shared_wide), lambda i: (i, 0))
    if sizes == (8, 4):
        (
            normed_tokens,
            grads_slots,
            rows_slots,
            mix_slots,
            shared_hidden,
            shared_gate_grad,
            shared_lift_grad,
        ) = gather_tokens(
            normed_wide,
            cotangent_all,
            here,
            twice,
            down_part,
            gate_part,
            up_part,
            local_experts,
            slot_rows,
            pair_rows,
            2,
        )
        normed_tokens = normed_tokens.reshape(all_rows, -1)
    else:
        normed_tokens = lax.all_gather(normed_wide, both, axis=0, tiled=True)

        def grads_alone(*refs):
            grads_kernel(pair_rows, refs[:3], refs[3:])

        grads_slots, shared_raw = call(
            grads_alone,
            quads,
            [whole(here), (cotangent_all, pair_spec(cotangent_all, quads)), whole(down_part)],
            [
                (slots, slots_spec(slots, quads)),
                (shape((all_rows, shared_wide), jnp.float32), pl.BlockSpec((quad_rows, shared_wide), lambda i: (i, 0))),
            ],
            gather_flops,
        )
        token_shape = shape((all_rows, shared_wide), jnp.bfloat16)
        rows_slots, mix_slots, shared_hidden, shared_gate_grad, shared_lift_grad = call(
            functools.partial(rows_kernel, pair_rows),
            quads,
            [
                whole(here),
                whole(twice),
                marks,
                (normed_tokens, pair_spec(normed_tokens, quads)),
                (shared_raw, token_spec),
                whole(gate_part),
                whole(up_part),
            ],
            [
                (slots, slots_spec(slots, quads)),
                (slots_one, slots_spec(slots_one, quads)),
                (token_shape, token_spec),
                (token_shape, token_spec),
                (token_shape, token_spec),
            ],
            gather_flops + 2 * all_rows * width * shared_wide,
        )
    hidden_here = expert_gate.shape[2]
    gate_rows, up_rows = expert_gate.transpose(0, 2, 1), expert_up.transpose(0, 2, 1)

    def tile_spec(rows, n):
        per = slot_rows // rows
        return pl.BlockSpec((1, rows, n), lambda i: (i // per, i % per, 0))

    def expert_spec(rows, matrix):
        per = slot_rows // rows
        return pl.BlockSpec((1,) + matrix.shape[1:], lambda i: (i // per, 0, 0))

    large, small = 32 * CAP, 16 * CAP
    narrow = shape((local_experts, slot_rows, hidden_here), jnp.bfloat16)
    one_matmul = 2 * local_experts * slot_rows * width * hidden_here
    routed_hidden, mixed_hidden, slope, active, produced = call(
        forward_kernel,
        local_experts * (slot_rows // large),
        [
            (rows_slots, tile_spec(large, width)),
            (mix_slots, tile_spec(large, lanes)),
            (gate_rows, expert_spec(large, gate_rows)),
            (up_rows, expert_spec(large, up_rows)),
            (expert_down, expert_spec(large, expert_down)),
        ],
        [(narrow, tile_spec(large, hidden_here))] * 4 + [(slots, tile_spec(large, width))],
        3 * one_matmul,
    )
    dense = shape((all_rows, width), jnp.bfloat16)
    dense_wide = shape((all_rows, width + lanes), jnp.bfloat16)
    (out_dense,) = call(
        functools.partial(out_kernel, pair_rows),
        quads,
        [
            whole(here),
            marks,
            (produced, slots_spec(slots, quads)),
            (shared_hidden, token_spec),
            whole(down_part),
        ],
        [(dense, pair_spec(dense, quads))],
        gather_flops,
    )
    narrow_tile = tile_spec(small, hidden_here)
    routed_out, (gate_grad, lift_grad, returned, mix_grad_slots) = sum_all(
        out_dense.reshape(blocks, token_rows, width),
        6,
        backward_kernel,
        local_experts * (slot_rows // small),
        [
            (grads_slots, tile_spec(small, width)),
            (routed_hidden, narrow_tile),
            (slope, narrow_tile),
            (active, narrow_tile),
            (gate_rows, expert_spec(small, gate_rows)),
            (up_rows, expert_spec(small, up_rows)),
            (expert_down, expert_spec(small, expert_down)),
        ],
        [
            (narrow, narrow_tile),
            (narrow, narrow_tile),
            (slots, tile_spec(small, width)),
            (slots_one, tile_spec(small, lanes)),
        ],
        3 * one_matmul,
    )
    (back_dense,) = call(
        functools.partial(back_kernel, pair_rows),
        quads,
        [
            whole(here),
            whole(high_at),
            whole(low_at),
            marks,
            (returned, slots_spec(slots, quads)),
            (mix_grad_slots, slots_spec(slots_one, quads)),
            (shared_gate_grad, token_spec),
            (shared_lift_grad, token_spec),
            whole(gate_part),
            whole(up_part),
        ],
        [(dense_wide, pair_spec(dense_wide, quads))],
        gather_flops + 2 * all_rows * width * shared_wide,
    )
    shared_sum = shape((shared_wide, width), jnp.float32)
    shared_out = (shared_sum, whole_spec(shared_sum))
    plain_spec = pl.BlockSpec((pair_rows, width), lambda i: (i, 0))
    shared_spec = pl.BlockSpec((pair_rows, shared_wide), lambda i: (i, 0))
    column_half = width // 2
    half_spec = lambda m: pl.BlockSpec((1, m, column_half), lambda i: (i // 2, 0, i % 2))
    narrow_spec = pl.BlockSpec((1, slot_rows, hidden_here), lambda i: (i // 2, 0, 0))
    shared_ins = [
        (normed_tokens, plain_spec),
        (cotangent_all, plain_spec),
        (shared_gate_grad, shared_spec),
        (shared_lift_grad, shared_spec),
        (shared_hidden, shared_spec),
    ]
    weight_ins = [
        (rows_slots, half_spec(slot_rows)),
        (grads_slots, half_spec(slot_rows)),
        (gate_grad, narrow_spec),
        (lift_grad, narrow_spec),
        (mixed_hidden, narrow_spec),
    ]
    back_blocks = back_dense.reshape(blocks, token_rows, -1)
    shared_flops = 6 * all_rows * width * shared_wide
    together = pairs == 2 * local_experts
    weight_type = jnp.bfloat16 if together else jnp.float32
    weight_shape = shape((local_experts, hidden_here, width), weight_type)
    weight_outs = [(weight_shape, half_spec(hidden_here))] * 3
    if together:
        back_here, sums = sum_all(
            back_blocks,
            3,
            gradients_kernel,
            pairs,
            shared_ins + weight_ins,
            [shared_out] * 3 + weight_outs,
            shared_flops + 3 * one_matmul,
        )
        shared_sums = sums[:3]
        weight_grads = [value.astype(jnp.float32) for value in sums[3:]]
    else:
        back_here, shared_sums = sum_all(
            back_blocks, 3, shared_kernel, pairs, shared_ins, [shared_out] * 3, shared_flops
        )
        weight_grads = call(
            weights_alone, 2 * local_experts, weight_ins, weight_outs, 3 * one_matmul
        )
    routed_back = back_here[:, :width]
    mix_grad = back_here[:, width : width + 2 * weight_count * routes.shape[1]]
    mix_grad = jnp.sum(mix_grad.reshape(token_rows, routes.shape[1], -1), axis=2)
    shared_grads = jnp.concatenate([total[:shared_here] for total in shared_sums], axis=0)
    shared_grads = shared_grads.astype(jnp.bfloat16)
    swapped = lax.all_to_all(shared_grads, "expert", split_axis=1, concat_axis=0, tiled=True)
    swapped = swapped.reshape(expert_lanes, 3, shared_here, -1).astype(jnp.float32)
    shared_gradients = [swapped[:, i].reshape(expert_lanes * shared_here, -1) for i in range(3)]
    chosen_grad = route_scale * (
        mix_grad / chosen_total
        - jnp.sum(mix_grad * chosen, axis=1, keepdims=True) / chosen_total**2
    )
    logit_grad = jnp.sum(choose * chosen_grad[:, :, None], axis=1) * gates * (1.0 - gates)
    normed_two_grad = (
        routed_back
        + jnp.dot(logit_grad, router_weight.astype(jnp.float32).T, precision=highest)
    )
    router_gradient = jnp.dot(logit_grad.T, normed_two.astype(jnp.float32), precision=highest)
    back_two, second_gain_gradient = norm_back(
        normed_two_grad, hidden_one, second_scale, second_gain
    )
    hidden_grad = upstream + back_two
    hidden_group = gather_group(hidden_grad.astype(jnp.bfloat16), 4)
    output_gradient = trans_times(hidden_group, mixed).astype(jnp.bfloat16)
    hidden_group, output_gradient = lax.optimization_barrier((hidden_group, output_gradient))
    output_shard = sum_shards(output_gradient)
    mixed_grad = (
        times_trans(hidden_group, output_weight)
        .astype(jnp.bfloat16)
        .reshape(group_rows, heads_here, VDIM)
    )
    probs = jnp.exp(score_block() - log_total)
    prob_grad = jnp.einsum("ihd,jhd->hij", mixed_grad, values, preferred_element_type=jnp.float32)
    centre = jnp.sum(probs * prob_grad, axis=-1, keepdims=True)
    score_grad = (probs * (prob_grad - centre)).astype(jnp.bfloat16)
    value_grad = jnp.einsum(
        "hij,ihd->jhd", probs.astype(jnp.bfloat16), mixed_grad, preferred_element_type=jnp.float32
    )
    query_nope_grad = (
        jnp.einsum("hij,jhd->ihd", score_grad, key_nope, preferred_element_type=jnp.float32)
        * score_scale
    )
    query_rope_grad = (
        jnp.einsum("hij,jd->ihd", score_grad, key_rope, preferred_element_type=jnp.float32)
        * score_scale
    )
    key_nope_grad = (
        jnp.einsum(
            "hij,ihd->jhd", score_grad, query[..., :NOPE], preferred_element_type=jnp.float32
        )
        * score_scale
    )
    key_rope_grad = (
        jnp.einsum("hij,ihd->jd", score_grad, query[..., NOPE:], preferred_element_type=jnp.float32)
        * score_scale
    )
    query_grad = jnp.concatenate(
        [query_nope_grad, unrotate(query_rope_grad, cosine[:, None, :], sine[:, None, :])], axis=-1
    )
    query_grad = query_grad.astype(jnp.bfloat16).reshape(group_rows, heads_here * query_width)
    expand_grad = (
        jnp.concatenate([key_nope_grad, value_grad], axis=-1)
        .astype(jnp.bfloat16)
        .reshape(group_rows, heads_here * (NOPE + VDIM))
    )
    expert_grads = (weight_grads[0].transpose(0, 2, 1), weight_grads[1].transpose(0, 2, 1), weight_grads[2])
    layer_out = (hidden_one + routed_out).astype(jnp.bfloat16)
    query_gradient = trans_times(normed_all, query_grad)
    expand_gradient = trans_times(latent_normed, expand_grad).astype(jnp.bfloat16)
    latent_normed_grad = times_trans(expand_grad, expand_weight)
    latent_back, latent_gain_gradient = norm_back(
        latent_normed_grad, latent, latent_scale, latent_gain
    )
    compressed_grad = jnp.concatenate([latent_back, unrotate(key_rope_grad, cosine, sine)], axis=-1)
    compressed_grad = compressed_grad.astype(jnp.bfloat16)
    latent_weight_gradient = trans_times(compressed_grad, normed_all)
    normed_part = times_trans(query_grad, query_weight) + times_trans(compressed_grad, latent_weight)
    first_gain_gradient = jnp.sum(normed_part * normed_all.astype(jnp.float32), axis=0) / first_gain
    rows_each = query_gradient.shape[0]
    joined = jnp.concatenate(
        [query_gradient.astype(jnp.bfloat16), expand_gradient.reshape(rows_each, -1)], axis=1
    )
    joined = sum_shards(joined).astype(jnp.float32)
    query_columns = query_gradient.shape[1]
    shards = (
        joined[:, :query_columns],
        joined[:, query_columns:].reshape(-1, expand_gradient.shape[1]),
        output_shard.T.astype(jnp.float32),
    )
    latent_columns = latent_weight.shape[1]
    rest = jnp.concatenate(
        [
            router_gradient,
            first_gain_gradient[None],
            second_gain_gradient[None],
            jnp.pad(latent_gain_gradient, (0, width - LATENT))[None],
        ],
        axis=0,
    ).astype(jnp.bfloat16)
    wanted = -(-(latent_columns + rest.shape[0]) // 64) * 64 - latent_columns
    rest = jnp.pad(rest, ((0, wanted - rest.shape[0]), (0, 0)))
    total, normed_grad = total_over_all(
        latent_weight_gradient.astype(jnp.bfloat16), rest, normed_part.astype(jnp.bfloat16), 7
    )
    back_one, _ = norm_back(normed_grad, activations, first_scale, first_gain)
    token_gradient = hidden_grad + back_one
    gains_at = latent_columns + expert_count
    wide = lambda value: value.astype(jnp.float32)
    totals = (
        wide(total[:latent_columns]).T,
        wide(total[gains_at + 2, :LATENT]),
        wide(total[latent_columns:gains_at]).T,
        wide(total[gains_at]),
        wide(total[gains_at + 1]),
    )
    return (
        layer_out,
        token_gradient,
        totals[3],
        shards[0],
        totals[0],
        totals[1],
        shards[1],
        shards[2],
        totals[4],
        totals[2],
        shared_gradients[0].T,
        shared_gradients[1].T,
        shared_gradients[2],
        expert_grads[0],
        expert_grads[1],
        expert_grads[2],
    )


def solution(mesh):
    return jax.shard_map(
        per_device,
        mesh=mesh,
        in_specs=(
            P(("expert", "weight"), None),
            P(("expert", "weight"), None),
            P("expert", None),
            P(("expert", "weight"), None),
            P(),
            P(None, "weight"),
            P(),
            P(),
            P(None, "weight"),
            P("weight", None),
            P(),
            P(),
            P(None, "weight"),
            P(None, "weight"),
            P("weight", None),
            P("expert", None, "weight"),
            P("expert", None, "weight"),
            P("expert", "weight", None),
        ),
        out_specs=(
            P(("expert", "weight"), None),
            P(("expert", "weight"), None),
            P(),
            P("expert", "weight"),
            P(),
            P(),
            P("expert", "weight"),
            P("weight", "expert"),
            P(),
            P(),
            P("expert", "weight"),
            P("expert", "weight"),
            P("weight", "expert"),
            P("expert", None, "weight"),
            P("expert", None, "weight"),
            P("expert", "weight", None),
        ),
        check_vma=False,
    )
```

```python
import functools

import jax
import jax.numpy as jnp
from jax import lax
from jax.experimental import pallas as pl
from jax.experimental.pallas import tpu as pltpu
from jax.sharding import PartitionSpec as P

NOPE = 128
ROPE = 64
VDIM = 128
LATENT = 512
CAP = 20


eps = 1e-06
route_scale = 2.446
rope_base = 50000.0
highest = lax.Precision.HIGHEST


def matmul(left, right):
    return jnp.dot(left, right, preferred_element_type=jnp.float32)


def trans_times(left, right):
    return lax.dot_general(
        left, right, (((0,), (0,)), ((), ())), preferred_element_type=jnp.float32
    )


def times_trans(left, right):
    return lax.dot_general(
        left, right, (((1,), (1,)), ((), ())), preferred_element_type=jnp.float32
    )


def inv_rms(value):
    return lax.rsqrt(jnp.mean(value * value, axis=-1, keepdims=True) + eps)


def norm_back(grad_out, value, scale, gain):
    scaled = grad_out * gain
    grad_in = scale * scaled - value * scale**3 * jnp.mean(scaled * value, axis=-1, keepdims=True)
    gain_grad = jnp.sum(grad_out * value * scale, axis=0)
    return (grad_in, gain_grad)


def rope_tables(seg):
    size = seg.shape[0]
    index = jnp.arange(size, dtype=jnp.int32)
    earlier = jnp.sum((seg[None, :] < seg[:, None]).astype(jnp.int32), axis=1)
    place = (index - earlier).astype(jnp.float32)
    half = ROPE // 2
    freqs = rope_base ** (-(jnp.arange(half, dtype=jnp.float32) * 2.0 / ROPE))
    angle = place[:, None] * freqs[None, :]
    return (jnp.cos(angle), jnp.sin(angle))


def attention_mask(seg):
    index = jnp.arange(seg.shape[0], dtype=jnp.int32)
    return (seg[:, None] == seg[None, :]) & (index[None, :] <= index[:, None])


def rotate(value, cosine, sine):
    half = value.shape[-1] // 2
    first, second = (value[..., :half], value[..., half:])
    return jnp.concatenate(
        [first * cosine - second * sine, second * cosine + first * sine], axis=-1
    )


def unrotate(value, cosine, sine):
    half = value.shape[-1] // 2
    first, second = (value[..., :half], value[..., half:])
    return jnp.concatenate(
        [first * cosine + second * sine, second * cosine - first * sine], axis=-1
    )


lanes = 128
vmem_limit = 64 * 1024 * 1024 - 131072


def token_slots(marks, here, local_experts, half):
    codes = times_trans(here, marks)
    count = codes.shape[1]
    rank = jnp.floor(codes * (1.0 / 32.0))
    place = codes - 32.0 * rank
    token = lax.broadcasted_iota(jnp.int32, codes.shape, 1)
    slot = jnp.where(codes >= 0, place + jnp.where(token >= half, float(CAP), 0.0), -1.0)
    row = lax.broadcasted_iota(jnp.int32, (2 * CAP, count), 0).astype(jnp.float32)
    picks = [jnp.where(row == slot[e : e + 1], 1.0, 0.0) for e in range(local_experts)]
    return picks, rank


def pair_slots(marks_ref, here_ref, local_experts, pair):
    count = marks_ref.shape[0] // pair
    return [
        token_slots(marks_ref[j * pair : (j + 1) * pair], here_ref[...], local_experts, pair // 2)
        for j in range(count)
    ]


def slot_part(value, e):
    return value[e * 2 * CAP : (e + 1) * 2 * CAP]


def gather_rows(slots, values, pair, out_ref):
    rows = [
        jnp.dot(
            jnp.concatenate(picks, axis=0).astype(jnp.bfloat16),
            values[j * pair : (j + 1) * pair],
            preferred_element_type=jnp.float32,
        )
        for j, (picks, _) in enumerate(slots)
    ]
    for e in range(out_ref.shape[0]):
        together = jnp.concatenate([slot_part(value, e) for value in rows], axis=0)
        out_ref[e] = together.astype(jnp.bfloat16)


def spread_rows(slots, rows_ref):
    local_experts = rows_ref.shape[0]
    rows = [rows_ref[e].astype(jnp.float32) for e in range(local_experts)]
    totals = []
    for j, (picks, _) in enumerate(slots):
        part = jnp.concatenate([slot_part(value, j) for value in rows], axis=0)
        pick = jnp.concatenate(picks, axis=0).astype(jnp.bfloat16)
        totals.append(trans_times(pick, part.astype(jnp.bfloat16)))
    return jnp.concatenate(totals, axis=0)


def grads_kernel(pair, ins, outs):
    here_ref, value_ref, down_ref = ins
    rows_ref, back_ref = outs
    width = rows_ref.shape[2]
    slots = pair_slots(value_ref.at[:, width:], here_ref, rows_ref.shape[0], pair)
    values = value_ref[:, :width]
    gather_rows(slots, values, pair, rows_ref)
    back_ref[...] = times_trans(values, down_ref[...])


def rows_kernel(
    pair,
    here_ref,
    twice_ref,
    marks_ref,
    value_ref,
    back_ref,
    gate_ref,
    up_ref,
    rows_ref,
    mix_ref,
    hidden_ref,
    gate_grad_ref,
    lift_grad_ref,
):
    width = rows_ref.shape[2]
    slots = pair_slots(marks_ref, here_ref, rows_ref.shape[0], pair)
    values = value_ref[:, :width]
    gather_rows(slots, values, pair, rows_ref)
    for j, (picks, _) in enumerate(slots):
        mixing = times_trans(twice_ref[...], value_ref[j * pair : (j + 1) * pair, width:])
        for e, pick in enumerate(picks):
            column = jnp.sum(pick * mixing[e : e + 1], axis=1, keepdims=True)
            column = jnp.broadcast_to(column, (2 * CAP, lanes))
            mix_ref[e, j * 2 * CAP : (j + 1) * 2 * CAP] = column
    gate = times_trans(values, gate_ref[...])
    lift = times_trans(values, up_ref[...])
    back = back_ref[...]
    sigma = jax.nn.sigmoid(gate)
    active = gate * sigma
    hidden_ref[...] = (active * lift).astype(jnp.bfloat16)
    gate_grad_ref[...] = (back * lift * sigma * (1.0 + gate * (1.0 - sigma))).astype(jnp.bfloat16)
    lift_grad_ref[...] = (back * active).astype(jnp.bfloat16)


def forward_kernel(
    rows_ref,
    mix_ref,
    gate_ref,
    up_ref,
    down_ref,
    hidden_ref,
    mixed_ref,
    slope_ref,
    active_ref,
    produced_ref,
):
    rows = rows_ref[0]
    gate = times_trans(rows, gate_ref[0])
    lift = times_trans(rows, up_ref[0])
    mix = mix_ref[0][:, :1]
    sigma = jax.nn.sigmoid(gate)
    active = gate * sigma
    hidden = active * lift
    mixed_hidden = (mix * hidden).astype(jnp.bfloat16)
    hidden_ref[0] = hidden.astype(jnp.bfloat16)
    mixed_ref[0] = mixed_hidden
    slope_ref[0] = (mix * lift * sigma * (1.0 + gate * (1.0 - sigma))).astype(jnp.bfloat16)
    active_ref[0] = (mix * active).astype(jnp.bfloat16)
    produced_ref[0] = matmul(mixed_hidden, down_ref[0]).astype(jnp.bfloat16)


def backward_kernel(turn, ins, outs):
    grads_ref, hidden_ref, slope_ref, active_ref, gate_ref, up_ref, down_ref = ins
    gate_grad_ref, lift_grad_ref, returned_ref, mix_grad_ref = outs
    back = times_trans(grads_ref[0], down_ref[0])
    mix_grad = jnp.sum(hidden_ref[0].astype(jnp.float32) * back, axis=1, keepdims=True)
    mix_grad_ref[0] = jnp.broadcast_to(mix_grad, mix_grad_ref.shape[1:])
    gate_grad = (back * slope_ref[0].astype(jnp.float32)).astype(jnp.bfloat16)
    lift_grad = (back * active_ref[0].astype(jnp.float32)).astype(jnp.bfloat16)
    gate_grad_ref[0] = gate_grad
    lift_grad_ref[0] = lift_grad
    returned = matmul(gate_grad, gate_ref[0]) + matmul(lift_grad, up_ref[0])
    returned_ref[0] = returned.astype(jnp.bfloat16)


def back_kernel(
    pair,
    here_ref,
    high_ref,
    low_ref,
    marks_ref,
    rows_ref,
    mix_grad_ref,
    gate_grad_ref,
    lift_grad_ref,
    gate_ref,
    up_ref,
    out_ref,
):
    width = rows_ref.shape[2]
    slots = pair_slots(marks_ref, here_ref, rows_ref.shape[0], pair)
    total = spread_rows(slots, rows_ref)
    total = total + matmul(gate_grad_ref[...], gate_ref[...])
    total = total + matmul(lift_grad_ref[...], up_ref[...])
    out_ref[:, :width] = total.astype(jnp.bfloat16)
    for j, (picks, rank) in enumerate(slots):
        choice = lax.broadcasted_iota(jnp.int32, rank.shape, 0).astype(jnp.float32)
        mix_grad = jnp.zeros(rank.shape, jnp.float32)
        for e, pick in enumerate(picks):
            column = slot_part(mix_grad_ref[e], j)[:, :1]
            row = jnp.sum(pick * column, axis=0, keepdims=True)
            mix_grad = mix_grad + jnp.where(choice == rank[e : e + 1], row, 0.0)
        high = mix_grad.astype(jnp.bfloat16)
        low = (mix_grad - high.astype(jnp.float32)).astype(jnp.bfloat16)
        sent = trans_times(high, high_ref[...]) + trans_times(low, low_ref[...])
        out_ref[j * pair : (j + 1) * pair, width:] = sent.astype(jnp.bfloat16)


def out_kernel(pair, here_ref, marks_ref, rows_ref, hidden_ref, down_ref, out_ref):
    slots = pair_slots(marks_ref, here_ref, rows_ref.shape[0], pair)
    total = spread_rows(slots, rows_ref)
    total = total + matmul(hidden_ref[...], down_ref[...])
    out_ref[...] = total.astype(jnp.bfloat16)


def whole_spec(array):
    zeros = (0,) * array.ndim
    return pl.BlockSpec(array.shape, lambda i: zeros)


def pair_spec(array, pairs):
    block = (array.shape[0] // pairs,) + array.shape[1:]
    zeros = (0,) * (array.ndim - 1)
    return pl.BlockSpec(block, lambda i: (i,) + zeros)


def slots_spec(array, pairs):
    block = (array.shape[0], array.shape[1] // pairs) + array.shape[2:]
    return pl.BlockSpec(block, lambda i: (0, i, 0))


def cost(flops, *arrays):
    moved = sum(a.size * a.dtype.itemsize for a in arrays)
    return pl.CostEstimate(flops=int(flops), bytes_accessed=int(moved), transcendentals=0)


def call(kernel, grid, ins, outs, flops):
    arrays = [a for a, _ in ins]
    shapes = [s for s, _ in outs]
    return pl.pallas_call(
        kernel,
        grid=(grid,),
        in_specs=[s for _, s in ins],
        out_specs=[s for _, s in outs],
        out_shape=shapes,
        cost_estimate=cost(flops, *arrays, *shapes),
        compiler_params=pltpu.CompilerParams(vmem_limit_bytes=vmem_limit),
    )(*arrays)


MESH = pl.DeviceIdType.MESH


def places():
    expert, weight = lax.axis_index("expert"), lax.axis_index("weight")
    return lax.div(expert, 2), lax.rem(expert, 2), lax.div(weight, 2), lax.rem(weight, 2)


def device(z, x, y, c):
    return (z * 2 + x, y * 2 + c)


def shard(z, x, y, c):
    return z * 8 + x * 4 + y * 2 + c


def push(source, target, send, receive, to):
    return pltpu.make_async_remote_copy(
        src_ref=source,
        dst_ref=target,
        send_sem=send,
        recv_sem=receive,
        device_id=to,
        device_id_type=MESH,
    )


class Sends:
    def __init__(self, semaphores):
        self.semaphores = semaphores
        self.started = []

    def plan(self, source, target, receive, to, when=None):
        copy = push(source, target, self.semaphores.at[len(self.started)], receive, to)
        self.started.append((copy, when))
        return copy

    def start(self, source, target, receive, to, when=None):
        copy = self.plan(source, target, receive, to, when)
        if when is None:
            copy.start()
        else:
            pl.when(when)(copy.start)

    def finish(self):
        for copy, when in self.started:
            if when is None:
                copy.wait_send()
            else:
                pl.when(when)(copy.wait_send)


def landed(target, receive, to):
    push(target, target, receive, receive, to).wait_recv()


def greet(devices):
    barrier = pltpu.get_barrier_semaphore()
    count = 0
    for to, when in devices:
        signal = functools.partial(
            pl.semaphore_signal, barrier, inc=1, device_id=to, device_id_type=MESH
        )
        if when is None:
            signal()
            count = count + 1
        else:
            pl.when(when)(signal)
            count = count + when.astype(jnp.int32)
    pl.semaphore_wait(barrier, count)


def add_rows(target, sources, start, rows):
    step = 16

    def body(i, carry):
        part = pl.ds(pl.multiple_of(start + i * step, step), step)
        total = target[part].astype(jnp.float32)
        for source, offset in sources:
            there = pl.ds(pl.multiple_of(start - offset + i * step, step), step)
            total = total + source[there].astype(jnp.float32)
        target[part] = total.astype(target.dtype)
        return carry

    lax.fori_loop(0, rows // step, body, 0)


def ordered(z, first, second):
    upper = lax.div(z, 2)
    inner = z + upper * (3 - 2 * z)
    value = first + inner * (second - first)
    return value + upper * (3 - 2 * value)


class Gather:
    def __init__(self, x_ref, out_ref, sends, recv_sems, local_sem, place, cut=None):
        z, x, y, c = place
        rows = x_ref.shape[0]
        cut = rows // 2 if cut is None else cut
        self.parts = [pl.ds(0, cut), pl.ds(cut, rows - cut)]
        over, side, mate = device(z, 1 - x, y, c), device(z, x, 1 - y, c), device(z, x, y, 1 - c)
        up, down = device(z + 1, x, y, c), device(z - 1, x, y, c)
        self.out_ref, self.recv_sems, self.mate = out_ref, recv_sems, mate
        planes = [ordered(z, (0, 1, 2, 3)[step], (1, 0, 2, 3)[step]) for step in range(4)]
        self.rising = [(zz <= z) & (z < 3) for zz in planes]
        self.falling = [(zz >= z) & (z > 0) for zz in planes]
        self.mine = [shard(zz, x, y, c) for zz in planes]
        self.overs = [shard(zz, 1 - x, y, c) for zz in planes]
        self.sides = [shard(zz, x, 1 - y, c) for zz in planes]
        self.corners = [shard(zz, 1 - x, 1 - y, c) for zz in planes]
        self.mates = [
            (shard(zz, x, y, 1 - c), shard(zz, 1 - x, y, 1 - c), shard(zz, x, 1 - y, 1 - c))
            for zz in planes
        ]
        self.mate_corners = [shard(zz, 1 - x, 1 - y, 1 - c) for zz in planes]
        self.keep = pltpu.make_async_copy(x_ref, out_ref.at[self.mine[0]], local_sem)
        self.whole_copies, self.relay_copies, self.corner_copies = [], [], []

        def copy(ref, receive, to, when=None, source=None):
            return sends.plan(ref if source is None else source, ref, receive, to, when)

        for step in range(4):
            i = self.mine[step]
            source = x_ref if step == 0 else None
            there, receive = out_ref.at[i], recv_sems.at[i, 0]
            self.whole_copies.append(
                [
                    (copy(there, receive, up, self.rising[step], source), self.rising[step]),
                    (copy(there, receive, down, self.falling[step], source), self.falling[step]),
                    (copy(there, receive, over, None, source), None),
                    (copy(there, receive, side, None, source), None),
                    (copy(there, receive, mate, None, source), None),
                ]
            )
            i, j = self.overs[step], self.sides[step]
            self.relay_copies.append(
                [
                    copy(self.halves(i, 0), recv_sems.at[i, 0], side),
                    copy(out_ref.at[i], recv_sems.at[i, 0], mate),
                    copy(self.halves(j, 1), recv_sems.at[j, 1], over),
                    copy(out_ref.at[j], recv_sems.at[j, 0], mate),
                ]
            )
            i = self.corners[step]
            self.corner_copies.append(
                [copy(self.halves(i, h), recv_sems.at[i, h], mate) for h in range(2)]
            )

    def halves(self, i, h):
        return self.out_ref.at[i, self.parts[h]]

    def full_here(self, i):
        landed(self.out_ref.at[i], self.recv_sems.at[i, 0], self.mate)

    def half_here(self, i, h):
        landed(self.halves(i, h), self.recv_sems.at[i, h], self.mate)

    def whole(self, step):
        if step == 0:
            self.keep.start()
        else:
            self.full_here(self.mine[step])
        for copy, when in self.whole_copies[step]:
            if when is None:
                copy.start()
            else:
                pl.when(when)(copy.start)

    def relay(self, step):
        self.full_here(self.overs[step])
        self.relay_copies[step][0].start()
        self.relay_copies[step][1].start()
        self.full_here(self.sides[step])
        self.relay_copies[step][2].start()
        self.relay_copies[step][3].start()

    def corner(self, step):
        for h in range(2):
            self.half_here(self.corners[step], h)
            self.corner_copies[step][h].start()

    def rest(self, step):
        for i in self.mates[step]:
            self.full_here(i)
        for h in range(2):
            self.half_here(self.mate_corners[step], h)
        if step == 0:
            self.keep.wait()

    def last(self):
        for step in range(4):
            self.rest(step)


def gather_neighbours(place):
    z, x, y, c = place
    return [
        (device(z, 1 - x, y, c), None),
        (device(z, x, 1 - y, c), None),
        (device(z, x, y, 1 - c), None),
        (device(z + 1, x, y, c), z < 3),
        (device(z - 1, x, y, c), z > 0),
    ]


def token_kernel(
    pair,
    x_ref,
    here_ref,
    value_ref,
    down_ref,
    twice_ref,
    gate_ref,
    up_ref,
    cotangent_hbm,
    out_ref,
    grads_ref,
    rows_hbm,
    mix_ref,
    hidden_ref,
    gate_grad_ref,
    lift_grad_ref,
    raw,
    arrived,
    marks,
    stage,
    send_sems,
    recv_sems,
    local_sem,
    load_sems,
    store_sems,
):
    turn, turns = pl.program_id(0), pl.num_programs(0)
    place = places()
    sends = Sends(send_sems)
    gather = Gather(x_ref, out_ref, sends, recv_sems, local_sem, place)
    quad, rows = value_ref.shape[0], x_ref.shape[0]
    count = quad // rows
    width = grads_ref.shape[2]
    slot_rows = grads_ref.shape[1]

    def begin():
        greet(gather_neighbours(place))
        gather.whole(0)

    def early():
        gather.relay(1)
        gather.corner(0)

    def part(index, size):
        return pl.ds(pl.multiple_of(index * size, 16), size)

    first_plane = turns - 4
    step = turn - first_plane
    second = step + (1 - 2 * step) * (1 - lax.div(step, 2))
    zz = ordered(place[0], step, second)

    def store(k):
        group = zz * 2 + k
        return pltpu.make_async_copy(
            stage.at[k], rows_hbm.at[:, part(group, slot_rows)], store_sems.at[k]
        )

    def loads(k):
        group = zz * 2 + k
        copies = [
            pltpu.make_async_copy(
                out_ref.at[group * count + i],
                arrived.at[k, pl.ds(i * rows, rows)],
                load_sems.at[k, i],
            )
            for i in range(count)
        ]
        copies.append(
            pltpu.make_async_copy(
                cotangent_hbm.at[part(group, quad), pl.ds(width, lanes)],
                marks.at[k],
                load_sems.at[k, count],
            )
        )
        return copies

    def plane():
        for k in range(2):
            for copy in loads(k):
                copy.start()

        def one(k, carry):
            for copy in loads(k):
                copy.wait()
            pl.when(step > 0)(lambda: store(k).wait())
            group = zz * 2 + k
            tokens = part(group, quad)
            rows_kernel(
                pair,
                here_ref,
                twice_ref,
                marks.at[k],
                arrived.at[k],
                raw.at[tokens],
                gate_ref,
                up_ref,
                stage.at[k],
                mix_ref.at[:, part(group, slot_rows)],
                hidden_ref.at[tokens],
                gate_grad_ref.at[tokens],
                lift_grad_ref.at[tokens],
            )
            store(k).start()
            return carry

        lax.fori_loop(0, 2, one, 0)

    def second_plane():
        gather.relay(2)
        gather.corner(1)
        gather.rest(1)

    def third_plane():
        gather.relay(3)
        gather.corner(2)
        gather.rest(2)

    def fourth_plane():
        gather.corner(3)
        gather.rest(3)

    def end():
        for k in range(2):
            store(k).wait()
        sends.finish()

    pieces = [
        begin,
        lambda: None,
        functools.partial(gather.whole, 1),
        functools.partial(gather.relay, 0),
        functools.partial(gather.whole, 2),
        lambda: None,
        early,
        functools.partial(gather.whole, 3),
        functools.partial(gather.rest, 0),
        second_plane,
        third_plane,
        fourth_plane,
    ]
    for number, piece in enumerate(pieces):
        pl.when(turn == number)(piece)

    @pl.when(turn < first_plane)
    def _():
        grads_kernel(pair, (here_ref, value_ref, down_ref), (grads_ref, raw.at[part(turn, quad)]))

    pl.when(turn >= first_plane)(plane)
    pl.when(turn == turns - 1)(end)


def gather_tokens(
    value, cotangent, here, twice, down, gate, up, local_experts, slot_rows, pair, number
):
    rows, wide = value.shape
    width = down.shape[1]
    quad, all_rows, turns = 4 * rows, 32 * rows, 8
    shared_wide = down.shape[0]
    shape, low = jax.ShapeDtypeStruct, jnp.bfloat16
    slots = shape((local_experts, slot_rows, width), low)
    token_part = shape((all_rows, shared_wide), low)
    mix = shape((local_experts, slot_rows, lanes), jnp.float32)
    away = pl.BlockSpec(memory_space=pl.ANY)
    last = turns - 1
    quad_spec = pl.BlockSpec((quad, cotangent.shape[1]), lambda i: (jnp.minimum(i, last), 0))
    part = slot_rows // turns
    slot_spec = pl.BlockSpec((local_experts, part, width), lambda i: (0, jnp.minimum(i, last), 0))
    ins = [
        (value, whole_spec(value)),
        (here, whole_spec(here)),
        (cotangent, quad_spec),
        (down, whole_spec(down)),
        (twice, whole_spec(twice)),
        (gate, whole_spec(gate)),
        (up, whole_spec(up)),
        (cotangent, away),
    ]
    outs = [
        (shape((32,) + value.shape, low), away),
        (slots, slot_spec),
        (slots, away),
        (mix, whole_spec(mix)),
        (token_part, whole_spec(token_part)),
        (token_part, whole_spec(token_part)),
        (token_part, whole_spec(token_part)),
    ]
    flops = 4 * all_rows * width * (2 * CAP * local_experts + 2 * shared_wide)
    return pl.pallas_call(
        functools.partial(token_kernel, pair),
        grid=(turns + 4,),
        out_shape=[o for o, _ in outs],
        in_specs=[spec for _, spec in ins],
        out_specs=[spec for _, spec in outs],
        scratch_shapes=[
            pltpu.VMEM((all_rows, shared_wide), jnp.float32),
            pltpu.VMEM((2, quad, wide), low),
            pltpu.VMEM((2, quad, lanes), low),
            pltpu.VMEM((2, local_experts, part, width), low),
            pltpu.SemaphoreType.DMA((44,)),
            pltpu.SemaphoreType.DMA((32, 2)),
            pltpu.SemaphoreType.DMA,
            pltpu.SemaphoreType.DMA((2, 5)),
            pltpu.SemaphoreType.DMA((2,)),
        ],
        compiler_params=pltpu.CompilerParams(
            collective_id=number, has_side_effects=True, vmem_limit_bytes=vmem_limit
        ),
        cost_estimate=cost(flops, *[a for a, _ in ins], *[o for o, _ in outs]),
    )(*[a for a, _ in ins])


def attention_kernel(
    score_scale,
    normed_ref,
    value_ref,
    cosine_ref,
    sine_ref,
    segment_row_ref,
    segment_column_ref,
    gain_ref,
    tokens_ref,
    second_gain_ref,
    router_ref,
    query_hbm,
    latent_hbm,
    expand_hbm,
    output_hbm,
    value_out,
    normed_out,
    query_out,
    latent_out,
    scale_out,
    latent_normed_out,
    key_rope_out,
    expanded_out,
    log_out,
    mixed_out,
    hidden_out,
    second_scale_out,
    gates_out,
    wide_out,
    query_matrix,
    latent_matrix,
    expand_matrix,
    output_matrix,
    partial,
    mates,
    sides,
    carried,
    send_sems,
    recv_sems,
    local_sems,
    group_sends,
    group_sems,
    sum_sends,
    mate_sems,
    side_sems,
):
    place = places()
    z, x, y, c = place
    side, mate = device(z, x, 1 - y, c), device(z, x, y, 1 - c)
    rows = normed_ref.shape[0]
    half = rows // 2
    heads = query_out.shape[0]
    greet(gather_neighbours(place))
    near = Sends(group_sends)
    own, across = y * 2 + c, (1 - y) * 2 + c
    keep = pltpu.make_async_copy(normed_ref, normed_out.at[own], local_sems.at[0])
    keep.start()

    def part(i, h):
        return normed_out.at[i, pl.ds(h * half, half)]

    for to in (side, mate):
        for h in range(2):
            piece = normed_ref.at[pl.ds(h * half, half)]
            near.start(piece, part(own, h), group_sems.at[own, h], to)
    sends = Sends(send_sems)
    gather = Gather(value_ref, value_out, sends, recv_sems, local_sems.at[1], place, 48)
    gather.whole(0)
    loads = [
        pltpu.make_async_copy(source, target, local_sems.at[2 + i])
        for i, (source, target) in enumerate(
            (
                (query_hbm, query_matrix),
                (latent_hbm, latent_matrix),
                (expand_hbm, expand_matrix),
                (output_hbm, output_matrix),
            )
        )
    ]
    for load in loads:
        load.start()
    for h in range(2):
        landed(part(across, h), group_sems.at[across, h], mate)
        near.start(part(across, h), part(across, h), group_sems.at[across, h], mate)
    for i in (y * 2 + 1 - c, (1 - y) * 2 + 1 - c):
        for h in range(2):
            landed(part(i, h), group_sems.at[i, h], mate)
    keep.wait()
    normed = normed_out[...].reshape(4 * rows, normed_out.shape[2])
    cosine, sine = cosine_ref[...], sine_ref[...]
    turn_half = ROPE // 2

    def turned(first, second):
        return jnp.concatenate(
            [first * cosine - second * sine, second * cosine + first * sine], axis=1
        )

    loads[0].wait()
    full = matmul(normed, query_matrix[...])
    for h in range(heads):
        start = h * (NOPE + ROPE)
        first = full[:, start + NOPE : start + NOPE + turn_half]
        second = full[:, start + NOPE + turn_half : start + NOPE + ROPE]
        query = jnp.concatenate([full[:, start : start + NOPE], turned(first, second)], axis=1)
        query_out[h] = query.astype(jnp.bfloat16)
    gather.whole(1)
    loads[1].wait()
    compressed = times_trans(normed, latent_matrix[...])
    latent = compressed[:, :LATENT]
    scale = inv_rms(latent)
    latent_out[...] = latent
    scale_out[...] = jnp.broadcast_to(scale, scale_out.shape)
    latent_normed_out[...] = (latent * scale * gain_ref[...]).astype(jnp.bfloat16)
    first = compressed[:, LATENT : LATENT + turn_half]
    second = compressed[:, LATENT + turn_half : LATENT + ROPE]
    key_rope_out[...] = turned(first, second).astype(jnp.bfloat16)
    gather.relay(0)
    loads[2].wait()
    expanded_out[...] = matmul(latent_normed_out[...], expand_matrix[...]).astype(jnp.bfloat16)

    def head(h):
        start = h * (NOPE + VDIM)
        query = query_out[h]
        raw = times_trans(query[:, :NOPE], expanded_out[:, columns(start, NOPE)])
        raw = raw + times_trans(query[:, NOPE:], key_rope_out[...])
        row = lax.broadcasted_iota(jnp.int32, raw.shape, 0)
        column = lax.broadcasted_iota(jnp.int32, raw.shape, 1)
        allowed = (segment_column_ref[...] == segment_row_ref[...]) & (column <= row)
        scores = jnp.where(allowed, raw * score_scale, -1e30)
        peak = jnp.max(scores, axis=1, keepdims=True)
        weights = jnp.exp(scores - peak)
        total = jnp.sum(weights, axis=1, keepdims=True)
        log_out[h] = jnp.broadcast_to(peak + jnp.log(total), log_out.shape[1:])
        probs = (weights / total).astype(jnp.bfloat16)
        mixed = matmul(probs, expanded_out[:, columns(start + NOPE, VDIM)])
        mixed_out[:, columns(h * VDIM, VDIM)] = mixed.astype(jnp.bfloat16)

    middle = [
        None,
        functools.partial(gather.whole, 2),
        functools.partial(gather.relay, 1),
        functools.partial(gather.corner, 0),
    ]

    def step(h, carry):
        head(h)
        for number, piece in enumerate(middle):
            if piece is not None:
                pl.when(h == number)(piece)
        return carry

    lax.fori_loop(0, heads, step, 0)
    loads[3].wait()
    for i in range(4):
        block = matmul(mixed_out[i * rows : (i + 1) * rows], output_matrix[...])
        partial[i] = block.astype(jnp.bfloat16)
    sums = Sends(sum_sends)
    for j, yy in enumerate((1 - y, y)):
        for h in range(2):
            some = pl.ds(h * half, half)
            sums.start(
                partial.at[yy * 2 + 1 - c, some], mates.at[j, some], mate_sems.at[j, h], mate
            )
    gather.whole(3)
    for h in range(2):
        some = pl.ds(h * half, half)
        landed(mates.at[0, some], mate_sems.at[0, h], mate)
        add_into(carried, [partial.at[(1 - y) * 2 + c], mates.at[0]], h * half, half)
        sums.start(carried.at[some], sides.at[some], side_sems.at[h], side)
    gather.relay(2)
    gather.corner(1)
    for h in range(2):
        some = pl.ds(h * half, half)
        landed(mates.at[1, some], mate_sems.at[1, h], mate)
        landed(sides.at[some], side_sems.at[h], mate)
        add_into(hidden_out, [partial.at[y * 2 + c], mates.at[1], sides], h * half, half)
    hidden = tokens_ref[...].astype(jnp.float32) + hidden_out[...]
    hidden_out[...] = hidden
    second_scale = inv_rms(hidden)
    second_scale_out[...] = jnp.broadcast_to(second_scale, second_scale_out.shape)
    normed_two = (hidden * second_scale * second_gain_ref[...]).astype(jnp.bfloat16)
    width = hidden.shape[1]
    wide_out[:, :width] = normed_two
    gates = jax.nn.sigmoid(times_trans(normed_two, router_ref[...]))
    gates_out[...] = gates
    codes = value_ref[:, width:].astype(jnp.float32)[:, : gates.shape[1]]
    weighted = jnp.where(codes >= 0, gates, 0.0)
    mixing = route_scale * weighted / jnp.sum(weighted, axis=1, keepdims=True)
    high = mixing.astype(jnp.bfloat16).astype(jnp.float32)
    wide_out[:, width:] = jnp.concatenate([high, mixing - high], axis=1).astype(jnp.bfloat16)
    gather.relay(3)
    gather.corner(2)
    gather.corner(3)
    gather.last()
    near.finish()
    sends.finish()
    sums.finish()


def add_into(target, sources, start, rows):
    step = 16

    def body(i, carry):
        part = pl.ds(pl.multiple_of(start + i * step, step), step)
        total = sources[0][part].astype(jnp.float32)
        for source in sources[1:]:
            total = total + source[part].astype(jnp.float32)
        target[part] = total.astype(target.dtype)
        return carry

    lax.fori_loop(0, rows // step, body, 0)


def attention_forward(
    score_scale,
    normed,
    value,
    cosine,
    sine,
    segment,
    gain,
    tokens,
    second_gain,
    router,
    query,
    latent,
    expand,
    output,
    number,
):
    rows, width = normed.shape
    group, heads = 4 * rows, query.shape[1] // (NOPE + ROPE)
    shape, low = jax.ShapeDtypeStruct, jnp.bfloat16
    vmem, away = pl.BlockSpec(memory_space=pltpu.VMEM), pl.BlockSpec(memory_space=pl.ANY)
    segment = segment.astype(jnp.float32)
    inputs = [normed, value, cosine, sine, segment[None], segment[:, None], gain[None]]
    inputs += [tokens, second_gain[None], router.T]
    matrices = [query, latent.T, expand, output]
    outs = [
        shape((32,) + value.shape, low),
        shape((4, rows, width), low),
        shape((heads, group, NOPE + ROPE), low),
        shape((group, LATENT), jnp.float32),
        shape((group, lanes), jnp.float32),
        shape((group, LATENT), low),
        shape((group, ROPE), low),
        shape((group, heads * (NOPE + VDIM)), low),
        shape((heads, group, lanes), jnp.float32),
        shape((group, heads * VDIM), low),
        shape((rows, width), jnp.float32),
        shape((rows, lanes), jnp.float32),
        shape((rows, router.shape[1]), jnp.float32),
        shape(value.shape, low),
    ]
    flops = 2 * group * (width * (query.shape[1] + latent.shape[1]) + output.size + expand.size)
    return pl.pallas_call(
        functools.partial(attention_kernel, score_scale),
        out_shape=outs,
        in_specs=[vmem] * len(inputs) + [away] * 4,
        out_specs=[away] + [vmem] * (len(outs) - 1),
        scratch_shapes=[pltpu.VMEM(m.shape, low) for m in matrices]
        + [
            pltpu.VMEM((4, rows, width), low),
            pltpu.VMEM((2, rows, width), low),
            pltpu.VMEM((rows, width), low),
            pltpu.VMEM((rows, width), low),
            pltpu.SemaphoreType.DMA((44,)),
            pltpu.SemaphoreType.DMA((32, 2)),
            pltpu.SemaphoreType.DMA((6,)),
            pltpu.SemaphoreType.DMA((6,)),
            pltpu.SemaphoreType.DMA((4, 2)),
            pltpu.SemaphoreType.DMA((6,)),
            pltpu.SemaphoreType.DMA((2, 2)),
            pltpu.SemaphoreType.DMA((2,)),
        ],
        compiler_params=pltpu.CompilerParams(
            collective_id=number, has_side_effects=True, vmem_limit_bytes=vmem_limit
        ),
        cost_estimate=cost(flops, *inputs, *matrices, *outs),
    )(*inputs, *matrices)


def sum_all_kernel(inner, cover_ins, cover_outs, p_ref, *refs):
    ins, refs = refs[:cover_ins], refs[cover_ins:]
    out_ref, refs = refs[0], refs[1:]
    outs, refs = refs[:cover_outs], refs[cover_outs:]
    own, mates, over_half, side_half, over_full, side_full, below, above = refs[:8]
    send_sems, mate_sems, half_sems, full_sems, line_sems, local_sems = refs[8:]
    z, x, y, c = places()
    turn, turns = pl.program_id(0), pl.num_programs(0)
    rows = out_ref.shape[0]
    half = rows // 2
    over, side, mate = device(z, 1 - x, y, c), device(z, x, 1 - y, c), device(z, x, y, 1 - c)
    up, down = device(z + 1, x, y, c), device(z - 1, x, y, c)
    sends = Sends(send_sems)
    targets = [ordered(z, (3, 2, 1, 0)[step], (3, 0, 2, 1)[step]) for step in range(4)]
    spots = [(1 - x, 1 - y), (1 - x, y), (x, 1 - y), (x, y)]
    shards = [[shard(zz, xx, yy, 1 - c) for xx, yy in spots] for zz in targets]
    mine = [[shard(zz, xx, yy, c) for xx, yy in spots] for zz in targets]
    higher = [zz > z for zz in targets]
    lower = [zz < z for zz in targets]
    loads = [
        pltpu.make_async_copy(p_ref.at[mine[slot // 4][slot % 4]], own.at[slot], local_sems.at[slot])
        for slot in range(16)
    ]

    mate_copies = [
        sends.plan(p_ref.at[shards[slot // 4][slot % 4]], mates.at[slot], mate_sems.at[slot], mate)
        for slot in range(16)
    ]
    corner_copies, relay_copies, line_copies = [], [], []
    for step in range(4):
        corner_copies.append(
            (
                sends.plan(
                    own.at[step * 4, pl.ds(half, half)],
                    over_half.at[step],
                    half_sems.at[step, 0],
                    over,
                ),
                sends.plan(
                    own.at[step * 4, pl.ds(0, half)], side_half.at[step], half_sems.at[step, 1], side
                ),
            )
        )
        relay_copies.append(
            (
                sends.plan(
                    own.at[step * 4 + 1], over_full.at[step], full_sems.at[step, 0], over
                ),
                sends.plan(
                    own.at[step * 4 + 2], side_full.at[step], full_sems.at[step, 1], side
                ),
            )
        )
    for step in range(3):
        zz, slot = targets[step], step * 4 + 3
        line_copies.append(
            (
                sends.plan(own.at[slot], below.at[zz], line_sems.at[zz, 0], up, higher[step]),
                sends.plan(own.at[slot], above.at[zz], line_sems.at[zz, 1], down, lower[step]),
            )
        )

    def begin():
        greet([(over, None), (side, None), (mate, None), (up, z < 3), (down, z > 0)])
        for slot in range(16):
            mate_copies[slot].start()
            loads[slot].start()

    def join(slot):
        loads[slot].wait()
        landed(mates.at[slot], mate_sems.at[slot], mate)

    def corner(step):
        slot = step * 4
        join(slot)
        add_rows(own.at[slot], [(mates.at[slot], 0)], 0, rows)
        for copy in corner_copies[step]:
            copy.start()

    def relay(step):
        slot = step * 4 + 1
        join(slot)
        add_rows(own.at[slot], [(mates.at[slot], 0)], half, half)
        landed(side_half.at[step], half_sems.at[step, 1], mate)
        add_rows(own.at[slot], [(mates.at[slot], 0), (side_half.at[step], 0)], 0, half)
        relay_copies[step][0].start()
        slot = step * 4 + 2
        join(slot)
        add_rows(own.at[slot], [(mates.at[slot], 0)], 0, half)
        landed(over_half.at[step], half_sems.at[step, 0], mate)
        add_rows(own.at[slot], [(mates.at[slot], 0), (over_half.at[step], half)], half, half)
        relay_copies[step][1].start()

    def whole(step):
        zz = targets[step]
        slot = step * 4 + 3
        join(slot)
        landed(over_full.at[step], full_sems.at[step, 0], mate)
        landed(side_full.at[step], full_sems.at[step, 1], mate)
        add_rows(
            own.at[slot],
            [(mates.at[slot], 0), (over_full.at[step], 0), (side_full.at[step], 0)],
            0,
            rows,
        )

        @pl.when((zz >= z) & (z > 0))
        def _():
            landed(below.at[zz], line_sems.at[zz, 0], mate)
            add_rows(own.at[slot], [(below.at[zz], 0)], 0, rows)

        @pl.when((zz <= z) & (z < 3))
        def _():
            landed(above.at[zz], line_sems.at[zz, 1], mate)
            add_rows(own.at[slot], [(above.at[zz], 0)], 0, rows)

        if step < 3:
            pl.when(higher[step])(line_copies[step][0].start)
            pl.when(lower[step])(line_copies[step][1].start)

    def end():
        whole(3)
        out_ref[...] = own[15].astype(out_ref.dtype)
        sends.finish()

    pieces = [
        begin,
        functools.partial(corner, 0),
        functools.partial(corner, 1),
        functools.partial(relay, 0),
        functools.partial(corner, 2),
        functools.partial(relay, 1),
        functools.partial(whole, 0),
        functools.partial(corner, 3),
        functools.partial(relay, 2),
        functools.partial(whole, 1),
        functools.partial(relay, 3),
        functools.partial(whole, 2),
    ]
    for number, piece in enumerate(pieces):
        pl.when(turn == number)(piece)
    inner(turn, ins, outs)
    pl.when(turn == turns - 1)(end)


def sum_all(value, number, inner, turns, ins, outs, flops):
    if lax.axis_size("expert") != 8 or lax.axis_size("weight") != 4:
        summed = lax.psum_scatter(
            value.reshape(-1, value.shape[2]), ("expert", "weight"), scatter_dimension=0, tiled=True
        )

        def alone(*refs):
            inner(pl.program_id(0), refs[: len(ins)], refs[len(ins) :])

        return summed.astype(jnp.float32), call(alone, turns, ins, outs, flops)
    _, rows, width = value.shape
    out = jax.ShapeDtypeStruct((rows, width), jnp.float32)
    buffer = lambda n, r: pltpu.VMEM((n, r, width), value.dtype)
    arrays, shapes = [a for a, _ in ins], [o for o, _ in outs]
    results = pl.pallas_call(
        functools.partial(sum_all_kernel, inner, len(ins), len(outs)),
        grid=(turns,),
        out_shape=[out] + shapes,
        in_specs=[pl.BlockSpec(memory_space=pl.ANY)] + [spec for _, spec in ins],
        out_specs=[pl.BlockSpec((rows, width), lambda i: (0, 0))] + [spec for _, spec in outs],
        scratch_shapes=[
            buffer(16, rows),
            buffer(16, rows),
            buffer(4, rows // 2),
            buffer(4, rows // 2),
            buffer(4, rows),
            buffer(4, rows),
            buffer(4, rows),
            buffer(4, rows),
            pltpu.SemaphoreType.DMA((40,)),
            pltpu.SemaphoreType.DMA((16,)),
            pltpu.SemaphoreType.DMA((4, 2)),
            pltpu.SemaphoreType.DMA((4, 2)),
            pltpu.SemaphoreType.DMA((4, 2)),
            pltpu.SemaphoreType.DMA((16,)),
        ],
        compiler_params=pltpu.CompilerParams(
            collective_id=number, has_side_effects=True, vmem_limit_bytes=vmem_limit
        ),
        cost_estimate=cost(flops, value, out, *arrays, *shapes),
    )(value, *arrays)
    return results[0], results[1:]


def gather_group_kernel(x_ref, out_ref, send_sems, recv_sems, local_sem):
    z, x, y, c = places()
    half = x_ref.shape[0] // 2
    side, mate = device(z, x, 1 - y, c), device(z, x, y, 1 - c)
    greet([(side, None), (mate, None)])
    sends = Sends(send_sems)
    own, across = y * 2 + c, (1 - y) * 2 + c
    keep = pltpu.make_async_copy(x_ref, out_ref.at[own], local_sem)
    keep.start()

    def part(i, h):
        return out_ref.at[i, pl.ds(h * half, half)]

    for h in range(2):
        piece = x_ref.at[pl.ds(h * half, half)]
        sends.start(piece, part(own, h), recv_sems.at[own, h], side)
    for h in range(2):
        piece = x_ref.at[pl.ds(h * half, half)]
        sends.start(piece, part(own, h), recv_sems.at[own, h], mate)
    for h in range(2):
        landed(part(across, h), recv_sems.at[across, h], mate)
        sends.start(part(across, h), part(across, h), recv_sems.at[across, h], mate)
    for i in (y * 2 + 1 - c, (1 - y) * 2 + 1 - c):
        for h in range(2):
            landed(part(i, h), recv_sems.at[i, h], mate)
    sends.finish()
    keep.wait()


def gather_group(value, number):
    if lax.axis_size("expert") != 8 or lax.axis_size("weight") != 4:
        return lax.all_gather(value, "weight", axis=0, tiled=True)
    out = jax.ShapeDtypeStruct((4,) + value.shape, value.dtype)
    return pl.pallas_call(
        gather_group_kernel,
        out_shape=out,
        in_specs=[pl.BlockSpec(memory_space=pltpu.VMEM)],
        out_specs=pl.BlockSpec(memory_space=pltpu.VMEM),
        scratch_shapes=[
            pltpu.SemaphoreType.DMA((6,)),
            pltpu.SemaphoreType.DMA((4, 2)),
            pltpu.SemaphoreType.DMA,
        ],
        compiler_params=pltpu.CompilerParams(collective_id=number, has_side_effects=True),
        cost_estimate=cost(0, value, out),
    )(value).reshape(-1, value.shape[1])


def sum_group_kernel(p_ref, out_ref, mates, sides, carried, send_sems, mate_sems, side_sems):
    z, x, y, c = places()
    rows = out_ref.shape[0]
    half = rows // 2
    side, mate = device(z, x, 1 - y, c), device(z, x, y, 1 - c)
    greet([(side, None), (mate, None)])
    sends = Sends(send_sems)

    for j, yy in enumerate((1 - y, y)):
        for h in range(2):
            part = pl.ds(h * half, half)
            sends.start(
                p_ref.at[yy * 2 + 1 - c, part], mates.at[j, part], mate_sems.at[j, h], mate
            )

    def add(target, sources, h):
        step = 16

        def body(i, carry):
            part = pl.ds(pl.multiple_of(h * half + i * step, step), step)
            total = sources[0][part].astype(jnp.float32)
            for source in sources[1:]:
                total = total + source[part].astype(jnp.float32)
            target[part] = total.astype(target.dtype)
            return carry

        lax.fori_loop(0, half // step, body, 0)

    for h in range(2):
        part = pl.ds(h * half, half)
        landed(mates.at[0, part], mate_sems.at[0, h], mate)
        add(carried, [p_ref.at[(1 - y) * 2 + c], mates.at[0]], h)
        sends.start(carried.at[part], sides.at[part], side_sems.at[h], side)
    for h in range(2):
        part = pl.ds(h * half, half)
        landed(mates.at[1, part], mate_sems.at[1, h], mate)
        landed(sides.at[part], side_sems.at[h], mate)
        add(out_ref, [p_ref.at[y * 2 + c], mates.at[1], sides], h)
    sends.finish()


def sum_group(value, number):
    if lax.axis_size("expert") != 8 or lax.axis_size("weight") != 4:
        summed = lax.psum_scatter(value, "weight", scatter_dimension=0, tiled=True)
        return summed.astype(jnp.float32)
    rows, width = value.shape[0] // 4, value.shape[1]
    value = value.reshape(4, rows, width)
    out = jax.ShapeDtypeStruct((rows, width), jnp.float32)
    return pl.pallas_call(
        sum_group_kernel,
        out_shape=out,
        in_specs=[pl.BlockSpec(memory_space=pltpu.VMEM)],
        out_specs=pl.BlockSpec(memory_space=pltpu.VMEM),
        scratch_shapes=[
            pltpu.VMEM((2, rows, width), value.dtype),
            pltpu.VMEM((rows, width), value.dtype),
            pltpu.VMEM((rows, width), value.dtype),
            pltpu.SemaphoreType.DMA((6,)),
            pltpu.SemaphoreType.DMA((2, 2)),
            pltpu.SemaphoreType.DMA((2,)),
        ],
        compiler_params=pltpu.CompilerParams(collective_id=number, has_side_effects=True),
        cost_estimate=cost(0, value, out),
    )(value)


def columns(start, size):
    return pl.ds(pl.multiple_of(start, lanes), size)


def add_block(target, sources, rows, row_start=0):
    step = 16

    def body(i, carry):
        part = pl.ds(pl.multiple_of(row_start + i * step, step), step)
        total = target[part].astype(jnp.float32)
        for source in sources:
            there = pl.ds(pl.multiple_of(i * step, step), step)
            total = total + source[there].astype(jnp.float32)
        target[part] = total.astype(target.dtype)
        return carry

    lax.fori_loop(0, rows // step, body, 0)


def total_kernel(
    top_ref,
    rest_ref,
    group_ref,
    out_ref,
    group_out,
    acc,
    mates,
    first_over,
    first_side,
    next_side,
    next_over,
    line,
    group_mates,
    group_sides,
    carried,
    send_sems,
    sems,
    mate_sems,
    side_sems,
):
    z, x, y, c = places()
    rows, width = out_ref.shape
    group_half = group_out.shape[0] // 2
    group_parts = [pl.ds(h * group_half, group_half) for h in range(2)]
    sources = [(top_ref, 0, 0), (rest_ref, top_ref.shape[0], 24)]
    half, quarter, eighth, sixteenth = width // 2, width // 4, width // 8, width // 16
    strip = rows // 4
    over, side, mate = device(z, 1 - x, y, c), device(z, x, 1 - y, c), device(z, x, y, 1 - c)
    others = [lax.rem(z + d, 4) for d in (1, 2, 3)]
    greet(
        [(over, None), (side, None), (mate, None)] + [(device(zz, x, y, c), None) for zz in others]
    )
    sends = Sends(send_sems)
    base = c * half
    for j in range(2):
        for p_ref, top, sem in sources:
            sends.start(
                p_ref.at[:, columns((1 - c) * half + j * quarter, quarter)],
                mates.at[pl.ds(top, p_ref.shape[0]), columns(j * quarter, quarter)],
                sems.at[sem + j],
                mate,
            )
    for i, yy in enumerate((1 - y, y)):
        for h, some in enumerate(group_parts):
            sends.start(
                group_ref.at[yy * 2 + 1 - c, some],
                group_mates.at[i, some],
                mate_sems.at[i, h],
                mate,
            )
    kept = (x * eighth + y * sixteenth, quarter + y * eighth + x * sixteenth)
    firsts, nexts = (first_over, first_side), (next_side, next_over)
    for j in range(2):
        part = columns(j * quarter, quarter)
        wide = 16
        for p_ref, top, sem in sources:
            landed(mates.at[pl.ds(top, p_ref.shape[0]), part], sems.at[sem + j], mate)

            def join(i, carry, j=j, p_ref=p_ref, top=top):
                mine = pl.ds(pl.multiple_of(i * wide, wide), wide)
                some = pl.ds(pl.multiple_of(top + i * wide, wide), wide)
                total = p_ref[mine, columns(base + j * quarter, quarter)].astype(jnp.float32)
                total = total + mates[some, columns(j * quarter, quarter)].astype(jnp.float32)
                acc[some, columns(j * quarter, quarter)] = total.astype(acc.dtype)
                return carry

            lax.fori_loop(0, p_ref.shape[0] // wide, join, 0)
        away = (1 - x) * eighth if j == 0 else quarter + (1 - y) * eighth
        sends.start(
            acc.at[:, columns(away, eighth)], firsts[j], sems.at[2 + j], (over, side)[j]
        )
    for h, some in enumerate(group_parts):
        landed(group_mates.at[0, some], mate_sems.at[0, h], mate)
        add_into(
            carried,
            [group_ref.at[(1 - y) * 2 + c], group_mates.at[0]],
            h * group_half,
            group_half,
        )
        sends.start(carried.at[some], group_sides.at[some], side_sems.at[h], side)
    for j in range(2):
        landed(firsts[j], sems.at[2 + j], mate)
        near = x * eighth if j == 0 else quarter + y * eighth
        add_block(acc.at[:, columns(near, eighth)], [firsts[j]], rows)
        away = near + ((1 - y) if j == 0 else (1 - x)) * sixteenth
        sends.start(
            acc.at[:, columns(away, sixteenth)], nexts[j], sems.at[4 + j], (side, over)[j]
        )
    for j in range(2):
        landed(nexts[j], sems.at[4 + j], mate)
        add_block(acc.at[:, columns(kept[j], sixteenth)], [nexts[j]], rows)
        for d, zz in enumerate(others):
            sends.start(
                acc.at[pl.ds(pl.multiple_of(zz * strip, 16), strip), columns(kept[j], sixteenth)],
                line.at[j, d],
                sems.at[6 + j * 3 + d],
                device(zz, x, y, c),
            )
    strip_here = pl.multiple_of(z * strip, 16)
    for j in range(2):
        for d in range(3):
            landed(line.at[j, d], sems.at[6 + j * 3 + d], mate)
        block = acc.at[:, columns(kept[j], sixteenth)]
        add_block(block, [line.at[j, d] for d in range(3)], strip, strip_here)

        def place(i, carry, j=j):
            some = pl.ds(pl.multiple_of(strip_here + i * 16, 16), 16)
            out_ref[some, columns(base + kept[j], sixteenth)] = acc[
                some, columns(kept[j], sixteenth)
            ]
            return carry

        lax.fori_loop(0, strip // 16, place, 0)
        done = out_ref.at[pl.ds(strip_here, strip), columns(base + kept[j], sixteenth)]
        for d, zz in enumerate(others):
            sends.start(done, done, sems.at[12 + j * 3 + d], device(zz, x, y, c))
    for j in range(2):
        for d in range(3):
            source = pl.multiple_of(lax.rem(z + 3 - d, 4) * strip, 16)
            landed(
                out_ref.at[pl.ds(source, strip), columns(base + kept[j], sixteenth)],
                sems.at[12 + j * 3 + d],
                mate,
            )
        part = out_ref.at[:, columns(base + kept[j], sixteenth)]
        sends.start(part, part, sems.at[18 + j], (side, over)[j])
    others_kept = (
        x * eighth + (1 - y) * sixteenth,
        quarter + y * eighth + (1 - x) * sixteenth,
    )
    for j in range(2):
        landed(out_ref.at[:, columns(base + others_kept[j], sixteenth)], sems.at[18 + j], mate)
        near = x * eighth if j == 0 else quarter + y * eighth
        part = out_ref.at[:, columns(base + near, eighth)]
        sends.start(part, part, sems.at[20 + j], (over, side)[j])
    for j in range(2):
        away = (1 - x) * eighth if j == 0 else quarter + (1 - y) * eighth
        landed(out_ref.at[:, columns(base + away, eighth)], sems.at[20 + j], mate)
        part = out_ref.at[:, columns(base + j * quarter, quarter)]
        sends.start(part, part, sems.at[22 + j], mate)
    for h, some in enumerate(group_parts):
        landed(group_mates.at[1, some], mate_sems.at[1, h], mate)
        landed(group_sides.at[some], side_sems.at[h], mate)
        add_into(
            group_out,
            [group_ref.at[y * 2 + c], group_mates.at[1], group_sides],
            h * group_half,
            group_half,
        )
    for j in range(2):
        landed(
            out_ref.at[:, columns((1 - c) * half + j * quarter, quarter)], sems.at[22 + j], mate
        )
    sends.finish()


def total_over_all(top, rest, group, number):
    if lax.axis_size("expert") != 8 or lax.axis_size("weight") != 4:
        value = jnp.concatenate([top, rest], axis=0).astype(jnp.float32)
        return lax.psum(value, ("expert", "weight")), sum_group(group, number)
    rows, width = top.shape[0] + rest.shape[0], top.shape[1]
    group = group.reshape(4, -1, width)
    group_rows = group.shape[1]
    out = jax.ShapeDtypeStruct((rows, width), top.dtype)
    group_out = jax.ShapeDtypeStruct((group_rows, width), jnp.float32)
    buffer = lambda n: pltpu.VMEM((rows, n), top.dtype)
    return pl.pallas_call(
        total_kernel,
        out_shape=[out, group_out],
        in_specs=[pl.BlockSpec(memory_space=pltpu.VMEM)] * 3,
        out_specs=[pl.BlockSpec(memory_space=pltpu.VMEM)] * 2,
        scratch_shapes=[
            buffer(width // 2),
            buffer(width // 2),
            buffer(width // 8),
            buffer(width // 8),
            buffer(width // 16),
            buffer(width // 16),
            pltpu.VMEM((2, 3, rows // 4, width // 16), top.dtype),
            pltpu.VMEM((2, group_rows, width), group.dtype),
            pltpu.VMEM((group_rows, width), group.dtype),
            pltpu.VMEM((group_rows, width), group.dtype),
            pltpu.SemaphoreType.DMA((32,)),
            pltpu.SemaphoreType.DMA((26,)),
            pltpu.SemaphoreType.DMA((2, 2)),
            pltpu.SemaphoreType.DMA((2,)),
        ],
        compiler_params=pltpu.CompilerParams(
            collective_id=number, has_side_effects=True, vmem_limit_bytes=vmem_limit
        ),
        cost_estimate=cost(0, top, rest, group, out, group_out),
    )(top, rest, group)


def shared_kernel(turn, ins, outs):
    normed_ref, cotangent_ref, gate_grad_ref, lift_grad_ref, hidden_ref = ins

    @pl.when(turn == 0)
    def _():
        for out_ref in outs:
            out_ref[...] = jnp.zeros_like(out_ref)

    normed, cotangent = normed_ref[...], cotangent_ref[...]
    outs[0][...] += trans_times(gate_grad_ref[...], normed)
    outs[1][...] += trans_times(lift_grad_ref[...], normed)
    outs[2][...] += trans_times(hidden_ref[...], cotangent)


def weight_kernel(ins, outs):
    rows_ref, grads_ref, gate_grad_ref, lift_grad_ref, hidden_ref = ins
    rows = rows_ref[0]
    for out_ref, left_ref, right in (
        (outs[0], gate_grad_ref, rows),
        (outs[1], lift_grad_ref, rows),
        (outs[2], hidden_ref, grads_ref[0]),
    ):
        out_ref[0] = trans_times(left_ref[0], right).astype(out_ref.dtype)


def weights_alone(*refs):
    weight_kernel(refs[:5], refs[5:])


def gradients_kernel(turn, ins, outs):
    shared_kernel(turn, ins[:5], outs[:3])
    weight_kernel(ins[5:], outs[3:])


def sum_shards(value):
    return lax.psum_scatter(value, "expert", scatter_dimension=0, tiled=True)


def per_device(
    tokens,
    cotangent,
    segments,
    routes,
    first_gain,
    query_weight,
    latent_weight,
    latent_gain,
    expand_weight,
    output_weight,
    second_gain,
    router_weight,
    shared_gate,
    shared_up,
    shared_down,
    expert_gate,
    expert_up,
    expert_down,
):
    weight_count = lax.axis_size("weight")
    token_rows = tokens.shape[0]
    width = tokens.shape[1]
    group_rows = token_rows * weight_count
    query_width = NOPE + ROPE
    heads_here = query_weight.shape[1] // query_width
    expert_count = router_weight.shape[1]
    local_experts = expert_gate.shape[0]
    score_scale = query_width ** (-0.5)
    activations = tokens.astype(jnp.float32)
    first_scale = inv_rms(activations)
    normed = (activations * first_scale * first_gain).astype(jnp.bfloat16)
    both = ("expert", "weight")
    expert_index = lax.axis_index("expert")
    expert_lanes = lax.axis_size("expert")
    blocks = expert_lanes * weight_count
    pairs, quads = blocks // 2, blocks // 4
    pair_rows, quad_rows = 2 * token_rows, 4 * token_rows
    all_rows = blocks * token_rows
    slot_rows = blocks * CAP
    choose = (
        routes[:, :, None] == jnp.arange(expert_count, dtype=jnp.int32)[None, None, :]
    ).astype(jnp.float32)
    hit = jnp.sum(choose, axis=1)
    order = jnp.arange(token_rows, dtype=jnp.int32)
    before = (order[None, :] < order[:, None]).astype(jnp.bfloat16)
    place = matmul(before, hit.astype(jnp.bfloat16))
    rank = jnp.sum(choose * jnp.arange(routes.shape[1], dtype=jnp.float32)[None, :, None], axis=1)
    code = jnp.where(hit > 0, 32.0 * rank + place, -1.0)
    extra = jnp.pad(code, ((0, 0), (0, lanes - expert_count)), constant_values=-1.0)
    cotangent_wide = jnp.concatenate([cotangent, extra.astype(jnp.bfloat16)], axis=1)
    column = jnp.arange(lanes, dtype=jnp.int32)[None, :]
    row = jnp.arange(8, dtype=jnp.int32)[:, None]
    first_here = expert_index * local_experts
    here = (row < local_experts) & (column == first_here + row)
    twice = here | ((row < local_experts) & (column == first_here + row + expert_count))
    here, twice = here.astype(jnp.bfloat16), twice.astype(jnp.bfloat16)
    weight_index = lax.axis_index("weight")
    high_column = 2 * (row * weight_count + weight_index)
    known = row < routes.shape[1]
    high_at = (known & (column == high_column)).astype(jnp.bfloat16)
    low_at = (known & (column == high_column + 1)).astype(jnp.bfloat16)
    shared_here = shared_gate.shape[1] // expert_lanes
    shared_wide = -(-shared_here // lanes) * lanes
    start = expert_index * shared_here

    def shared_part(matrix):
        part = lax.dynamic_slice_in_dim(matrix, start, shared_here, axis=0)
        return jnp.pad(part, ((0, shared_wide - shared_here), (0, 0)))

    gate_part = shared_part(shared_gate.T)
    up_part = shared_part(shared_up.T)
    down_part = shared_part(shared_down)
    shape = jax.ShapeDtypeStruct
    whole = lambda array: (array, whole_spec(array))
    slots = shape((local_experts, slot_rows, width), jnp.bfloat16)
    slots_one = shape((local_experts, slot_rows, lanes), jnp.float32)
    gather_flops = 2 * all_rows * width * (2 * CAP * local_experts + shared_wide)
    cosine, sine = rope_tables(segments[0])
    allowed = attention_mask(segments[0])
    sizes = (expert_lanes, weight_count)
    if sizes == (8, 4):
        (
            cotangent_all,
            normed_all,
            query,
            latent,
            latent_scale,
            latent_normed,
            key_rope,
            expanded,
            log_total,
            mixed,
            hidden_one,
            second_scale,
            gates,
            normed_wide,
        ) = attention_forward(
            score_scale,
            normed,
            cotangent_wide,
            cosine,
            sine,
            segments[0],
            latent_gain,
            tokens,
            second_gain,
            router_weight,
            query_weight,
            latent_weight,
            expand_weight,
            output_weight,
            0,
        )
        second_scale, normed_two = second_scale[:, :1], normed_wide[:, :width]
        cotangent_all = cotangent_all.reshape(all_rows, -1)
        normed_all = normed_all.reshape(group_rows, width)
        latent_scale, log_total = latent_scale[:, :1], log_total[:, :, :1]
        query = query.transpose(1, 0, 2)
        expanded = expanded.reshape(group_rows, heads_here, NOPE + VDIM)
    else:
        cotangent_all = lax.all_gather(cotangent_wide, both, axis=0, tiled=True)
        normed_all = gather_group(normed, 0)
        query_full = matmul(normed_all, query_weight).reshape(group_rows, heads_here, query_width)
        query = jnp.concatenate(
            [
                query_full[..., :NOPE],
                rotate(query_full[..., NOPE:], cosine[:, None, :], sine[:, None, :]),
            ],
            axis=-1,
        ).astype(jnp.bfloat16)
        compressed = matmul(normed_all, latent_weight)
        latent = compressed[:, :LATENT]
        latent_scale = inv_rms(latent)
        latent_normed = (latent * latent_scale * latent_gain).astype(jnp.bfloat16)
        key_rope = rotate(compressed[:, LATENT:], cosine, sine).astype(jnp.bfloat16)
        expanded = (
            matmul(latent_normed, expand_weight)
            .astype(jnp.bfloat16)
            .reshape(group_rows, heads_here, NOPE + VDIM)
        )
    key_nope = expanded[..., :NOPE]
    values = expanded[..., NOPE:]

    def score_block():
        raw = jnp.einsum(
            "ihd,jhd->hij", query[..., :NOPE], key_nope, preferred_element_type=jnp.float32
        )
        raw = raw + jnp.einsum(
            "ihd,jd->hij", query[..., NOPE:], key_rope, preferred_element_type=jnp.float32
        )
        return jnp.where(allowed[None], raw * score_scale, -1e30)

    if sizes != (8, 4):
        scores = score_block()
        peak = jnp.max(scores, axis=-1, keepdims=True)
        weights = jnp.exp(scores - peak)
        total = jnp.sum(weights, axis=-1, keepdims=True)
        log_total = peak + jnp.log(total)
        mixed = jnp.einsum(
            "hij,jhd->ihd",
            (weights / total).astype(jnp.bfloat16),
            values,
            preferred_element_type=jnp.float32,
        )
        mixed = mixed.astype(jnp.bfloat16).reshape(group_rows, heads_here * VDIM)
        attended = sum_group(matmul(mixed, output_weight).astype(jnp.bfloat16), 1)
        hidden_one = activations + attended
        second_scale = inv_rms(hidden_one)
        normed_two = (hidden_one * second_scale * second_gain).astype(jnp.bfloat16)
        gates = jax.nn.sigmoid(matmul(normed_two, router_weight))
        weighted = hit * gates
        mixing_at = route_scale * weighted / jnp.sum(weighted, axis=1, keepdims=True)
        mixing_high = mixing_at.astype(jnp.bfloat16)
        mixing_low = (mixing_at - mixing_high.astype(jnp.float32)).astype(jnp.bfloat16)
        normed_wide = jnp.concatenate([normed_two, mixing_high, mixing_low], axis=1)
    chosen = jnp.sum(choose * gates[:, None, :], axis=-1)
    chosen_total = jnp.sum(chosen, axis=1, keepdims=True)
    upstream = cotangent.astype(jnp.float32)
    marks = (cotangent_all, pl.BlockSpec((quad_rows, lanes), lambda i: (i, width // lanes)))
    token_spec = pl.BlockSpec((quad_rows, shared_wide), lambda i: (i, 0))
    if sizes == (8, 4):
        (
            normed_tokens,
            grads_slots,
            rows_slots,
            mix_slots,
            shared_hidden,
            shared_gate_grad,
            shared_lift_grad,
        ) = gather_tokens(
            normed_wide,
            cotangent_all,
            here,
            twice,
            down_part,
            gate_part,
            up_part,
            local_experts,
            slot_rows,
            pair_rows,
            2,
        )
        normed_tokens = normed_tokens.reshape(all_rows, -1)
    else:
        normed_tokens = lax.all_gather(normed_wide, both, axis=0, tiled=True)

        def grads_alone(*refs):
            grads_kernel(pair_rows, refs[:3], refs[3:])

        grads_slots, shared_raw = call(
            grads_alone,
            quads,
            [whole(here), (cotangent_all, pair_spec(cotangent_all, quads)), whole(down_part)],
            [
                (slots, slots_spec(slots, quads)),
                (shape((all_rows, shared_wide), jnp.float32), pl.BlockSpec((quad_rows, shared_wide), lambda i: (i, 0))),
            ],
            gather_flops,
        )
        token_shape = shape((all_rows, shared_wide), jnp.bfloat16)
        rows_slots, mix_slots, shared_hidden, shared_gate_grad, shared_lift_grad = call(
            functools.partial(rows_kernel, pair_rows),
            quads,
            [
                whole(here),
                whole(twice),
                marks,
                (normed_tokens, pair_spec(normed_tokens, quads)),
                (shared_raw, token_spec),
                whole(gate_part),
                whole(up_part),
            ],
            [
                (slots, slots_spec(slots, quads)),
                (slots_one, slots_spec(slots_one, quads)),
                (token_shape, token_spec),
                (token_shape, token_spec),
                (token_shape, token_spec),
            ],
            gather_flops + 2 * all_rows * width * shared_wide,
        )
    hidden_here = expert_gate.shape[2]
    gate_rows, up_rows = expert_gate.transpose(0, 2, 1), expert_up.transpose(0, 2, 1)

    def tile_spec(rows, n):
        per = slot_rows // rows
        return pl.BlockSpec((1, rows, n), lambda i: (i // per, i % per, 0))

    def expert_spec(rows, matrix):
        per = slot_rows // rows
        return pl.BlockSpec((1,) + matrix.shape[1:], lambda i: (i // per, 0, 0))

    large, small = 32 * CAP, 16 * CAP
    narrow = shape((local_experts, slot_rows, hidden_here), jnp.bfloat16)
    one_matmul = 2 * local_experts * slot_rows * width * hidden_here
    routed_hidden, mixed_hidden, slope, active, produced = call(
        forward_kernel,
        local_experts * (slot_rows // large),
        [
            (rows_slots, tile_spec(large, width)),
            (mix_slots, tile_spec(large, lanes)),
            (gate_rows, expert_spec(large, gate_rows)),
            (up_rows, expert_spec(large, up_rows)),
            (expert_down, expert_spec(large, expert_down)),
        ],
        [(narrow, tile_spec(large, hidden_here))] * 4 + [(slots, tile_spec(large, width))],
        3 * one_matmul,
    )
    dense = shape((all_rows, width), jnp.bfloat16)
    dense_wide = shape((all_rows, width + lanes), jnp.bfloat16)
    (out_dense,) = call(
        functools.partial(out_kernel, pair_rows),
        quads,
        [
            whole(here),
            marks,
            (produced, slots_spec(slots, quads)),
            (shared_hidden, token_spec),
            whole(down_part),
        ],
        [(dense, pair_spec(dense, quads))],
        gather_flops,
    )
    narrow_tile = tile_spec(small, hidden_here)
    routed_out, (gate_grad, lift_grad, returned, mix_grad_slots) = sum_all(
        out_dense.reshape(blocks, token_rows, width),
        6,
        backward_kernel,
        local_experts * (slot_rows // small),
        [
            (grads_slots, tile_spec(small, width)),
            (routed_hidden, narrow_tile),
            (slope, narrow_tile),
            (active, narrow_tile),
            (gate_rows, expert_spec(small, gate_rows)),
            (up_rows, expert_spec(small, up_rows)),
            (expert_down, expert_spec(small, expert_down)),
        ],
        [
            (narrow, narrow_tile),
            (narrow, narrow_tile),
            (slots, tile_spec(small, width)),
            (slots_one, tile_spec(small, lanes)),
        ],
        3 * one_matmul,
    )
    (back_dense,) = call(
        functools.partial(back_kernel, pair_rows),
        quads,
        [
            whole(here),
            whole(high_at),
            whole(low_at),
            marks,
            (returned, slots_spec(slots, quads)),
            (mix_grad_slots, slots_spec(slots_one, quads)),
            (shared_gate_grad, token_spec),
            (shared_lift_grad, token_spec),
            whole(gate_part),
            whole(up_part),
        ],
        [(dense_wide, pair_spec(dense_wide, quads))],
        gather_flops + 2 * all_rows * width * shared_wide,
    )
    shared_sum = shape((shared_wide, width), jnp.float32)
    shared_out = (shared_sum, whole_spec(shared_sum))
    plain_spec = pl.BlockSpec((pair_rows, width), lambda i: (i, 0))
    shared_spec = pl.BlockSpec((pair_rows, shared_wide), lambda i: (i, 0))
    column_half = width // 2
    half_spec = lambda m: pl.BlockSpec((1, m, column_half), lambda i: (i // 2, 0, i % 2))
    narrow_spec = pl.BlockSpec((1, slot_rows, hidden_here), lambda i: (i // 2, 0, 0))
    shared_ins = [
        (normed_tokens, plain_spec),
        (cotangent_all, plain_spec),
        (shared_gate_grad, shared_spec),
        (shared_lift_grad, shared_spec),
        (shared_hidden, shared_spec),
    ]
    weight_ins = [
        (rows_slots, half_spec(slot_rows)),
        (grads_slots, half_spec(slot_rows)),
        (gate_grad, narrow_spec),
        (lift_grad, narrow_spec),
        (mixed_hidden, narrow_spec),
    ]
    back_blocks = back_dense.reshape(blocks, token_rows, -1)
    shared_flops = 6 * all_rows * width * shared_wide
    together = pairs == 2 * local_experts
    weight_type = jnp.bfloat16 if together else jnp.float32
    weight_shape = shape((local_experts, hidden_here, width), weight_type)
    weight_outs = [(weight_shape, half_spec(hidden_here))] * 3
    if together:
        back_here, sums = sum_all(
            back_blocks,
            3,
            gradients_kernel,
            pairs,
            shared_ins + weight_ins,
            [shared_out] * 3 + weight_outs,
            shared_flops + 3 * one_matmul,
        )
        shared_sums = sums[:3]
        weight_grads = [value.astype(jnp.float32) for value in sums[3:]]
    else:
        back_here, shared_sums = sum_all(
            back_blocks, 3, shared_kernel, pairs, shared_ins, [shared_out] * 3, shared_flops
        )
        weight_grads = call(
            weights_alone, 2 * local_experts, weight_ins, weight_outs, 3 * one_matmul
        )
    routed_back = back_here[:, :width]
    mix_grad = back_here[:, width : width + 2 * weight_count * routes.shape[1]]
    mix_grad = jnp.sum(mix_grad.reshape(token_rows, routes.shape[1], -1), axis=2)
    shared_grads = jnp.concatenate([total[:shared_here] for total in shared_sums], axis=0)
    shared_grads = shared_grads.astype(jnp.bfloat16)
    swapped = lax.all_to_all(shared_grads, "expert", split_axis=1, concat_axis=0, tiled=True)
    swapped = swapped.reshape(expert_lanes, 3, shared_here, -1).astype(jnp.float32)
    shared_gradients = [swapped[:, i].reshape(expert_lanes * shared_here, -1) for i in range(3)]
    chosen_grad = route_scale * (
        mix_grad / chosen_total
        - jnp.sum(mix_grad * chosen, axis=1, keepdims=True) / chosen_total**2
    )
    logit_grad = jnp.sum(choose * chosen_grad[:, :, None], axis=1) * gates * (1.0 - gates)
    normed_two_grad = (
        routed_back
        + jnp.dot(logit_grad, router_weight.astype(jnp.float32).T, precision=highest)
    )
    router_gradient = jnp.dot(logit_grad.T, normed_two.astype(jnp.float32), precision=highest)
    back_two, second_gain_gradient = norm_back(
        normed_two_grad, hidden_one, second_scale, second_gain
    )
    hidden_grad = upstream + back_two
    hidden_group = gather_group(hidden_grad.astype(jnp.bfloat16), 4)
    output_gradient = trans_times(hidden_group, mixed).astype(jnp.bfloat16)
    hidden_group, output_gradient = lax.optimization_barrier((hidden_group, output_gradient))
    output_shard = sum_shards(output_gradient)
    mixed_grad = (
        times_trans(hidden_group, output_weight)
        .astype(jnp.bfloat16)
        .reshape(group_rows, heads_here, VDIM)
    )
    probs = jnp.exp(score_block() - log_total)
    prob_grad = jnp.einsum("ihd,jhd->hij", mixed_grad, values, preferred_element_type=jnp.float32)
    centre = jnp.sum(probs * prob_grad, axis=-1, keepdims=True)
    score_grad = (probs * (prob_grad - centre)).astype(jnp.bfloat16)
    value_grad = jnp.einsum(
        "hij,ihd->jhd", probs.astype(jnp.bfloat16), mixed_grad, preferred_element_type=jnp.float32
    )
    query_nope_grad = (
        jnp.einsum("hij,jhd->ihd", score_grad, key_nope, preferred_element_type=jnp.float32)
        * score_scale
    )
    query_rope_grad = (
        jnp.einsum("hij,jd->ihd", score_grad, key_rope, preferred_element_type=jnp.float32)
        * score_scale
    )
    key_nope_grad = (
        jnp.einsum(
            "hij,ihd->jhd", score_grad, query[..., :NOPE], preferred_element_type=jnp.float32
        )
        * score_scale
    )
    key_rope_grad = (
        jnp.einsum("hij,ihd->jd", score_grad, query[..., NOPE:], preferred_element_type=jnp.float32)
        * score_scale
    )
    query_grad = jnp.concatenate(
        [query_nope_grad, unrotate(query_rope_grad, cosine[:, None, :], sine[:, None, :])], axis=-1
    )
    query_grad = query_grad.astype(jnp.bfloat16).reshape(group_rows, heads_here * query_width)
    expand_grad = (
        jnp.concatenate([key_nope_grad, value_grad], axis=-1)
        .astype(jnp.bfloat16)
        .reshape(group_rows, heads_here * (NOPE + VDIM))
    )
    expert_grads = (weight_grads[0].transpose(0, 2, 1), weight_grads[1].transpose(0, 2, 1), weight_grads[2])
    layer_out = (hidden_one + routed_out).astype(jnp.bfloat16)
    query_gradient = trans_times(normed_all, query_grad)
    expand_gradient = trans_times(latent_normed, expand_grad).astype(jnp.bfloat16)
    latent_normed_grad = times_trans(expand_grad, expand_weight)
    latent_back, latent_gain_gradient = norm_back(
        latent_normed_grad, latent, latent_scale, latent_gain
    )
    compressed_grad = jnp.concatenate([latent_back, unrotate(key_rope_grad, cosine, sine)], axis=-1)
    compressed_grad = compressed_grad.astype(jnp.bfloat16)
    latent_weight_gradient = trans_times(compressed_grad, normed_all)
    normed_part = times_trans(query_grad, query_weight) + times_trans(compressed_grad, latent_weight)
    first_gain_gradient = jnp.sum(normed_part * normed_all.astype(jnp.float32), axis=0) / first_gain
    rows_each = query_gradient.shape[0]
    joined = jnp.concatenate(
        [query_gradient.astype(jnp.bfloat16), expand_gradient.reshape(rows_each, -1)], axis=1
    )
    joined = sum_shards(joined).astype(jnp.float32)
    query_columns = query_gradient.shape[1]
    shards = (
        joined[:, :query_columns],
        joined[:, query_columns:].reshape(-1, expand_gradient.shape[1]),
        output_shard.T.astype(jnp.float32),
    )
    latent_columns = latent_weight.shape[1]
    rest = jnp.concatenate(
        [
            router_gradient,
            first_gain_gradient[None],
            second_gain_gradient[None],
            jnp.pad(latent_gain_gradient, (0, width - LATENT))[None],
        ],
        axis=0,
    ).astype(jnp.bfloat16)
    wanted = -(-(latent_columns + rest.shape[0]) // 64) * 64 - latent_columns
    rest = jnp.pad(rest, ((0, wanted - rest.shape[0]), (0, 0)))
    total, normed_grad = total_over_all(
        latent_weight_gradient.astype(jnp.bfloat16), rest, normed_part.astype(jnp.bfloat16), 7
    )
    back_one, _ = norm_back(normed_grad, activations, first_scale, first_gain)
    token_gradient = hidden_grad + back_one
    gains_at = latent_columns + expert_count
    wide = lambda value: value.astype(jnp.float32)
    totals = (
        wide(total[:latent_columns]).T,
        wide(total[gains_at + 2, :LATENT]),
        wide(total[latent_columns:gains_at]).T,
        wide(total[gains_at]),
        wide(total[gains_at + 1]),
    )
    return (
        layer_out,
        token_gradient,
        totals[3],
        shards[0],
        totals[0],
        totals[1],
        shards[1],
        shards[2],
        totals[4],
        totals[2],
        shared_gradients[0].T,
        shared_gradients[1].T,
        shared_gradients[2],
        expert_grads[0],
        expert_grads[1],
        expert_grads[2],
    )


def solution(mesh):
    return jax.shard_map(
        per_device,
        mesh=mesh,
        in_specs=(
            P(("expert", "weight"), None),
            P(("expert", "weight"), None),
            P("expert", None),
            P(("expert", "weight"), None),
            P(),
            P(None, "weight"),
            P(),
            P(),
            P(None, "weight"),
            P("weight", None),
            P(),
            P(),
            P(None, "weight"),
            P(None, "weight"),
            P("weight", None),
            P("expert", None, "weight"),
            P("expert", None, "weight"),
            P("expert", "weight", None),
        ),
        out_specs=(
            P(("expert", "weight"), None),
            P(("expert", "weight"), None),
            P(),
            P("expert", "weight"),
            P(),
            P(),
            P("expert", "weight"),
            P("weight", "expert"),
            P(),
            P(),
            P("expert", "weight"),
            P("expert", "weight"),
            P("weight", "expert"),
            P("expert", None, "weight"),
            P("expert", None, "weight"),
            P("expert", "weight", None),
        ),
        check_vma=False,
    )
```
